128 devices in a mesh: tp: 2 (over core), fsdp: 64 (over z, y, x).
Axes of the slice: x: 4, y: 4, z: 4, core: 2. Of those that a mesh axis runs over, the one named last changes fastest.
Arguments:
- x: bfloat16 [128, 1024, 1024], P('fsdp')
- grad_y: bfloat16 [128, 1024, 1024], P('fsdp')
- w_qkv: bfloat16 [1024, 3, 16, 64], P('fsdp', None, 'tp')
- w_out: bfloat16 [16, 64, 1024], P('tp', None, 'fsdp')
- w_ff: bfloat16 [1024, 2, 2816], P('fsdp', None, 'tp')
- w_down: bfloat16 [2816, 1024], P('tp', 'fsdp')
Outputs:
- output 1: bfloat16 [128, 1024, 1024], P('fsdp')
- output 2: bfloat16 [128, 1024, 1024], P('fsdp')
- output 3: float32 [1024, 3, 16, 64], P('fsdp', None, 'tp')
- output 4: float32 [16, 64, 1024], P('tp', None, 'fsdp')
- output 5: float32 [1024, 2, 2816], P('fsdp', None, 'tp')
- output 6: float32 [2816, 1024], P('tp', 'fsdp')
All inputs are finite; a program needn't handle non-finite values.
Results may differ from the reference program's by a relative error of at most 0.0160394.
Values are sent between devices in bfloat16 or wider.
A program may use at most 1 GiB of HBM per device.

```python
import jax
import jax.numpy as jnp
from jax import lax

BATCH = 128
SEQ = 1024
D = 1024
HEADS = 16
HEAD = 64
FF = 2816
CLIP = 8.0
EPS = 1e-5
THETA = 10000.0


def setup_inputs(seed: int = 0) -> dict:
    rng_keys = jax.random.split(jax.random.key(seed), 6)
    x = jax.random.normal(rng_keys[0], (BATCH, SEQ, D), jnp.float32)
    grad_y = jax.random.normal(rng_keys[1], (BATCH, SEQ, D), jnp.float32)
    part_scale = jnp.array([1.0, 1.0, 5.0], jnp.float32)[None, :, None, None]
    w_qkv = jax.random.normal(rng_keys[2], (D, 3, HEADS, HEAD), jnp.float32) * (D ** -0.5) * part_scale
    w_out = jax.random.normal(rng_keys[3], (HEADS, HEAD, D), jnp.float32) * (2.0 * D ** -0.5)
    w_ff = jax.random.normal(rng_keys[4], (D, 2, FF), jnp.float32) * (D ** -0.5)
    w_down = jax.random.normal(rng_keys[5], (FF, D), jnp.float32) * (FF ** -0.5)
    return {'x': x.astype(jnp.bfloat16), 'grad_y': grad_y.astype(jnp.bfloat16), 'w_qkv': w_qkv.astype(jnp.bfloat16), 'w_out': w_out.astype(jnp.bfloat16), 'w_ff': w_ff.astype(jnp.bfloat16), 'w_down': w_down.astype(jnp.bfloat16)}


def layer_norm(values):
    mean_val = jnp.mean(values, axis=-1, keepdims=True)
    centered = values - mean_val
    variance = jnp.mean(centered * centered, axis=-1, keepdims=True)
    return centered * lax.rsqrt(variance + EPS)


def rope_tables():
    inv_freq = THETA ** (-jnp.arange(0, HEAD, 2, dtype=jnp.float32) / HEAD)
    angles = jnp.arange(SEQ, dtype=jnp.float32)[:, None] * inv_freq[None, :]
    return jnp.cos(angles)[:, None, :], jnp.sin(angles)[:, None, :]


def rotate(values, cos_tab, sin_tab):
    half_dim = HEAD // 2
    x_first = values[..., :half_dim]
    x_second = values[..., half_dim:]
    return jnp.concatenate([x_first * cos_tab - x_second * sin_tab, x_second * cos_tab + x_first * sin_tab], axis=-1)


def sequence_layer(x_seq, w_qkv, w_out, w_ff, w_down):
    cos_tab, sin_tab = rope_tables()
    normed1 = layer_norm(x_seq.astype(jnp.float32)).astype(jnp.bfloat16)
    qkv_raw = jnp.dot(normed1, w_qkv.astype(jnp.bfloat16).reshape(D, 3 * D), preferred_element_type=jnp.float32)
    qkv_cl = jnp.clip(qkv_raw, -CLIP, CLIP).reshape(SEQ, 3, HEADS, HEAD)
    q_rot = rotate(qkv_cl[:, 0], cos_tab, sin_tab).astype(jnp.bfloat16)
    k_rot = rotate(qkv_cl[:, 1], cos_tab, sin_tab).astype(jnp.bfloat16)
    v_val = qkv_cl[:, 2].astype(jnp.bfloat16)
    scores = jnp.einsum('qhe,khe->hqk', q_rot.astype(jnp.float32), k_rot.astype(jnp.float32)) * (HEAD ** -0.5)
    causal = jnp.arange(SEQ)[:, None] >= jnp.arange(SEQ)[None, :]
    scores = jnp.where(causal[None], scores, -1e30)
    prob_b16 = jax.nn.softmax(scores, axis=-1).astype(jnp.bfloat16)
    attn_o = jnp.einsum('hqk,khe->qhe', prob_b16.astype(jnp.float32), v_val.astype(jnp.float32)).astype(jnp.bfloat16)
    attn_proj = jnp.dot(attn_o.reshape(SEQ, D), w_out.astype(jnp.bfloat16).reshape(D, D), preferred_element_type=jnp.float32)
    hidden = (x_seq.astype(jnp.float32) + attn_proj).astype(jnp.bfloat16)
    normed2 = layer_norm(hidden.astype(jnp.float32)).astype(jnp.bfloat16)
    up_gate = jnp.dot(normed2, w_ff.astype(jnp.bfloat16).reshape(D, 2 * FF), preferred_element_type=jnp.float32).reshape(SEQ, 2, FF)
    mlp_act = (jax.nn.silu(up_gate[:, 1]) * up_gate[:, 0]).astype(jnp.bfloat16)
    mlp_proj = jnp.dot(mlp_act, w_down.astype(jnp.bfloat16), preferred_element_type=jnp.float32)
    return (hidden.astype(jnp.float32) + mlp_proj).astype(jnp.bfloat16)


def reference(x, grad_y, w_qkv, w_out, w_ff, w_down):
    def whole_layer(x_all, qkv_w, out_w, ff_w, down_w):
        layer_fn = jax.checkpoint(lambda x_seq: sequence_layer(x_seq, qkv_w, out_w, ff_w, down_w))
        return lax.map(layer_fn, x_all)

    y_out, pull_back = jax.vjp(whole_layer, x, w_qkv.astype(jnp.float32), w_out.astype(jnp.float32), w_ff.astype(jnp.float32), w_down.astype(jnp.float32))
    grad_x, grad_qkv, grad_out, grad_ff, grad_down = pull_back(grad_y)
    return y_out, grad_x, grad_qkv, grad_out, grad_ff, grad_down
```

```python
import functools
import jax, jax.numpy as jnp
from jax import lax
from jax.experimental import pallas as pl
from jax.experimental.pallas import tpu as pltpu
from jax.sharding import PartitionSpec as P

MESH_ID = pl.DeviceIdType.MESH
ORDERS = ((2, 1, 0), (1, 0, 2), (0, 2, 1))


class Torus:
    def __init__(self, send_sem, recv_sem):
        self.tp = lax.axis_index('tp')
        me = lax.axis_index('fsdp')
        self.at = (me // 16, (me // 4) % 4, me % 4)
        self.send_sem, self.recv_sem = send_sem, recv_sem
        self.n = 0
        self.sent = []

    def shift(self, axis, by):
        return (self.at[axis] + by + 4) % 4

    def peer(self, axis, by):
        pos = list(self.at)
        pos[axis] = self.shift(axis, by)
        return (self.tp, pos[0] * 16 + pos[1] * 4 + pos[2])

    def copy(self, src, dst, device):
        desc = pltpu.make_async_remote_copy(src, dst, self.send_sem.at[self.n], self.recv_sem.at[self.n], device_id=device, device_id_type=MESH_ID)
        self.n += 1
        self.sent.append(desc)
        return desc

    def local(self, src, dst):
        desc = pltpu.make_async_copy(src, dst, self.send_sem.at[self.n])
        self.n += 1
        return desc

    def barrier(self, partner=False):
        sem = pltpu.get_barrier_semaphore()
        peers = [self.peer(axis, by) for axis in range(3) for by in (1, -1)]
        if partner:
            peers.append((1 - self.tp, self.at[0] * 16 + self.at[1] * 4 + self.at[2]))
        for device in peers:
            pl.semaphore_signal(sem, inc=1, device_id=device, device_id_type=MESH_ID)
        pl.semaphore_wait(sem, len(peers))

    def finish(self):
        for desc in self.sent:
            desc.wait_send()
        self.sent = []


def window(ref, picks, rows, cols):
    return ref.at[picks[0], picks[1], picks[2], rows, cols]


def gather_stages(net, shards, outs, segs):
    whole = slice(None)
    state = {}

    def picks(order, phase, coord):
        got = [None] * 3
        for pos, axis in enumerate(order):
            got[axis] = pl.ds(0, 4) if pos < phase else net.at[axis]
        got[order[phase]] = coord
        return got

    def halves(order, phase, coord, off, width):
        if phase == 0:
            left = (width // 256) * 128 if width >= 256 else width
            parts = [(picks(order, phase, coord), pl.ds(off, left))]
            parts.append((picks(order, phase, coord), pl.ds(off + left, width - left)) if width > left else None)
            return parts
        parts = []
        for lo in (0, 2):
            got = picks(order, phase, coord)
            got[order[0]] = pl.ds(lo, 2)
            parts.append((got, pl.ds(off, width)))
        return parts

    def local_copies():
        state['own'] = []
        for shard, out in zip(shards, outs):
            desc = net.local(shard, out.at[net.at[0], net.at[1], net.at[2]])
            desc.start()
            state['own'].append(desc)

    def wait_own():
        for desc in state['own']:
            desc.wait()

    def start(phase):
        for colour, order in enumerate(ORDERS):
            axis = order[phase]
            for seg, (arr, off, width) in enumerate(segs[colour]):
                where = picks(order, phase, net.at[axis])
                dst = window(outs[arr], where, whole, pl.ds(off, width))
                src = shards[arr].at[:, pl.ds(off, width)] if phase == 0 else dst
                for by in (1, -1):
                    desc = net.copy(src, dst, net.peer(axis, by))
                    desc.start()
                    state[colour, phase, seg, by] = desc

    def forward(phase):
        for by in (1, -1):
            for colour, order in enumerate(ORDERS):
                axis = order[phase]
                for seg, (arr, off, width) in enumerate(segs[colour]):
                    state[colour, phase, seg, by].wait_recv()
                    part = halves(order, phase, net.shift(axis, -by), off, width)[0 if by == 1 else 1]
                    if part is None:
                        continue
                    ref = window(outs[arr], part[0], whole, part[1])
                    desc = net.copy(ref, ref, net.peer(axis, by))
                    desc.start()
                    state[colour, phase, seg, 'f', by] = desc

    def settle(phase):
        for by in (1, -1):
            for colour in range(3):
                for seg in range(len(segs[colour])):
                    if (colour, phase, seg, 'f', by) in state:
                        state[colour, phase, seg, 'f', by].wait_recv()

    def first():
        local_copies()
        start(0)

    def second():
        settle(0)
        wait_own()
        start(1)

    def third():
        settle(1)
        start(2)

    def last():
        settle(2)
        net.finish()

    return [first, functools.partial(forward, 0), second, functools.partial(forward, 1), third, functools.partial(forward, 2), last]


def gather_kernel(n_arr, segs, *refs):
    shards, outs = refs[:n_arr], refs[n_arr:2 * n_arr]
    send_sem, recv_sem = refs[2 * n_arr:]
    net = Torus(send_sem, recv_sem)
    net.barrier()
    for stage in gather_stages(net, shards, outs, segs):
        stage()


def all_gather(shards, segs, collective_id, sems=160):
    n_arr = len(shards)
    outs = [jax.ShapeDtypeStruct((4, 4, 4) + s.shape, s.dtype) for s in shards]
    got = pl.pallas_call(
        functools.partial(gather_kernel, n_arr, segs),
        out_shape=outs,
        in_specs=[pl.BlockSpec(memory_space=pltpu.VMEM)] * n_arr,
        out_specs=[pl.BlockSpec(memory_space=pltpu.HBM)] * n_arr,
        scratch_shapes=[pltpu.SemaphoreType.DMA((sems,)), pltpu.SemaphoreType.DMA((sems,))],
        compiler_params=pltpu.CompilerParams(collective_id=collective_id, has_side_effects=True),
        name='torus_gather',
    )(*shards)
    return [g.reshape(-1, g.shape[-1]) for g in got]


def scatter_buffers(widths):
    shapes = []
    for w in widths:
        shapes += [
            (2, 2, 4, 16, w), (2, 2, 4, 16, w), (2, 2, 4, 16, w), (2, 2, 4, 16, w), (4, 4, 16, w),
            (3, 2, 2, 16, w), (3, 2, 8, w),
        ]
    return [pltpu.VMEM(s, jnp.float32) for s in shapes]


def scatter_stages(net, parts, outs, segs, bufs):
    state = {}
    rows = slice(None)

    def buf(colour):
        return bufs[7 * colour:7 * colour + 7]

    def rest(order):
        return sorted(order[1:])

    def src1(order, coord, half):
        got = [pl.ds(0, 4)] * 3
        got[order[0]] = coord
        if half is not None:
            got[rest(order)[0]] = pl.ds(2 * half, 2)
        return got

    def part1(colour, seg, coord, half):
        arr, off, width = segs[colour][seg]
        return window(parts[arr], src1(ORDERS[colour], coord, half), rows, pl.ds(off, width))

    def spans(colour):
        at = 0
        for seg, (_, _, width) in enumerate(segs[colour]):
            yield seg, pl.ds(at, width)
            at += width

    def start1():
        for kind in ('x', 'y'):
            for colour, order in enumerate(ORDERS):
                axis = order[0]
                xb, yb = buf(colour)[0], buf(colour)[1]
                for seg, cols in spans(colour):
                    for d, by in ((0, 1), (1, -1)):
                        if kind == 'x':
                            src, dst = part1(colour, seg, net.shift(axis, 2), d), xb.at[d, :, :, :, cols]
                        else:
                            src, dst = part1(colour, seg, net.shift(axis, by), 1 - d), yb.at[d, :, :, :, cols]
                        desc = net.copy(src, dst, net.peer(axis, by))
                        desc.start()
                        state[1, kind, colour, seg, d] = desc
        for colour, order in enumerate(ORDERS):
            axis = order[0]
            fb, rb = buf(colour)[3], buf(colour)[4]
            for seg, cols in spans(colour):
                for d, by in ((0, 1), (1, -1)):
                    desc = net.local(part1(colour, seg, net.shift(axis, by), d), fb.at[d, :, :, :, cols])
                    desc.start()
                    state[1, 'f', colour, seg, d] = desc
                desc = net.local(part1(colour, seg, net.at[axis], None), rb.at[:, :, :, cols])
                desc.start()
                state[1, 'r', colour, seg] = desc

    def relay1():
        for colour, order in enumerate(ORDERS):
            axis = order[0]
            xb, zb, fb = buf(colour)[0], buf(colour)[2], buf(colour)[3]
            for d, by in ((0, 1), (1, -1)):
                for seg, _ in spans(colour):
                    state[1, 'x', colour, seg, d].wait_recv()
                    state[1, 'f', colour, seg, d].wait()

                def body(i, carry, xb=xb, fb=fb, d=d):
                    fb[d, i // 4, i % 4] = fb[d, i // 4, i % 4] + xb[d, i // 4, i % 4]
                    return carry

                lax.fori_loop(0, 8, body, 0)
                desc = net.copy(fb.at[d], zb.at[d], net.peer(axis, by))
                desc.start()
                state[1, 'z', colour, d] = desc

    def merge1():
        for colour in range(3):
            yb, zb, rb = buf(colour)[1], buf(colour)[2], buf(colour)[4]
            for seg, _ in spans(colour):
                state[1, 'r', colour, seg].wait()
                for d in (0, 1):
                    state[1, 'y', colour, seg, d].wait_recv()
            for d in (0, 1):
                state[1, 'z', colour, d].wait_recv()

            def body(i, carry, yb=yb, zb=zb, rb=rb):
                b, c = i // 4, i % 4
                rb[b, c] = rb[b, c] + yb[1, b, c] + zb[0, b, c]
                rb[b + 2, c] = rb[b + 2, c] + yb[0, b, c] + zb[1, b, c]
                return carry

            lax.fori_loop(0, 8, body, 0)

    def block2(colour, coord, half):
        order = ORDERS[colour]
        rb = buf(colour)[4]
        keep = pl.ds(0, 4) if half is None else pl.ds(2 * half, 2)
        return rb.at[coord, keep] if rest(order)[0] == order[1] else rb.at[keep, coord]

    def piece2(colour, coord, i):
        order = ORDERS[colour]
        rb = buf(colour)[4]
        return rb.at[coord, i] if rest(order)[0] == order[1] else rb.at[i, coord]

    def start2():
        for kind in ('x', 'y'):
            for colour, order in enumerate(ORDERS):
                axis, b2 = order[1], buf(colour)[5]
                for d, by in ((0, 1), (1, -1)):
                    src = block2(colour, net.shift(axis, 2), d) if kind == 'x' else block2(colour, net.shift(axis, by), 1 - d)
                    desc = net.copy(src, b2.at[0 if kind == 'x' else 1, d], net.peer(axis, by))
                    desc.start()
                    state[2, kind, colour, d] = desc

    def relay2():
        for colour, order in enumerate(ORDERS):
            axis, b2 = order[1], buf(colour)[5]
            for d, by in ((0, 1), (1, -1)):
                state[2, 'x', colour, d].wait_recv()
                for i in range(2):
                    b2[0, d, i] = b2[0, d, i] + piece2(colour, net.shift(axis, by), 2 * d + i)[...]
                desc = net.copy(b2.at[0, d], b2.at[2, d], net.peer(axis, by))
                desc.start()
                state[2, 'z', colour, d] = desc

    def merge2():
        for colour, order in enumerate(ORDERS):
            axis, b2 = order[1], buf(colour)[5]
            for d in (0, 1):
                state[2, 'y', colour, d].wait_recv()
                state[2, 'z', colour, d].wait_recv()
            for i in range(2):
                lo, hi = piece2(colour, net.at[axis], i), piece2(colour, net.at[axis], 2 + i)
                lo[...] = lo[...] + b2[1, 1, i] + b2[2, 0, i]
                hi[...] = hi[...] + b2[1, 0, i] + b2[2, 1, i]

    def block3(colour, coord, half):
        order = ORDERS[colour]
        ref = piece2(colour, net.at[order[1]], coord)
        return ref if half is None else ref.at[pl.ds(8 * half, 8)]

    def start3():
        for kind in ('x', 'y'):
            for colour, order in enumerate(ORDERS):
                axis, b3 = order[2], buf(colour)[6]
                for d, by in ((0, 1), (1, -1)):
                    src = block3(colour, net.shift(axis, 2), d) if kind == 'x' else block3(colour, net.shift(axis, by), 1 - d)
                    desc = net.copy(src, b3.at[0 if kind == 'x' else 1, d], net.peer(axis, by))
                    desc.start()
                    state[3, kind, colour, d] = desc

    def relay3():
        for colour, order in enumerate(ORDERS):
            axis, b3 = order[2], buf(colour)[6]
            for d, by in ((0, 1), (1, -1)):
                state[3, 'x', colour, d].wait_recv()
                b3[0, d] = b3[0, d] + block3(colour, net.shift(axis, by), d)[...]
                desc = net.copy(b3.at[0, d], b3.at[2, d], net.peer(axis, by))
                desc.start()
                state[3, 'z', colour, d] = desc

    def merge3():
        for colour, order in enumerate(ORDERS):
            axis, b3 = order[2], buf(colour)[6]
            for d in (0, 1):
                state[3, 'y', colour, d].wait_recv()
                state[3, 'z', colour, d].wait_recv()
            lo, hi = block3(colour, net.at[axis], 0), block3(colour, net.at[axis], 1)
            low = lo[...] + b3[1, 1] + b3[2, 0]
            high = hi[...] + b3[1, 0] + b3[2, 1]
            at = 0
            for arr, off, width in segs[colour]:
                outs[arr][pl.ds(0, 8), pl.ds(off, width)] = low[:, at:at + width]
                outs[arr][pl.ds(8, 8), pl.ds(off, width)] = high[:, at:at + width]
                at += width
        net.finish()

    def join(*fns):
        def run():
            for fn in fns:
                fn()
        return run

    return [start1, relay1, join(merge1, start2), relay2, join(merge2, start3), relay3, merge3]


def scatter_kernel(n_arr, segs, *refs):
    parts, outs = refs[:n_arr], refs[n_arr:2 * n_arr]
    send_sem, recv_sem = refs[2 * n_arr:2 * n_arr + 2]
    bufs = refs[2 * n_arr + 2:]
    net = Torus(send_sem, recv_sem)
    net.barrier()
    for stage in scatter_stages(net, parts, outs, segs, bufs):
        stage()


def reduce_scatter(parts, segs, collective_id, sems=160):
    n_arr = len(parts)
    widths = [sum(w for _, _, w in seg) for seg in segs]
    return pl.pallas_call(
        functools.partial(scatter_kernel, n_arr, segs),
        out_shape=[jax.ShapeDtypeStruct((16, p.shape[-1]), jnp.float32) for p in parts],
        in_specs=[pl.BlockSpec(memory_space=pltpu.HBM)] * n_arr,
        out_specs=[pl.BlockSpec(memory_space=pltpu.VMEM)] * n_arr,
        scratch_shapes=[pltpu.SemaphoreType.DMA((sems,)), pltpu.SemaphoreType.DMA((sems,))] + scatter_buffers(widths),
        compiler_params=pltpu.CompilerParams(collective_id=collective_id, has_side_effects=True, vmem_limit_bytes=60 * 2**20),
        name='torus_scatter',
    )(*[p.reshape(4, 4, 4, 16, p.shape[-1]) for p in parts])


SEGS = (((2, 0, 2048),), ((2, 2048, 768), (3, 0, 1280)), ((3, 1280, 128), (1, 0, 512), (0, 0, 1536)))


def layer_norm(values):
    mean_val = jnp.mean(values, axis=-1, keepdims=True)
    centered = values - mean_val
    inv_std = lax.rsqrt(jnp.mean(centered * centered, axis=-1, keepdims=True) + 1e-5)
    return centered * inv_std, inv_std


def norm_backward(grad_norm, normed, inv_std):
    grad_mean = jnp.mean(grad_norm, axis=-1, keepdims=True)
    proj_mean = jnp.mean(grad_norm * normed, axis=-1, keepdims=True)
    return inv_std * (grad_norm - grad_mean - normed * proj_mean)


def rope_tables(seq_len, head_dim):
    inv_freq = 10000.0 ** (-jnp.arange(0, head_dim, 2, dtype=jnp.float32) / head_dim)
    angles = jnp.arange(seq_len, dtype=jnp.float32)[:, None] * inv_freq[None, :]
    return jnp.cos(angles)[:, None, :], jnp.sin(angles)[:, None, :]


def rotate(values, cos_tab, sin_tab):
    half_dim = values.shape[-1] // 2
    x_first = values[..., :half_dim]
    x_second = values[..., half_dim:]
    return jnp.concatenate([x_first * cos_tab - x_second * sin_tab, x_second * cos_tab + x_first * sin_tab], axis=-1)


def device_step(x, grad_y, w_qkv, w_out, w_ff, w_down):
    seq_len = x.shape[1]
    head_dim = w_qkv.shape[3]
    score_scale = head_dim ** -0.5
    cos_tab, sin_tab = rope_tables(seq_len, head_dim)
    causal = jnp.arange(seq_len)[:, None] >= jnp.arange(seq_len)[None, :]

    heads = w_qkv.shape[2]
    ff = w_ff.shape[2]
    shards = [w_qkv.reshape(16, -1), w_out.reshape(heads * head_dim, 16).T, w_ff.reshape(16, -1), w_down.T]
    qkv_full, out_full, ff_full, down_full = all_gather(shards, SEGS, 0)
    qkv_full = qkv_full.reshape(-1, 3, heads, head_dim)
    out_full = out_full.reshape(-1, heads, head_dim)
    ff_full = ff_full.reshape(-1, 2, ff)

    x_f32 = x.astype(jnp.float32)
    normed1, inv_std1 = layer_norm(x_f32)
    normed1_b = normed1.astype(jnp.bfloat16)
    qkv_raw = jnp.einsum('btd,dchn->btchn', normed1_b, qkv_full, preferred_element_type=jnp.float32)
    clip_keep = jnp.abs(qkv_raw) < 8.0
    qkv_cl = jnp.clip(qkv_raw, -8.0, 8.0)
    q_rot = rotate(qkv_cl[:, :, 0], cos_tab, sin_tab).astype(jnp.bfloat16)
    k_rot = rotate(qkv_cl[:, :, 1], cos_tab, sin_tab).astype(jnp.bfloat16)
    v_val = qkv_cl[:, :, 2].astype(jnp.bfloat16)
    scores = jnp.einsum('bqhe,bkhe->bhqk', q_rot, k_rot, preferred_element_type=jnp.float32) * score_scale
    prob_f32 = jax.nn.softmax(jnp.where(causal, scores, -1e30), axis=-1)
    prob_b16 = prob_f32.astype(jnp.bfloat16)
    attn_o = jnp.einsum('bhqk,bkhe->bqhe', prob_b16, v_val, preferred_element_type=jnp.float32).astype(jnp.bfloat16)
    attn_part = jnp.einsum('crif,eif->cre', attn_o, out_full, preferred_element_type=jnp.float32)
    hidden = (x_f32 + lax.psum(attn_part, 'tp')).astype(jnp.bfloat16)
    hidden_f32 = hidden.astype(jnp.float32)
    normed2, inv_std2 = layer_norm(hidden_f32)
    normed2_b = normed2.astype(jnp.bfloat16)
    up_gate = jnp.einsum('btd,dcf->btcf', normed2_b, ff_full, preferred_element_type=jnp.float32)
    up_val = up_gate[:, :, 0]
    gate_val = up_gate[:, :, 1]
    gate_sig = jax.nn.sigmoid(gate_val)
    gate_act = gate_val * gate_sig
    mlp_act = (gate_act * up_val).astype(jnp.bfloat16)
    mlp_part = jnp.einsum('btf,df->btd', mlp_act, down_full, preferred_element_type=jnp.float32)
    y_out = (hidden_f32 + lax.psum(mlp_part, 'tp')).astype(jnp.bfloat16)

    grad_y32 = grad_y.astype(jnp.float32)
    grad_down = jnp.einsum('btd,btf->df', grad_y, mlp_act, preferred_element_type=jnp.float32)
    grad_act = jnp.einsum('btd,df->btf', grad_y, down_full, preferred_element_type=jnp.float32)
    grad_up = grad_act * gate_act
    grad_gate = grad_act * up_val * gate_sig * (1.0 + gate_val * (1.0 - gate_sig))
    grad_upgate = jnp.stack([grad_up, grad_gate], axis=2).astype(jnp.bfloat16)
    grad_ff = jnp.einsum('btd,btcf->dcf', normed2_b, grad_upgate, preferred_element_type=jnp.float32)
    grad_norm2 = lax.psum(jnp.einsum('btcf,dcf->btd', grad_upgate, ff_full, preferred_element_type=jnp.float32), 'tp')
    grad_hidden = grad_y32 + norm_backward(grad_norm2, normed2, inv_std2)
    grad_hidden_b = grad_hidden.astype(jnp.bfloat16)
    grad_out = jnp.einsum('cre,crif->eif', grad_hidden_b, attn_o, preferred_element_type=jnp.float32)
    grad_o = jnp.einsum('cre,eif->crif', grad_hidden_b, out_full, preferred_element_type=jnp.float32).astype(jnp.bfloat16)
    grad_prob = jnp.einsum('bqhe,bkhe->bhqk', grad_o, v_val, preferred_element_type=jnp.float32)
    grad_v = jnp.einsum('bhqk,bqhe->bkhe', prob_b16, grad_o, preferred_element_type=jnp.float32)
    grad_score = prob_f32 * (grad_prob - jnp.sum(grad_prob * prob_f32, axis=-1, keepdims=True))
    grad_score_b = (grad_score * score_scale).astype(jnp.bfloat16)
    grad_q = jnp.einsum('bhqk,bkhe->bqhe', grad_score_b, k_rot, preferred_element_type=jnp.float32)
    grad_k = jnp.einsum('bhqk,bqhe->bkhe', grad_score_b, q_rot, preferred_element_type=jnp.float32)
    grad_qkv_all = jnp.stack([rotate(grad_q, cos_tab, -sin_tab), rotate(grad_k, cos_tab, -sin_tab), grad_v], axis=2)
    grad_qkv_b = jnp.where(clip_keep, grad_qkv_all, 0.0).astype(jnp.bfloat16)
    grad_qkv = jnp.einsum('btd,btchn->dchn', normed1_b, grad_qkv_b, preferred_element_type=jnp.float32)
    grad_norm1 = lax.psum(jnp.einsum('btchn,dchn->btd', grad_qkv_b, qkv_full, preferred_element_type=jnp.float32), 'tp')
    grad_x = (grad_hidden + norm_backward(grad_norm1, normed1, inv_std1)).astype(jnp.bfloat16)
    full = [g.reshape(1024, -1) for g in (grad_qkv, grad_out, grad_ff, grad_down)]
    own_qkv, own_out, own_ff, own_down = reduce_scatter(full, SEGS, 1)
    own_out = own_out.T.reshape(heads, head_dim, 16)
    return y_out, grad_x, own_qkv.reshape(16, 3, heads, head_dim), own_out, own_ff.reshape(16, 2, ff), own_down.T


def solution(mesh):
    act_spec = P('fsdp', None, None)
    weight_specs = (P('fsdp', None, 'tp', None), P('tp', None, 'fsdp'), P('fsdp', None, 'tp'), P('tp', 'fsdp'))
    return jax.shard_map(device_step, mesh=mesh, in_specs=(act_spec, act_spec) + weight_specs, out_specs=(act_spec, act_spec) + weight_specs, check_vma=False)
```

```python
import functools

import jax
import jax.numpy as jnp
import numpy as np
from jax import lax
from jax.experimental import pallas as pl
from jax.experimental.pallas import tpu as pltpu
from jax.sharding import PartitionSpec as P

MESH_ID = pl.DeviceIdType.MESH
SIDE = 4
PIECE = 16
ORDERS = ((2, 1, 0), (1, 0, 2), (0, 2, 1))
BOTH = ((0, 1), (1, -1))
PHASES = range(3)


class Torus:
    def __init__(self):
        self.core = lax.axis_index('tp')
        self.index = lax.axis_index('fsdp')
        self.at = (self.index // (SIDE * SIDE), (self.index // SIDE) % SIDE, self.index % SIDE)
        self.partner = (1 - self.core, self.index)

    def shift(self, axis, by):
        return (self.at[axis] + by + SIDE) % SIDE

    def peer(self, axis, by):
        pos = list(self.at)
        pos[axis] = self.shift(axis, by)
        return (self.core, (pos[0] * SIDE + pos[1]) * SIDE + pos[2])

    def neighbours(self):
        return [self.peer(axis, by) for axis in range(3) for _, by in BOTH]

    def tell(self, sem, devices):
        for device in devices:
            pl.semaphore_signal(sem, inc=1, device_id=device, device_id_type=MESH_ID)

    def barrier(self, devices):
        sem = pltpu.get_barrier_semaphore()
        self.tell(sem, devices)
        pl.semaphore_wait(sem, len(devices))


def in_order(*calls):
    def run():
        for call in calls:
            call()
    return run


class Gather:
    COPIES = 36

    def __init__(self, net, shard, out, widths, sems, first):
        self.net, self.shard, self.out, self.sems, self.first = net, shard, out, sems, first
        self.cols = [(sum(widths[:i]), w) for i, w in enumerate(widths)]

    def block(self, colour, phase, coord, half=None):
        order = ORDERS[colour]
        off, width = self.cols[colour]
        pick = list(self.net.at)
        for axis in order[:phase]:
            pick[axis] = pl.ds(0, SIDE)
        pick[order[phase]] = coord
        if half is not None and phase:
            pick[order[0]] = pl.ds(half * 2, 2)
        elif half is not None:
            cut = width - width // 256 * 128
            off, width = (off + cut, width - cut) if half else (off, cut)
        return self.out.at[pick[0], pick[1], pick[2], :, pl.ds(off, width)] if width else None

    def copy(self, phase, colour, relay, d, by, came=False):
        axis = ORDERS[colour][phase]
        back = -by if relay else 0
        coord = self.net.shift(axis, back - by if came else back)
        dst = src = self.block(colour, phase, coord, d if relay else None)
        if dst is None:
            return None
        if not (phase or relay or came):
            off, width = self.cols[colour]
            src = self.shard.at[:, pl.ds(off, width)]
        at = self.first + ((phase * 3 + colour) * 2 + relay) * 2 + d
        return pltpu.make_async_remote_copy(src, dst, self.sems.at[0, at], self.sems.at[1, at], device_id=self.net.peer(axis, by), device_id_type=MESH_ID)

    def each(self, phase, relay, act, came=False):
        for d, by in BOTH:
            for colour in range(3):
                desc = self.copy(phase, colour, relay, d, by, came)
                if desc is not None:
                    act(desc)

    def own(self):
        at = self.net.at
        return pltpu.make_async_copy(self.shard, self.out.at[at[0], at[1], at[2]], self.sems.at[0, self.first + self.COPIES])

    def start(self, phase):
        if phase:
            self.each(phase - 1, 1, lambda c: c.wait_recv(), True)
        if phase == 1:
            self.own().wait()
        self.each(phase, 0, lambda c: c.start())
        if not phase:
            self.own().start()

    def relay(self, phase):
        for d, by in BOTH:
            for colour in range(3):
                self.copy(phase, colour, 0, d, by, True).wait_recv()
                desc = self.copy(phase, colour, 1, d, by)
                if desc is not None:
                    desc.start()

    def finish(self):
        self.each(PHASES[-1], 1, lambda c: c.wait_recv(), True)
        for phase in PHASES:
            for relay in range(2):
                self.each(phase, relay, lambda c: c.wait_send())

    def stages(self):
        return [functools.partial(f, p) for p in PHASES for f in (self.start, self.relay)] + [self.finish]


def gather_kernel(widths, shard, out, sems):
    net = Torus()
    net.barrier(net.neighbours())
    for stage in Gather(net, shard, out, widths, sems, 0).stages():
        stage()


def all_gather(shard, widths, collective_id):
    out = pl.pallas_call(
        functools.partial(gather_kernel, widths),
        out_shape=jax.ShapeDtypeStruct((SIDE, SIDE, SIDE) + shard.shape, shard.dtype),
        in_specs=[pl.BlockSpec(memory_space=pltpu.VMEM)],
        out_specs=pl.BlockSpec(memory_space=pltpu.HBM),
        scratch_shapes=[pltpu.SemaphoreType.DMA((2, Gather.COPIES + 1))],
        compiler_params=pltpu.CompilerParams(collective_id=collective_id, has_side_effects=True),
        name='torus_gather',
    )(shard)
    return out.reshape(-1, shard.shape[-1])


class Scatter:
    COPIES = 54

    def __init__(self, net, part, cols, bufs, sems, first):
        self.net, self.part, self.cols, self.bufs, self.sems, self.first = net, part, cols, bufs, sems, first

    @staticmethod
    def scratch(cols):
        shapes = []
        for _, w in cols:
            shapes += [(3, 2, 2, SIDE, PIECE, w), (3, 2, 2, PIECE, w), (3, 2, PIECE // 2, w)]
        return [pltpu.VMEM(s, jnp.float32) for s in shapes]

    def buf(self, colour, phase):
        return self.bufs[colour * len(PHASES) + phase]

    def block(self, colour, phase, coord, half):
        order = ORDERS[colour]
        off, width = self.cols[colour]
        pick = [pl.ds(0, SIDE)] * 3
        for axis in order[:phase]:
            pick[axis] = self.net.at[axis]
        pick[order[phase]] = coord
        rows = pl.ds(0, PIECE)
        rest = sorted(order[phase + 1:])
        if rest:
            pick[rest[0]] = pl.ds(2 * half, 2)
        else:
            rows = pl.ds(PIECE // 2 * half, PIECE // 2)
        return self.part.at[pick[0], pick[1], pick[2], rows, pl.ds(off, width)]

    def copy(self, phase, colour, kind, d, by):
        axis = ORDERS[colour][phase]
        buf = self.buf(colour, phase)
        if kind == 2:
            src = buf.at[0, d]
        elif kind:
            src = self.block(colour, phase, self.net.shift(axis, by), 1 - d)
        else:
            src = self.block(colour, phase, self.net.shift(axis, 2), d)
        at = self.first + ((phase * 3 + colour) * 3 + kind) * 2 + d
        return pltpu.make_async_remote_copy(src, buf.at[kind, d], self.sems.at[0, at], self.sems.at[1, at], device_id=self.net.peer(axis, by), device_id_type=MESH_ID)

    def start(self, phase):
        for kind in range(2):
            for d, by in BOTH:
                for colour in range(3):
                    self.copy(phase, colour, kind, d, by).start()

    def relay(self, phase):
        for colour in range(3):
            buf = self.buf(colour, phase)
            for d, by in BOTH:
                self.copy(phase, colour, 0, d, by).wait_recv()
                buf[0, d] = buf[0, d] + self.block(colour, phase, self.net.shift(ORDERS[colour][phase], by), d)[...]
                self.copy(phase, colour, 2, d, by).start()

    def merge(self, phase):
        for colour in range(3):
            buf = self.buf(colour, phase)
            for d, by in BOTH:
                for kind in (1, 2):
                    self.copy(phase, colour, kind, d, by).wait_recv()
            for half in range(2):
                mine = self.block(colour, phase, self.net.at[ORDERS[colour][phase]], half)
                mine[...] = mine[...] + buf[1, 1 - half] + buf[2, half]
        if phase + 1 < len(PHASES):
            self.start(phase + 1)

    def finish(self):
        for phase in PHASES:
            for colour in range(3):
                for kind in PHASES:
                    for d, by in BOTH:
                        self.copy(phase, colour, kind, d, by).wait_send()

    def stages(self):
        calls = [functools.partial(self.start, 0)]
        for phase in PHASES:
            calls += [functools.partial(self.relay, phase), functools.partial(self.merge, phase)]
        return calls[:-1] + [in_order(calls[-1], self.finish)]

    def result(self):
        at = self.net.at
        return self.part[at[0], at[1], at[2]]


def cut_three(width, off=0):
    tiles = width // 128
    sizes = [(tiles + 2 - i) // 3 * 128 for i in range(3)]
    return [(off + sum(sizes[:i]), s) for i, s in enumerate(sizes)]


def plan(text, *sets):
    left = [iter(s) for s in sets]
    return [(hook, next(left[int(which)])) for hook, field in enumerate(text.split(',')) for which in field]


def halves_of(calls, first=0):
    return [[((when - first) // 2, call) for when, call in calls if when >= first and (when - first) % 2 == odd] for odd in range(2)]


def run_at(hook, calls):
    for when, call in calls:
        pl.when(hook == when)(call)


F32, BF16 = jnp.float32, jnp.bfloat16
QB = 256
LANES = 128
MIB = 2**20


def nt(a, b):
    return lax.dot_general(a, b, (((1,), (1,)), ((), ())), preferred_element_type=F32)


def nn(a, b):
    return jnp.dot(a, b, preferred_element_type=F32)


def tn(a, b):
    return lax.dot_general(a, b, (((0,), (0,)), ((), ())), preferred_element_type=F32)


def over_keys(reduce, values):
    return reduce(values, axis=0, keepdims=True)


def over_lanes(values):
    return jnp.mean(values, axis=-1, keepdims=True)


def head_masks(paired):
    lane = lax.broadcasted_iota(jnp.int32, (1, LANES), 1)
    first = (lane % 64) < 32 if paired else lane < 64
    return first, jnp.logical_not(first)


def causal_block():
    return lax.broadcasted_iota(jnp.int32, (QB, QB), 0) <= lax.broadcasted_iota(jnp.int32, (QB, QB), 1)


def attend_pair(q_ref, k_ref, v_ref, o_ref, lse_ref, hook):
    seq = q_ref.shape[0]
    zero = jnp.zeros((), BF16)
    masks = head_masks(True)
    key = k_ref[...]
    keys = [jnp.where(m, key, zero) for m in masks]
    vt = v_ref[...].astype(F32).T.astype(BF16)
    causal = causal_block()
    for i in reversed(range(seq // QB)):
        lo, hi = i * QB, (i + 1) * QB
        query = q_ref[lo:hi, :]
        outs = []
        for h in range(2):
            diag = jnp.where(causal, nt(keys[h][lo:hi], query), -1e30)
            top = over_keys(jnp.max, diag)
            if i:
                past = nt(keys[h][:lo], query)
                top = jnp.maximum(top, over_keys(jnp.max, past))
                past = jnp.exp(past - top)
            diag = jnp.exp(diag - top)
            total = over_keys(jnp.sum, diag)
            if i:
                total = total + over_keys(jnp.sum, past)
            scale = 1.0 / total
            lse_ref[h:h + 1, lo:hi] = top + jnp.log(total)
            vh = vt[64 * h:64 * h + 64]
            acc = nn(vh[:, lo:hi], (diag * scale).astype(BF16))
            if i:
                acc = acc + nn(vh[:, :lo], (past * scale).astype(BF16))
            outs.append(acc)
        o_ref[lo:hi, :] = jnp.concatenate(outs, axis=0).T.astype(BF16)
        if hi == seq:
            hook()


def attend_pair_back(q_ref, k_ref, v_ref, do_ref, lse_ref, dk_ref, dv_ref, put_dq, hook):
    seq = q_ref.shape[0]
    zero = jnp.zeros((), BF16)
    qmask, vmask = head_masks(True), head_masks(False)
    key, val = k_ref[...], v_ref[...]
    keys = [jnp.where(m, key, zero) for m in qmask]
    vals = [jnp.where(m, val, zero) for m in vmask]
    keys_t = [k.astype(F32).T.astype(BF16) for k in keys]
    causal = causal_block()
    for i in reversed(range(seq // QB)):
        lo, hi = i * QB, (i + 1) * QB
        query, dout = q_ref[lo:hi, :], do_ref[lo:hi, :]
        probs, dscores = [], []
        for h in range(2):
            lse = lse_ref[h:h + 1, lo:hi]
            prob = jnp.where(causal, jnp.exp(nt(keys[h][lo:hi], query) - lse), 0.0)
            grad = nt(vals[h][lo:hi], dout)
            drop = over_keys(jnp.sum, prob * grad)
            if i:
                prob_p = jnp.exp(nt(keys[h][:lo], query) - lse)
                grad_p = nt(vals[h][:lo], dout)
                drop = drop + over_keys(jnp.sum, prob_p * grad_p)
            ds = (prob * (grad - drop)).astype(BF16)
            prob = prob.astype(BF16)
            if i:
                ds = jnp.concatenate([(prob_p * (grad_p - drop)).astype(BF16), ds], axis=0)
                prob = jnp.concatenate([prob_p.astype(BF16), prob], axis=0)
            probs.append(prob)
            dscores.append(ds)
        dq_t = nn(keys_t[0][:, :hi], dscores[0]) + nn(keys_t[1][:, :hi], dscores[1])
        put_dq(lo, hi, dq_t.T)
        both = jnp.concatenate([jnp.where(m, dout, zero) for m in vmask], axis=0)
        dv = nn(jnp.concatenate(probs, axis=1), both)
        both = jnp.concatenate([jnp.where(m, query, zero) for m in qmask], axis=0)
        dk = nn(jnp.concatenate(dscores, axis=1), both)
        if hi == seq:
            dv_ref[...] = dv
            dk_ref[...] = dk
            hook()
        else:
            dv_ref[:hi, :] += dv
            dk_ref[:hi, :] += dk


def swap_halves(values):
    return pltpu.roll(values, LANES // 2, axis=1)


def tables(seq, head):
    freq = 10000.0 ** (-np.arange(0, head, 2, dtype=np.float64) / head)
    angle = np.arange(seq, dtype=np.float64)[:, None] * freq[None, :]
    cos, sin = np.cos(angle).astype(np.float32), np.sin(angle).astype(np.float32)
    return np.concatenate([cos] * 4, axis=1), np.concatenate([-sin, -sin, sin, sin], axis=1)


def norm_rows(values):
    mean = over_lanes(values)
    centered = values - mean
    inv = lax.rsqrt(over_lanes(centered * centered) + 1e-5)
    return centered * inv, inv


def norm_grad(grad, normed, inv):
    mean = over_lanes(grad)
    proj = over_lanes(grad * normed)
    return inv * (grad - mean - normed * proj)


def params(collective_id=None):
    return pltpu.CompilerParams(collective_id=collective_id, has_side_effects=collective_id is not None, vmem_limit_bytes=63 * MIB)


def dma(*shape):
    return pltpu.SemaphoreType.DMA(shape)


def shape(dtype, *dims):
    return jax.ShapeDtypeStruct(dims, dtype)


HBM = pl.BlockSpec(memory_space=pltpu.HBM)
WHOLE = pl.BlockSpec(memory_space=pltpu.VMEM)


def fixed(block, index=(0, 0)):
    return pl.BlockSpec(block, lambda *grid: index, pipeline_mode=pl.Buffered(buffer_count=1))


def qkv_kernel(x_ref, w_ref, cos_ref, sin_ref, qkv_ref, keep_ref):
    normed, _ = norm_rows(x_ref[...].astype(F32))
    raw = nn(normed.astype(BF16), w_ref[...])
    keep_ref[...] = (jnp.abs(raw) < 8.0).astype(F32).astype(BF16)
    cut = jnp.clip(raw, -8.0, 8.0)
    cos, sin = cos_ref[...], sin_ref[...]
    tiles = raw.shape[1] // LANES
    for j in range(tiles):
        cols = slice(LANES * j, LANES * (j + 1))
        tile = cut[:, cols]
        if j < 2 * tiles // 3:
            tile = tile * cos + swap_halves(tile) * sin
        if j < tiles // 3:
            tile = tile * 0.125
        qkv_ref[:, cols] = tile.astype(BF16)


def qkv_proj(x, w, cos, sin, block=512):
    rows, d = x.shape
    cols = w.shape[1]
    per = cos.shape[0] // block
    row = lambda width: pl.BlockSpec((block, width), lambda i: (i, 0))
    tab = pl.BlockSpec((block, LANES), lambda i: (i % per, 0))
    return pl.pallas_call(
        qkv_kernel,
        grid=(rows // block,),
        in_specs=[row(d), fixed((d, cols)), tab, tab],
        out_specs=[row(cols)] * 2,
        out_shape=[shape(BF16, rows, cols)] * 2,
        compiler_params=params(),
        name='project',
    )(x, w, cos, sin)


CHUNK = 256
GATHER_PLAN = '01,01,01,01,0,0,01,,,,1,,,,,,1'
SCATTER_PLAN = ',,,0,,,0,1,,,,20,0,01,01,0,,1,1,12,2,1,2,,2,,2,2'
LAST_PLAN = ',,0,0,0,0,0'


def aligned(at, size):
    return pl.ds(pl.multiple_of(at, size), size)


def to_partner(net, src, dst, send, recv):
    return pltpu.make_async_remote_copy(src, dst, send, recv, device_id=net.partner, device_id_type=MESH_ID)


def attn_out_kernel(widths, q_ref, k_ref, v_ref, x_ref, out_shard, ff_shard, o_ref, lse_ref, h_hbm, wo_hbm, wf_hbm,
                    o_all, part, got, h_buf, wo, sems, gather_sems, local_sem):
    b, p = pl.program_id(0), pl.program_id(1)
    pairs = pl.num_programs(1)
    step = b * pairs + p
    seq = q_ref.shape[0]
    half = CHUNK // 2
    chunks = seq // CHUNK
    net = Torus()
    g_out = Gather(net, out_shard, wo_hbm, widths[0], gather_sems, 0)
    g_ff = Gather(net, ff_shard, wf_hbm, widths[1], gather_sems, Gather.COPIES + 1)
    calls = plan(GATHER_PLAN, g_out.stages(), g_ff.stages())

    @pl.when(step == 0)
    def _():
        net.barrier(net.neighbours() + [net.partner])

    begin, middle = halves_of(calls)
    run_at(step, begin)
    attend_pair(q_ref, k_ref, v_ref, o_ref, lse_ref.at[0, 0], lambda: run_at(step, middle))
    o_all[p] = o_ref[...]

    def rows_in(c, core):
        return aligned(c * CHUNK + core * half, half)

    def part_copy(c):
        return to_partner(net, part.at[rows_in(c, 1 - net.core)], got.at[b, c], sems.at[0, b, c], sems.at[1, b, c])

    def h_rows(c, core):
        return h_hbm.at[aligned(b * seq + c * CHUNK + core * half, half)]

    def h_copy(c, core):
        return to_partner(net, h_buf.at[b, c], h_rows(c, core), sems.at[2, b, c], sems.at[3, b, c])

    def h_local(c):
        return pltpu.make_async_copy(h_buf.at[b, c], h_rows(c, net.core), local_sem.at[b, c])

    @pl.when(step == pairs - 1)
    def _():
        load = pltpu.make_async_copy(wo_hbm, wo, local_sem.at[0, 0])
        load.start()
        load.wait()

    @pl.when(p == pairs - 1)
    def _():
        o_full = jnp.concatenate([o_all[j] for j in range(o_all.shape[0])], axis=1)
        weight = wo[...].reshape(part.shape[1], -1)
        for c in range(chunks):
            rows = slice(c * CHUNK, (c + 1) * CHUNK)
            part[rows, :] = nt(o_full[rows], weight)
            part_copy(c).start()
        for c in range(chunks):
            part_copy(c).wait()
            own = rows_in(c, net.core)
            h_buf[b, c] = (x_ref[own, :].astype(F32) + (part[own, :] + got[b, c])).astype(BF16)
            h_copy(c, net.core).start()
            h_local(c).start()
        for c in range(chunks):
            h_copy(c, net.core).wait_send()
            h_local(c).wait()
            h_copy(c, 1 - net.core).wait_recv()

    run_at(step + 1, begin[-1:])


def attn_out(qkv, x, out_shard, ff_shard, batch, seq, pairs, collective_id):
    spec = lambda part: pl.BlockSpec((seq, LANES), lambda b, p: (b, part * pairs + p))
    d = x.shape[1]
    chunks = seq // CHUNK
    vm = pltpu.VMEM
    widths = tuple(tuple(w for _, w in cut_three(s.shape[1])) for s in (out_shard, ff_shard))
    torus = (SIDE, SIDE, SIDE)
    return pl.pallas_call(
        functools.partial(attn_out_kernel, widths),
        grid=(batch, pairs),
        in_specs=[spec(0), spec(1), spec(2), pl.BlockSpec((seq, d), lambda b, p: (b, 0)), WHOLE, WHOLE],
        out_specs=[spec(0), pl.BlockSpec((1, 1, 2, seq), lambda b, p: (b, p, 0, 0)), HBM, HBM, HBM],
        out_shape=[shape(BF16, batch * seq, LANES * pairs), shape(F32, batch, pairs, 2, seq), shape(BF16, batch * seq, d),
                   shape(BF16, *torus, *out_shard.shape), shape(BF16, *torus, *ff_shard.shape)],
        scratch_shapes=[vm((pairs, seq, LANES), BF16), vm((seq, d), F32), vm((batch, chunks, CHUNK // 2, d), F32), vm((batch, chunks, CHUNK // 2, d), BF16),
                        vm(torus + out_shard.shape, BF16), dma(4, batch, chunks), dma(2, 2 * (Gather.COPIES + 1)), dma(batch, chunks)],
        compiler_params=params(collective_id),
        name='attend_out',
    )(qkv, qkv, qkv, x, out_shard, ff_shard)


class Exchange:
    def __init__(self, net, step, rows, partials, results, sems, local_sem):
        self.net, self.step, self.rows, self.partials, self.results, self.sems, self.local_sem = net, step, rows, partials, results, sems, local_sem

    def half(self, core, at=0):
        return aligned(at * self.rows + core * (self.rows // 2), self.rows // 2)

    def sem(self, which, parity):
        return self.sems.at[0, which, parity], self.sems.at[1, which, parity]

    def part(self, which):
        part, got = self.partials[which]
        slot = self.step % 2
        return to_partner(self.net, part.at[self.half(1 - self.net.core)], got.at[slot], *self.sem(which, slot))

    def total(self, which):
        part, got = self.partials[which]
        self.part(which).wait()
        return part[self.half(self.net.core), :] + got[self.step % 2]

    def copies(self, at, core):
        out = []
        for i, (buf, hbm) in enumerate(self.results):
            rows = hbm.at[self.half(core, at)]
            out.append((to_partner(self.net, buf, rows, *self.sem(len(self.partials) + i, at % 2)), pltpu.make_async_copy(buf, rows, self.local_sem.at[i])))
        return out

    def publish(self):
        for remote, local in self.copies(self.step, self.net.core):
            remote.start()
            local.start()

    def settle(self, at):
        for remote, local in self.copies(at, self.net.core):
            remote.wait_send()
            local.wait()
        for remote, _ in self.copies(at, 1 - self.net.core):
            remote.wait_recv()


def mlp_kernel(h_ref, gy_ref, wff_ref, wd_ref, y_hbm, gh_hbm, gh32_ref, act, gug, n2_ref,
               part_y, part_g, got_y, got_g, y_buf, gh_buf, sems, local_sem):
    step, steps = pl.program_id(0), pl.num_programs(0)
    rows, d = h_ref.shape
    ff = wd_ref.shape[1]
    net = Torus()
    swap = Exchange(net, step, rows, ((part_y, got_y), (part_g, got_g)), ((y_buf, y_hbm), (gh_buf, gh_hbm)), sems, local_sem)

    @pl.when(step == 0)
    def _():
        net.barrier([net.partner])

    n2, _ = norm_rows(h_ref[...].astype(F32))
    n2 = n2.astype(BF16)
    n2_ref[...] = n2
    gy = gy_ref[...]
    for j in range(0, ff, QB):
        w = min(QB, ff - j)
        gact = nn(gy, wd_ref[:, j:j + w])
        for i in range(j, j + w, LANES):
            at, mid, end = 2 * i, 2 * i + LANES, 2 * i + QB
            ug = nn(n2, wff_ref[:, at:end])
            up, gate = ug[:, :LANES], ug[:, LANES:]
            sig = 1.0 / (1.0 + jnp.exp(-gate))
            silu = gate * sig
            act[:, i:i + LANES] = (silu * up).astype(BF16)
            ga = gact[:, i - j:i - j + LANES]
            gug[:, at:mid] = (ga * silu).astype(BF16)
            gug[:, mid:end] = (ga * up * sig * (1.0 + gate * (1.0 - sig))).astype(BF16)

    for which, left, right, part in ((0, act, wd_ref, part_y), (1, gug, wff_ref, part_g)):
        for j in range(0, d, QB):
            part[:, j:j + QB] = nt(left[...], right[j:j + QB, :])
        swap.part(which).start()

    @pl.when(step > 0)
    def _():
        swap.settle(step - 1)

    own = swap.half(net.core)
    h_own = h_ref[own, :].astype(F32)
    normed, inv = norm_rows(h_own)
    y_buf[...] = (h_own + swap.total(0)).astype(BF16)
    gh = gy_ref[own, :].astype(F32) + norm_grad(swap.total(1), normed, inv)
    gh32_ref[...] = gh
    gh_buf[...] = gh.astype(BF16)
    swap.publish()

    @pl.when(step == steps - 1)
    def _():
        swap.settle(step)


def mlp(h, gy, weights, collective_id, block=512):
    rows, d = h.shape
    ff = weights.shape[1] // 3
    half = block // 2
    row = lambda n, width: pl.BlockSpec((n, width), lambda i: (i, 0))
    vm = pltpu.VMEM
    return pl.pallas_call(
        mlp_kernel,
        grid=(rows // block,),
        in_specs=[row(block, d), row(block, d), fixed((d, 2 * ff)), fixed((d, ff), (0, 2))],
        out_specs=[HBM, HBM, row(half, d), row(block, ff), row(block, 2 * ff), row(block, d)],
        out_shape=[shape(BF16, rows, d), shape(BF16, rows, d), shape(F32, rows // 2, d), shape(BF16, rows, ff), shape(BF16, rows, 2 * ff), shape(BF16, rows, d)],
        scratch_shapes=[vm((block, d), F32), vm((block, d), F32), vm((2, half, d), F32), vm((2, half, d), F32), vm((half, d), BF16), vm((half, d), BF16),
                        dma(2, 4, 2), dma(2)],
        compiler_params=params(collective_id),
        name='mlp',
    )(h, gy, weights, weights)


def accumulate(part, cols, first, left, right):
    for j in range(0, right.shape[1], QB):
        w = min(QB, right.shape[1] - j)
        prod = tn(left, right[:, j:j + w]).reshape(part.shape[:-1] + (w,))
        at = slice(cols + j, cols + j + w)
        part[..., at] = jnp.where(first, 0.0, part[..., at]) + prod


CHUNK_STEPS = 4
SETS = 3
HEAD_STEP = SETS * CHUNK_STEPS


def back_kernel(cols, pairs, gy_ref, n2_ref, act_ref, gug_ref, q_ref, k_ref, v_ref, lse_ref, gh_ref, wo_ref, o_ref, keep_q, keep_k, keep_v, cos_ref, sin_ref,
                gq_ref, gk_ref, gv_ref, gw_ref, grads_ref, do_ref, dk_ref, dv_ref, parts, sems, *bufs):
    step = pl.program_id(0)
    turn = step - HEAD_STEP
    p = turn % pairs
    net = Torus()
    per = len(bufs) // SETS
    scatters = [Scatter(net, parts.at[i], cols, bufs[per * i:per * i + per], sems, i * Scatter.COPIES) for i in range(SETS)]
    calls = plan(SCATTER_PLAN, *(s.stages() for s in scatters))
    middle, end = halves_of(calls, HEAD_STEP)

    @pl.when(step == 0)
    def _():
        net.barrier(net.neighbours())

    first = step % CHUNK_STEPS == 0

    @pl.when(step < CHUNK_STEPS)
    def _():
        accumulate(parts.at[0], 0, first, gy_ref[...], act_ref)

    @pl.when((step >= CHUNK_STEPS) & (step < HEAD_STEP))
    def _():
        accumulate(parts.at[step // CHUNK_STEPS], 0, first, n2_ref[...], gug_ref)

    run_at(step, [c for c in calls if c[0] < HEAD_STEP])

    def back(values, lo, hi, keep):
        turned = values * cos_ref[lo:hi, :] - swap_halves(values) * sin_ref[lo:hi, :]
        return (turned * keep[lo:hi, :].astype(F32)).astype(BF16)

    def put_dq(lo, hi, dq):
        gq_ref[lo:hi, :] = back(dq * 0.125, lo, hi, keep_q)

    @pl.when(turn >= 0)
    def _():
        @pl.when(p == 0)
        def _():
            gh = gh_ref[...]
            dout = nn(gh, wo_ref[...]).astype(BF16)
            for j in range(pairs):
                do_ref[j] = dout[:, LANES * j:LANES * (j + 1)]
            gw_ref[...] = jnp.where(turn == 0, 0.0, gw_ref[...]) + tn(gh, o_ref[...])

        attend_pair_back(q_ref, k_ref, v_ref, do_ref.at[p], lse_ref.at[0, 0], dk_ref, dv_ref, put_dq, lambda: run_at(turn, middle))
        seq = q_ref.shape[0]
        gk_ref[...] = back(dk_ref[...], 0, seq, keep_k)
        gv_ref[...] = (dv_ref[...] * keep_v[...].astype(F32)).astype(BF16)
        run_at(turn, end)

    @pl.when(step == pl.num_programs(0) - 1)
    def _():
        for i, scatter in enumerate(scatters):
            grads_ref[i] = scatter.result()


def back(gy, n2, act, gug, qkv, lse, gh, wo_t, o, keep, cos, sin, batch, seq, pairs, collective_id):
    rows, d = gy.shape
    ff = act.shape[1]
    block = rows // CHUNK_STEPS
    turn = lambda s: jnp.maximum(s - HEAD_STEP, 0)
    head = lambda part: pl.BlockSpec((seq, LANES), lambda s: (turn(s) // pairs, part * pairs + turn(s) % pairs))
    chunk = lambda s, i: jnp.clip(s - i * CHUNK_STEPS, 0, CHUNK_STEPS - 1)
    late = lambda s: jnp.where(s < 2 * CHUNK_STEPS, chunk(s, 1), chunk(s, 2))
    cols = cut_three(ff)
    vm = pltpu.VMEM
    once = pl.Buffered(buffer_count=1)
    per_seq = lambda width: pl.BlockSpec((seq, width), lambda s: (turn(s) // pairs, 0), pipeline_mode=once)
    return pl.pallas_call(
        functools.partial(back_kernel, cols, pairs),
        grid=(HEAD_STEP + batch * pairs,),
        in_specs=[pl.BlockSpec((block, d), lambda s: (chunk(s, 0), 0)), pl.BlockSpec((block, d), lambda s: (late(s), 0)),
                  pl.BlockSpec((block, ff), lambda s: (chunk(s, 0), 0)), pl.BlockSpec((block, ff), lambda s: (late(s), jnp.where(s < 2 * CHUNK_STEPS, 0, 1))),
                  head(0), head(1), head(2), pl.BlockSpec((1, 1, 2, seq), lambda s: (turn(s) // pairs, turn(s) % pairs, 0, 0)),
                  per_seq(d), fixed(wo_t.shape), per_seq(LANES * pairs), head(0), head(1), head(2), fixed(cos.shape), fixed(sin.shape)],
        out_specs=[head(0)] * 3 + [fixed(wo_t.shape), fixed((SETS, PIECE, ff), (0, 0, 0))],
        out_shape=[shape(BF16, rows, LANES * pairs)] * 3 + [shape(F32, *wo_t.shape), shape(F32, SETS, PIECE, ff)],
        scratch_shapes=[vm((pairs, seq, LANES), BF16), vm((seq, LANES), F32), vm((seq, LANES), F32), vm((SETS, SIDE, SIDE, SIDE, PIECE, ff), F32),
                        dma(2, SETS * Scatter.COPIES)] + Scatter.scratch(cols) * SETS,
        compiler_params=params(collective_id),
        name='back',
    )(gy, n2, act, gug, qkv, qkv, qkv, lse, gh, wo_t, o, keep, keep, keep, cos, sin)


def last_kernel(cols, blocks, x_ref, gq_ref, gk_ref, gv_ref, gh_ref, w_ref, gout_hbm, gx_hbm, gw_ref,
                parts, part, got, buf, sems, scatter_sems, local_sem, *bufs):
    step = pl.program_id(0)
    turn = step - blocks
    rows, d = x_ref.shape
    net = Torus()
    scatter = Scatter(net, parts, cols, bufs, scatter_sems, 0)
    stages = scatter.stages()
    swap = Exchange(net, turn, rows, ((part, got),), ((buf, gx_hbm),), sems, local_sem)
    grads = (gq_ref, gk_ref, gv_ref)
    third = gq_ref.shape[1]
    load = pltpu.make_async_copy(gout_hbm, parts.at[:, :, :, :, pl.ds(len(grads) * third, gout_hbm.shape[-1])], local_sem.at[1])

    @pl.when(step == 0)
    def _():
        load.start()
        net.barrier(net.neighbours() + [net.partner])

    @pl.when(turn < 0)
    def _():
        normed, _ = norm_rows(x_ref[...].astype(F32))
        for i, g in enumerate(grads):
            accumulate(parts, third * i, step == 0, normed.astype(BF16), g)

    @pl.when(turn == -1)
    def _():
        load.wait()
        stages[0]()

    @pl.when(turn >= 0)
    def _():
        for j in range(0, d, QB):
            part[:, j:j + QB] = sum(nt(g[...], w_ref[j:j + QB, third * i:third * (i + 1)]) for i, g in enumerate(grads))
        swap.part(0).start()
        run_at(turn, [(2, stages[1]), (3, stages[2])])

        @pl.when(turn > 0)
        def _():
            swap.settle(turn - 1)

        normed, inv = norm_rows(x_ref[swap.half(net.core), :].astype(F32))
        buf[...] = (gh_ref[...] + norm_grad(swap.total(0), normed, inv)).astype(BF16)
        swap.publish()

    @pl.when(turn == blocks - 1)
    def _():
        swap.settle(turn)
        for stage in stages[3:]:
            stage()
        gw_ref[...] = scatter.result()


def last(x, gq, gk, gv, gh32, w, gout, collective_id, block=512):
    rows, d = x.shape
    blocks = rows // block
    row = lambda n, width: pl.BlockSpec((n, width), lambda s: (s % blocks, 0))
    vm = pltpu.VMEM
    half = block // 2
    torus = (SIDE, SIDE, SIDE, PIECE)
    gout = gout.reshape(torus + (-1,))
    width = w.shape[1] + gout.shape[-1]
    cols = cut_three(width)
    return pl.pallas_call(
        functools.partial(last_kernel, cols, blocks),
        grid=(2 * blocks,),
        in_specs=[row(block, d)] + [row(block, gq.shape[1])] * 3 + [pl.BlockSpec((half, d), lambda s: (jnp.maximum(s - blocks, 0), 0)), fixed(w.shape), HBM],
        out_specs=[HBM, fixed((PIECE, width))],
        out_shape=[shape(BF16, rows, d), shape(F32, PIECE, width)],
        scratch_shapes=[vm(torus + (width,), F32), vm((block, d), F32), vm((2, half, d), F32), vm((half, d), BF16), dma(2, 2, 2), dma(2, Scatter.COPIES), dma(2)] + Scatter.scratch(cols),
        compiler_params=params(collective_id),
        name='last',
    )(x, gq, gk, gv, gh32, w, gout)


def pair_heads(w, head):
    n, width = w.shape
    cut = width // 3 * 2
    qk = w[:, :cut].reshape(n, -1, 2, 2, head // 2).swapaxes(2, 3)
    return jnp.concatenate([qk.reshape(n, cut), w[:, cut:]], axis=1)


def device_step(x, grad_y, w_qkv, w_out, w_ff, w_down):
    batch, seq, d = x.shape
    heads, head = w_qkv.shape[2:]
    pairs = heads // 2
    ff = w_ff.shape[2]
    tiles = ff // LANES
    cos, sin = (jnp.asarray(t) for t in tables(seq, head))
    inter = w_ff.reshape(-1, 2, tiles, LANES).swapaxes(1, 2).reshape(-1, 2 * ff)
    ff_shard = jnp.concatenate([inter, w_down.T], axis=1)
    out_shard = w_out.reshape(heads * head, -1).T
    wq = all_gather(pair_heads(w_qkv.reshape(PIECE, -1), head), (512,) * 3, 0)
    x2, gy = x.reshape(-1, d), grad_y.reshape(-1, d)
    qkv, keep = qkv_proj(x2, wq, cos, sin)
    o, lse, h, wo_t, wf = attn_out(qkv, x2, out_shard, ff_shard, batch, seq, pairs, 1)
    wo_t, wf = wo_t.reshape(d, -1), wf.reshape(d, -1)
    y, gh, gh32, act, gug, n2 = mlp(h, gy, wf, 2)
    gq, gk, gv, gout, grads = back(gy, n2, act, gug, qkv, lse, gh, wo_t, o, keep, cos, sin, batch, seq, pairs, 3)
    gx, gw = last(x2, gq, gk, gv, gh32, wq, gout, 4)
    gff = grads[1:].swapaxes(0, 1).reshape(-1, tiles, 2, LANES).swapaxes(1, 2).reshape(-1, 2, ff)
    gqkv, gout = gw[:, :wq.shape[1]], gw[:, wq.shape[1]:]
    return y.reshape(x.shape), gx.reshape(x.shape), pair_heads(gqkv, head).reshape(w_qkv.shape), gout.T.reshape(heads, head, -1), gff, grads[0].T


def solution(mesh):
    specs = (P('fsdp'), P('fsdp'), P('fsdp', None, 'tp'), P('tp', None, 'fsdp'), P('fsdp', None, 'tp'), P('tp', 'fsdp'))
    return jax.shard_map(device_step, mesh=mesh, in_specs=specs, out_specs=specs, check_vma=False)
```

```python
import functools

import jax
import jax.numpy as jnp
import numpy as np
from jax import lax
from jax.experimental import pallas as pl
from jax.experimental.pallas import tpu as pltpu
from jax.sharding import PartitionSpec as P

MESH_ID = pl.DeviceIdType.MESH
SIDE = 4
PIECE = 16
ORDERS = ((2, 1, 0), (1, 0, 2), (0, 2, 1))
BOTH = ((0, 1), (1, -1))
PHASES = range(3)


class Torus:
    def __init__(self):
        self.core = lax.axis_index('tp')
        self.index = lax.axis_index('fsdp')
        plane, x = lax.div(self.index, SIDE), lax.rem(self.index, SIDE)
        self.at = (lax.div(plane, SIDE), lax.rem(plane, SIDE), x)
        self.partner = (1 - self.core, self.index)
        self.moved = {(axis, by): lax.rem(at + (by + SIDE), SIDE) for axis, at in enumerate(self.at) for by in range(-2, 3)}
        self.peers = {(axis, by): self.place(axis, self.moved[axis, by]) for axis in range(3) for _, by in BOTH}

    def place(self, axis, coord):
        pos = list(self.at)
        pos[axis] = coord
        return (self.core, (pos[0] * SIDE + pos[1]) * SIDE + pos[2])

    def shift(self, axis, by):
        return self.moved[axis, by]

    def peer(self, axis, by):
        return self.peers[axis, by]

    def neighbours(self):
        return list(self.peers.values())

    def tell(self, sem, devices):
        for device in devices:
            pl.semaphore_signal(sem, inc=1, device_id=device, device_id_type=MESH_ID)

    def barrier(self, devices):
        sem = pltpu.get_barrier_semaphore()
        self.tell(sem, devices)
        pl.semaphore_wait(sem, len(devices))


def pair_of(sems, *at):
    return sems.at[(0,) + at], sems.at[(1,) + at]


def in_order(*calls):
    def run():
        for call in calls:
            call()
    return run


class Gather:
    COPIES = 36

    def __init__(self, net, shard, out, widths, sems, first):
        self.net, self.shard, self.out, self.sems, self.first = net, shard, out, sems, first
        self.cols = [(sum(widths[:i]), w) for i, w in enumerate(widths)]

    def block(self, colour, phase, coord, half=None):
        order = ORDERS[colour]
        off, width = self.cols[colour]
        pick = list(self.net.at)
        for axis in order[:phase]:
            pick[axis] = pl.ds(0, SIDE)
        pick[order[phase]] = coord
        if half is not None and phase:
            pick[order[0]] = pl.ds(half * 2, 2)
        elif half is not None:
            cut = width - width // 256 * 128
            off, width = (off + cut, width - cut) if half else (off, cut)
        return self.out.at[pick[0], pick[1], pick[2], :, pl.ds(off, width)] if width else None

    def copy(self, phase, colour, relay, d, by, came=False):
        axis = ORDERS[colour][phase]
        back = -by if relay else 0
        coord = self.net.shift(axis, back - by if came else back)
        dst = src = self.block(colour, phase, coord, d if relay else None)
        if dst is None:
            return None
        if not (phase or relay or came):
            off, width = self.cols[colour]
            src = self.shard.at[:, pl.ds(off, width)]
        at = self.first + ((phase * 3 + colour) * 2 + relay) * 2 + d
        return pltpu.make_async_remote_copy(src, dst, *pair_of(self.sems, at), device_id=self.net.peer(axis, by), device_id_type=MESH_ID)

    def each(self, phase, relay, act, came=False):
        for d, by in BOTH:
            for colour in range(3):
                desc = self.copy(phase, colour, relay, d, by, came)
                if desc is not None:
                    act(desc)

    def own(self):
        at = self.net.at
        return pltpu.make_async_copy(self.shard, self.out.at[at[0], at[1], at[2]], self.sems.at[0, self.first + self.COPIES])

    def start(self, phase):
        if phase:
            self.each(phase - 1, 1, lambda c: c.wait_recv(), True)
        if phase == 1:
            self.own().wait()
        self.each(phase, 0, lambda c: c.start())
        if not phase:
            self.own().start()

    def relay(self, phase):
        for d, by in BOTH:
            for colour in range(3):
                self.copy(phase, colour, 0, d, by, True).wait_recv()
                desc = self.copy(phase, colour, 1, d, by)
                if desc is not None:
                    desc.start()

    def finish(self):
        self.each(PHASES[-1], 1, lambda c: c.wait_recv(), True)
        for phase in PHASES:
            for relay in range(2):
                self.each(phase, relay, lambda c: c.wait_send())

    def stages(self):
        return [functools.partial(f, p) for p in PHASES for f in (self.start, self.relay)] + [self.finish]


def gather_kernel(widths, shard, out, sems):
    net = Torus()
    net.barrier(net.neighbours())
    for stage in Gather(net, shard, out, widths, sems, 0).stages():
        stage()


def all_gather(shard, widths, collective_id):
    out = pl.pallas_call(
        functools.partial(gather_kernel, widths),
        out_shape=jax.ShapeDtypeStruct((SIDE, SIDE, SIDE) + shard.shape, shard.dtype),
        in_specs=[pl.BlockSpec(memory_space=pltpu.VMEM)],
        out_specs=pl.BlockSpec(memory_space=pltpu.HBM),
        scratch_shapes=[pltpu.SemaphoreType.DMA((2, Gather.COPIES + 1))],
        compiler_params=pltpu.CompilerParams(collective_id=collective_id, has_side_effects=True),
        name='torus_gather',
    )(shard)
    return out.reshape(-1, shard.shape[-1])


class Scatter:
    COPIES = 54

    def __init__(self, net, part, cols, bufs, sems, first):
        self.net, self.part, self.cols, self.bufs, self.sems, self.first = net, part, cols, bufs, sems, first

    @staticmethod
    def scratch(cols):
        shapes = []
        for _, w in cols:
            shapes += [(3, 2, 2, SIDE, PIECE, w), (3, 2, 2, PIECE, w), (3, 2, PIECE // 2, w)]
        return [pltpu.VMEM(s, jnp.float32) for s in shapes]

    def buf(self, colour, phase):
        return self.bufs[colour * len(PHASES) + phase]

    def block(self, colour, phase, coord, half):
        order = ORDERS[colour]
        off, width = self.cols[colour]
        pick = [pl.ds(0, SIDE)] * 3
        for axis in order[:phase]:
            pick[axis] = self.net.at[axis]
        pick[order[phase]] = coord
        rows = pl.ds(0, PIECE)
        rest = sorted(order[phase + 1:])
        if rest:
            pick[rest[0]] = pl.ds(2 * half, 2)
        else:
            rows = pl.ds(PIECE // 2 * half, PIECE // 2)
        return self.part.at[pick[0], pick[1], pick[2], rows, pl.ds(off, width)]

    def copy(self, phase, colour, kind, d, by):
        axis = ORDERS[colour][phase]
        buf = self.buf(colour, phase)
        if kind == 2:
            src = buf.at[0, d]
        elif kind:
            src = self.block(colour, phase, self.net.shift(axis, by), 1 - d)
        else:
            src = self.block(colour, phase, self.net.shift(axis, 2), d)
        at = self.first + ((phase * 3 + colour) * 3 + kind) * 2 + d
        return pltpu.make_async_remote_copy(src, buf.at[kind, d], *pair_of(self.sems, at), device_id=self.net.peer(axis, by), device_id_type=MESH_ID)

    def start(self, phase, kind):
        for d, by in BOTH:
            for colour in range(3):
                self.copy(phase, colour, kind, d, by).start()

    def relay(self, phase):
        for colour in range(3):
            buf = self.buf(colour, phase)
            for d, by in BOTH:
                self.copy(phase, colour, 0, d, by).wait_recv()
                buf[0, d] = buf[0, d] + self.block(colour, phase, self.net.shift(ORDERS[colour][phase], by), d)[...]
                self.copy(phase, colour, 2, d, by).start()

    def merge(self, phase):
        for colour in range(3):
            buf = self.buf(colour, phase)
            for d, by in BOTH:
                for kind in (1, 2):
                    self.copy(phase, colour, kind, d, by).wait_recv()
            for half in range(2):
                mine = self.block(colour, phase, self.net.at[ORDERS[colour][phase]], half)
                mine[...] = mine[...] + buf[1, 1 - half] + buf[2, half]
        if phase + 1 < len(PHASES):
            for kind in range(2):
                self.start(phase + 1, kind)

    def finish(self):
        for phase in PHASES:
            for colour in range(3):
                for kind in PHASES:
                    for d, by in BOTH:
                        self.copy(phase, colour, kind, d, by).wait_send()

    def stages(self):
        calls = [functools.partial(self.start, 0, kind) for kind in range(2)]
        for phase in PHASES:
            calls += [functools.partial(self.relay, phase), functools.partial(self.merge, phase)]
        return calls[:-1] + [in_order(calls[-1], self.finish)]

    def result(self):
        at = self.net.at
        return self.part[at[0], at[1], at[2]]


def cut_three(width, off=0):
    tiles = width // 128
    sizes = [(tiles + 2 - i) // 3 * 128 for i in range(3)]
    return [(off + sum(sizes[:i]), s) for i, s in enumerate(sizes)]


def plan(text, *sets):
    left = [iter(s) for s in sets]
    return [(hook, next(left[int(which)])) for hook, field in enumerate(text.split(',')) for which in field]


def halves_of(calls, first=0):
    return [[((when - first) // 2, call) for when, call in calls if when >= first and (when - first) % 2 == odd] for odd in range(2)]


def run_at(hook, calls):
    for when, call in calls:
        pl.when(hook == when)(call)


F32, BF16 = jnp.float32, jnp.bfloat16
QB = 256
LANES = 128
MIB = 2**20


def nt(a, b):
    return lax.dot_general(a, b, (((1,), (1,)), ((), ())), preferred_element_type=F32)


def nn(a, b):
    return jnp.dot(a, b, preferred_element_type=F32)


def tn(a, b):
    return lax.dot_general(a, b, (((0,), (0,)), ((), ())), preferred_element_type=F32)


def over_keys(reduce, values):
    return reduce(values, axis=0, keepdims=True)


def over_lanes(values):
    return jnp.mean(values, axis=-1, keepdims=True)


def head_masks(paired):
    lane = lax.broadcasted_iota(jnp.int32, (1, LANES), 1)
    first = (lane % 64) < 32 if paired else lane < 64
    return first, jnp.logical_not(first)


def causal_block():
    return lax.broadcasted_iota(jnp.int32, (QB, QB), 0) <= lax.broadcasted_iota(jnp.int32, (QB, QB), 1)


def attend_pair(q_ref, k_ref, v_ref, o_ref, lse_ref, hook):
    seq = q_ref.shape[0]
    zero = jnp.zeros((), BF16)
    masks = head_masks(True)
    key = k_ref[...]
    keys = [jnp.where(m, key, zero) for m in masks]
    vt = v_ref[...].astype(F32).T.astype(BF16)
    causal = causal_block()
    for i in reversed(range(seq // QB)):
        lo, hi = i * QB, (i + 1) * QB
        query = q_ref[lo:hi, :]
        outs = []
        for h in range(2):
            diag = jnp.where(causal, nt(keys[h][lo:hi], query), -1e30)
            top = over_keys(jnp.max, diag)
            if i:
                past = nt(keys[h][:lo], query)
                top = jnp.maximum(top, over_keys(jnp.max, past))
                past = jnp.exp(past - top)
            diag = jnp.exp(diag - top)
            total = over_keys(jnp.sum, diag)
            if i:
                total = total + over_keys(jnp.sum, past)
            scale = 1.0 / total
            lse_ref[h:h + 1, lo:hi] = top + jnp.log(total)
            vh = vt[64 * h:64 * h + 64]
            acc = nn(vh[:, lo:hi], (diag * scale).astype(BF16))
            if i:
                acc = acc + nn(vh[:, :lo], (past * scale).astype(BF16))
            outs.append(acc)
        o_ref[lo:hi, :] = jnp.concatenate(outs, axis=0).T.astype(BF16)
        if hi == seq:
            hook()


def attend_pair_back(q_ref, k_ref, v_ref, do_ref, lse_ref, dk_ref, dv_ref, put_dq, hook):
    seq = q_ref.shape[0]
    zero = jnp.zeros((), BF16)
    qmask, vmask = head_masks(True), head_masks(False)
    key, val = k_ref[...], v_ref[...]
    keys = [jnp.where(m, key, zero) for m in qmask]
    vals = [jnp.where(m, val, zero) for m in vmask]
    keys_t = [k.astype(F32).T.astype(BF16) for k in keys]
    causal = causal_block()
    for i in reversed(range(seq // QB)):
        lo, hi = i * QB, (i + 1) * QB
        query, dout = q_ref[lo:hi, :], do_ref[lo:hi, :]
        probs, dscores = [], []
        for h in range(2):
            lse = lse_ref[h:h + 1, lo:hi]
            prob = jnp.where(causal, jnp.exp(nt(keys[h][lo:hi], query) - lse), 0.0)
            grad = nt(vals[h][lo:hi], dout)
            drop = over_keys(jnp.sum, prob * grad)
            if i:
                prob_p = jnp.exp(nt(keys[h][:lo], query) - lse)
                grad_p = nt(vals[h][:lo], dout)
                drop = drop + over_keys(jnp.sum, prob_p * grad_p)
            ds = (prob * (grad - drop)).astype(BF16)
            prob = prob.astype(BF16)
            if i:
                ds = jnp.concatenate([(prob_p * (grad_p - drop)).astype(BF16), ds], axis=0)
                prob = jnp.concatenate([prob_p.astype(BF16), prob], axis=0)
            probs.append(prob)
            dscores.append(ds)
        dq_t = nn(keys_t[0][:, :hi], dscores[0]) + nn(keys_t[1][:, :hi], dscores[1])
        put_dq(lo, hi, dq_t.T)
        both = jnp.concatenate([jnp.where(m, dout, zero) for m in vmask], axis=0)
        dv = nn(jnp.concatenate(probs, axis=1), both)
        both = jnp.concatenate([jnp.where(m, query, zero) for m in qmask], axis=0)
        dk = nn(jnp.concatenate(dscores, axis=1), both)
        if hi == seq:
            dv_ref[...] = dv
            dk_ref[...] = dk
            hook()
        else:
            dv_ref[:hi, :] += dv
            dk_ref[:hi, :] += dk


def swap_halves(values):
    return pltpu.roll(values, LANES // 2, axis=1)


def tables(seq, head):
    freq = 10000.0 ** (-np.arange(0, head, 2, dtype=np.float64) / head)
    angle = np.arange(seq, dtype=np.float64)[:, None] * freq[None, :]
    cos, sin = np.cos(angle).astype(np.float32), np.sin(angle).astype(np.float32)
    return np.concatenate([cos] * 4, axis=1), np.concatenate([-sin, -sin, sin, sin], axis=1)


def norm_rows(values):
    mean = over_lanes(values)
    centered = values - mean
    inv = lax.rsqrt(over_lanes(centered * centered) + 1e-5)
    return centered * inv, inv


def norm_grad(grad, normed, inv):
    mean = over_lanes(grad)
    proj = over_lanes(grad * normed)
    return inv * (grad - mean - normed * proj)


def params(collective_id=None):
    return pltpu.CompilerParams(collective_id=collective_id, has_side_effects=collective_id is not None, vmem_limit_bytes=63 * MIB)


def dma(*shape):
    return pltpu.SemaphoreType.DMA(shape)


def shape(dtype, *dims):
    return jax.ShapeDtypeStruct(dims, dtype)


HBM = pl.BlockSpec(memory_space=pltpu.HBM)
WHOLE = pl.BlockSpec(memory_space=pltpu.VMEM)


def strips(width, size):
    return range(0, width, size)


def rows_of(size, width, index):
    return pl.BlockSpec((size, width), lambda step: (index(step), 0))


def fixed(block, index=(0, 0)):
    return pl.BlockSpec(block, lambda *grid: index, pipeline_mode=pl.Buffered(buffer_count=1))


def qkv_kernel(x_ref, w_ref, cos_ref, sin_ref, qkv_ref, keep_ref, n1_ref):
    normed, _ = norm_rows(x_ref[...].astype(F32))
    normed = normed.astype(BF16)
    n1_ref[...] = normed
    cos, sin = cos_ref[...], sin_ref[...]
    width = w_ref.shape[1]
    third = width // 3
    for j in strips(width, QB):
        raw = nn(normed, w_ref[:, j:j + QB])
        keep_ref[:, j:j + QB] = (jnp.abs(raw) < 8.0).astype(F32).astype(BF16)
        raw = jnp.clip(raw, -8.0, 8.0)
        for at in strips(QB, LANES):
            tile = raw[:, at:at + LANES]
            if j < 2 * third:
                tile = tile * cos + swap_halves(tile) * sin
            if j < third:
                tile = tile * 0.125
            qkv_ref[:, j + at:j + at + LANES] = tile.astype(BF16)


def qkv_proj(x, w, cos, sin, block=512):
    rows, d = x.shape
    cols = w.shape[1]
    per = cos.shape[0] // block
    row = lambda width: rows_of(block, width, lambda i: i)
    tab = rows_of(block, LANES, lambda i: i % per)
    return pl.pallas_call(
        qkv_kernel,
        grid=(rows // block,),
        in_specs=[row(d), fixed((d, cols)), tab, tab],
        out_specs=[row(cols), row(cols), row(d)],
        out_shape=[shape(BF16, rows, cols)] * 2 + [shape(BF16, rows, d)],
        compiler_params=params(),
        name='project',
    )(x, w, cos, sin)


CHUNK = 256
GATHER_PLAN = '01,0,01,0,01,,01,1,,0,,,,,1,,1'
SCATTER_PLAN = ',,,0,,,0,0,,,,21,,2,,,02,11,,,,02,,12,10,210,21,120'
LAST_PLAN = '0,1,,020,,1,2,413,,023,434,2,0,3142,30142,3140,23,14,34102'


def aligned(at, size):
    return pl.ds(pl.multiple_of(at, size), size)


def to_partner(net, src, dst, send, recv):
    return pltpu.make_async_remote_copy(src, dst, send, recv, device_id=net.partner, device_id_type=MESH_ID)


def attn_out_kernel(widths, q_ref, k_ref, v_ref, x_ref, out_shard, ff_shard, o_ref, lse_ref, h_hbm, wo_hbm, wf_hbm,
                    o_all, part, got, h_buf, wo, sems, gather_sems, local_sem):
    step, last = pl.program_id(0), pl.num_programs(0) - 1
    seq = q_ref.shape[0]
    batch, pairs = o_all.shape[:2]
    half = CHUNK // 2
    chunks = seq // CHUNK
    net = Torus()
    g_out = Gather(net, out_shard, wo_hbm, widths[0], gather_sems, 0)
    g_ff = Gather(net, ff_shard, wf_hbm, widths[1], gather_sems, Gather.COPIES + 1)
    begin, middle = halves_of(plan(GATHER_PLAN, g_out.stages(), g_ff.stages()))

    @pl.when(step == 0)
    def _():
        net.barrier(net.neighbours() + [net.partner])

    run_at(step, begin)
    attend_pair(q_ref, k_ref, v_ref, o_ref, lse_ref.at[0, 0], lambda: run_at(step, middle))
    o_all[step // pairs, step % pairs] = o_ref[...]

    def rows_in(c, core):
        return aligned(c * CHUNK + core * half, half)

    def part_copy(b, c):
        return to_partner(net, part.at[b, rows_in(c, 1 - net.core)], got.at[b, c], *pair_of(sems, 0, b, c))

    def h_rows(b, c, core):
        return h_hbm.at[aligned(b * seq + c * CHUNK + core * half, half)]

    def h_copy(b, c, core):
        return to_partner(net, h_buf.at[b, c], h_rows(b, c, core), *pair_of(sems, 1, b, c))

    def h_local(b, c):
        return pltpu.make_async_copy(h_buf.at[b, c], h_rows(b, c, net.core), local_sem.at[b, c])

    def project(b):
        o_full = jnp.concatenate([o_all[b, j] for j in range(pairs)], axis=1)
        weight = wo[...].reshape(part.shape[2], -1)
        for c in range(chunks):
            rows = slice(c * CHUNK, (c + 1) * CHUNK)
            part[b, rows, :] = nt(o_full[rows], weight)
            part_copy(b, c).start()

    def combine(b):
        for c in range(chunks):
            part_copy(b, c).wait()
            own = rows_in(c, net.core)
            h_buf[b, c] = (x_ref[own, :].astype(F32) + (part[b, own, :] + got[b, c])).astype(BF16)
            h_copy(b, c, net.core).start()
            h_local(b, c).start()

    def settle():
        for b in range(batch):
            for c in range(chunks):
                h_copy(b, c, net.core).wait_send()
                h_local(b, c).wait()
                h_copy(b, c, 1 - net.core).wait_recv()

    load = pltpu.make_async_copy(wo_hbm, wo, local_sem.at[0, 0])
    finish = in_order(functools.partial(project, 1), functools.partial(combine, 1), settle)
    run_at(last - step, [(2, in_order(load.start, load.wait, functools.partial(project, 0))), (1, functools.partial(combine, 0)), (0, finish)])
    run_at(step + 1, begin[-1:])


def attn_out(qkv, x, out_shard, ff_shard, batch, seq, pairs, collective_id):
    steps = batch * pairs
    spec = lambda part: pl.BlockSpec((seq, LANES), lambda s: (s // pairs, part * pairs + s % pairs))
    d = x.shape[1]
    chunks = seq // CHUNK
    vm = pltpu.VMEM
    widths = tuple(tuple(w for _, w in cut_three(s.shape[1])) for s in (out_shard, ff_shard))
    torus = (SIDE, SIDE, SIDE)
    return pl.pallas_call(
        functools.partial(attn_out_kernel, widths),
        grid=(steps,),
        in_specs=[spec(0), spec(1), spec(2), rows_of(seq, d, lambda s: s // (steps - 1)), WHOLE, WHOLE],
        out_specs=[spec(0), pl.BlockSpec((1, 1, 2, seq), lambda s: (s // pairs, s % pairs, 0, 0)), HBM, HBM, HBM],
        out_shape=[shape(BF16, batch * seq, LANES * pairs), shape(F32, batch, pairs, 2, seq), shape(BF16, batch * seq, d),
                   shape(BF16, *torus, *out_shard.shape), shape(BF16, *torus, *ff_shard.shape)],
        scratch_shapes=[vm((batch, pairs, seq, LANES), BF16), vm((batch, seq, d), F32), vm((batch, chunks, CHUNK // 2, d), F32), vm((batch, chunks, CHUNK // 2, d), BF16),
                        vm(torus + out_shard.shape, BF16), dma(2, 2, batch, chunks), dma(2, 2 * (Gather.COPIES + 1)), dma(batch, chunks)],
        compiler_params=params(collective_id),
        name='attend_out',
    )(qkv, qkv, qkv, x, out_shard, ff_shard)


class Exchange:
    def __init__(self, net, rows, partials, results, sems, local_sem):
        self.net, self.rows, self.partials, self.results, self.sems, self.local_sem = net, rows, partials, results, sems, local_sem

    def half(self, core, at=0):
        return aligned(at * self.rows + core * (self.rows // 2), self.rows // 2)

    def part(self, which, at):
        part, got = self.partials[which]
        return to_partner(self.net, part.at[at % 2, self.half(1 - self.net.core)], got.at[at], *pair_of(self.sems, which, at))

    def total(self, which, at):
        part, got = self.partials[which]
        self.part(which, at).wait()
        return part[at % 2, self.half(self.net.core), :] + got[at]

    def results_of(self, at, core, act):
        for i, (buf, hbm) in enumerate(self.results):
            act(buf, hbm.at[self.half(core, at)], pair_of(self.sems, len(self.partials) + i, at), self.local_sem.at[i])

    def publish(self, at):
        def act(buf, rows, sem, local_sem):
            to_partner(self.net, buf, rows, *sem).start()
            pltpu.make_async_copy(buf, rows, local_sem).start()
        self.results_of(at, self.net.core, act)

    def settle(self, at):
        def act(buf, rows, sem, local_sem):
            to_partner(self.net, buf, rows, *sem).wait_send()
            pltpu.make_async_copy(buf, rows, local_sem).wait()
        self.results_of(at, self.net.core, act)
        self.results_of(at, 1 - self.net.core, lambda buf, rows, sem, local_sem: to_partner(self.net, buf, rows, *sem).wait_recv())


def mlp_kernel(blocks, h_ref, gy_ref, wff_ref, wd_ref, y_hbm, gh_hbm, gh32_ref, act, gug, n2_ref,
               part_y, part_g, got_y, got_g, y_buf, gh_buf, h_own, gy_own, sems, local_sem):
    step = pl.program_id(0)
    rows, d = h_ref.shape
    ff = wd_ref.shape[1]
    net = Torus()
    swap = Exchange(net, rows, ((part_y, got_y), (part_g, got_g)), ((y_buf, y_hbm), (gh_buf, gh_hbm)), sems, local_sem)

    @pl.when(step == 0)
    def _():
        net.barrier([net.partner])

    @pl.when(step < blocks)
    def _():
        n2, _ = norm_rows(h_ref[...].astype(F32))
        n2 = n2.astype(BF16)
        n2_ref[...] = n2
        gy = gy_ref[...]
        for j in strips(ff, QB):
            w = min(QB, ff - j)
            gact = nn(gy, wd_ref[:, j:j + w])
            for i in range(j, j + w, LANES):
                at, mid, end = 2 * i, 2 * i + LANES, 2 * i + QB
                ug = nn(n2, wff_ref[:, at:end])
                up, gate = ug[:, :LANES], ug[:, LANES:]
                sig = 1.0 / (1.0 + jnp.exp(-gate))
                silu = gate * sig
                act[:, i:i + LANES] = (silu * up).astype(BF16)
                ga = gact[:, i - j:i - j + LANES]
                gug[:, at:mid] = (ga * silu).astype(BF16)
                gug[:, mid:end] = (ga * up * sig * (1.0 + gate * (1.0 - sig))).astype(BF16)

        for which, left, right, part in ((0, act, wd_ref, part_y), (1, gug, wff_ref, part_g)):
            for j in strips(d, QB):
                part[step % 2, :, j:j + QB] = nt(left[...], right[j:j + QB, :])
            swap.part(which, step).start()

    @pl.when(step > 1)
    def _():
        swap.settle(step - 2)

    @pl.when(step > 0)
    def _():
        done = step - 1
        hidden = h_own[...].astype(F32)
        normed, inv = norm_rows(hidden)
        y_buf[...] = (hidden + swap.total(0, done)).astype(BF16)
        gh = gy_own[...].astype(F32) + norm_grad(swap.total(1, done), normed, inv)
        gh32_ref[...] = gh
        gh_buf[...] = gh.astype(BF16)
        swap.publish(done)

    own = swap.half(net.core)
    h_own[...] = h_ref[own, :]
    gy_own[...] = gy_ref[own, :]

    @pl.when(step == blocks)
    def _():
        swap.settle(step - 1)


def mlp(h, gy, weights, collective_id, block=512):
    rows, d = h.shape
    ff = weights.shape[1] // 3
    half = block // 2
    blocks = rows // block
    row = lambda width: rows_of(block, width, lambda i: jnp.minimum(i, blocks - 1))
    vm = pltpu.VMEM
    return pl.pallas_call(
        functools.partial(mlp_kernel, blocks),
        grid=(blocks + 1,),
        in_specs=[row(d), row(d), fixed((d, 2 * ff)), fixed((d, ff), (0, 2))],
        out_specs=[HBM, HBM, rows_of(half, d, lambda i: jnp.maximum(i - 1, 0)), row(ff), row(2 * ff), row(d)],
        out_shape=[shape(BF16, rows, d), shape(BF16, rows, d), shape(F32, rows // 2, d), shape(BF16, rows, ff), shape(BF16, rows, 2 * ff), shape(BF16, rows, d)],
        scratch_shapes=[vm((2, block, d), F32)] * 2 + [vm((blocks, half, d), F32)] * 2 + [vm((half, d), BF16)] * 4 + [dma(2, 4, blocks), dma(2)],
        compiler_params=params(collective_id),
        name='mlp',
    )(h, gy, weights, weights)


def accumulate(part, cols, first, left, right):
    for j in strips(right.shape[1], QB):
        w = min(QB, right.shape[1] - j)
        prod = tn(left, right[:, j:j + w]).reshape(part.shape[:-1] + (w,))
        at = slice(cols + j, cols + j + w)
        part[..., at] = jnp.where(first, 0.0, part[..., at]) + prod


CHUNK_STEPS = 4
SETS = 3
HEAD_STEP = SETS * CHUNK_STEPS


def back_kernel(cols, pairs, gy_ref, n2_ref, act_ref, gug_ref, q_ref, k_ref, v_ref, lse_ref, gh_ref, wo_ref, o_ref, keep_q, keep_k, keep_v, cos_ref, sin_ref,
                gq_ref, gk_ref, gv_ref, gw_ref, grads_ref, do_ref, dk_ref, dv_ref, parts, sems, *bufs):
    step = pl.program_id(0)
    turn = step - HEAD_STEP
    p = turn % pairs
    net = Torus()
    per = len(bufs) // SETS
    scatters = [Scatter(net, parts.at[i], cols, bufs[per * i:per * i + per], sems, i * Scatter.COPIES) for i in range(SETS)]
    calls = plan(SCATTER_PLAN, *(s.stages() for s in scatters))
    middle, end = halves_of(calls, HEAD_STEP)

    @pl.when(step == 0)
    def _():
        net.barrier(net.neighbours())

    first = step % CHUNK_STEPS == 0

    @pl.when(step < CHUNK_STEPS)
    def _():
        accumulate(parts.at[0], 0, first, gy_ref[...], act_ref)

    @pl.when((step >= CHUNK_STEPS) & (step < HEAD_STEP))
    def _():
        accumulate(parts.at[step // CHUNK_STEPS], 0, first, n2_ref[...], gug_ref)

    run_at(step, [c for c in calls if c[0] < HEAD_STEP])

    def back(values, lo, hi, keep):
        turned = values * cos_ref[lo:hi, :] - swap_halves(values) * sin_ref[lo:hi, :]
        return (turned * keep[lo:hi, :].astype(F32)).astype(BF16)

    def put_dq(lo, hi, dq):
        gq_ref[lo:hi, :] = back(dq * 0.125, lo, hi, keep_q)

    @pl.when(turn >= 0)
    def _():
        @pl.when(p == 0)
        def _():
            gh = gh_ref[...]
            dout = nn(gh, wo_ref[...]).astype(BF16)
            for j in range(pairs):
                do_ref[j] = dout[:, LANES * j:LANES * (j + 1)]
            gw_ref[...] = jnp.where(turn == 0, 0.0, gw_ref[...]) + tn(gh, o_ref[...])

        attend_pair_back(q_ref, k_ref, v_ref, do_ref.at[p], lse_ref.at[0, 0], dk_ref, dv_ref, put_dq, lambda: run_at(turn, middle))
        seq = q_ref.shape[0]
        gk_ref[...] = back(dk_ref[...], 0, seq, keep_k)
        gv_ref[...] = (dv_ref[...] * keep_v[...].astype(F32)).astype(BF16)
        run_at(turn, end)

    @pl.when(step == pl.num_programs(0) - 1)
    def _():
        for i, scatter in enumerate(scatters):
            grads_ref[i] = scatter.result()


def back(gy, n2, act, gug, qkv, lse, gh, wo_t, o, keep, cos, sin, batch, seq, pairs, collective_id):
    rows, d = gy.shape
    ff = act.shape[1]
    block = rows // CHUNK_STEPS
    turn = lambda s: jnp.maximum(s - HEAD_STEP, 0)
    head = lambda part: pl.BlockSpec((seq, LANES), lambda s: (turn(s) // pairs, part * pairs + turn(s) % pairs))
    chunk = lambda s, i: jnp.clip(s - i * CHUNK_STEPS, 0, CHUNK_STEPS - 1)
    early = lambda s: chunk(s, 0)
    late = lambda s: jnp.where(s < 2 * CHUNK_STEPS, chunk(s, 1), chunk(s, 2))
    cols = cut_three(ff)
    vm = pltpu.VMEM
    once = pl.Buffered(buffer_count=1)
    per_seq = lambda width: pl.BlockSpec((seq, width), lambda s: (turn(s) // pairs, 0), pipeline_mode=once)
    return pl.pallas_call(
        functools.partial(back_kernel, cols, pairs),
        grid=(HEAD_STEP + batch * pairs,),
        in_specs=[rows_of(block, d, early), rows_of(block, d, late),
                  rows_of(block, ff, early), pl.BlockSpec((block, ff), lambda s: (late(s), jnp.where(s < 2 * CHUNK_STEPS, 0, 1))),
                  head(0), head(1), head(2), pl.BlockSpec((1, 1, 2, seq), lambda s: (turn(s) // pairs, turn(s) % pairs, 0, 0)),
                  per_seq(d), fixed(wo_t.shape), per_seq(LANES * pairs), head(0), head(1), head(2), fixed(cos.shape), fixed(sin.shape)],
        out_specs=[head(0)] * 3 + [fixed(wo_t.shape), fixed((SETS, PIECE, ff), (0, 0, 0))],
        out_shape=[shape(BF16, rows, LANES * pairs)] * 3 + [shape(F32, *wo_t.shape), shape(F32, SETS, PIECE, ff)],
        scratch_shapes=[vm((pairs, seq, LANES), BF16), vm((seq, LANES), F32), vm((seq, LANES), F32), vm((SETS, SIDE, SIDE, SIDE, PIECE, ff), F32),
                        dma(2, SETS * Scatter.COPIES)] + Scatter.scratch(cols) * SETS,
        compiler_params=params(collective_id),
        name='back',
    )(gy, n2, act, gug, qkv, qkv, qkv, lse, gh, wo_t, o, keep, keep, keep, cos, sin)


def last_kernel(pairs, blocks, n1_ref, gq_ref, gk_ref, gv_ref, x_ref, gq_row, gk_row, gv_row, gh_ref, w_ref, gout_hbm, gx_hbm, gout_ref, gw_ref,
                part_out, part_qkv, part, got, buf, sems, scatter_sems, local_sem, *bufs):
    step = pl.program_id(0)
    turn = step - pairs
    rows, d = x_ref.shape
    net = Torus()
    grads = (gq_row, gk_row, gv_row)
    third = gq_row.shape[1]
    per = len(bufs) // (pairs + 1)
    parts = [part_out] + [part_qkv.at[j] for j in range(pairs)]
    scatters = [Scatter(net, s, cut_three(s.shape[-1]), bufs[per * i:per * i + per], scatter_sems, i * Scatter.COPIES) for i, s in enumerate(parts)]
    calls = plan(LAST_PLAN, *(s.stages() for s in scatters))
    swap = Exchange(net, rows, ((part, got),), ((buf, gx_hbm),), sems, local_sem)

    @pl.when(step == 0)
    def _():
        load = pltpu.make_async_copy(gout_hbm, part_out, local_sem.at[1])
        load.start()
        net.barrier(net.neighbours() + [net.partner])
        load.wait()

    begin, end = halves_of(calls)
    run_at(step, begin)

    @pl.when(turn < 0)
    def _():
        right = jnp.concatenate([g[...] for g in (gq_ref, gk_ref, gv_ref)], axis=1)
        accumulate(part_qkv.at[step], 0, True, n1_ref[...], right)

    @pl.when((turn >= 0) & (turn < blocks))
    def _():
        for j in strips(d, QB):
            part[turn % 2, :, j:j + QB] = sum(nt(g[...], w_ref[j:j + QB, third * i:third * (i + 1)]) for i, g in enumerate(grads))
        swap.part(0, turn).start()

    run_at(step, end)

    @pl.when(turn > 1)
    def _():
        swap.settle(turn - 2)

    @pl.when(turn > 0)
    def _():
        done = turn - 1
        normed, inv = norm_rows(x_ref[swap.half(net.core), :].astype(F32))
        buf[...] = (gh_ref[...] + norm_grad(swap.total(0, done), normed, inv)).astype(BF16)
        swap.publish(done)

    @pl.when(turn == blocks)
    def _():
        for when, call in calls:
            if when > 2 * (pairs + blocks) + 1:
                call()
        swap.settle(turn - 1)
        gout_ref[...] = scatters[0].result()
        for j, s in enumerate(scatters[1:]):
            sums = s.result()
            for i in range(len(grads)):
                gw_ref[:, third * i + LANES * j:third * i + LANES * (j + 1)] = sums[:, LANES * i:LANES * (i + 1)]


def last(x, n1, gq, gk, gv, gh32, w, gout, pairs, collective_id, block=512):
    rows, d = x.shape
    blocks = rows // block
    late = lambda n, width, by: rows_of(n, width, lambda s: jnp.clip(s - pairs - by, 0, blocks - 1))
    head = pl.BlockSpec((rows, LANES), lambda s: (0, jnp.minimum(s, pairs - 1)))
    vm = pltpu.VMEM
    half = block // 2
    torus = (SIDE, SIDE, SIDE, PIECE)
    gout = gout.reshape(torus + (-1,))
    return pl.pallas_call(
        functools.partial(last_kernel, pairs, blocks),
        grid=(pairs + blocks + 1,),
        in_specs=[fixed((rows, d))] + [head] * 3 + [late(block, d, 1)] + [late(block, gq.shape[1], 0)] * 3 + [late(half, d, 1), fixed(w.shape), HBM],
        out_specs=[HBM, WHOLE, WHOLE],
        out_shape=[shape(BF16, rows, d), shape(F32, PIECE, gout.shape[-1]), shape(F32, PIECE, w.shape[1])],
        scratch_shapes=[vm(gout.shape, F32), vm((pairs,) + torus + (3 * LANES,), F32), vm((2, block, d), F32), vm((blocks, half, d), F32), vm((half, d), BF16),
                        dma(2, 2, blocks), dma(2, (pairs + 1) * Scatter.COPIES), dma(2)] + Scatter.scratch(cut_three(gout.shape[-1])) + Scatter.scratch(cut_three(3 * LANES)) * pairs,
        compiler_params=params(collective_id),
        name='last',
    )(n1, gq, gk, gv, x, gq, gk, gv, gh32, w, gout)


def pair_heads(w, head):
    n, width = w.shape
    cut = width // 3 * 2
    qk = w[:, :cut].reshape(n, -1, 2, 2, head // 2).swapaxes(2, 3)
    return jnp.concatenate([qk.reshape(n, cut), w[:, cut:]], axis=1)


def device_step(x, grad_y, w_qkv, w_out, w_ff, w_down):
    batch, seq, d = x.shape
    heads, head = w_qkv.shape[2:]
    ids = iter(range(5))
    pairs = heads // 2
    ff = w_ff.shape[2]
    tiles = ff // LANES
    cos, sin = (jnp.asarray(t) for t in tables(seq, head))
    inter = w_ff.reshape(-1, 2, tiles, LANES).swapaxes(1, 2).reshape(-1, 2 * ff)
    ff_shard = jnp.concatenate([inter, w_down.T], axis=1)
    out_shard = w_out.reshape(heads * head, -1).T
    wq = all_gather(pair_heads(w_qkv.reshape(PIECE, -1), head), [w for _, w in cut_three(w_qkv[0].size)], next(ids))
    x2, gy = x.reshape(-1, d), grad_y.reshape(-1, d)
    qkv, keep, n1 = qkv_proj(x2, wq, cos, sin)
    o, lse, h, wo_t, wf = attn_out(qkv, x2, out_shard, ff_shard, batch, seq, pairs, next(ids))
    wo_t, wf = wo_t.reshape(d, -1), wf.reshape(d, -1)
    y, gh, gh32, act, gug, n2 = mlp(h, gy, wf, next(ids))
    gq, gk, gv, gout, grads = back(gy, n2, act, gug, qkv, lse, gh, wo_t, o, keep, cos, sin, batch, seq, pairs, next(ids))
    gx, gout, gqkv = last(x2, n1, gq, gk, gv, gh32, wq, gout, pairs, next(ids))
    gff = grads[1:].swapaxes(0, 1).reshape(-1, tiles, 2, LANES).swapaxes(1, 2).reshape(-1, 2, ff)
    return y.reshape(x.shape), gx.reshape(x.shape), pair_heads(gqkv, head).reshape(w_qkv.shape), gout.T.reshape(heads, head, -1), gff, grads[0].T


def solution(mesh):
    specs = (P('fsdp'), P('fsdp'), P('fsdp', None, 'tp'), P('tp', None, 'fsdp'), P('fsdp', None, 'tp'), P('tp', 'fsdp'))
    return jax.shard_map(device_step, mesh=mesh, in_specs=specs, out_specs=specs, check_vma=False)
```

```python
import functools

import jax
import jax.numpy as jnp
import numpy as np
from jax import lax
from jax.experimental import pallas as pl
from jax.experimental.pallas import tpu as pltpu
from jax.sharding import PartitionSpec as P

MESH_ID = pl.DeviceIdType.MESH
SIDE = 4
PIECE = 16
ORDERS = ((2, 1, 0), (1, 0, 2), (0, 2, 1))
BOTH = ((0, 1), (1, -1))
PHASES = range(3)


class Torus:
    def __init__(self):
        self.core = lax.axis_index('tp')
        self.index = lax.axis_index('fsdp')
        plane, x = lax.div(self.index, SIDE), lax.rem(self.index, SIDE)
        self.at = (lax.div(plane, SIDE), lax.rem(plane, SIDE), x)
        self.partner = (1 - self.core, self.index)
        self.moved = {(axis, by): lax.rem(at + (by + SIDE), SIDE) for axis, at in enumerate(self.at) for by in range(-2, 3)}
        self.peers = {(axis, by): self.place(axis, self.moved[axis, by]) for axis in range(3) for _, by in BOTH}

    def place(self, axis, coord):
        pos = list(self.at)
        pos[axis] = coord
        return (self.core, (pos[0] * SIDE + pos[1]) * SIDE + pos[2])

    def shift(self, axis, by):
        return self.moved[axis, by]

    def peer(self, axis, by):
        return self.peers[axis, by]

    def neighbours(self):
        return list(self.peers.values())

    def tell(self, sem, devices):
        for device in devices:
            pl.semaphore_signal(sem, inc=1, device_id=device, device_id_type=MESH_ID)

    def barrier(self, devices):
        sem = pltpu.get_barrier_semaphore()
        self.tell(sem, devices)
        pl.semaphore_wait(sem, len(devices))


def pair_of(sems, *at):
    return sems.at[(0,) + at], sems.at[(1,) + at]


def in_order(*calls):
    def run():
        for call in calls:
            call()
    return run


class Gather:
    COPIES = 36

    def __init__(self, net, shard, out, widths, sems, first):
        self.net, self.shard, self.out, self.sems, self.first = net, shard, out, sems, first
        self.cols = [(sum(widths[:i]), w) for i, w in enumerate(widths)]

    def block(self, colour, phase, coord, half=None):
        order = ORDERS[colour]
        off, width = self.cols[colour]
        pick = list(self.net.at)
        for axis in order[:phase]:
            pick[axis] = pl.ds(0, SIDE)
        pick[order[phase]] = coord
        if half is not None and phase:
            pick[order[0]] = pl.ds(half * 2, 2)
        elif half is not None:
            cut = width - width // 256 * 128
            off, width = (off + cut, width - cut) if half else (off, cut)
        return self.out.at[pick[0], pick[1], pick[2], :, pl.ds(off, width)] if width else None

    def copy(self, phase, colour, relay, d, by, came=False):
        axis = ORDERS[colour][phase]
        back = -by if relay else 0
        coord = self.net.shift(axis, back - by if came else back)
        dst = src = self.block(colour, phase, coord, d if relay else None)
        if dst is None:
            return None
        if not (phase or relay or came):
            off, width = self.cols[colour]
            src = self.shard.at[:, pl.ds(off, width)]
        at = self.first + ((phase * 3 + colour) * 2 + relay) * 2 + d
        return pltpu.make_async_remote_copy(src, dst, *pair_of(self.sems, at), device_id=self.net.peer(axis, by), device_id_type=MESH_ID)

    def each(self, phase, relay, act, came=False):
        for d, by in BOTH:
            for colour in range(3):
                desc = self.copy(phase, colour, relay, d, by, came)
                if desc is not None:
                    act(desc)

    def own(self):
        at = self.net.at
        return pltpu.make_async_copy(self.shard, self.out.at[at[0], at[1], at[2]], self.sems.at[0, self.first + self.COPIES])

    def start(self, phase):
        if phase:
            self.each(phase - 1, 1, lambda c: c.wait_recv(), True)
        if phase == 1:
            self.own().wait()
        self.each(phase, 0, lambda c: c.start())
        if not phase:
            self.own().start()

    def relay(self, phase):
        for d, by in BOTH:
            for colour in range(3):
                self.copy(phase, colour, 0, d, by, True).wait_recv()
                desc = self.copy(phase, colour, 1, d, by)
                if desc is not None:
                    desc.start()

    def finish(self):
        self.each(PHASES[-1], 1, lambda c: c.wait_recv(), True)
        for phase in PHASES:
            for relay in range(2):
                self.each(phase, relay, lambda c: c.wait_send())

    def stages(self):
        return [functools.partial(f, p) for p in PHASES for f in (self.start, self.relay)] + [self.finish]


class Scatter:
    COPIES = 54

    def __init__(self, net, part, cols, bufs, sems, first):
        self.net, self.part, self.cols, self.bufs, self.sems, self.first = net, part, cols, bufs, sems, first

    @staticmethod
    def scratch(cols):
        shapes = []
        for _, w in cols:
            shapes += [(3, 2, 2, SIDE, PIECE, w), (3, 2, 2, PIECE, w), (3, 2, PIECE // 2, w)]
        return [pltpu.VMEM(s, jnp.float32) for s in shapes]

    def buf(self, colour, phase):
        return self.bufs[colour * len(PHASES) + phase]

    def block(self, colour, phase, coord, half):
        order = ORDERS[colour]
        off, width = self.cols[colour]
        pick = [pl.ds(0, SIDE)] * 3
        for axis in order[:phase]:
            pick[axis] = self.net.at[axis]
        pick[order[phase]] = coord
        rows = pl.ds(0, PIECE)
        rest = sorted(order[phase + 1:])
        if rest:
            pick[rest[0]] = pl.ds(2 * half, 2)
        else:
            rows = pl.ds(PIECE // 2 * half, PIECE // 2)
        return self.part.at[pick[0], pick[1], pick[2], rows, pl.ds(off, width)]

    def copy(self, phase, colour, kind, d, by):
        axis = ORDERS[colour][phase]
        buf = self.buf(colour, phase)
        if kind == 2:
            src = buf.at[0, d]
        elif kind:
            src = self.block(colour, phase, self.net.shift(axis, by), 1 - d)
        else:
            src = self.block(colour, phase, self.net.shift(axis, 2), d)
        at = self.first + ((phase * 3 + colour) * 3 + kind) * 2 + d
        return pltpu.make_async_remote_copy(src, buf.at[kind, d], *pair_of(self.sems, at), device_id=self.net.peer(axis, by), device_id_type=MESH_ID)

    def start(self, phase, kind):
        for d, by in BOTH:
            for colour in range(3):
                self.copy(phase, colour, kind, d, by).start()

    def relay(self, phase):
        for colour in range(3):
            buf = self.buf(colour, phase)
            for d, by in BOTH:
                self.copy(phase, colour, 0, d, by).wait_recv()
                buf[0, d] = buf[0, d] + self.block(colour, phase, self.net.shift(ORDERS[colour][phase], by), d)[...]
                self.copy(phase, colour, 2, d, by).start()

    def merge(self, phase):
        for colour in range(3):
            buf = self.buf(colour, phase)
            for d, by in BOTH:
                for kind in (1, 2):
                    self.copy(phase, colour, kind, d, by).wait_recv()
            for half in range(2):
                mine = self.block(colour, phase, self.net.at[ORDERS[colour][phase]], half)
                mine[...] = mine[...] + buf[1, 1 - half] + buf[2, half]
        if phase + 1 < len(PHASES):
            for kind in range(2):
                self.start(phase + 1, kind)

    def finish(self):
        for phase in PHASES:
            for colour in range(3):
                for kind in PHASES:
                    for d, by in BOTH:
                        self.copy(phase, colour, kind, d, by).wait_send()

    def stages(self):
        calls = [functools.partial(self.start, 0, kind) for kind in range(2)]
        for phase in PHASES:
            calls += [functools.partial(self.relay, phase), functools.partial(self.merge, phase)]
        return calls[:-1] + [in_order(calls[-1], self.finish)]

    def result(self):
        at = self.net.at
        return self.part[at[0], at[1], at[2]]


def cut_three(width, off=0):
    tiles = width // 128
    sizes = [(tiles + 2 - i) // 3 * 128 for i in range(3)]
    return [(off + sum(sizes[:i]), s) for i, s in enumerate(sizes)]


def plan(text, *sets):
    left = [iter(s) for s in sets]
    return [(hook, next(left[int(which)])) for hook, field in enumerate(text.split(',')) for which in field]


def halves_of(calls, first=0):
    return [[((when - first) // 2, call) for when, call in calls if when >= first and (when - first) % 2 == odd] for odd in range(2)]


def run_at(hook, calls):
    for when, call in calls:
        pl.when(hook == when)(call)


F32, BF16 = jnp.float32, jnp.bfloat16
QB = 256
LANES = 128
MIB = 2**20


def nt(a, b):
    return lax.dot_general(a, b, (((1,), (1,)), ((), ())), preferred_element_type=F32)


def nn(a, b):
    return jnp.dot(a, b, preferred_element_type=F32)


def tn(a, b):
    return lax.dot_general(a, b, (((0,), (0,)), ((), ())), preferred_element_type=F32)


def over_keys(reduce, values):
    return reduce(values, axis=0, keepdims=True)


def over_lanes(values):
    return jnp.mean(values, axis=-1, keepdims=True)


def head_masks(paired):
    lane = lax.broadcasted_iota(jnp.int32, (1, LANES), 1)
    first = (lane % 64) < 32 if paired else lane < 64
    return first, jnp.logical_not(first)


def causal_block():
    return lax.broadcasted_iota(jnp.int32, (QB, QB), 0) <= lax.broadcasted_iota(jnp.int32, (QB, QB), 1)


def attend_pair(q_ref, k_ref, v_ref, o_ref, lse_ref, hook):
    seq = q_ref.shape[0]
    zero = jnp.zeros((), BF16)
    masks = head_masks(True)
    key = k_ref[...]
    keys = [jnp.where(m, key, zero) for m in masks]
    vt = v_ref[...].astype(F32).T.astype(BF16)
    causal = causal_block()
    for i in reversed(range(seq // QB)):
        lo, hi = i * QB, (i + 1) * QB
        query = q_ref[lo:hi, :]
        outs = []
        for h in range(2):
            diag = jnp.where(causal, nt(keys[h][lo:hi], query), -1e30)
            top = over_keys(jnp.max, diag)
            if i:
                past = nt(keys[h][:lo], query)
                top = jnp.maximum(top, over_keys(jnp.max, past))
                past = jnp.exp(past - top)
            diag = jnp.exp(diag - top)
            total = over_keys(jnp.sum, diag)
            if i:
                total = total + over_keys(jnp.sum, past)
            scale = 1.0 / total
            lse_ref[h:h + 1, lo:hi] = top + jnp.log(total)
            vh = vt[64 * h:64 * h + 64]
            acc = nn(vh[:, lo:hi], (diag * scale).astype(BF16))
            if i:
                acc = acc + nn(vh[:, :lo], (past * scale).astype(BF16))
            outs.append(acc)
        o_ref[lo:hi, :] = jnp.concatenate(outs, axis=0).T.astype(BF16)
        if hi == seq:
            hook()


def attend_pair_back(q_ref, k_ref, v_ref, do_ref, lse_ref, dk_ref, dv_ref, put_dq, hook):
    seq = q_ref.shape[0]
    zero = jnp.zeros((), BF16)
    qmask, vmask = head_masks(True), head_masks(False)
    key, val = k_ref[...], v_ref[...]
    keys = [jnp.where(m, key, zero) for m in qmask]
    vals = [jnp.where(m, val, zero) for m in vmask]
    keys_t = [k.astype(F32).T.astype(BF16) for k in keys]
    causal = causal_block()
    for i in reversed(range(seq // QB)):
        lo, hi = i * QB, (i + 1) * QB
        query, dout = q_ref[lo:hi, :], do_ref[lo:hi, :]
        probs, dscores = [], []
        for h in range(2):
            lse = lse_ref[h:h + 1, lo:hi]
            prob = jnp.where(causal, jnp.exp(nt(keys[h][lo:hi], query) - lse), 0.0)
            grad = nt(vals[h][lo:hi], dout)
            drop = over_keys(jnp.sum, prob * grad)
            if i:
                prob_p = jnp.exp(nt(keys[h][:lo], query) - lse)
                grad_p = nt(vals[h][:lo], dout)
                drop = drop + over_keys(jnp.sum, prob_p * grad_p)
            ds = (prob * (grad - drop)).astype(BF16)
            prob = prob.astype(BF16)
            if i:
                ds = jnp.concatenate([(prob_p * (grad_p - drop)).astype(BF16), ds], axis=0)
                prob = jnp.concatenate([prob_p.astype(BF16), prob], axis=0)
            probs.append(prob)
            dscores.append(ds)
        dq_t = nn(keys_t[0][:, :hi], dscores[0]) + nn(keys_t[1][:, :hi], dscores[1])
        put_dq(lo, hi, dq_t.T)
        both = jnp.concatenate([jnp.where(m, dout, zero) for m in vmask], axis=0)
        dv = nn(jnp.concatenate(probs, axis=1), both)
        both = jnp.concatenate([jnp.where(m, query, zero) for m in qmask], axis=0)
        dk = nn(jnp.concatenate(dscores, axis=1), both)
        if hi == seq:
            dv_ref[...] = dv
            dk_ref[...] = dk
            hook()
        else:
            dv_ref[:hi, :] += dv
            dk_ref[:hi, :] += dk


def swap_halves(values):
    return pltpu.roll(values, LANES // 2, axis=1)


def tables(seq, head):
    freq = 10000.0 ** (-np.arange(0, head, 2, dtype=np.float64) / head)
    angle = np.arange(seq, dtype=np.float64)[:, None] * freq[None, :]
    cos, sin = np.cos(angle).astype(np.float32), np.sin(angle).astype(np.float32)
    return np.concatenate([cos] * 4, axis=1), np.concatenate([-sin, -sin, sin, sin], axis=1)


def norm_rows(values):
    mean = over_lanes(values)
    centered = values - mean
    inv = lax.rsqrt(over_lanes(centered * centered) + 1e-5)
    return centered * inv, inv


def norm_grad(grad, normed, inv):
    mean = over_lanes(grad)
    proj = over_lanes(grad * normed)
    return inv * (grad - mean - normed * proj)


def params(collective_id=None):
    return pltpu.CompilerParams(collective_id=collective_id, has_side_effects=collective_id is not None, vmem_limit_bytes=63 * MIB)


def dma(*shape):
    return pltpu.SemaphoreType.DMA(shape)


def shape(dtype, *dims):
    return jax.ShapeDtypeStruct(dims, dtype)


HBM = pl.BlockSpec(memory_space=pltpu.HBM)
WHOLE = pl.BlockSpec(memory_space=pltpu.VMEM)


def strips(width, size):
    return range(0, width, size)


def rows_of(size, width, index):
    return pl.BlockSpec((size, width), lambda step: (index(step), 0))


def fixed(block, index=(0, 0)):
    return pl.BlockSpec(block, lambda *grid: index, pipeline_mode=pl.Buffered(buffer_count=1))


def project_pair(normed, weight, cos_ref, sin_ref, qkv_ref, keep_ref):
    for part in range(3):
        cols = slice(LANES * part, LANES * (part + 1))
        raw = nn(normed, weight[:, cols])
        keep_ref[:, cols] = (jnp.abs(raw) < 8.0).astype(F32).astype(BF16)
        tile = jnp.clip(raw, -8.0, 8.0)
        if part < 2:
            tile = tile * cos_ref[...] + swap_halves(tile) * sin_ref[...]
        if not part:
            tile = tile * 0.125
        qkv_ref[:, cols] = tile.astype(BF16)


def swap_middle(tile):
    quarter = lax.broadcasted_iota(jnp.int32, tile.shape, 1) // (LANES // 4)
    up, down = pltpu.roll(tile, LANES // 4, axis=1), pltpu.roll(tile, LANES - LANES // 4, axis=1)
    return jnp.where(quarter == 1, down, jnp.where(quarter == 2, up, tile))


CHUNK = 256
CHUNK_STEPS = 4
FRONT_PLAN = '060160160160100,12,234,12345,2345,12345,234,35,45,23,4,,,,,5,,5'
SCATTER_PLAN = ',,,0,,,0,0,,,,21,,2,,,02,11,,,,02,,12,10,210,21,120'
LAST_PLAN = '0,1,,020,,1,2,413,,023,434,2,0,3142,30142,3140,23,14,34102'


def aligned(at, size):
    return pl.ds(pl.multiple_of(at, size), size)


def to_partner(net, src, dst, send, recv):
    return pltpu.make_async_remote_copy(src, dst, send, recv, device_id=net.partner, device_id_type=MESH_ID)


def front_kernel(x_hbm, qkv_shard, out_shard, ff_shard, down_shard, cos_ref, sin_ref, qkv_ref, keep_ref, o_ref, lse_ref, h_hbm, n1_hbm, wq_hbm, wo_hbm, wf_hbm,
                 x_all, n1, w, shards, o_all, part, got, h_buf, wo, sems, gather_sems, load_sem, h_sem, *kept):
    step, last = pl.program_id(0), pl.num_programs(0) - 1
    turn = step - 1
    batch, pairs, seq = o_all.shape[:3]
    b, p = turn % batch, turn // batch
    half = CHUNK // 2
    chunks = seq // CHUNK
    ff = down_shard.shape[1]
    net = Torus()
    width = 3 * LANES
    places = [(width, w.at[j]) for j in range(pairs)] + [(LANES * pairs, wo_hbm), (3 * ff, wf_hbm)]
    gathers, at = [], 0
    for i, (cols, out) in enumerate(places):
        gathers.append(Gather(net, shards.at[:, pl.ds(at, cols)], out, [size for _, size in cut_three(cols)], gather_sems, i * (Gather.COPIES + 1)))
        at += cols
    strip = x_all.shape[0] // CHUNK_STEPS

    def load(i):
        return pltpu.make_async_copy(x_hbm.at[pl.ds(strip * i, strip)], x_all.at[pl.ds(strip * i, strip)], load_sem.at[i])

    def save(i):
        return pltpu.make_async_copy(n1.at[pl.ds(strip * i, strip)], n1_hbm.at[pl.ds(strip * i, strip)], load_sem.at[i])

    def save_weight(j):
        return pltpu.make_async_copy(w.at[j], wq_hbm.at[:, :, :, :, pl.ds(width * j, width)], load_sem.at[CHUNK_STEPS + j])

    def normalize(i):
        load(i).wait()
        rows = slice(strip * i, strip * (i + 1))
        n1[rows, :] = norm_rows(x_all[rows, :].astype(F32))[0].astype(BF16)
        save(i).start()

    calls = plan(FRONT_PLAN, *([*g.stages()] for g in gathers), [functools.partial(normalize, i) for i in range(CHUNK_STEPS)])

    @pl.when(step == 0)
    def _():
        for i in range(CHUNK_STEPS):
            load(i).start()
        for j in range(pairs):
            for i in range(3):
                tile = qkv_shard[:, LANES * (pairs * i + j):LANES * (pairs * i + j + 1)].astype(F32)
                shards[:, width * j + LANES * i:width * j + LANES * (i + 1)] = (swap_middle(tile) if i < 2 else tile).astype(BF16)
        at = width * pairs
        shards[:, at:at + LANES * pairs] = out_shard[...]
        at += LANES * pairs
        for i in strips(ff, LANES):
            for j in range(2):
                shards[:, at + LANES * j:at + LANES * (j + 1)] = ff_shard[j, :, i:i + LANES]
            at += 2 * LANES
        shards[:, at:] = down_shard[...]
        net.barrier(net.neighbours() + [net.partner])
        for when, call in calls:
            if not when:
                call()

    begin, middle = halves_of(calls, 1)
    run_at(turn, begin)

    @pl.when(turn >= 0)
    def _():
        project_pair(n1[aligned(b * seq, seq), :], w[p].reshape(n1.shape[1], width), cos_ref, sin_ref, qkv_ref, keep_ref)
        q_ref, k_ref, v_ref = (qkv_ref.at[:, pl.ds(LANES * i, LANES)] for i in range(3))
        attend_pair(q_ref, k_ref, v_ref, o_ref, lse_ref.at[0, 0], lambda: run_at(turn, middle))
        o_all[b, p] = o_ref[...]

    def rows_in(c, core):
        return aligned(c * CHUNK + core * half, half)

    def part_copy(b, c):
        return to_partner(net, part.at[b, rows_in(c, 1 - net.core)], got.at[b, c], *pair_of(sems, 0, b, c))

    def rows_out(b, c, core):
        return aligned(b * seq + c * CHUNK + core * half, half)

    def h_copy(b, c, core):
        return to_partner(net, h_buf.at[b, c], h_hbm.at[rows_out(b, c, core)], *pair_of(sems, 1, b, c))

    def h_local(b, c):
        return pltpu.make_async_copy(h_buf.at[b, c], h_hbm.at[rows_out(b, c, net.core)], h_sem.at[b, c])

    def project(b):
        o_full = jnp.concatenate([o_all[b, j] for j in range(pairs)], axis=1)
        weight = wo[...].reshape(part.shape[2], -1)
        for c in range(chunks):
            rows = slice(c * CHUNK, (c + 1) * CHUNK)
            part[b, rows, :] = nt(o_full[rows], weight)
            part_copy(b, c).start()

    def combine(b):
        for c in range(chunks):
            part_copy(b, c).wait()
            own = rows_in(c, net.core)
            h_buf[b, c] = (x_all[rows_out(b, c, net.core), :].astype(F32) + (part[b, own, :] + got[b, c])).astype(BF16)
            h_copy(b, c, net.core).start()
            h_local(b, c).start()

    def settle():
        for b in range(batch):
            for c in range(chunks):
                h_copy(b, c, net.core).wait_send()
                h_local(b, c).wait()
                h_copy(b, c, 1 - net.core).wait_recv()
        for i in range(CHUNK_STEPS):
            save(i).wait()
        for j in range(pairs):
            save_weight(j).wait()

    def fetch():
        copy = pltpu.make_async_copy(wo_hbm, wo, h_sem.at[0, 0])
        copy.start()
        for j in range(pairs):
            save_weight(j).start()
        copy.wait()
        project(0)

    def finish():
        combine(0)
        project(1)
        combine(1)
        settle()

    run_at(last - step, [(1, fetch), (0, finish)])
    run_at(turn + 1, begin[-1:])


def front(x, qkv_shard, out_shard, ff_shard, down_shard, cos, sin, batch, seq, collective_id):
    pairs = out_shard.shape[1] // LANES
    rows, d = x.shape
    width = 3 * LANES
    chunks = seq // CHUNK
    vm = pltpu.VMEM
    torus = (SIDE, SIDE, SIDE, PIECE)
    shards = [s.size // PIECE for s in (qkv_shard, out_shard, ff_shard, down_shard)]
    turn = lambda s: jnp.maximum(s - 1, 0)
    head = lambda width: pl.BlockSpec((seq, width), lambda s: (turn(s) % batch, turn(s) // batch))
    return pl.pallas_call(
        front_kernel,
        grid=(1 + batch * pairs,),
        in_specs=[HBM] + [WHOLE] * 4 + [fixed(cos.shape)] * 2,
        out_specs=[head(width), head(width), head(LANES), pl.BlockSpec((1, 1, 2, seq), lambda s: (turn(s) % batch, turn(s) // batch, 0, 0))] + [HBM] * 5,
        out_shape=[shape(BF16, rows, width * pairs)] * 2 + [shape(BF16, rows, LANES * pairs), shape(F32, batch, pairs, 2, seq), shape(BF16, rows, d), shape(BF16, rows, d),
                   shape(BF16, *torus, shards[0]), shape(BF16, *torus, shards[1]), shape(BF16, *torus, shards[2] + shards[3])],
        scratch_shapes=[vm((rows, d), BF16), vm((rows, d), BF16), vm((pairs,) + torus + (width,), BF16), vm((PIECE, sum(shards)), BF16),
                        vm((batch, pairs, seq, LANES), BF16), vm((batch, seq, d), F32), vm((batch, chunks, CHUNK // 2, d), F32), vm((batch, chunks, CHUNK // 2, d), BF16),
                        vm(torus + (shards[1],), BF16), dma(2, 2, batch, chunks), dma(2, (pairs + 2) * (Gather.COPIES + 1)), dma(CHUNK_STEPS + pairs), dma(batch, chunks)],
        compiler_params=params(collective_id),
        name='front',
    )(x, qkv_shard, out_shard, ff_shard, down_shard, cos, sin)


class Exchange:
    def __init__(self, net, rows, partials, results, sems, local_sem):
        self.net, self.rows, self.partials, self.results, self.sems, self.local_sem = net, rows, partials, results, sems, local_sem

    def half(self, core, at=0):
        return aligned(at * self.rows + core * (self.rows // 2), self.rows // 2)

    def part(self, which, at):
        part, got = self.partials[which]
        return to_partner(self.net, part.at[at % 2, self.half(1 - self.net.core)], got.at[at], *pair_of(self.sems, which, at))

    def total(self, which, at):
        part, got = self.partials[which]
        self.part(which, at).wait()
        return part[at % 2, self.half(self.net.core), :] + got[at]

    def results_of(self, at, core, act):
        for i, (buf, hbm) in enumerate(self.results):
            act(buf, hbm.at[self.half(core, at)], pair_of(self.sems, len(self.partials) + i, at), self.local_sem.at[i])

    def publish(self, at):
        def act(buf, rows, sem, local_sem):
            to_partner(self.net, buf, rows, *sem).start()
            pltpu.make_async_copy(buf, rows, local_sem).start()
        self.results_of(at, self.net.core, act)

    def settle(self, at):
        def act(buf, rows, sem, local_sem):
            to_partner(self.net, buf, rows, *sem).wait_send()
            pltpu.make_async_copy(buf, rows, local_sem).wait()
        self.results_of(at, self.net.core, act)
        self.results_of(at, 1 - self.net.core, lambda buf, rows, sem, local_sem: to_partner(self.net, buf, rows, *sem).wait_recv())


def mlp_kernel(blocks, h_ref, gy_ref, wff_ref, wd_ref, y_hbm, gh_hbm, gh32_ref, act, gug, n2_ref,
               part_y, part_g, got_y, got_g, y_buf, gh_buf, h_own, gy_own, sems, local_sem):
    step = pl.program_id(0)
    rows, d = h_ref.shape
    ff = wd_ref.shape[1]
    net = Torus()
    swap = Exchange(net, rows, ((part_y, got_y), (part_g, got_g)), ((y_buf, y_hbm), (gh_buf, gh_hbm)), sems, local_sem)

    @pl.when(step == 0)
    def _():
        net.barrier([net.partner])

    @pl.when(step < blocks)
    def _():
        n2, _ = norm_rows(h_ref[...].astype(F32))
        n2 = n2.astype(BF16)
        n2_ref[...] = n2
        gy = gy_ref[...]
        for j in strips(ff, QB):
            w = min(QB, ff - j)
            gact = nn(gy, wd_ref[:, j:j + w])
            for i in range(j, j + w, LANES):
                at, mid, end = 2 * i, 2 * i + LANES, 2 * i + QB
                ug = nn(n2, wff_ref[:, at:end])
                up, gate = ug[:, :LANES], ug[:, LANES:]
                sig = 1.0 / (1.0 + jnp.exp(-gate))
                silu = gate * sig
                act[:, i:i + LANES] = (silu * up).astype(BF16)
                ga = gact[:, i - j:i - j + LANES]
                gug[:, at:mid] = (ga * silu).astype(BF16)
                gug[:, mid:end] = (ga * up * sig * (1.0 + gate * (1.0 - sig))).astype(BF16)

        for which, left, right, part in ((0, act, wd_ref, part_y), (1, gug, wff_ref, part_g)):
            for j in strips(d, QB):
                part[step % 2, :, j:j + QB] = nt(left[...], right[j:j + QB, :])
            swap.part(which, step).start()

    @pl.when(step > 1)
    def _():
        swap.settle(step - 2)

    @pl.when(step > 0)
    def _():
        done = step - 1
        hidden = h_own[...].astype(F32)
        normed, inv = norm_rows(hidden)
        y_buf[...] = (hidden + swap.total(0, done)).astype(BF16)
        gh = gy_own[...].astype(F32) + norm_grad(swap.total(1, done), normed, inv)
        gh32_ref[...] = gh
        gh_buf[...] = gh.astype(BF16)
        swap.publish(done)

    own = swap.half(net.core)
    h_own[...] = h_ref[own, :]
    gy_own[...] = gy_ref[own, :]

    @pl.when(step == blocks)
    def _():
        swap.settle(step - 1)


def mlp(h, gy, weights, collective_id, block=512):
    rows, d = h.shape
    ff = weights.shape[1] // 3
    half = block // 2
    blocks = rows // block
    row = lambda width: rows_of(block, width, lambda i: jnp.minimum(i, blocks - 1))
    vm = pltpu.VMEM
    return pl.pallas_call(
        functools.partial(mlp_kernel, blocks),
        grid=(blocks + 1,),
        in_specs=[row(d), row(d), fixed((d, 2 * ff)), fixed((d, ff), (0, 2))],
        out_specs=[HBM, HBM, rows_of(half, d, lambda i: jnp.maximum(i - 1, 0)), row(ff), row(2 * ff), row(d)],
        out_shape=[shape(BF16, rows, d), shape(BF16, rows, d), shape(F32, rows // 2, d), shape(BF16, rows, ff), shape(BF16, rows, 2 * ff), shape(BF16, rows, d)],
        scratch_shapes=[vm((2, block, d), F32)] * 2 + [vm((blocks, half, d), F32)] * 2 + [vm((half, d), BF16)] * 4 + [dma(2, 4, blocks), dma(2)],
        compiler_params=params(collective_id),
        name='mlp',
    )(h, gy, weights, weights)


def accumulate(part, cols, first, left, right):
    for j in strips(right.shape[1], QB):
        w = min(QB, right.shape[1] - j)
        prod = tn(left, right[:, j:j + w]).reshape(part.shape[:-1] + (w,))
        at = slice(cols + j, cols + j + w)
        part[..., at] = jnp.where(first, 0.0, part[..., at]) + prod


SETS = 3
HEAD_STEP = SETS * CHUNK_STEPS


def back_kernel(cols, pairs, gy_ref, n2_ref, act_ref, gug_ref, qkv_ref, lse_ref, gh_ref, wo_ref, o_ref, keep_ref, cos_ref, sin_ref,
                g_ref, gw_ref, gd_ref, gff_ref, do_ref, dk_ref, dv_ref, parts, sems, *bufs):
    step = pl.program_id(0)
    turn = step - HEAD_STEP
    p = turn % pairs
    net = Torus()
    per = len(bufs) // SETS
    scatters = [Scatter(net, parts.at[i], cols, bufs[per * i:per * i + per], sems, i * Scatter.COPIES) for i in range(SETS)]
    calls = plan(SCATTER_PLAN, *(s.stages() for s in scatters))
    middle, end = halves_of(calls, HEAD_STEP)

    @pl.when(step == 0)
    def _():
        net.barrier(net.neighbours())

    first = step % CHUNK_STEPS == 0

    @pl.when(step < CHUNK_STEPS)
    def _():
        accumulate(parts.at[0], 0, first, gy_ref[...], act_ref)

    @pl.when((step >= CHUNK_STEPS) & (step < HEAD_STEP))
    def _():
        accumulate(parts.at[step // CHUNK_STEPS], 0, first, n2_ref[...], gug_ref)

    run_at(step, [c for c in calls if c[0] < HEAD_STEP])

    def put(part, lo, hi, values):
        cols = slice(LANES * part, LANES * (part + 1))
        if part < 2:
            values = values * cos_ref[lo:hi, :] - swap_halves(values) * sin_ref[lo:hi, :]
        g_ref[lo:hi, cols] = (values * keep_ref[lo:hi, cols].astype(F32)).astype(BF16)

    def put_dq(lo, hi, dq):
        put(0, lo, hi, dq * 0.125)

    @pl.when(turn >= 0)
    def _():
        @pl.when(p == 0)
        def _():
            gh = gh_ref[...]
            dout = nn(gh, wo_ref[...]).astype(BF16)
            for j in range(pairs):
                do_ref[j] = dout[:, LANES * j:LANES * (j + 1)]
            gw_ref[...] = jnp.where(turn == 0, 0.0, gw_ref[...]) + tn(gh, o_ref[...])

        q_ref, k_ref, v_ref = (qkv_ref.at[:, pl.ds(LANES * i, LANES)] for i in range(3))
        attend_pair_back(q_ref, k_ref, v_ref, do_ref.at[p], lse_ref.at[0, 0], dk_ref, dv_ref, put_dq, lambda: run_at(turn, middle))
        seq = q_ref.shape[0]
        put(1, 0, seq, dk_ref[...])
        put(2, 0, seq, dv_ref[...])
        run_at(turn, end)

    @pl.when(step == pl.num_programs(0) - 1)
    def _():
        gd_ref[...], *halves = [s.result() for s in scatters]
        tiles = jnp.concatenate(halves, axis=1)
        for i in strips(tiles.shape[1], LANES):
            at = i // QB * LANES
            gff_ref[i // LANES % 2, :, at:at + LANES] = tiles[:, i:i + LANES]


def back(gy, n2, act, gug, qkv, lse, gh, wo_t, o, keep, cos, sin, batch, seq, pairs, collective_id):
    rows, d = gy.shape
    ff = act.shape[1]
    block = rows // CHUNK_STEPS
    turn = lambda s: jnp.maximum(s - HEAD_STEP, 0)
    head = pl.BlockSpec((seq, 3 * LANES), lambda s: (turn(s) // pairs, turn(s) % pairs))
    chunk = lambda s, i: jnp.clip(s - i * CHUNK_STEPS, 0, CHUNK_STEPS - 1)
    early = lambda s: chunk(s, 0)
    late = lambda s: jnp.where(s < 2 * CHUNK_STEPS, chunk(s, 1), chunk(s, 2))
    cols = cut_three(ff)
    vm = pltpu.VMEM
    once = pl.Buffered(buffer_count=1)
    per_seq = lambda width: pl.BlockSpec((seq, width), lambda s: (turn(s) // pairs, 0), pipeline_mode=once)
    return pl.pallas_call(
        functools.partial(back_kernel, cols, pairs),
        grid=(HEAD_STEP + batch * pairs,),
        in_specs=[rows_of(block, d, early), rows_of(block, d, late),
                  rows_of(block, ff, early), pl.BlockSpec((block, ff), lambda s: (late(s), jnp.where(s < 2 * CHUNK_STEPS, 0, 1))),
                  head, pl.BlockSpec((1, 1, 2, seq), lambda s: (turn(s) // pairs, turn(s) % pairs, 0, 0)),
                  per_seq(d), fixed(wo_t.shape), per_seq(LANES * pairs), head, fixed(cos.shape), fixed(sin.shape)],
        out_specs=[head, fixed(wo_t.shape), fixed((PIECE, ff)), fixed((2, PIECE, ff), (0, 0, 0))],
        out_shape=[shape(BF16, *qkv.shape), shape(F32, *wo_t.shape), shape(F32, PIECE, ff), shape(F32, 2, PIECE, ff)],
        scratch_shapes=[vm((pairs, seq, LANES), BF16), vm((seq, LANES), F32), vm((seq, LANES), F32), vm((SETS, SIDE, SIDE, SIDE, PIECE, ff), F32),
                        dma(2, SETS * Scatter.COPIES)] + Scatter.scratch(cols) * SETS,
        compiler_params=params(collective_id),
        name='back',
    )(gy, n2, act, gug, qkv, lse, gh, wo_t, o, keep, cos, sin)


def last_kernel(pairs, blocks, n1_ref, g_ref, x_ref, g_row, gh_ref, w_ref, gout_hbm, gx_hbm, gout_ref, gw_ref,
                part_out, part_qkv, part, got, buf, sems, scatter_sems, local_sem, *bufs):
    step = pl.program_id(0)
    turn = step - pairs
    rows, d = x_ref.shape
    net = Torus()
    per = len(bufs) // (pairs + 1)
    parts = [part_out] + [part_qkv.at[j] for j in range(pairs)]
    scatters = [Scatter(net, s, cut_three(s.shape[-1]), bufs[per * i:per * i + per], scatter_sems, i * Scatter.COPIES) for i, s in enumerate(parts)]
    calls = plan(LAST_PLAN, *(s.stages() for s in scatters))
    swap = Exchange(net, rows, ((part, got),), ((buf, gx_hbm),), sems, local_sem)

    @pl.when(step == 0)
    def _():
        load = pltpu.make_async_copy(gout_hbm, part_out, local_sem.at[1])
        load.start()
        net.barrier(net.neighbours() + [net.partner])
        load.wait()

    begin, end = halves_of(calls)
    run_at(step, begin)

    @pl.when(turn < 0)
    def _():
        accumulate(part_qkv.at[step], 0, True, n1_ref[...], g_ref)

    @pl.when((turn >= 0) & (turn < blocks))
    def _():
        for j in strips(d, QB):
            part[turn % 2, :, j:j + QB] = nt(g_row[...], w_ref[j:j + QB, :])
        swap.part(0, turn).start()

    run_at(step, end)

    @pl.when(turn > 1)
    def _():
        swap.settle(turn - 2)

    @pl.when(turn > 0)
    def _():
        done = turn - 1
        normed, inv = norm_rows(x_ref[swap.half(net.core), :].astype(F32))
        buf[...] = (gh_ref[...] + norm_grad(swap.total(0, done), normed, inv)).astype(BF16)
        swap.publish(done)

    @pl.when(turn == blocks)
    def _():
        for when, call in calls:
            if when > 2 * (pairs + blocks) + 1:
                call()
        swap.settle(turn - 1)
        gout_ref[...] = scatters[0].result()
        for j, s in enumerate(scatters[1:]):
            sums = s.result()
            for i in range(3):
                tile = sums[:, LANES * i:LANES * (i + 1)]
                gw_ref[:, LANES * (pairs * i + j):LANES * (pairs * i + j + 1)] = swap_middle(tile) if i < 2 else tile


def last(x, n1, g, gh32, w, gout, pairs, collective_id, block=512):
    rows, d = x.shape
    blocks = rows // block
    late = lambda n, width, by: rows_of(n, width, lambda s: jnp.clip(s - pairs - by, 0, blocks - 1))
    head = pl.BlockSpec((rows, 3 * LANES), lambda s: (0, jnp.minimum(s, pairs - 1)))
    vm = pltpu.VMEM
    half = block // 2
    torus = (SIDE, SIDE, SIDE, PIECE)
    gout = gout.reshape(torus + (-1,))
    return pl.pallas_call(
        functools.partial(last_kernel, pairs, blocks),
        grid=(pairs + blocks + 1,),
        in_specs=[fixed((rows, d)), head, late(block, d, 1), late(block, g.shape[1], 0), late(half, d, 1), fixed(w.shape), HBM],
        out_specs=[HBM, WHOLE, WHOLE],
        out_shape=[shape(BF16, rows, d), shape(F32, PIECE, gout.shape[-1]), shape(F32, PIECE, w.shape[1])],
        scratch_shapes=[vm(gout.shape, F32), vm((pairs,) + torus + (3 * LANES,), F32), vm((2, block, d), F32), vm((blocks, half, d), F32), vm((half, d), BF16),
                        dma(2, 2, blocks), dma(2, (pairs + 1) * Scatter.COPIES), dma(2)] + Scatter.scratch(cut_three(gout.shape[-1])) + Scatter.scratch(cut_three(3 * LANES)) * pairs,
        compiler_params=params(collective_id),
        name='last',
    )(n1, g, x, g, gh32, w, gout)


def device_step(x, grad_y, w_qkv, w_out, w_ff, w_down):
    batch, seq, d = x.shape
    heads, head = w_qkv.shape[2:]
    pairs = heads // 2
    cos, sin = (jnp.asarray(t) for t in tables(seq, head))
    ids = iter(range(4))
    x2, gy = x.reshape(-1, d), grad_y.reshape(-1, d)
    shards = (w_qkv.reshape(PIECE, -1), w_out.reshape(heads * head, -1).T, w_ff.swapaxes(0, 1), w_down.T)
    qkv, keep, o, lse, h, n1, wq, wo_t, wf = front(x2, *shards, cos, sin, batch, seq, next(ids))
    wq, wo_t, wf = (w.reshape(d, -1) for w in (wq, wo_t, wf))
    y, gh, gh32, act, gug, n2 = mlp(h, gy, wf, next(ids))
    g, gout, gd, gff = back(gy, n2, act, gug, qkv, lse, gh, wo_t, o, keep, cos, sin, batch, seq, pairs, next(ids))
    gx, gout, gqkv = last(x2, n1, g, gh32, wq, gout, pairs, next(ids))
    return y.reshape(x.shape), gx.reshape(x.shape), gqkv.reshape(w_qkv.shape), gout.T.reshape(w_out.shape), gff.swapaxes(0, 1), gd.T


def solution(mesh):
    specs = (P('fsdp'), P('fsdp'), P('fsdp', None, 'tp'), P('tp', None, 'fsdp'), P('fsdp', None, 'tp'), P('tp', 'fsdp'))
    return jax.shard_map(device_step, mesh=mesh, in_specs=specs, out_specs=specs, check_vma=False)
```

```python
import functools

import jax
import jax.numpy as jnp
import numpy as np
from jax import lax
from jax.experimental import pallas as pl
from jax.experimental.pallas import tpu as pltpu
from jax.sharding import PartitionSpec as P

MESH_ID = pl.DeviceIdType.MESH
SIDE = 4
PIECE = 16
ORDERS = ((2, 1, 0), (1, 0, 2), (0, 2, 1))
BOTH = ((0, 1), (1, -1))
PHASES = THREE = range(3)
TWO = range(2)


class Torus:
    def __init__(self):
        self.core = lax.axis_index('tp')
        self.index = lax.axis_index('fsdp')
        plane, x = lax.div(self.index, SIDE), lax.rem(self.index, SIDE)
        self.at = (lax.div(plane, SIDE), lax.rem(plane, SIDE), x)
        self.partner = (1 - self.core, self.index)
        self.moved = {(axis, by): lax.rem(at + (by + SIDE), SIDE) for axis, at in enumerate(self.at) for by in range(-2, 3)}
        self.peers = {(axis, by): self.place(axis, self.moved[axis, by]) for axis in THREE for by in (-1, 1, 2)}

    def place(self, axis, coord):
        pos = list(self.at)
        pos[axis] = coord
        return (self.core, (pos[0] * SIDE + pos[1]) * SIDE + pos[2])

    def shift(self, axis, by):
        return self.moved[axis, by]

    def peer(self, axis, by):
        return self.peers[axis, by]

    def neighbours(self, reach=1):
        return [device for (_, by), device in self.peers.items() if by <= reach]

    def tell(self, sem, devices):
        for device in devices:
            pl.semaphore_signal(sem, inc=1, device_id=device, device_id_type=MESH_ID)

    def barrier(self, devices):
        sem = pltpu.get_barrier_semaphore()
        self.tell(sem, devices)
        pl.semaphore_wait(sem, len(devices))


def pair_of(sems, *at):
    return sems.at[(0,) + at], sems.at[(1,) + at]


def in_order(*calls):
    def run():
        for call in calls:
            call()
    return run


class Gather:
    COPIES = 36

    def __init__(self, net, shard, out, cols, shift, sems, first, direct=False):
        self.net, self.shard, self.out, self.cols, self.moved, self.sems, self.first, self.direct = net, shard, out, cols, shift, sems, first, direct

    def block(self, colour, phase, coord, half=None):
        order = ORDERS[colour]
        off, width = self.cols[colour]
        pick = list(self.net.at)
        for axis in order[:phase]:
            pick[axis] = pl.ds(0, SIDE)
        pick[order[phase]] = coord
        if half is not None and phase:
            pick[order[0]] = pl.ds(half * 2, 2)
        elif half is not None:
            cut = width - width // 256 * 128
            off, width = (off + cut, width - cut) if half else (off, cut)
        return self.out.at[pick[0], pick[1], pick[2], :, pl.ds(off, width)] if width else None

    def copy(self, phase, colour, relay, d, by, came=False):
        axis = ORDERS[colour][phase]
        far = relay and self.direct
        if far and d:
            return None
        by = 2 if far else by
        back = -by if relay and not far else 0
        dst = src = self.block(colour, phase, self.net.shift(axis, back - by if came else back), d if relay and not far else None)
        if dst is None:
            return None
        if not phase and not came and (far or not relay):
            off, width = self.cols[colour]
            src = self.shard.at[:, pl.ds(off + self.moved, width)]
        at = self.first + ((phase * 3 + colour) * 2 + relay) * 2 + d
        return pltpu.make_async_remote_copy(src, dst, *pair_of(self.sems, at), device_id=self.net.peer(axis, by), device_id_type=MESH_ID)

    def each(self, phase, relay, act, came=False):
        for d, by in BOTH:
            for colour in THREE:
                desc = self.copy(phase, colour, relay, d, by, came)
                if desc is not None:
                    act(desc)

    def own(self):
        at = self.net.at
        off, width = self.cols[0][0], sum(w for _, w in self.cols)
        src = self.shard.at[:, pl.ds(off + self.moved, width)]
        return pltpu.make_async_copy(src, self.out.at[at[0], at[1], at[2], :, pl.ds(off, width)], self.sems.at[0, self.first + self.COPIES])

    def arrive(self, phase):
        for relay in TWO:
            if relay or self.direct:
                self.each(phase, relay, lambda c: c.wait_recv(), True)

    def start(self, phase):
        if phase:
            self.arrive(phase - 1)
        if phase == 1:
            self.own().wait()
        for relay in range(1 + self.direct):
            self.each(phase, relay, lambda c: c.start())
        if not phase:
            self.own().start()

    def relay(self, phase):
        for d, by in BOTH:
            for colour in THREE:
                self.copy(phase, colour, 0, d, by, True).wait_recv()
                desc = self.copy(phase, colour, 1, d, by)
                if desc is not None:
                    desc.start()

    def finish(self):
        self.arrive(PHASES[-1])
        for phase in PHASES:
            for relay in TWO:
                self.each(phase, relay, lambda c: c.wait_send())

    def stages(self):
        steps = (self.start,) if self.direct else (self.start, self.relay)
        return [functools.partial(f, p) for p in PHASES for f in steps] + [self.finish]


class Scatter:
    COPIES = 54

    def __init__(self, net, part, cols, bufs, sems, first):
        self.net, self.part, self.cols, self.bufs, self.sems, self.first = net, part, cols, bufs, sems, first

    @staticmethod
    def scratch(cols):
        shapes = []
        for _, w in cols:
            shapes += [(3, 2, 2, SIDE, PIECE, w), (3, 2, 2, PIECE, w), (3, 2, PIECE // 2, w)]
        return [pltpu.VMEM(s, jnp.float32) for s in shapes]

    def buf(self, colour, phase):
        return self.bufs[colour * len(PHASES) + phase]

    def block(self, colour, phase, coord, half):
        order = ORDERS[colour]
        off, width = self.cols[colour]
        pick = [pl.ds(0, SIDE)] * 3
        for axis in order[:phase]:
            pick[axis] = self.net.at[axis]
        pick[order[phase]] = coord
        rows = pl.ds(0, PIECE)
        rest = sorted(order[phase + 1:])
        if rest:
            pick[rest[0]] = pl.ds(2 * half, 2)
        else:
            rows = pl.ds(PIECE // 2 * half, PIECE // 2)
        return self.part.at[pick[0], pick[1], pick[2], rows, pl.ds(off, width)]

    def copy(self, phase, colour, kind, d, by):
        axis = ORDERS[colour][phase]
        buf = self.buf(colour, phase)
        if kind == 2:
            src = buf.at[0, d]
        elif kind:
            src = self.block(colour, phase, self.net.shift(axis, by), 1 - d)
        else:
            src = self.block(colour, phase, self.net.shift(axis, 2), d)
        at = self.first + ((phase * 3 + colour) * 3 + kind) * 2 + d
        return pltpu.make_async_remote_copy(src, buf.at[kind, d], *pair_of(self.sems, at), device_id=self.net.peer(axis, by), device_id_type=MESH_ID)

    def start(self, phase, kind):
        for d, by in BOTH:
            for colour in THREE:
                self.copy(phase, colour, kind, d, by).start()

    def relay(self, phase):
        for colour in THREE:
            buf = self.buf(colour, phase)
            for d, by in BOTH:
                self.copy(phase, colour, 0, d, by).wait_recv()
                buf[0, d] = buf[0, d] + self.block(colour, phase, self.net.shift(ORDERS[colour][phase], by), d)[...]
                self.copy(phase, colour, 2, d, by).start()

    def merge(self, phase):
        for colour in THREE:
            buf = self.buf(colour, phase)
            for d, by in BOTH:
                for kind in (1, 2):
                    self.copy(phase, colour, kind, d, by).wait_recv()
            for half in TWO:
                mine = self.block(colour, phase, self.net.at[ORDERS[colour][phase]], half)
                mine[...] = mine[...] + buf[1, 1 - half] + buf[2, half]
        if phase + 1 < len(PHASES):
            for kind in TWO:
                self.start(phase + 1, kind)

    def finish(self):
        for phase in PHASES:
            for colour in THREE:
                for kind in PHASES:
                    for d, by in BOTH:
                        self.copy(phase, colour, kind, d, by).wait_send()

    def stages(self):
        calls = [functools.partial(self.start, 0, kind) for kind in TWO]
        for phase in PHASES:
            calls += [functools.partial(self.relay, phase), functools.partial(self.merge, phase)]
        return calls[:-1] + [in_order(calls[-1], self.finish)]

    def result(self):
        at = self.net.at
        return self.part[at[0], at[1], at[2]]


def cut_three(width, off=0):
    tiles = width // 128
    sizes = [(tiles + 2 - i) // 3 * 128 for i in THREE]
    return [(off + sum(sizes[:i]), s) for i, s in enumerate(sizes)]


def plan(text, *sets):
    left = [iter(s) for s in sets]
    return [(hook, next(left[int(which)])) for hook, field in enumerate(text.split(',')) for which in field]


def halves_of(calls, first=0):
    return [[((when - first) // 2, call) for when, call in calls if when >= first and (when - first) % 2 == odd] for odd in TWO]


def run_at(hook, calls):
    for when, call in calls:
        pl.when(hook == when)(call)


F32, BF16 = jnp.float32, jnp.bfloat16
QB = 256
LANES = 128
MIB = 2**20


def nt(a, b):
    return lax.dot_general(a, b, (((1,), (1,)), ((), ())), preferred_element_type=F32)


def nn(a, b):
    return jnp.dot(a, b, preferred_element_type=F32)


def tn(a, b):
    return lax.dot_general(a, b, (((0,), (0,)), ((), ())), preferred_element_type=F32)


def along(reduce, values):
    return reduce(values, axis=-1, keepdims=True)


def head_masks(paired):
    lane = lax.broadcasted_iota(jnp.int32, (1, LANES), 1)
    first = (lane % 64) < 32 if paired else lane < 64
    return first, jnp.logical_not(first)


def causal_tile(key_axis):
    dims = (QB, 2 * QB) if key_axis == 0 else (2 * QB, QB)
    return lax.broadcasted_iota(jnp.int32, dims, key_axis) <= lax.broadcasted_iota(jnp.int32, dims, 1 - key_axis) % QB


def by_head(values, masks):
    return jnp.concatenate([jnp.where(m, values, jnp.zeros((), BF16)) for m in masks], axis=0)


def attend_pair(q_ref, k_ref, v_ref, o_ref, lse_ref):
    masks = head_masks(True)
    key, val = k_ref[...], v_ref[...]
    causal = causal_tile(1)
    first = head_masks(False)[0]
    for lo in reversed(strips(q_ref.shape[0], QB)):
        hi = lo + QB
        query = by_head(q_ref[lo:hi, :], masks)
        diag = jnp.where(causal, nt(query, key[lo:hi]), -1e30)
        top = along(jnp.max, diag)
        if lo:
            past = nt(query, key[:lo])
            top = jnp.maximum(top, along(jnp.max, past))
            past = jnp.exp(past - top)
        diag = jnp.exp(diag - top)
        total = along(jnp.sum, diag)
        if lo:
            total = total + along(jnp.sum, past)
        scale = 1.0 / total
        acc = nn((diag * scale).astype(BF16), val[lo:hi])
        if lo:
            acc = acc + nn((past * scale).astype(BF16), val[:lo])
        o_ref[lo:hi, :] = jnp.where(first, acc[:QB], acc[QB:]).astype(BF16)
        lse = jnp.broadcast_to(top + jnp.log(total), acc.shape).T
        for h in TWO:
            lse_ref[h:h + 1, lo:hi] = lse[:1, h * QB:(h + 1) * QB]


def attend_pair_back(q_ref, k_ref, v_ref, do_ref, lse_ref, dk_ref, dv_ref, put_dq):
    seq = q_ref.shape[0]
    qmask, vmask = head_masks(True), head_masks(False)
    key, val = k_ref[...], v_ref[...]
    key_t = key.astype(F32).T.astype(BF16)
    causal = causal_tile(0)
    first = lax.broadcasted_iota(jnp.int32, (LANES, 1), 0) % 64 < 32

    def products(lo):
        hi = lo + QB
        query, dout = by_head(q_ref[lo:hi, :], qmask), by_head(do_ref[lo:hi, :], vmask)
        return query, dout, nt(key[:hi], query), nt(val[:hi], dout)

    ahead = products(seq - QB)
    for lo in reversed(strips(seq, QB)):
        hi = lo + QB
        query, dout, score, grad = ahead
        if lo:
            ahead = products(lo - QB)
        prob = jnp.exp(score - jnp.concatenate([lse_ref[h:h + 1, lo:hi] for h in TWO], axis=1))
        diag = jnp.where(causal, prob[lo:], 0.0)
        prob = jnp.concatenate([prob[:lo], diag], axis=0) if lo else diag
        ds = (prob * (grad - jnp.sum(prob * grad, axis=0, keepdims=True))).astype(BF16)
        both = nn(key_t[:, :hi], ds)
        put_dq(lo, hi, jnp.where(first, both[:, :QB], both[:, QB:]).T)
        dv, dk = nn(prob.astype(BF16), dout), nn(ds, query)
        if hi == seq:
            dv_ref[...] = dv
            dk_ref[...] = dk
        else:
            dv_ref[:hi, :] += dv
            dk_ref[:hi, :] += dk


def swap_halves(values):
    return pltpu.roll(values, LANES // 2, axis=1)


def tables(seq, head):
    freq = 10000.0 ** (-np.arange(0, head, 2, dtype=np.float64) / head)
    angle = np.arange(seq, dtype=np.float64)[:, None] * freq[None, :]
    cos, sin = np.cos(angle).astype(np.float32), np.sin(angle).astype(np.float32)
    return np.concatenate([cos] * 4, axis=1), np.concatenate([-sin, -sin, sin, sin], axis=1)


def norm_rows(values):
    mean = along(jnp.mean, values)
    centered = values - mean
    inv = lax.rsqrt(along(jnp.mean, centered * centered) + 1e-5)
    return centered * inv, inv


def norm_grad(grad, normed, inv):
    mean = along(jnp.mean, grad)
    proj = along(jnp.mean, grad * normed)
    return inv * (grad - mean - normed * proj)


def params(collective_id=None):
    return pltpu.CompilerParams(collective_id=collective_id, has_side_effects=collective_id is not None, vmem_limit_bytes=63 * MIB)


def dma(*shape):
    return pltpu.SemaphoreType.DMA(shape)


def shape(dtype, *dims):
    return jax.ShapeDtypeStruct(dims, dtype)


HBM = pl.BlockSpec(memory_space=pltpu.HBM)
WHOLE = pl.BlockSpec(memory_space=pltpu.VMEM)


def lanes(part):
    return slice(LANES * part, LANES * (part + 1))


def strips(width, size):
    return range(0, width, size)


def rows_of(size, width, index):
    return pl.BlockSpec((size, width), lambda step: (index(step), 0))


def fixed(block, index=(0, 0)):
    return pl.BlockSpec(block, lambda *grid: index, pipeline_mode=pl.Buffered(buffer_count=1))


def project_pair(n1_ref, weight, cos_ref, sin_ref, qkv_ref, keep_ref):
    for lo in strips(n1_ref.shape[0], QB):
        rows = slice(lo, lo + QB)
        raw = nn(n1_ref[rows, :], weight)
        keep_ref[rows, :] = (jnp.abs(raw) < 8.0).astype(F32).astype(BF16)
        raw = jnp.clip(raw, -8.0, 8.0)
        for part in THREE:
            cols = lanes(part)
            tile = raw[:, cols]
            if part < 2:
                tile = tile * cos_ref[rows, :] + swap_halves(tile) * sin_ref[rows, :]
            if not part:
                tile = tile * 0.125
            qkv_ref[rows, cols] = tile.astype(BF16)


def swap_middle(tile):
    quarter = lax.broadcasted_iota(jnp.int32, tile.shape, 1) // (LANES // 4)
    up, down = pltpu.roll(tile, LANES // 4, axis=1), pltpu.roll(tile, LANES - LANES // 4, axis=1)
    return jnp.where(quarter == 1, down, jnp.where(quarter == 2, up, tile))


CHUNK = 256
CHUNK_STEPS = 4
FRONT_PLAN = '015501255012340,234,234,,23,1,342,,34,2,3,,,,,,4,4'
SCATTER_PLAN = ',,,00,,,,,11,,,,2,0,,2,2,1,,,02,1,0,,21,021,201,102'
LAST_PLAN = '0,,011,,0,,3,4,1323,44,,2201,34,201,432,0,31,420,134230142'


def aligned(at, size):
    return pl.ds(pl.multiple_of(at, size), size)


def to_partner(net, src, dst, send, recv):
    return pltpu.make_async_remote_copy(src, dst, send, recv, device_id=net.partner, device_id_type=MESH_ID)


def front_kernel(x_hbm, qkv_shard, out_shard, ff_shard, down_shard, cos_ref, sin_ref, qkv_ref, keep_ref, o_ref, lse_ref, h_hbm, n1_hbm, wq_hbm, wo_hbm, wf_hbm,
                 x_all, n1, w, shards, o_all, part, got, h_buf, wo, sems, gather_sems, load_sem, h_sem, *kept):
    step, last = pl.program_id(0), pl.num_programs(0) - 1
    turn = step - 1
    batch, pairs, seq = o_all.shape[:3]
    b, p = turn % batch, turn // batch
    half = CHUNK // 2
    chunks = seq // CHUNK
    ff = down_shard.shape[1]
    net = Torus()
    width = 3 * LANES
    heads_end, out_end = width * pairs, (width + LANES) * pairs
    places = [(w, cut_three(width), 0), (w, cut_three(width, width), 0), (w, cut_three(heads_end - 2 * width, 2 * width), 0),
              (wo_hbm, cut_three(LANES * pairs), heads_end), (wf_hbm, cut_three(3 * ff), out_end)]
    gathers = [Gather(net, shards, out, cols, shift, gather_sems, i * (Gather.COPIES + 1), i < 2) for i, (out, cols, shift) in enumerate(places)]
    strip = x_all.shape[0] // CHUNK_STEPS

    def load(i):
        return pltpu.make_async_copy(x_hbm.at[pl.ds(strip * i, strip)], x_all.at[pl.ds(strip * i, strip)], load_sem.at[i])

    def save(i):
        return pltpu.make_async_copy(n1.at[pl.ds(strip * i, strip)], n1_hbm.at[pl.ds(strip * i, strip)], load_sem.at[i])

    save_weight = pltpu.make_async_copy(w, wq_hbm, load_sem.at[CHUNK_STEPS])

    def normalize(i):
        load(i).wait()
        rows = slice(strip * i, strip * (i + 1))
        n1[rows, :] = norm_rows(x_all[rows, :].astype(F32))[0].astype(BF16)
        save(i).start()

    calls = plan(FRONT_PLAN, *([*g.stages()] for g in gathers), [functools.partial(normalize, i) for i in range(CHUNK_STEPS)])

    @pl.when(step == 0)
    def _():
        for i in range(CHUNK_STEPS):
            load(i).start()
        for j in range(pairs):
            for i in THREE:
                tile = qkv_shard[:, lanes(pairs * i + j)].astype(F32)
                shards[:, lanes(3 * j + i)] = (swap_middle(tile) if i < 2 else tile).astype(BF16)
        at = width * pairs
        shards[:, at:at + LANES * pairs] = out_shard[...]
        at += LANES * pairs
        for i in strips(ff, LANES):
            for j in TWO:
                shards[:, at + LANES * j:at + LANES * (j + 1)] = ff_shard[j, :, i:i + LANES]
            at += 2 * LANES
        shards[:, at:] = down_shard[...]
        net.barrier(net.neighbours(2) + [net.partner])
        for when, call in calls:
            if not when:
                call()

    begin, end = halves_of(calls, 1)
    run_at(turn, begin)

    @pl.when(turn >= 0)
    def _():
        weight = w[:, :, :, :, pl.ds(pl.multiple_of(width * p, LANES), width)].reshape(n1.shape[1], width)
        project_pair(n1.at[aligned(b * seq, seq)], weight, cos_ref, sin_ref, qkv_ref, keep_ref)
        q_ref, k_ref, v_ref = (qkv_ref.at[:, pl.ds(LANES * i, LANES)] for i in THREE)
        attend_pair(q_ref, k_ref, v_ref, o_ref, lse_ref.at[0, 0])
        o_all[b, p] = o_ref[...]

    run_at(turn, end)

    def rows_in(c, core):
        return aligned(c * CHUNK + core * half, half)

    def part_copy(b, c):
        return to_partner(net, part.at[b, rows_in(c, 1 - net.core)], got.at[b, c], *pair_of(sems, 0, b, c))

    def rows_out(b, c, core):
        return aligned(b * seq + c * CHUNK + core * half, half)

    def h_copy(b, c, core):
        return to_partner(net, h_buf.at[b, c], h_hbm.at[rows_out(b, c, core)], *pair_of(sems, 1, b, c))

    def h_local(b, c):
        return pltpu.make_async_copy(h_buf.at[b, c], h_hbm.at[rows_out(b, c, net.core)], h_sem.at[b, c])

    def project(b):
        o_full = jnp.concatenate([o_all[b, j] for j in range(pairs)], axis=1)
        weight = wo[...].reshape(part.shape[2], -1)
        for c in range(chunks):
            rows = slice(c * CHUNK, (c + 1) * CHUNK)
            part[b, rows, :] = nt(o_full[rows], weight)
            part_copy(b, c).start()

    def combine(b):
        for c in range(chunks):
            part_copy(b, c).wait()
            own = rows_in(c, net.core)
            h_buf[b, c] = (x_all[rows_out(b, c, net.core), :].astype(F32) + (part[b, own, :] + got[b, c])).astype(BF16)
            h_copy(b, c, net.core).start()
            h_local(b, c).start()

    def settle():
        for b in range(batch):
            for c in range(chunks):
                h_copy(b, c, net.core).wait_send()
                h_local(b, c).wait()
                h_copy(b, c, 1 - net.core).wait_recv()
        for i in range(CHUNK_STEPS):
            save(i).wait()
        save_weight.wait()

    def fetch():
        copy = pltpu.make_async_copy(wo_hbm, wo, h_sem.at[0, 0])
        copy.start()
        save_weight.start()
        copy.wait()
        project(0)

    def finish():
        combine(0)
        project(1)
        combine(1)
        settle()

    run_at(last - step, [(1, fetch), (0, finish)])
    run_at(turn + 1, begin[-1:])


def front(x, qkv_shard, out_shard, ff_shard, down_shard, cos, sin, batch, seq, collective_id):
    pairs = out_shard.shape[1] // LANES
    rows, d = x.shape
    width = 3 * LANES
    chunks = seq // CHUNK
    vm = pltpu.VMEM
    torus = (SIDE, SIDE, SIDE, PIECE)
    shards = [s.size // PIECE for s in (qkv_shard, out_shard, ff_shard, down_shard)]
    turn = lambda s: jnp.maximum(s - 1, 0)
    head = lambda width: pl.BlockSpec((seq, width), lambda s: (turn(s) % batch, turn(s) // batch))
    return pl.pallas_call(
        front_kernel,
        grid=(1 + batch * pairs,),
        in_specs=[HBM] + [WHOLE] * 4 + [fixed(cos.shape)] * 2,
        out_specs=[head(width), head(width), head(LANES), pl.BlockSpec((1, 1, 2, seq), lambda s: (turn(s) % batch, turn(s) // batch, 0, 0))] + [HBM] * 5,
        out_shape=[shape(BF16, rows, width * pairs)] * 2 + [shape(BF16, rows, LANES * pairs), shape(F32, batch, pairs, 2, seq), shape(BF16, rows, d), shape(BF16, rows, d),
                   shape(BF16, *torus, shards[0]), shape(BF16, *torus, shards[1]), shape(BF16, *torus, shards[2] + shards[3])],
        scratch_shapes=[vm((rows, d), BF16), vm((rows, d), BF16), vm(torus + (width * pairs,), BF16), vm((PIECE, sum(shards)), BF16),
                        vm((batch, pairs, seq, LANES), BF16), vm((batch, seq, d), F32), vm((batch, chunks, CHUNK // 2, d), F32), vm((batch, chunks, CHUNK // 2, d), BF16),
                        vm(torus + (shards[1],), BF16), dma(2, 2, batch, chunks), dma(2, 5 * (Gather.COPIES + 1)), dma(CHUNK_STEPS + 1), dma(batch, chunks)],
        compiler_params=params(collective_id),
        name='front',
    )(x, qkv_shard, out_shard, ff_shard, down_shard, cos, sin)


class Exchange:
    def __init__(self, net, rows, partials, results, sems, local_sem):
        self.net, self.rows, self.partials, self.results, self.sems, self.local_sem = net, rows, partials, results, sems, local_sem

    def half(self, core, at=0):
        return aligned(at * self.rows + core * (self.rows // 2), self.rows // 2)

    def part(self, which, at):
        part, got = self.partials[which]
        return to_partner(self.net, part.at[at % 2, self.half(1 - self.net.core)], got.at[at], *pair_of(self.sems, which, at))

    def total(self, which, at):
        part, got = self.partials[which]
        self.part(which, at).wait()
        return part[at % 2, self.half(self.net.core), :] + got[at]

    def results_of(self, at, core, act):
        for i, (buf, hbm) in enumerate(self.results):
            act(buf.at[at % 2], hbm.at[self.half(core, at)], pair_of(self.sems, len(self.partials) + i, at), self.local_sem.at[i, at % 2])

    def publish(self, at):
        def act(buf, rows, sem, local_sem):
            to_partner(self.net, buf, rows, *sem).start()
            pltpu.make_async_copy(buf, rows, local_sem).start()
        self.results_of(at, self.net.core, act)

    def settle(self, at):
        def act(buf, rows, sem, local_sem):
            to_partner(self.net, buf, rows, *sem).wait_send()
            pltpu.make_async_copy(buf, rows, local_sem).wait()
        self.results_of(at, self.net.core, act)
        self.results_of(at, 1 - self.net.core, lambda buf, rows, sem, local_sem: to_partner(self.net, buf, rows, *sem).wait_recv())


def mlp_kernel(blocks, h_ref, gy_ref, wff_ref, wd_ref, y_hbm, gh_hbm, gh32_ref, acts, n2_ref,
               part_y, part_g, got_y, got_g, y_buf, gh_buf, h_own, gy_own, sems, local_sem):
    step = pl.program_id(0)
    rows, d = h_ref.shape
    ff = wd_ref.shape[1]
    gug, act = acts.at[:, pl.ds(0, 2 * ff)], acts.at[:, pl.ds(2 * ff, ff)]
    net = Torus()
    swap = Exchange(net, rows, ((part_y, got_y), (part_g, got_g)), ((y_buf, y_hbm), (gh_buf, gh_hbm)), sems, local_sem)

    @pl.when(step == 0)
    def _():
        net.barrier([net.partner])

    @pl.when(step < blocks)
    def _():
        n2, _ = norm_rows(h_ref[...].astype(F32))
        n2 = n2.astype(BF16)
        n2_ref[...] = n2
        gy = gy_ref[...]
        for j in strips(ff, QB):
            w = min(QB, ff - j)
            gact = nn(gy, wd_ref[:, j:j + w])
            for i in range(j, j + w, LANES):
                at, mid, end = 2 * i, 2 * i + LANES, 2 * i + QB
                ug = nn(n2, wff_ref[:, at:end])
                up, gate = ug[:, :LANES], ug[:, LANES:]
                sig = 1.0 / (1.0 + jnp.exp(-gate))
                silu = gate * sig
                act[:, i:i + LANES] = (silu * up).astype(BF16)
                ga = gact[:, i - j:i - j + LANES]
                gug[:, at:mid] = (ga * silu).astype(BF16)
                gug[:, mid:end] = (ga * up * sig * (1.0 + gate * (1.0 - sig))).astype(BF16)

        for which, left, right, part in ((0, act, wd_ref, part_y), (1, gug, wff_ref, part_g)):
            for j in strips(d, QB):
                part[step % 2, :, j:j + QB] = nt(left[...], right[j:j + QB, :])
            swap.part(which, step).start()

    @pl.when(step > 2)
    def _():
        swap.settle(step - 3)

    @pl.when(step > 0)
    def _():
        done = step - 1
        hidden = h_own[...].astype(F32)
        normed, inv = norm_rows(hidden)
        y_buf[done % 2] = (hidden + swap.total(0, done)).astype(BF16)
        gh = gy_own[...].astype(F32) + norm_grad(swap.total(1, done), normed, inv)
        gh32_ref[...] = gh
        gh_buf[done % 2] = gh.astype(BF16)
        swap.publish(done)

    own = swap.half(net.core)
    h_own[...] = h_ref[own, :]
    gy_own[...] = gy_ref[own, :]

    @pl.when(step == blocks)
    def _():
        for at in (blocks - 2, blocks - 1):
            swap.settle(at)


def mlp(h, gy, weights, collective_id, block=512):
    rows, d = h.shape
    ff = weights.shape[1] // 3
    half = block // 2
    blocks = rows // block
    row = lambda width: rows_of(block, width, lambda i: jnp.minimum(i, blocks - 1))
    vm = pltpu.VMEM
    return pl.pallas_call(
        functools.partial(mlp_kernel, blocks),
        grid=(blocks + 1,),
        in_specs=[row(d), row(d), fixed((d, 2 * ff)), fixed((d, ff), (0, 2))],
        out_specs=[HBM, HBM, rows_of(half, d, lambda i: jnp.maximum(i - 1, 0)), row(3 * ff), row(d)],
        out_shape=[shape(BF16, rows, d), shape(BF16, rows, d), shape(F32, rows // 2, d), shape(BF16, rows, 3 * ff), shape(BF16, rows, d)],
        scratch_shapes=[vm((2, block, d), F32)] * 2 + [vm((blocks, half, d), F32)] * 2 + [vm((2, half, d), BF16)] * 2 + [vm((half, d), BF16)] * 2 + [dma(2, 4, blocks), dma(2, 2)],
        compiler_params=params(collective_id),
        name='mlp',
    )(h, gy, weights, weights)


def accumulate(part, cols, first, left, right):
    for j in strips(right.shape[1], QB):
        w = min(QB, right.shape[1] - j)
        prod = tn(left, right[:, j:j + w]).reshape(part.shape[:-1] + (w,))
        at = slice(cols + j, cols + j + w)
        part[..., at] = jnp.where(first, 0.0, part[..., at]) + prod


SETS = 3
HEAD_STEP = SETS * CHUNK_STEPS


def back_kernel(cols, pairs, gy_ref, n2_ref, act_ref, qkv_ref, lse_ref, gh_ref, wo_ref, o_ref, keep_ref, cos_ref, sin_ref,
                g_ref, gw_ref, gd_ref, gff_ref, do_ref, dk_ref, dv_ref, parts, sems, *bufs):
    step = pl.program_id(0)
    turn = step - HEAD_STEP
    p = turn % pairs
    net = Torus()
    per = len(bufs) // SETS
    scatters = [Scatter(net, parts.at[i], cols, bufs[per * i:per * i + per], sems, i * Scatter.COPIES) for i in range(SETS)]
    calls = plan(SCATTER_PLAN, *(s.stages() for s in scatters))
    begin, end = halves_of(calls, HEAD_STEP)

    @pl.when(step == 0)
    def _():
        net.barrier(net.neighbours())

    first = step % CHUNK_STEPS == 0

    @pl.when(step < CHUNK_STEPS)
    def _():
        accumulate(parts.at[0], 0, first, gy_ref[...], act_ref)

    @pl.when((step >= CHUNK_STEPS) & (step < HEAD_STEP))
    def _():
        accumulate(parts.at[step // CHUNK_STEPS], 0, first, n2_ref[...], act_ref)

    run_at(step, [c for c in calls if c[0] < HEAD_STEP])

    def put(part, lo, hi, values):
        cols = lanes(part)
        if part < 2:
            values = values * cos_ref[lo:hi, :] - swap_halves(values) * sin_ref[lo:hi, :]
        g_ref[lo:hi, cols] = (values * keep_ref[lo:hi, cols].astype(F32)).astype(BF16)

    def put_dq(lo, hi, dq):
        put(0, lo, hi, dq * 0.125)

    @pl.when(turn >= 0)
    def _():
        @pl.when(p == 0)
        def _():
            gh = gh_ref[...]
            dout = nn(gh, wo_ref[...]).astype(BF16)
            for j in range(pairs):
                do_ref[j] = dout[:, lanes(j)]
            gw_ref[...] = jnp.where(turn == 0, 0.0, gw_ref[...]) + tn(gh, o_ref[...])

        run_at(turn, begin)
        q_ref, k_ref, v_ref = (qkv_ref.at[:, pl.ds(LANES * i, LANES)] for i in THREE)
        attend_pair_back(q_ref, k_ref, v_ref, do_ref.at[p], lse_ref.at[0, 0], dk_ref, dv_ref, put_dq)
        seq = q_ref.shape[0]
        put(1, 0, seq, dk_ref[...])
        put(2, 0, seq, dv_ref[...])
        run_at(turn, end)

    @pl.when(step == pl.num_programs(0) - 1)
    def _():
        gd_ref[...], *halves = [s.result() for s in scatters]
        tiles = jnp.concatenate(halves, axis=1)
        for i in strips(tiles.shape[1], LANES):
            at = i // QB * LANES
            gff_ref[i // LANES % 2, :, at:at + LANES] = tiles[:, i:i + LANES]


def back(gy, n2, acts, qkv, lse, gh, wo_t, o, keep, cos, sin, batch, seq, pairs, collective_id):
    rows, d = gy.shape
    ff = acts.shape[1] // SETS
    block = rows // CHUNK_STEPS
    turn = lambda s: jnp.maximum(s - HEAD_STEP, 0)
    head = pl.BlockSpec((seq, 3 * LANES), lambda s: (turn(s) // pairs, turn(s) % pairs))
    chunk = lambda s, i: jnp.clip(s - i * CHUNK_STEPS, 0, CHUNK_STEPS - 1)
    late = lambda s: jnp.where(s < 2 * CHUNK_STEPS, chunk(s, 1), chunk(s, 2))
    acts_at = lambda s: (jnp.where(s < CHUNK_STEPS, s, late(s)), jnp.where(s < CHUNK_STEPS, 2, jnp.minimum(s // (2 * CHUNK_STEPS), 1)))
    cols = cut_three(ff)
    vm = pltpu.VMEM
    once = pl.Buffered(buffer_count=1)
    per_seq = lambda width: pl.BlockSpec((seq, width), lambda s: (turn(s) // pairs, 0), pipeline_mode=once)
    return pl.pallas_call(
        functools.partial(back_kernel, cols, pairs),
        grid=(HEAD_STEP + batch * pairs,),
        in_specs=[rows_of(block, d, lambda s: chunk(s, 0)), rows_of(block, d, late), pl.BlockSpec((block, ff), acts_at), head, pl.BlockSpec((1, 1, 2, seq), lambda s: (turn(s) // pairs, turn(s) % pairs, 0, 0)),
                  per_seq(d), fixed(wo_t.shape), per_seq(LANES * pairs), head, fixed(cos.shape), fixed(sin.shape)],
        out_specs=[head, fixed(wo_t.shape), fixed((PIECE, ff)), fixed((2, PIECE, ff), (0, 0, 0))],
        out_shape=[shape(BF16, *qkv.shape), shape(F32, *wo_t.shape), shape(F32, PIECE, ff), shape(F32, 2, PIECE, ff)],
        scratch_shapes=[vm((pairs, seq, LANES), BF16), vm((seq, LANES), F32), vm((seq, LANES), F32), vm((SETS, SIDE, SIDE, SIDE, PIECE, ff), F32),
                        dma(2, SETS * Scatter.COPIES)] + Scatter.scratch(cols) * SETS,
        compiler_params=params(collective_id),
        name='back',
    )(gy, n2, acts, qkv, lse, gh, wo_t, o, keep, cos, sin)


def last_kernel(pairs, blocks, n1_ref, g_ref, x_ref, g_row, gh_ref, w_ref, gout_hbm, gx_hbm, gout_ref, gw_ref,
                part_out, part_qkv, part, got, buf, sems, scatter_sems, local_sem, *bufs):
    step = pl.program_id(0)
    turn = step - pairs
    rows, d = x_ref.shape
    net = Torus()
    per = len(bufs) // (pairs + 1)
    parts = [part_out] + [part_qkv.at[j] for j in range(pairs)]
    scatters = [Scatter(net, s, cut_three(s.shape[-1]), bufs[per * i:per * i + per], scatter_sems, i * Scatter.COPIES) for i, s in enumerate(parts)]
    calls = plan(LAST_PLAN, *(s.stages() for s in scatters))
    swap = Exchange(net, rows, ((part, got),), ((buf, gx_hbm),), sems, local_sem)

    @pl.when(step == 0)
    def _():
        load = pltpu.make_async_copy(gout_hbm, part_out, local_sem.at[1, 0])
        load.start()
        net.barrier(net.neighbours() + [net.partner])
        load.wait()

    begin, end = halves_of(calls)
    run_at(step, begin)

    @pl.when(turn < 0)
    def _():
        accumulate(part_qkv.at[step], 0, True, n1_ref[...], g_ref)

    @pl.when((turn >= 0) & (turn < blocks))
    def _():
        for j in strips(d, QB):
            part[turn % 2, :, j:j + QB] = nt(g_row[...], w_ref[j:j + QB, :])
        swap.part(0, turn).start()

    run_at(step, end)

    @pl.when(turn > 2)
    def _():
        swap.settle(turn - 3)

    @pl.when(turn > 0)
    def _():
        done = turn - 1
        normed, inv = norm_rows(x_ref[swap.half(net.core), :].astype(F32))
        buf[done % 2] = (gh_ref[...] + norm_grad(swap.total(0, done), normed, inv)).astype(BF16)
        swap.publish(done)

    @pl.when(turn == blocks)
    def _():
        for when, call in calls:
            if when > 2 * (pairs + blocks) + 1:
                call()
        for at in (blocks - 2, blocks - 1):
            swap.settle(at)
        gout_ref[...] = scatters[0].result()
        for j, s in enumerate(scatters[1:]):
            sums = s.result()
            for i in THREE:
                tile = sums[:, lanes(i)]
                gw_ref[:, lanes(pairs * i + j)] = swap_middle(tile) if i < 2 else tile


def last(x, n1, g, gh32, w, gout, pairs, collective_id, block=512):
    rows, d = x.shape
    blocks = rows // block
    late = lambda n, width, by: rows_of(n, width, lambda s: jnp.clip(s - pairs - by, 0, blocks - 1))
    head = pl.BlockSpec((rows, 3 * LANES), lambda s: (0, jnp.minimum(s, pairs - 1)))
    vm = pltpu.VMEM
    half = block // 2
    torus = (SIDE, SIDE, SIDE, PIECE)
    gout = gout.reshape(torus + (-1,))
    return pl.pallas_call(
        functools.partial(last_kernel, pairs, blocks),
        grid=(pairs + blocks + 1,),
        in_specs=[fixed((rows, d)), head, late(block, d, 1), late(block, g.shape[1], 0), late(half, d, 1), fixed(w.shape), HBM],
        out_specs=[HBM, WHOLE, WHOLE],
        out_shape=[shape(BF16, rows, d), shape(F32, PIECE, gout.shape[-1]), shape(F32, PIECE, w.shape[1])],
        scratch_shapes=[vm(gout.shape, F32), vm((pairs,) + torus + (3 * LANES,), F32), vm((2, block, d), F32), vm((blocks, half, d), F32), vm((2, half, d), BF16),
                        dma(2, 2, blocks), dma(2, (pairs + 1) * Scatter.COPIES), dma(2, 2)] + Scatter.scratch(cut_three(gout.shape[-1])) + Scatter.scratch(cut_three(3 * LANES)) * pairs,
        compiler_params=params(collective_id),
        name='last',
    )(n1, g, x, g, gh32, w, gout)


def device_step(x, grad_y, w_qkv, w_out, w_ff, w_down):
    batch, seq, d = x.shape
    heads, head = w_qkv.shape[2:]
    pairs = heads // 2
    cos, sin = (jnp.asarray(t) for t in tables(seq, head))
    ids = iter(range(4))
    x2, gy = x.reshape(-1, d), grad_y.reshape(-1, d)
    shards = (w_qkv.reshape(PIECE, -1), w_out.reshape(heads * head, -1).T, w_ff.swapaxes(0, 1), w_down.T)
    qkv, keep, o, lse, h, n1, wq, wo_t, wf = front(x2, *shards, cos, sin, batch, seq, next(ids))
    wq, wo_t, wf = (w.reshape(d, -1) for w in (wq, wo_t, wf))
    y, gh, gh32, acts, n2 = mlp(h, gy, wf, next(ids))
    g, gout, gd, gff = back(gy, n2, acts, qkv, lse, gh, wo_t, o, keep, cos, sin, batch, seq, pairs, next(ids))
    gx, gout, gqkv = last(x2, n1, g, gh32, wq, gout, pairs, next(ids))
    return y.reshape(x.shape), gx.reshape(x.shape), gqkv.reshape(w_qkv.shape), gout.T.reshape(w_out.shape), gff.swapaxes(0, 1), gd.T


def solution(mesh):
    specs = (P('fsdp'), P('fsdp'), P('fsdp', None, 'tp'), P('tp', None, 'fsdp'), P('fsdp', None, 'tp'), P('tp', 'fsdp'))
    return jax.shard_map(device_step, mesh=mesh, in_specs=specs, out_specs=specs, check_vma=False)
```

```python
import functools

import jax
import jax.numpy as jnp
import numpy as np
from jax import lax
from jax.experimental import pallas as pl
from jax.experimental.pallas import tpu as pltpu
from jax.sharding import PartitionSpec as P

MESH_ID = pl.DeviceIdType.MESH
SIDE = 4
PIECE = 16
ORDERS = ((2, 1, 0), (1, 0, 2), (0, 2, 1))
BOTH = ((0, 1), (1, -1))
PHASES = THREE = range(3)
TWO = range(2)


class Torus:
    def __init__(self):
        self.core = lax.axis_index('tp')
        self.index = lax.axis_index('fsdp')
        plane, x = lax.div(self.index, SIDE), lax.rem(self.index, SIDE)
        self.at = (lax.div(plane, SIDE), lax.rem(plane, SIDE), x)
        self.partner = (1 - self.core, self.index)
        self.moved = {(axis, by): lax.rem(at + (by + SIDE), SIDE) for axis, at in enumerate(self.at) for by in range(-2, 3)}
        self.peers = {(axis, by): self.place(axis, self.moved[axis, by]) for axis in THREE for by in (-1, 1, 2)}

    def place(self, axis, coord):
        pos = list(self.at)
        pos[axis] = coord
        z, y, x = pos
        return (self.core, (z * SIDE + y) * SIDE + x)

    def shift(self, axis, by):
        return self.moved[axis, by]

    def peer(self, axis, by):
        return self.peers[axis, by]

    def neighbours(self, reach=1):
        return [device for (_, by), device in self.peers.items() if by <= reach]

    def tell(self, sem, devices):
        for device in devices:
            pl.semaphore_signal(sem, inc=1, device_id=device, device_id_type=MESH_ID)

    def barrier(self, devices):
        sem = pltpu.get_barrier_semaphore()
        self.tell(sem, devices)
        pl.semaphore_wait(sem, len(devices))


def pair_of(sems, *at):
    return sems.at[(0,) + at], sems.at[(1,) + at]


def in_order(*calls):
    def run():
        for call in calls:
            call()
    return run


def span(cols):
    (off, width), *rest = cols
    return pl.ds(off, width + sum(w for _, w in rest))


class Gather:
    SEMS = 7

    def __init__(self, net, shard, out, cols, shift, sems, first, direct=False):
        self.net, self.shard, self.out, self.cols, self.moved, self.sems, self.first, self.direct = net, shard, out, cols, shift, sems, first, direct

    def block(self, colour, phase, coord, half=None):
        order = ORDERS[colour]
        off, width = self.cols[colour]
        pick = list(self.net.at)
        for axis in order[:phase]:
            pick[axis] = pl.ds(0, SIDE)
        pick[order[phase]] = coord
        if half is not None and phase:
            pick[order[0]] = pl.ds(half * 2, 2)
        elif half is not None:
            cut = width - width // 256 * 128
            off, width = (off + cut, width - cut) if half else (off, cut)
        return self.out.at[(*pick, slice(None), pl.ds(off, width))] if width else None

    def copy(self, phase, colour, relay, d, by):
        axis = ORDERS[colour][phase]
        far = relay and self.direct
        if far and d:
            return None
        by = 2 if far else by
        back = -by if relay and not far else 0
        dst = src = self.block(colour, phase, self.net.shift(axis, back), d if relay and not far else None)
        if dst is None:
            return None
        if not phase and (far or not relay):
            off, width = self.cols[colour]
            src = self.shard.at[:, pl.ds(off + self.moved, width)]
        return pltpu.make_async_remote_copy(src, dst, *self.sem(phase, relay), device_id=self.net.peer(axis, by), device_id_type=MESH_ID)

    def sem(self, phase, relay):
        return pair_of(self.sems, self.first + 2 * phase + relay)

    def each(self, phase, relay):
        for d, by in BOTH:
            for colour in THREE:
                desc = self.copy(phase, colour, relay, d, by)
                if desc is not None:
                    desc.start()

    def wait(self, phase, relay, side):
        pick = [pl.ds(0, SIDE)] * phase + [pl.ds(0, 2 - relay)] + [0, 0]
        ref = self.out.at[tuple(reversed(pick[:3])) + (slice(None), span(self.cols))]
        pltpu.make_async_copy(ref, ref, self.sem(phase, relay)[side]).wait()

    def own(self):
        at = self.net.at
        cols = span(self.cols)
        src = self.shard.at[:, pl.ds(cols.start + self.moved, cols.size)]
        return pltpu.make_async_copy(src, self.out.at[(*at, slice(None), cols)], self.sems.at[0, self.first + self.SEMS - 1])

    def arrive(self, phase):
        if self.direct:
            self.wait(phase, 0, 1)
        self.wait(phase, 1, 1)

    def start(self, phase):
        if phase:
            self.arrive(phase - 1)
        if phase == 1:
            self.own().wait()
        for relay in range(1 + self.direct):
            self.each(phase, relay)
        if not phase:
            self.own().start()

    def relay(self, phase):
        self.wait(phase, 0, 1)
        self.each(phase, 1)

    def finish(self):
        self.arrive(PHASES[-1])
        for phase in PHASES:
            for relay in TWO:
                self.wait(phase, relay, 0)

    def stages(self):
        steps = (self.start,) if self.direct else (self.start, self.relay)
        return [functools.partial(f, p) for p in PHASES for f in steps] + [self.finish]


class Scatter:
    SEMS = 9

    def __init__(self, net, part, cols, bufs, sems, first):
        self.net, self.part, self.cols, self.bufs, self.sems, self.first = net, part, cols, bufs, sems, first

    @staticmethod
    def scratch(cols):
        shapes = []
        for _, w in cols:
            shapes += [(3, 2, 2, SIDE, PIECE, w), (3, 2, 2, PIECE, w), (3, 2, PIECE // 2, w)]
        return [pltpu.VMEM(s, jnp.float32) for s in shapes]

    def buf(self, colour, phase):
        return self.bufs[colour * len(PHASES) + phase]

    def block(self, colour, phase, coord, half):
        order = ORDERS[colour]
        off, width = self.cols[colour]
        pick = [pl.ds(0, SIDE)] * 3
        for axis in order[:phase]:
            pick[axis] = self.net.at[axis]
        pick[order[phase]] = coord
        rows = pl.ds(0, PIECE)
        rest = sorted(order[phase + 1:])
        if rest:
            pick[rest[0]] = pl.ds(2 * half, 2)
        else:
            rows = pl.ds(PIECE // 2 * half, PIECE // 2)
        return self.part.at[(*pick, rows, pl.ds(off, width))]

    def copy(self, phase, colour, kind, d, by):
        axis = ORDERS[colour][phase]
        buf = self.buf(colour, phase)
        if kind == 2:
            src = buf.at[0, d]
        elif kind:
            src = self.block(colour, phase, self.net.shift(axis, by), 1 - d)
        else:
            src = self.block(colour, phase, self.net.shift(axis, 2), d)
        return pltpu.make_async_remote_copy(src, buf.at[kind, d], *self.sem(phase, kind), device_id=self.net.peer(axis, by), device_id_type=MESH_ID)

    def sem(self, phase, kind):
        return pair_of(self.sems, self.first + len(PHASES) * phase + kind)

    def wait(self, phase, kind, side):
        pick = [0] * (phase + 1) + [pl.ds(0, SIDE)] * (2 - phase)
        ref = self.part.at[tuple(pick) + (slice(None), span(self.cols))]
        pltpu.make_async_copy(ref, ref, self.sem(phase, kind)[side]).wait()

    def start(self, phase, kind):
        for d, by in BOTH:
            for colour in THREE:
                self.copy(phase, colour, kind, d, by).start()

    def relay(self, phase):
        self.wait(phase, 0, 1)
        for colour in THREE:
            buf = self.buf(colour, phase)
            for d, by in BOTH:
                buf[0, d] = buf[0, d] + self.block(colour, phase, self.net.shift(ORDERS[colour][phase], by), d)[...]
        self.start(phase, 2)

    def merge(self, phase):
        for kind in (1, 2):
            self.wait(phase, kind, 1)
        for colour in THREE:
            buf = self.buf(colour, phase)
            for half in TWO:
                mine = self.block(colour, phase, self.net.at[ORDERS[colour][phase]], half)
                mine[...] = mine[...] + buf[1, 1 - half] + buf[2, half]
        if phase + 1 < len(PHASES):
            for kind in TWO:
                self.start(phase + 1, kind)

    def finish(self):
        for phase in PHASES:
            for kind in PHASES:
                self.wait(phase, kind, 0)

    def stages(self):
        calls = [functools.partial(self.start, 0, kind) for kind in TWO]
        for phase in PHASES:
            calls += [functools.partial(self.relay, phase), functools.partial(self.merge, phase)]
        return calls[:-1] + [in_order(calls[-1], self.finish)]

    def result(self):
        return self.part[self.net.at]


def cut_three(width, off=0, turn=0):
    tiles = width // 128
    sizes = [(tiles + (2 + turn - i) % 3) // 3 * 128 for i in THREE]
    return [(off + sum(sizes[:i]), s) for i, s in enumerate(sizes)]


def plan(text, *sets):
    left = [iter(s) for s in sets]
    return [(hook, next(left[int(which)])) for hook, field in enumerate(text.split(',')) for which in field]


def halves_of(calls, first=0):
    return [[((when - first) // 2, call) for when, call in calls if when >= first and (when - first) % 2 == odd] for odd in TWO]


def run_at(hook, calls):
    for when, call in calls:
        pl.when(hook == when)(call)


F32, BF16 = jnp.float32, jnp.bfloat16
QB = 256
LANES = 128
CLIP = 8.0
MIB = 2**20


def nt(a, b):
    return lax.dot_general(a, b, (((1,), (1,)), ((), ())), preferred_element_type=F32)


def nn(a, b):
    return jnp.dot(a, b, preferred_element_type=F32)


def tn(a, b):
    return lax.dot_general(a, b, (((0,), (0,)), ((), ())), preferred_element_type=F32)


def along(reduce, values):
    return reduce(values, axis=-1, keepdims=True)


def head_masks(paired):
    lane = lax.broadcasted_iota(jnp.int32, (1, LANES), 1)
    first = (lane % 64) < 32 if paired else lane < 64
    return first, jnp.logical_not(first)


def causal_tile(key_axis):
    dims = (QB, 2 * QB) if key_axis == 0 else (2 * QB, QB)
    return lax.broadcasted_iota(jnp.int32, dims, key_axis) <= lax.broadcasted_iota(jnp.int32, dims, 1 - key_axis) % QB


def by_head(values, masks):
    return jnp.concatenate([jnp.where(m, values, jnp.zeros((), BF16)) for m in masks], axis=0)


def attend_pair(q_ref, k_ref, v_ref, o_ref, lse_ref):
    masks = head_masks(True)
    key, val = k_ref[...], v_ref[...]
    causal = causal_tile(1)
    first = head_masks(False)[0]
    for lo in reversed(strips(q_ref.shape[0], QB)):
        hi = lo + QB
        query = by_head(q_ref[lo:hi, :], masks)
        diag = jnp.where(causal, nt(query, key[lo:hi]), -1e30)
        top = along(jnp.max, diag)
        if lo:
            past = nt(query, key[:lo])
            top = jnp.maximum(top, along(jnp.max, past))
            past = jnp.exp(past - top)
        diag = jnp.exp(diag - top)
        total = along(jnp.sum, diag)
        if lo:
            total = total + along(jnp.sum, past)
        scale = 1.0 / total
        acc = nn((diag * scale).astype(BF16), val[lo:hi])
        if lo:
            acc = acc + nn((past * scale).astype(BF16), val[:lo])
        o_ref[lo:hi, :] = jnp.where(first, acc[:QB], acc[QB:]).astype(BF16)
        lse = jnp.broadcast_to(top + jnp.log(total), acc.shape).T
        for h in TWO:
            lse_ref[h:h + 1, lo:hi] = lse[:1, h * QB:(h + 1) * QB]


def attend_pair_back(q_ref, k_ref, v_ref, do_ref, lse_ref, dk_ref, dv_ref, put_dq):
    seq = q_ref.shape[0]
    qmask, vmask = head_masks(True), head_masks(False)
    key, val = k_ref[...], v_ref[...]
    key_t = key.astype(F32).T.astype(BF16)
    causal = causal_tile(0)
    first = lax.broadcasted_iota(jnp.int32, (LANES, 1), 0) % 64 < 32

    def products(lo):
        hi = lo + QB
        query, dout = by_head(q_ref[lo:hi, :], qmask), by_head(do_ref[lo:hi, :], vmask)
        return query, dout, nt(key[:hi], query), nt(val[:hi], dout)

    ahead = products(seq - QB)
    for lo in reversed(strips(seq, QB)):
        hi = lo + QB
        query, dout, score, grad = ahead
        if lo:
            ahead = products(lo - QB)
        prob = jnp.exp(score - jnp.concatenate([lse_ref[h:h + 1, lo:hi] for h in TWO], axis=1))
        diag = jnp.where(causal, prob[lo:], 0.0)
        prob = jnp.concatenate([prob[:lo], diag], axis=0) if lo else diag
        ds = (prob * (grad - jnp.sum(prob * grad, axis=0, keepdims=True))).astype(BF16)
        both = nn(key_t[:, :hi], ds)
        put_dq(lo, hi, jnp.where(first, both[:, :QB], both[:, QB:]).T)
        dv, dk = nn(prob.astype(BF16), dout), nn(ds, query)
        if hi == seq:
            dv_ref[...] = dv
            dk_ref[...] = dk
        else:
            dv_ref[:hi, :] += dv
            dk_ref[:hi, :] += dk


def swap_halves(values):
    return pltpu.roll(values, LANES // 2, axis=1)


def tables(seq, head):
    freq = 10000.0 ** (-np.arange(0, head, 2, dtype=np.float64) / head)
    angle = np.arange(seq, dtype=np.float64)[:, None] * freq[None, :]
    cos, sin = np.cos(angle).astype(np.float32), np.sin(angle).astype(np.float32)
    return np.concatenate([cos] * 4, axis=1), np.concatenate([-sin, -sin, sin, sin], axis=1)


def norm_rows(values):
    mean = along(jnp.mean, values)
    centered = values - mean
    inv = lax.rsqrt(along(jnp.mean, centered * centered) + 1e-5)
    return centered * inv, inv


def norm_grad(grad, normed, inv):
    mean = along(jnp.mean, grad)
    proj = along(jnp.mean, grad * normed)
    return inv * (grad - mean - normed * proj)


def params(collective_id=None):
    return pltpu.CompilerParams(collective_id=collective_id, has_side_effects=collective_id is not None, vmem_limit_bytes=63 * MIB)


def dma(*shape):
    return pltpu.SemaphoreType.DMA(shape)


def shape(dtype, *dims):
    return jax.ShapeDtypeStruct(dims, dtype)


HBM = pl.BlockSpec(memory_space=pltpu.HBM)
WHOLE = pl.BlockSpec(memory_space=pltpu.VMEM)


def lanes(part):
    return slice(LANES * part, LANES * (part + 1))


def strips(width, size):
    return range(0, width, size)


def rows_of(size, width, index):
    return pl.BlockSpec((size, width), lambda step: (index(step), 0))


def fixed(block, index=(0, 0)):
    return pl.BlockSpec(block, lambda *grid: index, pipeline_mode=pl.Buffered(buffer_count=1))


def project_pair(n1_ref, weight, cos_ref, sin_ref, qkv_ref, keep_ref):
    for lo in strips(n1_ref.shape[0], QB):
        rows = slice(lo, lo + QB)
        raw = nn(n1_ref[rows, :], weight)
        keep_ref[rows, :] = (jnp.abs(raw) < CLIP).astype(F32).astype(BF16)
        raw = jnp.clip(raw, -CLIP, CLIP)
        for part in THREE:
            cols = lanes(part)
            tile = raw[:, cols]
            if part < 2:
                tile = tile * cos_ref[rows, :] + swap_halves(tile) * sin_ref[rows, :]
            if not part:
                tile = tile * 0.125
            qkv_ref[rows, cols] = tile.astype(BF16)


def swap_middle(tile):
    quarter = lax.broadcasted_iota(jnp.int32, tile.shape, 1) // (LANES // 4)
    up, down = pltpu.roll(tile, LANES // 4, axis=1), pltpu.roll(tile, LANES - LANES // 4, axis=1)
    return jnp.where(quarter == 1, down, jnp.where(quarter == 2, up, tile))


CHUNK = 256
CHUNK_STEPS = 4
FRONT_PLAN = '01456601452660124530,34,2345,,1,,45,,24,,,,3,,5,,,5'
SCATTER_PLAN = '00,,,,,11,,,20,,,,12,,,20,1,,20,12,10,2,102,,102'
LAST_PLAN = '00,,1,202,,31,3,,413,442,31,04,231,402,13,402,,1,403201342'


def aligned(at, size):
    return pl.ds(pl.multiple_of(at, size), size)


def to_partner(net, src, dst, send, recv):
    return pltpu.make_async_remote_copy(src, dst, send, recv, device_id=net.partner, device_id_type=MESH_ID)


def front_kernel(x_hbm, qkv_shard, out_shard, ff_shard, down_shard, cos_ref, sin_ref, qkv_ref, keep_ref, o_ref, lse_ref, h_hbm, n1_hbm, wq_hbm, wo_hbm, wf_hbm,
                 x_all, n1, w, shards, o_all, part, got, h_buf, wo, sems, gather_sems, load_sem, h_sem, *kept):
    step, last = pl.program_id(0), pl.num_programs(0) - 1
    turn = step - 1
    batch, pairs, seq = o_all.shape[:3]
    b, p = turn % batch, turn // batch
    half = CHUNK // 2
    chunks = seq // CHUNK
    ff = down_shard.shape[1]
    net = Torus()
    width = 3 * LANES
    heads_end, out_end = width * pairs, (width + LANES) * pairs
    places = [(w, cut_three(width, width * j), 0) for j in range(pairs)] + [
              (wo_hbm, cut_three(LANES * pairs), heads_end), (wf_hbm, cut_three(3 * ff), out_end)]
    gathers = [Gather(net, shards, out, cols, shift, gather_sems, i * Gather.SEMS, i < pairs) for i, (out, cols, shift) in enumerate(places)]
    strip = x_all.shape[0] // CHUNK_STEPS

    def load(i):
        return pltpu.make_async_copy(x_hbm.at[pl.ds(strip * i, strip)], x_all.at[pl.ds(strip * i, strip)], load_sem.at[i])

    def save(i):
        return pltpu.make_async_copy(n1.at[pl.ds(strip * i, strip)], n1_hbm.at[pl.ds(strip * i, strip)], load_sem.at[i])

    save_weight = pltpu.make_async_copy(w, wq_hbm, load_sem.at[CHUNK_STEPS])

    def normalize(i):
        load(i).wait()
        rows = slice(strip * i, strip * (i + 1))
        n1[rows, :] = norm_rows(x_all[rows, :].astype(F32))[0].astype(BF16)
        save(i).start()

    calls = plan(FRONT_PLAN, *([*g.stages()] for g in gathers), [functools.partial(normalize, i) for i in range(CHUNK_STEPS)])

    @pl.when(step == 0)
    def _():
        for i in range(CHUNK_STEPS):
            load(i).start()
        for j in range(pairs):
            for i in THREE:
                tile = qkv_shard[:, lanes(pairs * i + j)].astype(F32)
                shards[:, lanes(3 * j + i)] = (swap_middle(tile) if i < 2 else tile).astype(BF16)
        at = width * pairs
        shards[:, at:at + LANES * pairs] = out_shard[...]
        at += LANES * pairs
        for i in strips(ff, LANES):
            for j in TWO:
                shards[:, at + LANES * j:at + LANES * (j + 1)] = ff_shard[j, :, i:i + LANES]
            at += 2 * LANES
        shards[:, at:] = down_shard[...]
        net.barrier(net.neighbours(2) + [net.partner])
        for when, call in calls:
            if not when:
                call()

    begin, end = halves_of(calls, 1)
    run_at(turn, begin)

    @pl.when(turn >= 0)
    def _():
        weight = w[:, :, :, :, pl.ds(pl.multiple_of(width * p, LANES), width)].reshape(n1.shape[1], width)
        project_pair(n1.at[aligned(b * seq, seq)], weight, cos_ref, sin_ref, qkv_ref, keep_ref)
        q_ref, k_ref, v_ref = (qkv_ref.at[:, pl.ds(LANES * i, LANES)] for i in THREE)
        attend_pair(q_ref, k_ref, v_ref, o_ref, lse_ref.at[0, 0])
        o_all[b, p] = o_ref[...]

    run_at(turn, end)

    def rows_in(c, core):
        return aligned(c * CHUNK + core * half, half)

    def part_copy(b, c):
        return to_partner(net, part.at[b, rows_in(c, 1 - net.core)], got.at[b, c], *pair_of(sems, 0, b, c))

    def rows_out(b, c, core):
        return aligned(b * seq + c * CHUNK + core * half, half)

    def h_copy(b, c, core):
        return to_partner(net, h_buf.at[b, c], h_hbm.at[rows_out(b, c, core)], *pair_of(sems, 1, b, c))

    def h_local(b, c):
        return pltpu.make_async_copy(h_buf.at[b, c], h_hbm.at[rows_out(b, c, net.core)], h_sem.at[b, c])

    def project(b):
        o_full = jnp.concatenate([o_all[b, j] for j in range(pairs)], axis=1)
        weight = wo[...].reshape(part.shape[2], -1)
        for c in range(chunks):
            rows = slice(c * CHUNK, (c + 1) * CHUNK)
            part[b, rows, :] = nt(o_full[rows], weight)
            part_copy(b, c).start()

    def combine(b):
        for c in range(chunks):
            part_copy(b, c).wait()
            own = rows_in(c, net.core)
            h_buf[b, c] = (x_all[rows_out(b, c, net.core), :].astype(F32) + (part[b, own, :] + got[b, c])).astype(BF16)
            h_copy(b, c, net.core).start()
            h_local(b, c).start()

    def settle():
        for b in range(batch):
            for c in range(chunks):
                h_copy(b, c, net.core).wait_send()
                h_local(b, c).wait()
                h_copy(b, c, 1 - net.core).wait_recv()
        for i in range(CHUNK_STEPS):
            save(i).wait()
        save_weight.wait()

    fetch = pltpu.make_async_copy(wo_hbm, wo, h_sem.at[0, 0])

    def early():
        fetch.start()
        save_weight.start()

    def halfway():
        fetch.wait()
        project(0)

    def finish():
        combine(0)
        project(1)
        combine(1)
        settle()

    run_at(last - step, [(2, early), (1, halfway), (0, finish)])
    run_at(turn + 1, begin[-1:])


def front(x, qkv_shard, out_shard, ff_shard, down_shard, cos, sin, batch, seq, collective_id):
    pairs = out_shard.shape[1] // LANES
    rows, d = x.shape
    width = 3 * LANES
    chunks = seq // CHUNK
    vm = pltpu.VMEM
    torus = (SIDE, SIDE, SIDE, PIECE)
    shards = [s.size // PIECE for s in (qkv_shard, out_shard, ff_shard, down_shard)]
    turn = lambda s: jnp.maximum(s - 1, 0)
    head = lambda width: pl.BlockSpec((seq, width), lambda s: (turn(s) % batch, turn(s) // batch))
    return pl.pallas_call(
        front_kernel,
        grid=(1 + batch * pairs,),
        in_specs=[HBM] + [WHOLE] * 4 + [fixed(cos.shape)] * 2,
        out_specs=[head(width), head(width), head(LANES), pl.BlockSpec((1, 1, 2, seq), lambda s: (turn(s) % batch, turn(s) // batch, 0, 0))] + [HBM] * 5,
        out_shape=[shape(BF16, rows, width * pairs)] * 2 + [shape(BF16, rows, LANES * pairs), shape(F32, batch, pairs, 2, seq), shape(BF16, rows, d), shape(BF16, rows, d),
                   shape(BF16, *torus, shards[0]), shape(BF16, *torus, shards[1]), shape(BF16, *torus, shards[2] + shards[3])],
        scratch_shapes=[vm((rows, d), BF16), vm((rows, d), BF16), vm(torus + (width * pairs,), BF16), vm((PIECE, sum(shards)), BF16),
                        vm((batch, pairs, seq, LANES), BF16), vm((batch, seq, d), F32), vm((batch, chunks, CHUNK // 2, d), F32), vm((batch, chunks, CHUNK // 2, d), BF16),
                        vm(torus + (shards[1],), BF16), dma(2, 2, batch, chunks), dma(2, (pairs + 2) * Gather.SEMS), dma(CHUNK_STEPS + 1), dma(batch, chunks)],
        compiler_params=params(collective_id),
        name='front',
    )(x, qkv_shard, out_shard, ff_shard, down_shard, cos, sin)


class Exchange:
    def __init__(self, net, rows, partials, results, sems, local_sem):
        self.net, self.rows, self.partials, self.results, self.sems, self.local_sem = net, rows, partials, results, sems, local_sem

    def half(self, core, at=0):
        return aligned(at * self.rows + core * (self.rows // 2), self.rows // 2)

    def part(self, which, at):
        part, got = self.partials[which]
        return to_partner(self.net, part.at[at % 2, self.half(1 - self.net.core)], got.at[at], *pair_of(self.sems, which, at))

    def total(self, which, at):
        part, got = self.partials[which]
        self.part(which, at).wait()
        return part[at % 2, self.half(self.net.core), :] + got[at]

    def results_of(self, at, core, act):
        for i, (buf, hbm) in enumerate(self.results):
            act(buf.at[at % 2], hbm.at[self.half(core, at)], pair_of(self.sems, len(self.partials) + i, at), self.local_sem.at[i, at % 2])

    def publish(self, at):
        def act(buf, rows, sem, local_sem):
            to_partner(self.net, buf, rows, *sem).start()
            pltpu.make_async_copy(buf, rows, local_sem).start()
        self.results_of(at, self.net.core, act)

    def settle(self, at):
        def act(buf, rows, sem, local_sem):
            to_partner(self.net, buf, rows, *sem).wait_send()
            pltpu.make_async_copy(buf, rows, local_sem).wait()
        self.results_of(at, self.net.core, act)
        self.results_of(at, 1 - self.net.core, lambda buf, rows, sem, local_sem: to_partner(self.net, buf, rows, *sem).wait_recv())


def mlp_kernel(blocks, h_ref, gy_ref, wff_ref, wd_ref, y_hbm, gh_hbm, gh32_ref, acts_hbm, n2_ref, gd_hbm,
               saved, grad_down, part_y, part_g, got_y, got_g, y_buf, gh_buf, h_own, gy_own, sems, local_sem, save_sem):
    step = pl.program_id(0)
    rows, d = h_ref.shape
    ff = wd_ref.shape[1]
    acts = saved.at[step % 2]
    gug, act = acts.at[:, pl.ds(0, 2 * ff)], acts.at[:, pl.ds(2 * ff, ff)]

    def save(at):
        return pltpu.make_async_copy(saved.at[at % 2], acts_hbm.at[aligned(at * rows, rows)], save_sem.at[at % 2])

    save_grad = pltpu.make_async_copy(grad_down, gd_hbm, save_sem.at[2])
    net = Torus()
    swap = Exchange(net, rows, ((part_y, got_y), (part_g, got_g)), ((y_buf, y_hbm), (gh_buf, gh_hbm)), sems, local_sem)

    @pl.when(step == 0)
    def _():
        net.barrier([net.partner])

    @pl.when((step > 1) & (step < blocks))
    def _():
        save(step - 2).wait()

    @pl.when(step < blocks)
    def _():
        n2, _ = norm_rows(h_ref[...].astype(F32))
        n2 = n2.astype(BF16)
        n2_ref[...] = n2
        gy = gy_ref[...]
        for j in strips(ff, QB):
            w = min(QB, ff - j)
            gact = nn(gy, wd_ref[:, j:j + w])
            for i in range(j, j + w, LANES):
                at, mid, end = 2 * i, 2 * i + LANES, 2 * i + QB
                ug = nn(n2, wff_ref[:, at:end])
                up, gate = ug[:, :LANES], ug[:, LANES:]
                sig = 1.0 / (1.0 + jnp.exp(-gate))
                silu = gate * sig
                act[:, i:i + LANES] = (silu * up).astype(BF16)
                ga = gact[:, i - j:i - j + LANES]
                gug[:, at:mid] = (ga * silu).astype(BF16)
                gug[:, mid:end] = (ga * up * sig * (1.0 + gate * (1.0 - sig))).astype(BF16)

        for which, left, right, part in ((0, act, wd_ref, part_y), (1, gug, wff_ref, part_g)):
            for j in strips(d, QB):
                part[step % 2, :, j:j + QB] = nt(left[...], right[j:j + QB, :])
            swap.part(which, step).start()
        save(step).start()
        accumulate(grad_down, 0, step == 0, gy, act)

    @pl.when(step == blocks - 1)
    def _():
        save_grad.start()

    @pl.when(step > 2)
    def _():
        swap.settle(step - 3)

    @pl.when(step > 0)
    def _():
        done = step - 1
        hidden = h_own[...].astype(F32)
        normed, inv = norm_rows(hidden)
        y_buf[done % 2] = (hidden + swap.total(0, done)).astype(BF16)
        gh = gy_own[...].astype(F32) + norm_grad(swap.total(1, done), normed, inv)
        gh32_ref[...] = gh
        gh_buf[done % 2] = gh.astype(BF16)
        swap.publish(done)

    own = swap.half(net.core)
    h_own[...] = h_ref[own, :]
    gy_own[...] = gy_ref[own, :]

    @pl.when(step == blocks)
    def _():
        for at in (blocks - 2, blocks - 1):
            swap.settle(at)
            save(at).wait()
        save_grad.wait()


def mlp(h, gy, weights, collective_id, block=512):
    rows, d = h.shape
    ff = weights.shape[1] // 3
    half = block // 2
    blocks = rows // block
    torus = (SIDE, SIDE, SIDE, PIECE)
    row = lambda width: rows_of(block, width, lambda i: jnp.minimum(i, blocks - 1))
    vm = pltpu.VMEM
    return pl.pallas_call(
        functools.partial(mlp_kernel, blocks),
        grid=(blocks + 1,),
        in_specs=[row(d), row(d), fixed((d, 2 * ff)), fixed((d, ff), (0, 2))],
        out_specs=[HBM, HBM, rows_of(half, d, lambda i: jnp.maximum(i - 1, 0)), HBM, row(d), HBM],
        out_shape=[shape(BF16, rows, d), shape(BF16, rows, d), shape(F32, rows // 2, d), shape(BF16, rows, 3 * ff), shape(BF16, rows, d), shape(F32, *torus, ff)],
        scratch_shapes=[vm((2, block, 3 * ff), BF16), vm(torus + (ff,), F32)] + [vm((2, block, d), F32)] * 2 + [vm((blocks, half, d), F32)] * 2 + [vm((2, half, d), BF16)] * 2 + [vm((half, d), BF16)] * 2 + [dma(2, 4, blocks), dma(2, 2), dma(3)],
        compiler_params=params(collective_id),
        name='mlp',
    )(h, gy, weights, weights)


def accumulate(part, cols, first, left, right):
    for j in strips(right.shape[1], QB):
        w = min(QB, right.shape[1] - j)
        prod = tn(left, right[:, j:j + w]).reshape(part.shape[:-1] + (w,))
        at = slice(cols + j, cols + j + w)
        part[..., at] = jnp.where(first, 0.0, part[..., at]) + prod


SETS = 3
HEAD_STEP = (SETS - 1) * CHUNK_STEPS


def back_kernel(pairs, gd_hbm, n2_ref, act_ref, qkv_ref, lse_ref, gh_ref, wo_ref, o_ref, keep_ref, cos_ref, sin_ref,
                g_ref, gw_ref, gd_ref, gff_ref, do_ref, dk_ref, dv_ref, parts, sems, load_sem, *bufs):
    step = pl.program_id(0)
    turn = step - HEAD_STEP
    p = turn % pairs
    net = Torus()
    per = len(bufs) // SETS
    scatters = [Scatter(net, parts.at[i], cut_three(parts.shape[-1], 0, i), bufs[per * i:per * i + per], sems, i * Scatter.SEMS) for i in range(SETS)]
    calls = plan(SCATTER_PLAN, *(s.stages() for s in scatters))
    begin, end = halves_of(calls, HEAD_STEP + 1)

    @pl.when(step == 0)
    def _():
        load = pltpu.make_async_copy(gd_hbm, parts.at[0], load_sem.at[0])
        load.start()
        net.barrier(net.neighbours())
        load.wait()
        for when, call in calls:
            if not when:
                call()

    @pl.when(turn < 0)
    def _():
        accumulate(parts.at[1 + step // CHUNK_STEPS], 0, step % CHUNK_STEPS == 0, n2_ref[...], act_ref)

    run_at(step + 1, [c for c in calls if 0 < c[0] <= HEAD_STEP])

    def put(part, lo, hi, values):
        cols = lanes(part)
        if part < 2:
            values = values * cos_ref[lo:hi, :] - swap_halves(values) * sin_ref[lo:hi, :]
        g_ref[lo:hi, cols] = (values * keep_ref[lo:hi, cols].astype(F32)).astype(BF16)

    def put_dq(lo, hi, dq):
        put(0, lo, hi, dq * 0.125)

    @pl.when(turn >= 0)
    def _():
        @pl.when(p == 0)
        def _():
            gh = gh_ref[...]
            dout = nn(gh, wo_ref[...]).astype(BF16)
            for j in range(pairs):
                do_ref[j] = dout[:, lanes(j)]
            gw_ref[...] = jnp.where(turn == 0, 0.0, gw_ref[...]) + tn(gh, o_ref[...])

        run_at(turn, begin)
        q_ref, k_ref, v_ref = (qkv_ref.at[:, pl.ds(LANES * i, LANES)] for i in THREE)
        attend_pair_back(q_ref, k_ref, v_ref, do_ref.at[p], lse_ref.at[0, 0], dk_ref, dv_ref, put_dq)
        seq = q_ref.shape[0]
        put(1, 0, seq, dk_ref[...])
        put(2, 0, seq, dv_ref[...])
        run_at(turn, end)

    @pl.when(step == pl.num_programs(0) - 1)
    def _():
        gd_ref[...], *halves = [s.result() for s in scatters]
        tiles = jnp.concatenate(halves, axis=1)
        for i in strips(tiles.shape[1], LANES):
            at = i // QB * LANES
            gff_ref[i // LANES % 2, :, at:at + LANES] = tiles[:, i:i + LANES]


def back(gd, n2, acts, qkv, lse, gh, wo_t, o, keep, cos, sin, batch, seq, pairs, collective_id):
    rows, d = n2.shape
    ff = acts.shape[1] // SETS
    block = rows // CHUNK_STEPS
    turn = lambda s: jnp.maximum(s - HEAD_STEP, 0)
    head = pl.BlockSpec((seq, 3 * LANES), lambda s: (turn(s) // pairs, turn(s) % pairs))
    late = lambda s: jnp.where(s < HEAD_STEP, s % CHUNK_STEPS, CHUNK_STEPS - 1)
    vm = pltpu.VMEM
    per_seq = lambda width: rows_of(seq, width, lambda s: turn(s) // pairs)
    return pl.pallas_call(
        functools.partial(back_kernel, pairs),
        grid=(HEAD_STEP + batch * pairs,),
        in_specs=[HBM, rows_of(block, d, late), pl.BlockSpec((block, ff), lambda s: (late(s), jnp.minimum(s // CHUNK_STEPS, 1))), head, pl.BlockSpec((1, 1, 2, seq), lambda s: (turn(s) // pairs, turn(s) % pairs, 0, 0)),
                  per_seq(d), fixed(wo_t.shape), per_seq(LANES * pairs), head, fixed(cos.shape), fixed(sin.shape)],
        out_specs=[head, fixed(wo_t.shape), fixed((PIECE, ff)), fixed((2, PIECE, ff), (0, 0, 0))],
        out_shape=[shape(BF16, *qkv.shape), shape(F32, *wo_t.shape), shape(F32, PIECE, ff), shape(F32, 2, PIECE, ff)],
        scratch_shapes=[vm((pairs, seq, LANES), BF16), vm((seq, LANES), F32), vm((seq, LANES), F32), vm((SETS, SIDE, SIDE, SIDE, PIECE, ff), F32),
                        dma(2, SETS * Scatter.SEMS), dma(1)] + [s for i in range(SETS) for s in Scatter.scratch(cut_three(ff, 0, i))],
        compiler_params=params(collective_id),
        name='back',
    )(gd, n2, acts, qkv, lse, gh, wo_t, o, keep, cos, sin)


def last_kernel(pairs, blocks, n1_ref, g_ref, x_ref, g_row, gh_ref, w_ref, gout_hbm, gx_hbm, gout_ref, gw_ref,
                part_out, part_qkv, part, got, buf, sems, scatter_sems, local_sem, *bufs):
    step = pl.program_id(0)
    turn = step - pairs
    rows, d = x_ref.shape
    net = Torus()
    per = len(bufs) // (pairs + 1)
    parts = [part_out] + [part_qkv.at[j] for j in range(pairs)]
    scatters = [Scatter(net, s, cut_three(s.shape[-1], 0, i), bufs[per * i:per * i + per], scatter_sems, i * Scatter.SEMS) for i, s in enumerate(parts)]
    calls = plan(LAST_PLAN, *(s.stages() for s in scatters))
    swap = Exchange(net, rows, ((part, got),), ((buf, gx_hbm),), sems, local_sem)

    @pl.when(step == 0)
    def _():
        load = pltpu.make_async_copy(gout_hbm, part_out, local_sem.at[1, 0])
        load.start()
        net.barrier(net.neighbours() + [net.partner])
        load.wait()

    begin, end = halves_of(calls)
    run_at(step, begin)

    @pl.when(turn < 0)
    def _():
        accumulate(part_qkv.at[step], 0, True, n1_ref[...], g_ref)

    @pl.when((turn >= 0) & (turn < blocks))
    def _():
        for j in strips(d, QB):
            part[turn % 2, :, j:j + QB] = nt(g_row[...], w_ref[j:j + QB, :])
        swap.part(0, turn).start()

    run_at(step, end)

    @pl.when(turn > 2)
    def _():
        swap.settle(turn - 3)

    @pl.when(turn > 0)
    def _():
        done = turn - 1
        normed, inv = norm_rows(x_ref[swap.half(net.core), :].astype(F32))
        buf[done % 2] = (gh_ref[...] + norm_grad(swap.total(0, done), normed, inv)).astype(BF16)
        swap.publish(done)

    @pl.when(turn == blocks)
    def _():
        for when, call in calls:
            if when > 2 * (pairs + blocks) + 1:
                call()
        for at in (blocks - 2, blocks - 1):
            swap.settle(at)
        gout_ref[...] = scatters[0].result()
        for j, s in enumerate(scatters[1:]):
            sums = s.result()
            for i in THREE:
                tile = sums[:, lanes(i)]
                gw_ref[:, lanes(pairs * i + j)] = swap_middle(tile) if i < 2 else tile


def last(x, n1, g, gh32, w, gout, pairs, collective_id, block=512):
    rows, d = x.shape
    blocks = rows // block
    late = lambda n, width, by: rows_of(n, width, lambda s: jnp.clip(s - pairs - by, 0, blocks - 1))
    head = pl.BlockSpec((rows, 3 * LANES), lambda s: (0, jnp.minimum(s, pairs - 1)))
    vm = pltpu.VMEM
    half = block // 2
    torus = (SIDE, SIDE, SIDE, PIECE)
    gout = gout.reshape(torus + (-1,))
    return pl.pallas_call(
        functools.partial(last_kernel, pairs, blocks),
        grid=(pairs + blocks + 1,),
        in_specs=[fixed((rows, d)), head, late(block, d, 1), late(block, g.shape[1], 0), late(half, d, 1), fixed(w.shape), HBM],
        out_specs=[HBM, WHOLE, WHOLE],
        out_shape=[shape(BF16, rows, d), shape(F32, PIECE, gout.shape[-1]), shape(F32, PIECE, w.shape[1])],
        scratch_shapes=[vm(gout.shape, F32), vm((pairs,) + torus + (3 * LANES,), F32), vm((2, block, d), F32), vm((blocks, half, d), F32), vm((2, half, d), BF16),
                        dma(2, 2, blocks), dma(2, (pairs + 1) * Scatter.SEMS), dma(2, 2)] + Scatter.scratch(cut_three(gout.shape[-1])) + Scatter.scratch(cut_three(3 * LANES)) * pairs,
        compiler_params=params(collective_id),
        name='last',
    )(n1, g, x, g, gh32, w, gout)


def device_step(x, grad_y, w_qkv, w_out, w_ff, w_down):
    batch, seq, d = x.shape
    heads, head = w_qkv.shape[2:]
    pairs = heads // 2
    cos, sin = (jnp.asarray(t) for t in tables(seq, head))
    ids = iter(range(4))
    x2, gy = (v.reshape(batch * seq, d) for v in (x, grad_y))
    turned = lambda w: w.swapaxes(0, 1)
    shards = (w_qkv.reshape(PIECE, w_qkv.size // PIECE), w_out.reshape(heads * head, PIECE).T, turned(w_ff), w_down.T)
    qkv, keep, o, lse, h, n1, *weights = front(x2, *shards, cos, sin, batch, seq, next(ids))
    wq, wo_t, wf = (w.reshape(d, w.shape[-1]) for w in weights)
    y, gh, gh32, acts, n2, gd = mlp(h, gy, wf, next(ids))
    g, gout, gd, gff = back(gd, n2, acts, qkv, lse, gh, wo_t, o, keep, cos, sin, batch, seq, pairs, next(ids))
    gx, gout, gqkv = last(x2, n1, g, gh32, wq, gout, pairs, next(ids))
    return y.reshape(x.shape), gx.reshape(x.shape), gqkv.reshape(w_qkv.shape), gout.T.reshape(w_out.shape), turned(gff), gd.T


def solution(mesh):
    specs = (P('fsdp'), P('fsdp'), P('fsdp', None, 'tp'), P('tp', None, 'fsdp'), P('fsdp', None, 'tp'), P('tp', 'fsdp'))
    return jax.shard_map(device_step, mesh=mesh, in_specs=specs, out_specs=specs, check_vma=False)
```

```python
import functools

import jax
import jax.numpy as jnp
import numpy as np
from jax import lax
from jax.experimental import pallas as pl
from jax.experimental.pallas import tpu as pltpu
from jax.sharding import PartitionSpec as P

MESH_ID = pl.DeviceIdType.MESH
SIDE = 4
PIECE = 16
ORDERS = ((2, 1, 0), (1, 0, 2), (0, 2, 1))
BOTH = ((0, 1), (1, -1))
PHASES = THREE = range(3)
TWO = range(2)


class Torus:
    def __init__(self):
        self.core = lax.axis_index('tp')
        self.index = lax.axis_index('fsdp')
        plane, x = lax.div(self.index, SIDE), lax.rem(self.index, SIDE)
        self.at = (lax.div(plane, SIDE), lax.rem(plane, SIDE), x)
        self.partner = (1 - self.core, self.index)
        self.moved = {(axis, by): lax.rem(at + (by + SIDE), SIDE) for axis, at in enumerate(self.at) for by in range(-2, 3)}
        self.peers = {(axis, by): self.place(axis, self.moved[axis, by]) for axis in THREE for by in (-1, 1, 2)}

    def place(self, axis, coord):
        pos = list(self.at)
        pos[axis] = coord
        z, y, x = pos
        return (self.core, (z * SIDE + y) * SIDE + x)

    def shift(self, axis, by):
        return self.moved[axis, by]

    def peer(self, axis, by):
        return self.peers[axis, by]

    def neighbours(self, reach=1):
        return [device for (_, by), device in self.peers.items() if by <= reach]

    def tell(self, sem, devices):
        for device in devices:
            pl.semaphore_signal(sem, inc=1, device_id=device, device_id_type=MESH_ID)

    def barrier(self, devices):
        sem = pltpu.get_barrier_semaphore()
        self.tell(sem, devices)
        pl.semaphore_wait(sem, len(devices))


def pair_of(sems, *at):
    return sems.at[(0,) + at], sems.at[(1,) + at]


def in_order(*calls):
    def run():
        for call in calls:
            call()
    return run


def span(cols):
    (off, width), *rest = cols
    return pl.ds(off, width + sum(w for _, w in rest))


class Gather:
    SEMS = 7

    def __init__(self, net, shard, out, cols, shift, sems, first, direct=False):
        self.net, self.shard, self.out, self.cols, self.moved, self.sems, self.first, self.direct = net, shard, out, cols, shift, sems, first, direct

    def block(self, colour, phase, coord, half=None):
        order = ORDERS[colour]
        off, width = self.cols[colour]
        pick = list(self.net.at)
        for axis in order[:phase]:
            pick[axis] = pl.ds(0, SIDE)
        pick[order[phase]] = coord
        if half is not None and phase:
            pick[order[0]] = pl.ds(half * 2, 2)
        elif half is not None:
            cut = width - width // 256 * 128
            off, width = (off + cut, width - cut) if half else (off, cut)
        return self.out.at[(*pick, slice(None), pl.ds(off, width))] if width else None

    def copy(self, phase, colour, relay, d, by):
        axis = ORDERS[colour][phase]
        far = relay and self.direct
        if far and d:
            return None
        by = 2 if far else by
        back = -by if relay and not far else 0
        dst = src = self.block(colour, phase, self.net.shift(axis, back), d if relay and not far else None)
        if dst is None:
            return None
        if not phase and (far or not relay):
            off, width = self.cols[colour]
            src = self.shard.at[:, pl.ds(off + self.moved, width)]
        return pltpu.make_async_remote_copy(src, dst, *self.sem(phase, relay), device_id=self.net.peer(axis, by), device_id_type=MESH_ID)

    def sem(self, phase, relay):
        return pair_of(self.sems, self.first + 2 * phase + relay)

    def each(self, phase, relay):
        for d, by in BOTH:
            for colour in THREE:
                desc = self.copy(phase, colour, relay, d, by)
                if desc is not None:
                    desc.start()

    def wait(self, phase, relay, side):
        pick = [pl.ds(0, SIDE)] * phase + [pl.ds(0, 2 - relay)] + [0, 0]
        ref = self.out.at[tuple(reversed(pick[:3])) + (slice(None), span(self.cols))]
        pltpu.make_async_copy(ref, ref, self.sem(phase, relay)[side]).wait()

    def own(self):
        at = self.net.at
        cols = span(self.cols)
        src = self.shard.at[:, pl.ds(cols.start + self.moved, cols.size)]
        return pltpu.make_async_copy(src, self.out.at[(*at, slice(None), cols)], self.sems.at[0, self.first + self.SEMS - 1])

    def arrive(self, phase):
        if self.direct:
            self.wait(phase, 0, 1)
        self.wait(phase, 1, 1)

    def start(self, phase):
        if phase:
            self.arrive(phase - 1)
        if phase == 1:
            self.own().wait()
        for relay in range(1 + self.direct):
            self.each(phase, relay)
        if not phase:
            self.own().start()

    def relay(self, phase):
        self.wait(phase, 0, 1)
        self.each(phase, 1)

    def finish(self):
        self.arrive(PHASES[-1])
        for phase in PHASES:
            for relay in TWO:
                self.wait(phase, relay, 0)

    def stages(self):
        steps = (self.start,) if self.direct else (self.start, self.relay)
        return [functools.partial(f, p) for p in PHASES for f in steps] + [self.finish]


class Scatter:
    SEMS = 9

    def __init__(self, net, part, cols, bufs, sems, first):
        self.net, self.part, self.cols, self.bufs, self.sems, self.first = net, part, cols, bufs, sems, first

    @staticmethod
    def scratch(cols):
        shapes = []
        for _, w in cols:
            shapes += [(3, 2, 2, SIDE, PIECE, w), (3, 2, 2, PIECE, w), (3, 2, PIECE // 2, w)]
        return [pltpu.VMEM(s, jnp.float32) for s in shapes]

    def buf(self, colour, phase):
        return self.bufs[colour * len(PHASES) + phase]

    def block(self, colour, phase, coord, half):
        order = ORDERS[colour]
        off, width = self.cols[colour]
        pick = [pl.ds(0, SIDE)] * 3
        for axis in order[:phase]:
            pick[axis] = self.net.at[axis]
        pick[order[phase]] = coord
        rows = pl.ds(0, PIECE)
        rest = sorted(order[phase + 1:])
        if rest:
            pick[rest[0]] = pl.ds(2 * half, 2)
        else:
            rows = pl.ds(PIECE // 2 * half, PIECE // 2)
        return self.part.at[(*pick, rows, pl.ds(off, width))]

    def copy(self, phase, colour, kind, d, by):
        axis = ORDERS[colour][phase]
        buf = self.buf(colour, phase)
        if kind == 2:
            src = buf.at[0, d]
        elif kind:
            src = self.block(colour, phase, self.net.shift(axis, by), 1 - d)
        else:
            src = self.block(colour, phase, self.net.shift(axis, 2), d)
        return pltpu.make_async_remote_copy(src, buf.at[kind, d], *self.sem(phase, kind), device_id=self.net.peer(axis, by), device_id_type=MESH_ID)

    def sem(self, phase, kind):
        return pair_of(self.sems, self.first + len(PHASES) * phase + kind)

    def wait(self, phase, kind, side):
        pick = [0] * (phase + 1) + [pl.ds(0, SIDE)] * (2 - phase)
        ref = self.part.at[tuple(pick) + (slice(None), span(self.cols))]
        pltpu.make_async_copy(ref, ref, self.sem(phase, kind)[side]).wait()

    def start(self, phase, kind):
        for d, by in BOTH:
            for colour in THREE:
                self.copy(phase, colour, kind, d, by).start()

    def relay(self, phase):
        self.wait(phase, 0, 1)
        for colour in THREE:
            buf = self.buf(colour, phase)
            for d, by in BOTH:
                buf[0, d] = buf[0, d] + self.block(colour, phase, self.net.shift(ORDERS[colour][phase], by), d)[...]
        self.start(phase, 2)

    def merge(self, phase):
        for kind in (1, 2):
            self.wait(phase, kind, 1)
        for colour in THREE:
            buf = self.buf(colour, phase)
            for half in TWO:
                mine = self.block(colour, phase, self.net.at[ORDERS[colour][phase]], half)
                mine[...] = mine[...] + buf[1, 1 - half] + buf[2, half]
        if phase + 1 < len(PHASES):
            for kind in TWO:
                self.start(phase + 1, kind)

    def finish(self):
        for phase in PHASES:
            for kind in PHASES:
                self.wait(phase, kind, 0)

    def stages(self):
        calls = [functools.partial(self.start, 0, kind) for kind in TWO]
        for phase in PHASES:
            calls += [functools.partial(self.relay, phase), functools.partial(self.merge, phase)]
        return calls[:-1] + [in_order(calls[-1], self.finish)]

    def result(self):
        return self.part[self.net.at]


def cut_three(width, off=0, turn=0):
    tiles = width // 128
    sizes = [(tiles + (2 + turn - i) % 3) // 3 * 128 for i in THREE]
    return [(off + sum(sizes[:i]), s) for i, s in enumerate(sizes)]


def plan(text, *sets):
    left = [iter(s) for s in sets]
    return [(hook, next(left[int(which)])) for hook, field in enumerate(text.split(',')) for which in field]


def halves_of(calls, first=0):
    return [[((when - first) // 2, call) for when, call in calls if when >= first and (when - first) % 2 == odd] for odd in TWO]


def run_at(hook, calls):
    for when, call in calls:
        pl.when(hook == when)(call)


F32, BF16 = jnp.float32, jnp.bfloat16
QB = 256
LANES = 128
HALF = LANES // 2
CLIP = 8.0
MIB = 2**20


def nt(a, b):
    return lax.dot_general(a, b, (((1,), (1,)), ((), ())), preferred_element_type=F32)


def nn(a, b):
    return jnp.dot(a, b, preferred_element_type=F32)


def tn(a, b):
    return lax.dot_general(a, b, (((0,), (0,)), ((), ())), preferred_element_type=F32)


def along(reduce, values):
    return reduce(values, axis=-1, keepdims=True)


def head_masks(paired):
    lane = lax.broadcasted_iota(jnp.int32, (1, LANES), 1)
    first = lane % HALF < HALF // 2 if paired else lane < HALF
    return first, jnp.logical_not(first)


def causal_tile(key_axis):
    dims = (QB, 2 * QB) if key_axis == 0 else (2 * QB, QB)
    return lax.broadcasted_iota(jnp.int32, dims, key_axis) <= lax.broadcasted_iota(jnp.int32, dims, 1 - key_axis) % QB


def by_head(values, masks):
    return jnp.concatenate([jnp.where(m, values, jnp.zeros((), BF16)) for m in masks], axis=0)


def attend_pair(q_ref, k_ref, v_ref, o_ref, lse_ref):
    masks = head_masks(True)
    key, val = k_ref[...], v_ref[...]
    causal = causal_tile(1)
    first = head_masks(False)[0]
    for lo in reversed(strips(q_ref.shape[0], QB)):
        hi = lo + QB
        query = by_head(q_ref[lo:hi, :], masks)
        diag = jnp.where(causal, nt(query, key[lo:hi]), -1e30)
        top = along(jnp.max, diag)
        if lo:
            past = nt(query, key[:lo])
            top = jnp.maximum(top, along(jnp.max, past))
            past = jnp.exp(past - top)
        diag = jnp.exp(diag - top)
        total = along(jnp.sum, diag)
        if lo:
            total = total + along(jnp.sum, past)
        scale = 1.0 / total
        acc = nn((diag * scale).astype(BF16), val[lo:hi])
        if lo:
            acc = acc + nn((past * scale).astype(BF16), val[:lo])
        o_ref[lo:hi, :] = jnp.where(first, acc[:QB], acc[QB:]).astype(BF16)
        lse = jnp.broadcast_to(top + jnp.log(total), acc.shape).T
        for h in TWO:
            lse_ref[h:h + 1, lo:hi] = lse[:1, h * QB:(h + 1) * QB]


def attend_pair_back(q_ref, k_ref, v_ref, do_ref, lse_ref, dk_ref, dv_ref, put_dq):
    seq = q_ref.shape[0]
    qmask, vmask = head_masks(True), head_masks(False)
    key, val = k_ref[...], v_ref[...]
    key_t = key.astype(F32).T.astype(BF16)
    causal = causal_tile(0)
    first = lax.broadcasted_iota(jnp.int32, (LANES, 1), 0) % HALF < HALF // 2

    def products(lo):
        hi = lo + QB
        query, dout = by_head(q_ref[lo:hi, :], qmask), by_head(do_ref[lo:hi, :], vmask)
        return query, dout, nt(key[:hi], query), nt(val[:hi], dout)

    ahead = products(seq - QB)
    for lo in reversed(strips(seq, QB)):
        hi = lo + QB
        query, dout, score, grad = ahead
        if lo:
            ahead = products(lo - QB)
        prob = jnp.exp(score - jnp.concatenate([lse_ref[h:h + 1, lo:hi] for h in TWO], axis=1))
        diag = jnp.where(causal, prob[lo:], 0.0)
        prob = jnp.concatenate([prob[:lo], diag], axis=0) if lo else diag
        ds = (prob * (grad - jnp.sum(prob * grad, axis=0, keepdims=True))).astype(BF16)
        both = nn(key_t[:, :hi], ds)
        put_dq(lo, hi, jnp.where(first, both[:, :QB], both[:, QB:]).T)
        dv, dk = nn(prob.astype(BF16), dout), nn(ds, query)
        if hi == seq:
            dv_ref[...] = dv
            dk_ref[...] = dk
        else:
            dv_ref[:hi, :] += dv
            dk_ref[:hi, :] += dk


def swap_halves(values):
    return pltpu.roll(values, HALF, axis=1)


COARSE = 32


def tables(seq, head):
    freq = 10000.0 ** (-np.arange(0, head, 2, dtype=np.float64) / head)
    angles = [np.tile(np.arange(seq // COARSE)[:, None] * step * freq, LANES // len(freq)) for step in (1, COARSE)]
    return np.stack([np.stack([np.cos(angle), np.sin(angle)]) for angle in angles]).astype(np.float32)


def spread_tables(table_ref, cos_ref, sin_ref):
    fine_cos, fine_sin = table_ref[0]
    sign = jnp.where(lax.broadcasted_iota(jnp.int32, (1, LANES), 1) < HALF, -1.0, 1.0)

    def body(i):
        rows = aligned(i * COARSE, COARSE)
        cos, sin = table_ref[1, :, pl.ds(i, 1), :]
        cos_ref[rows, :] = fine_cos * cos - fine_sin * sin
        sin_ref[rows, :] = (fine_sin * cos + fine_cos * sin) * sign

    repeat(cos_ref.shape[0] // COARSE, body)


def repeat(count, body):
    def step(i, carry):
        body(i)
        return carry

    lax.fori_loop(0, count, step, 0)


def side_by_side(halves, j):
    return jnp.concatenate([halves[2 * j], halves[2 * j + 1]], axis=1)


def aligned(at, size):
    return pl.ds(pl.multiple_of(at, size), size)


def norm_rows(values):
    mean = along(jnp.mean, values)
    centered = values - mean
    inv = lax.rsqrt(along(jnp.mean, centered * centered) + 1e-5)
    return centered * inv, inv


def norm_grad(grad, normed, inv):
    mean = along(jnp.mean, grad)
    proj = along(jnp.mean, grad * normed)
    return inv * (grad - mean - normed * proj)


def params(collective_id, limit=63):
    return pltpu.CompilerParams(collective_id=collective_id, has_side_effects=True, vmem_limit_bytes=limit * MIB)


def grid_step():
    return pl.program_id(0), pl.num_programs(0) - 1


def dma(*shape):
    return pltpu.SemaphoreType.DMA(shape)


def shape(dtype, *dims):
    return jax.ShapeDtypeStruct(dims, dtype)


HBM = pl.BlockSpec(memory_space=pltpu.HBM)
WHOLE = pl.BlockSpec(memory_space=pltpu.VMEM)


def lanes(part):
    return slice(LANES * part, LANES * (part + 1))


def strips(width, size):
    return range(0, width, size)


def rows_of(size, width, index):
    return pl.BlockSpec((size, width), lambda step: (index(step), 0))


def fixed(block, index=(0, 0)):
    return pl.BlockSpec(block, lambda *grid: index, pipeline_mode=pl.Buffered(buffer_count=1))


def project_pair(n1_ref, weight, cos_ref, sin_ref, qkv_ref, keep_ref):
    for lo in strips(n1_ref.shape[0], QB):
        rows = slice(lo, lo + QB)
        raw = nn(n1_ref[rows, :], weight)
        keep_ref[rows, :] = (jnp.abs(raw) < CLIP).astype(F32).astype(BF16)
        raw = jnp.clip(raw, -CLIP, CLIP)
        for part in THREE:
            cols = lanes(part)
            tile = raw[:, cols]
            if part < 2:
                tile = tile * cos_ref[rows, :] + swap_halves(tile) * sin_ref[rows, :]
            if not part:
                tile = tile * 0.125
            qkv_ref[rows, cols] = tile.astype(BF16)


def swap_middle(tile):
    quarter = lax.broadcasted_iota(jnp.int32, tile.shape, 1) // (LANES // 4)
    up, down = pltpu.roll(tile, LANES // 4, axis=1), pltpu.roll(tile, LANES - LANES // 4, axis=1)
    return jnp.where(quarter == 1, down, jnp.where(quarter == 2, up, tile))


CHUNK = 256
CHUNK_STEPS = 4
FRONT_PLAN = '014560145260124530,4,245,,13,,345,,2,,4,,3,,5,,,5'
SCATTER_PLAN = '00,,,,,11,,,20,,,,12,,,20,1,,20,12,10,2,102,,102'
LAST_PLAN = '00,,1,202,,31,3,,413,442,31,04,231,402,13,402,,1,403201342'


def to_partner(net, src, dst, send, recv):
    return pltpu.make_async_remote_copy(src, dst, send, recv, device_id=net.partner, device_id_type=MESH_ID)


def front_kernel(x_hbm, qkv_shard, out_shard, ff_shard, down_shard, table_ref, qkv_ref, keep_ref, o_ref, lse_ref, h_hbm, n1_hbm, wq_hbm, wo_hbm, wf_hbm,
                 x_all, n1, w, shards, o_all, part, got, h_buf, wo, sems, gather_sems, load_sem, h_sem, cos_ref, sin_ref, o_buf):
    step, last = grid_step()
    turn = step - 1
    batch, pairs, seq = o_all.shape[:3]
    b, p = turn % batch, turn // batch
    half = CHUNK // 2
    chunks = seq // CHUNK
    ff = down_shard.shape[1]
    net = Torus()
    width = 3 * LANES
    heads_end, out_end = width * pairs, (width + LANES) * pairs
    places = [(w, cut_three(width, width * j), 0) for j in range(pairs)] + [
              (wo_hbm, cut_three(LANES * pairs), heads_end), (wf_hbm, cut_three(3 * ff), out_end)]
    gathers = [Gather(net, shards, out, cols, shift, gather_sems, i * Gather.SEMS, i < pairs) for i, (out, cols, shift) in enumerate(places)]
    strip = x_all.shape[0] // CHUNK_STEPS

    def rows_at(i):
        return aligned(i * strip, strip)

    def load(i):
        return pltpu.make_async_copy(x_hbm.at[rows_at(i)], x_all.at[rows_at(i)], load_sem.at[i])

    def save(i):
        return pltpu.make_async_copy(n1.at[rows_at(i)], n1_hbm.at[rows_at(i)], load_sem.at[i])

    save_weight = pltpu.make_async_copy(w, wq_hbm, load_sem.at[CHUNK_STEPS])

    def normalize(i):
        load(i).wait()
        n1[rows_at(i), :] = norm_rows(x_all[rows_at(i), :].astype(F32))[0].astype(BF16)
        save(i).start()

    def normalize_half(first):
        repeat(CHUNK_STEPS // 2, lambda i: normalize(first + i))

    spread = functools.partial(spread_tables, table_ref, cos_ref, sin_ref)
    calls = plan(FRONT_PLAN, *([*g.stages()] for g in gathers), [in_order(spread, functools.partial(normalize_half, 0)), functools.partial(normalize_half, CHUNK_STEPS // 2)])

    @pl.when(step == 0)
    def _():
        for i in range(CHUNK_STEPS):
            load(i).start()
        for i in THREE:
            heads = qkv_shard[:, i].astype(F32).swapaxes(0, 1)
            for j in range(pairs):
                tile = side_by_side(heads, j)
                shards[:, lanes(3 * j + i)] = (swap_middle(tile) if i < 2 else tile).astype(BF16)
        for j in range(pairs):
            shards[:, lanes(3 * pairs + j)] = side_by_side(out_shard, j)
        both = ff_shard[...].astype(F32)
        for i in range(ff // LANES):
            for j in TWO:
                shards[:, lanes(4 * pairs + 2 * i + j)] = both[:, j, lanes(i)].astype(BF16)
        shards[:, out_end + 2 * ff:] = down_shard[...]
        net.barrier(net.neighbours(2) + [net.partner])
        for when, call in calls:
            if not when:
                call()

    begin, end = halves_of(calls, 1)
    run_at(turn, begin)

    @pl.when(turn >= 0)
    def _():
        weight = w[:, :, :, :, pl.ds(pl.multiple_of(width * p, LANES), width)].reshape(n1.shape[1], width)
        project_pair(n1.at[aligned(b * seq, seq)], weight, cos_ref, sin_ref, qkv_ref, keep_ref)
        q_ref, k_ref, v_ref = (qkv_ref.at[:, pl.ds(LANES * i, LANES)] for i in THREE)
        attend_pair(q_ref, k_ref, v_ref, o_ref, lse_ref.at[0, 0])
        o_all[b, p] = o_ref[...]

    run_at(turn, end)

    def rows_in(c, core):
        return aligned(c * CHUNK + core * half, half)

    def part_copy(b, c):
        return to_partner(net, part.at[b, rows_in(c, 1 - net.core)], got.at[b, c], *pair_of(sems, 0, b, c))

    def rows_out(b, c, core):
        return aligned(b * seq + c * CHUNK + core * half, half)

    def h_copy(b, c, core):
        return to_partner(net, h_buf.at[b, c], h_hbm.at[rows_out(b, c, core)], *pair_of(sems, 1, b, c))

    def h_local(b, c):
        return pltpu.make_async_copy(h_buf.at[b, c], h_hbm.at[rows_out(b, c, net.core)], h_sem.at[b, c])

    def project(b):
        o_buf[...] = jnp.concatenate([o_all[b, j] for j in range(pairs)], axis=1)
        weight = wo[...].reshape(part.shape[2], LANES * pairs)

        def body(c):
            rows = aligned(c * CHUNK, CHUNK)
            part[b, rows, :] = nt(o_buf[rows, :], weight)
            part_copy(b, c).start()

        repeat(chunks, body)

    def combine(b):
        def body(c):
            part_copy(b, c).wait()
            own = rows_in(c, net.core)
            h_buf[b, c] = (x_all[rows_out(b, c, net.core), :].astype(F32) + (part[b, own, :] + got[b, c])).astype(BF16)
            h_copy(b, c, net.core).start()
            h_local(b, c).start()

        repeat(chunks, body)

    def settle():
        for b in range(batch):
            for c in range(chunks):
                h_copy(b, c, net.core).wait_send()
                h_local(b, c).wait()
                h_copy(b, c, 1 - net.core).wait_recv()
        for i in range(CHUNK_STEPS):
            save(i).wait()
        save_weight.wait()

    fetch = pltpu.make_async_copy(wo_hbm, wo, h_sem.at[0, 0])
    run_at(last - step, [(2, fetch.start), (2, save_weight.start), (1, fetch.wait), (0, functools.partial(combine, 0))])

    @pl.when(step + 1 >= last)
    def _():
        project(step + 1 - last)

    run_at(last - step, [(0, functools.partial(combine, 1)), (0, settle)])
    run_at(turn + 1, begin[-1:])


def front(x, qkv_shard, out_shard, ff_shard, down_shard, table, batch, seq, collective_id):
    pairs = len(out_shard) // 2
    rows, d = x.shape
    width = 3 * LANES
    chunks = seq // CHUNK
    vm = pltpu.VMEM
    torus = (SIDE, SIDE, SIDE, PIECE)
    shards = [s.size // PIECE for s in (qkv_shard, out_shard, ff_shard, down_shard)]
    turn = lambda s: jnp.maximum(s - 1, 0)
    head = lambda width: pl.BlockSpec((seq, width), lambda s: (turn(s) % batch, turn(s) // batch))
    return pl.pallas_call(
        front_kernel,
        grid=(1 + batch * pairs,),
        in_specs=[HBM] + [WHOLE] * 5,
        out_specs=[head(width), head(width), head(LANES), pl.BlockSpec((1, 1, 2, seq), lambda s: (turn(s) % batch, turn(s) // batch, 0, 0))] + [HBM] * 5,
        out_shape=[shape(BF16, rows, width * pairs)] * 2 + [shape(BF16, rows, LANES * pairs), shape(F32, batch, pairs, 2, seq), shape(BF16, rows, d), shape(BF16, rows, d),
                   shape(BF16, *torus, shards[0]), shape(BF16, *torus, shards[1]), shape(BF16, *torus, shards[2] + shards[3])],
        scratch_shapes=[vm((rows, d), BF16), vm((rows, d), BF16), vm(torus + (width * pairs,), BF16), vm((PIECE, sum(shards)), BF16),
                        vm((batch, pairs, seq, LANES), BF16), vm((batch, seq, d), F32), vm((batch, chunks, CHUNK // 2, d), F32), vm((batch, chunks, CHUNK // 2, d), BF16),
                        vm(torus + (shards[1],), BF16), dma(2, 2, batch, chunks), dma(2, (pairs + 2) * Gather.SEMS), dma(CHUNK_STEPS + 1), dma(batch, chunks)] + [vm((seq, LANES), F32)] * 2 + [vm((seq, LANES * pairs), BF16)],
        compiler_params=params(collective_id),
        name='front',
    )(x, qkv_shard, out_shard, ff_shard, down_shard, table)


class Exchange:
    def __init__(self, net, rows, partials, results, sems, local_sem):
        self.net, self.rows, self.partials, self.results, self.sems, self.local_sem = net, rows, partials, results, sems, local_sem

    def half(self, core, at=0):
        return aligned(at * self.rows + core * (self.rows // 2), self.rows // 2)

    def part(self, which, at):
        part, got = self.partials[which]
        return to_partner(self.net, part.at[at % 2, self.half(1 - self.net.core)], got.at[at], *pair_of(self.sems, which, at))

    def total(self, which, at):
        part, got = self.partials[which]
        self.part(which, at).wait()
        return part[at % 2, self.half(self.net.core), :] + got[at]

    def results_of(self, at, core, act):
        for i, (buf, hbm) in enumerate(self.results):
            act(buf.at[at % 2], hbm.at[self.half(core, at)], pair_of(self.sems, len(self.partials) + i, at), self.local_sem.at[i, at % 2])

    def publish(self, at):
        def act(buf, rows, sem, local_sem):
            to_partner(self.net, buf, rows, *sem).start()
            pltpu.make_async_copy(buf, rows, local_sem).start()
        self.results_of(at, self.net.core, act)

    def settle(self, at):
        def act(buf, rows, sem, local_sem):
            to_partner(self.net, buf, rows, *sem).wait_send()
            pltpu.make_async_copy(buf, rows, local_sem).wait()
        self.results_of(at, self.net.core, act)
        self.results_of(at, 1 - self.net.core, lambda buf, rows, sem, local_sem: to_partner(self.net, buf, rows, *sem).wait_recv())


def mlp_kernel(blocks, h_ref, gy_ref, wff_ref, wd_ref, y_hbm, gh_hbm, gh32_ref, acts_hbm, n2_ref, gd_hbm,
               saved, grad_down, part_y, part_g, got_y, got_g, y_buf, gh_buf, h_own, gy_own, sems, local_sem, save_sem):
    step, final = grid_step()
    rows, d = h_ref.shape
    ff = wd_ref.shape[1]
    acts = saved.at[step % 2]
    gug, act = acts.at[:, pl.ds(0, 2 * ff)], acts.at[:, pl.ds(2 * ff, ff)]

    def save(at):
        return pltpu.make_async_copy(saved.at[at % 2], acts_hbm.at[aligned(at * rows, rows)], save_sem.at[at % 2])

    save_grad = pltpu.make_async_copy(grad_down, gd_hbm, save_sem.at[2])
    net = Torus()
    swap = Exchange(net, rows, ((part_y, got_y), (part_g, got_g)), ((y_buf, y_hbm), (gh_buf, gh_hbm)), sems, local_sem)

    @pl.when(step == 0)
    def _():
        net.barrier([net.partner])

    @pl.when((step > 1) & (step < blocks))
    def _():
        save(step - 2).wait()

    @pl.when(step < blocks)
    def _():
        n2, _ = norm_rows(h_ref[...].astype(F32))
        n2 = n2.astype(BF16)
        n2_ref[...] = n2
        gy = gy_ref[...]
        for j in strips(ff, QB):
            w = min(QB, ff - j)
            gact = nn(gy, wd_ref[:, j:j + w])
            for i in range(j, j + w, LANES):
                at, mid, end = 2 * i, 2 * i + LANES, 2 * i + QB
                ug = nn(n2, wff_ref[:, at:end])
                up, gate = ug[:, :LANES], ug[:, LANES:]
                sig = 1.0 / (1.0 + jnp.exp(-gate))
                silu = gate * sig
                act[:, i:i + LANES] = (silu * up).astype(BF16)
                ga = gact[:, i - j:i - j + LANES]
                gug[:, at:mid] = (ga * silu).astype(BF16)
                gug[:, mid:end] = (ga * up * sig * (1.0 + gate * (1.0 - sig))).astype(BF16)

        for which, left, right, part in ((0, act, wd_ref, part_y), (1, gug, wff_ref, part_g)):
            for j in strips(d, QB):
                part[step % 2, :, j:j + QB] = nt(left[...], right[j:j + QB, :])
            swap.part(which, step).start()
        save(step).start()
        accumulate(grad_down, step == 0, gy, act)

    @pl.when(step == blocks - 1)
    def _():
        save_grad.start()

    @pl.when(step > 2)
    def _():
        swap.settle(step - 3)

    @pl.when(step > 0)
    def _():
        done = step - 1
        hidden = h_own[...].astype(F32)
        normed, inv = norm_rows(hidden)
        y_buf[done % 2] = (hidden + swap.total(0, done)).astype(BF16)
        gh = gy_own[...].astype(F32) + norm_grad(swap.total(1, done), normed, inv)
        gh32_ref[...] = gh
        gh_buf[done % 2] = gh.astype(BF16)
        swap.publish(done)

    own = swap.half(net.core)
    h_own[...] = h_ref[own, :]
    gy_own[...] = gy_ref[own, :]

    @pl.when(step == blocks)
    def _():
        for at in (blocks - 2, blocks - 1):
            swap.settle(at)
            save(at).wait()
        save_grad.wait()


def mlp(h, gy, weights, collective_id, block=512):
    rows, d = h.shape
    ff = weights.shape[1] // 3
    half = block // 2
    blocks = rows // block
    torus = (SIDE, SIDE, SIDE, PIECE)
    row = lambda width: rows_of(block, width, lambda i: jnp.minimum(i, blocks - 1))
    vm = pltpu.VMEM
    return pl.pallas_call(
        functools.partial(mlp_kernel, blocks),
        grid=(blocks + 1,),
        in_specs=[row(d), row(d), fixed((d, 2 * ff)), fixed((d, ff), (0, 2))],
        out_specs=[HBM, HBM, rows_of(half, d, lambda i: jnp.maximum(i - 1, 0)), HBM, row(d), HBM],
        out_shape=[shape(BF16, rows, d), shape(BF16, rows, d), shape(F32, rows // 2, d), shape(BF16, rows, 3 * ff), shape(BF16, rows, d), shape(F32, *torus, ff)],
        scratch_shapes=[vm((2, block, 3 * ff), BF16), vm(torus + (ff,), F32)] + [vm((2, block, d), F32)] * 2 + [vm((blocks, half, d), F32)] * 2 + [vm((2, half, d), BF16)] * 2 + [vm((half, d), BF16)] * 2 + [dma(2, 4, blocks), dma(2, 2), dma(3)],
        compiler_params=params(collective_id),
        name='mlp',
    )(h, gy, weights, weights)


def accumulate(part, first, left, right):
    for j in strips(right.shape[1], QB):
        w = min(QB, right.shape[1] - j)
        prod = tn(left, right[:, j:j + w]).reshape(part.shape[:-1] + (w,))
        at = slice(j, j + w)
        part[..., at] = jnp.where(first, 0.0, part[..., at]) + prod


SETS = 3
HEAD_STEP = (SETS - 1) * CHUNK_STEPS


def back_kernel(pairs, gd_hbm, n2_ref, act_ref, qkv_ref, lse_ref, gh_ref, wo_ref, o_ref, keep_ref, table_ref,
                g_ref, gw_ref, gd_ref, gff_ref, cos_ref, sin_ref, do_ref, dk_ref, dv_ref, parts, sems, load_sem, *bufs):
    step, final = grid_step()
    turn = step - HEAD_STEP
    p = turn % pairs
    half = gh_ref.shape[0] // 2
    net = Torus()
    per = len(bufs) // SETS
    scatters = [Scatter(net, parts.at[i], cut_three(parts.shape[-1], turn=i), bufs[per * i:per * i + per], sems, i * Scatter.SEMS) for i in range(SETS)]
    calls = plan(SCATTER_PLAN, *(s.stages() for s in scatters))
    begin, end = halves_of(calls, HEAD_STEP + 1)

    @pl.when(step == 0)
    def _():
        load = pltpu.make_async_copy(gd_hbm, parts.at[0], load_sem.at[0])
        load.start()
        spread_tables(table_ref, cos_ref, sin_ref)
        net.barrier(net.neighbours())
        load.wait()
        for when, call in calls:
            if not when:
                call()

    @pl.when(turn < 0)
    def _():
        accumulate(parts.at[1 + step // CHUNK_STEPS], step % CHUNK_STEPS == 0, n2_ref[...], act_ref)

    run_at(step + 1, [c for c in calls if 0 < c[0] <= HEAD_STEP])

    def put(part, lo, hi, values):
        cols = lanes(part)
        if part < 2:
            values = values * cos_ref[lo:hi, :] - swap_halves(values) * sin_ref[lo:hi, :]
        g_ref[lo:hi, cols] = (values * keep_ref[lo:hi, cols].astype(F32)).astype(BF16)

    def put_dq(lo, hi, dq):
        put(0, lo, hi, dq * 0.125)

    @pl.when(turn >= 0)
    def _():
        @pl.when(p == 0)
        def _():
            gw_ref[...] = jnp.where(turn == 0, 0.0, gw_ref[...])

            def body(i):
                rows = aligned(i * half, half)
                gh = gh_ref[rows, :]
                dout = nn(gh, wo_ref[...]).astype(BF16)
                for j in range(pairs):
                    do_ref[j, rows, :] = dout[:, lanes(j)]
                gw_ref[...] += tn(gh, o_ref[rows, :])

            repeat(len(TWO), body)

        run_at(turn, begin)
        q_ref, k_ref, v_ref = (qkv_ref.at[:, pl.ds(LANES * i, LANES)] for i in THREE)
        attend_pair_back(q_ref, k_ref, v_ref, do_ref.at[p], lse_ref.at[0, 0], dk_ref, dv_ref, put_dq)
        seq = q_ref.shape[0]
        put(1, 0, seq, dk_ref[...])
        put(2, 0, seq, dv_ref[...])
        run_at(turn, end)

    @pl.when(step == final)
    def _():
        gd_ref[...], *halves = [s.result() for s in scatters]
        tiles = jnp.concatenate(halves, axis=1)
        for i in strips(tiles.shape[1], LANES):
            at = i // QB * LANES
            gff_ref[:, i // LANES % 2, at:at + LANES] = tiles[:, i:i + LANES]


def back(gd, n2, acts, qkv, lse, gh, wo_t, o, keep, table, batch, seq, pairs, collective_id):
    rows, d = n2.shape
    ff = acts.shape[1] // SETS
    block = rows // CHUNK_STEPS
    turn = lambda s: jnp.maximum(s - HEAD_STEP, 0)
    head = pl.BlockSpec((seq, 3 * LANES), lambda s: (turn(s) // pairs, turn(s) % pairs))
    late = lambda s: jnp.where(s < HEAD_STEP, s % CHUNK_STEPS, CHUNK_STEPS - 1)
    vm = pltpu.VMEM
    per_seq = lambda width: rows_of(seq, width, lambda s: turn(s) // pairs)
    return pl.pallas_call(
        functools.partial(back_kernel, pairs),
        grid=(HEAD_STEP + batch * pairs,),
        in_specs=[HBM, rows_of(block, d, late), pl.BlockSpec((block, ff), lambda s: (late(s), jnp.minimum(s // CHUNK_STEPS, 1))), head, pl.BlockSpec((1, 1, 2, seq), lambda s: (turn(s) // pairs, turn(s) % pairs, 0, 0)),
                  per_seq(d), fixed(wo_t.shape), per_seq(LANES * pairs), head, WHOLE],
        out_specs=[head, fixed(wo_t.shape), WHOLE, WHOLE],
        out_shape=[shape(BF16, *qkv.shape), shape(F32, *wo_t.shape), shape(F32, PIECE, ff), shape(F32, PIECE, 2, ff)],
        scratch_shapes=[vm((seq, LANES), F32)] * 2 + [vm((pairs, seq, LANES), BF16)] + [vm((seq, LANES), F32)] * 2 + [vm((SETS, SIDE, SIDE, SIDE, PIECE, ff), F32),
                        dma(2, SETS * Scatter.SEMS), dma(1)] + [s for i in range(SETS) for s in Scatter.scratch(cut_three(ff, turn=i))],
        compiler_params=params(collective_id),
        name='back',
    )(gd, n2, acts, qkv, lse, gh, wo_t, o, keep, table)


def last_kernel(pairs, blocks, n1_ref, g_ref, x_ref, g_row, gh_ref, w_ref, gout_hbm, gx_hbm, gout_ref, gw_ref,
                part_out, part_qkv, part, got, buf, sems, scatter_sems, local_sem, *bufs):
    step, final = grid_step()
    turn = step - pairs
    rows, d = x_ref.shape
    net = Torus()
    per = len(bufs) // (pairs + 1)
    parts = [part_out] + [part_qkv.at[j] for j in range(pairs)]
    scatters = [Scatter(net, s, cut_three(s.shape[-1], turn=i), bufs[per * i:per * i + per], scatter_sems, i * Scatter.SEMS) for i, s in enumerate(parts)]
    calls = plan(LAST_PLAN, *(s.stages() for s in scatters))
    swap = Exchange(net, rows, ((part, got),), ((buf, gx_hbm),), sems, local_sem)

    @pl.when(step == 0)
    def _():
        load = pltpu.make_async_copy(gout_hbm, part_out, local_sem.at[1, 0])
        load.start()
        net.barrier(net.neighbours() + [net.partner])
        load.wait()

    begin, end = halves_of(calls)
    run_at(step, begin)

    @pl.when(turn < 0)
    def _():
        size = n1_ref.shape[0] // len(TWO)

        def body(i):
            accumulate(part_qkv.at[step], i == 0, n1_ref[aligned(i * size, size), :], g_ref.at[aligned(i * size, size)])

        repeat(len(TWO), body)

    @pl.when((turn >= 0) & (turn < blocks))
    def _():
        for j in strips(d, QB):
            part[turn % 2, :, j:j + QB] = nt(g_row[...], w_ref[j:j + QB, :])
        swap.part(0, turn).start()

    run_at(step, end)

    @pl.when(turn > 2)
    def _():
        swap.settle(turn - 3)

    @pl.when(turn > 0)
    def _():
        done = turn - 1
        normed, inv = norm_rows(x_ref[swap.half(net.core), :].astype(F32))
        buf[done % 2] = (gh_ref[...] + norm_grad(swap.total(0, done), normed, inv)).astype(BF16)
        swap.publish(done)

    @pl.when(turn == blocks)
    def _():
        for when, call in calls:
            if when > 2 * (pairs + blocks) + 1:
                call()
        for at in (blocks - 2, blocks - 1):
            swap.settle(at)
        out, *sums = [s.result() for s in scatters]
        halves = slice(HALF), slice(HALF, LANES)
        for j in range(pairs):
            for h, cols in enumerate(halves):
                gout_ref[2 * j + h] = out[:, lanes(j)][:, cols]
        for i in THREE:
            tiles = [swap_middle(s[:, lanes(i)]) if i < 2 else s[:, lanes(i)] for s in sums]
            gw_ref[:, i] = jnp.stack([t[:, cols] for t in tiles for cols in halves]).swapaxes(0, 1)


def last(x, n1, g, gh32, w, gout, pairs, collective_id, block=512):
    rows, d = x.shape
    blocks = rows // block
    late = lambda n, width, by: rows_of(n, width, lambda s: jnp.clip(s - pairs - by, 0, blocks - 1))
    head = pl.BlockSpec((rows, 3 * LANES), lambda s: (0, jnp.minimum(s, pairs - 1)))
    vm = pltpu.VMEM
    half = block // 2
    torus = (SIDE, SIDE, SIDE, PIECE)
    gout = gout.reshape(torus + (-1,))
    return pl.pallas_call(
        functools.partial(last_kernel, pairs, blocks),
        grid=(pairs + blocks + 1,),
        in_specs=[fixed((rows, d)), head, late(block, d, 1), late(block, g.shape[1], 0), late(half, d, 1), fixed(w.shape), HBM],
        out_specs=[HBM, WHOLE, WHOLE],
        out_shape=[shape(BF16, rows, d), shape(F32, 2 * pairs, PIECE, HALF), shape(F32, PIECE, 3, 2 * pairs, HALF)],
        scratch_shapes=[vm(gout.shape, F32), vm((pairs,) + torus + (3 * LANES,), F32), vm((2, block, d), F32), vm((blocks, half, d), F32), vm((2, half, d), BF16),
                        dma(2, 2, blocks), dma(2, (pairs + 1) * Scatter.SEMS), dma(2, 2)] + Scatter.scratch(cut_three(gout.shape[-1])) + Scatter.scratch(cut_three(3 * LANES)) * pairs,
        compiler_params=params(collective_id, 46),
        name='last',
    )(n1, g, x, g, gh32, w, gout)


def device_step(x, grad_y, w_qkv, w_out, w_ff, w_down):
    batch, seq, d = x.shape
    heads, head = w_qkv.shape[2:]
    pairs = heads // 2
    table = jnp.asarray(tables(seq, head))
    ids = iter(range(4))
    x2, gy = (v.reshape(batch * seq, d) for v in (x, grad_y))
    qkv, keep, o, lse, h, n1, *weights = front(x2, w_qkv, w_out.swapaxes(1, 2), w_ff, w_down.T, table, batch, seq, next(ids))
    wq, wo_t, wf = (w.reshape(d, w.shape[-1]) for w in weights)
    y, gh, gh32, acts, n2, gd = mlp(h, gy, wf, next(ids))
    g, gout, gd, gff = back(gd, n2, acts, qkv, lse, gh, wo_t, o, keep, table, batch, seq, pairs, next(ids))
    gx, gout, gqkv = last(x2, n1, g, gh32, wq, gout, pairs, next(ids))
    return y.reshape(x.shape), gx.reshape(x.shape), gqkv, gout.swapaxes(1, 2), gff, gd.T


def solution(mesh):
    specs = (P('fsdp'), P('fsdp'), P('fsdp', None, 'tp'), P('tp', None, 'fsdp'), P('fsdp', None, 'tp'), P('tp', 'fsdp'))
    return jax.shard_map(device_step, mesh=mesh, in_specs=specs, out_specs=specs, check_vma=False)
```

```python
import functools

import jax
import jax.numpy as jnp
import numpy as np
from jax import lax
from jax.experimental import pallas as pl
from jax.experimental.pallas import tpu as pltpu
from jax.sharding import PartitionSpec as P

MESH_ID = pl.DeviceIdType.MESH
SIDE = 4
TILE = 128
PIECE = 16
ORDERS = ((2, 1, 0), (1, 0, 2), (0, 2, 1))
BOTH = ((0, 1), (1, -1))
PHASES = THREE = range(3)
TWO = range(2)


class Torus:
    def __init__(self):
        self.core = lax.axis_index('tp')
        self.index = lax.axis_index('fsdp')
        plane, x = lax.div(self.index, SIDE), lax.rem(self.index, SIDE)
        self.at = (lax.div(plane, SIDE), lax.rem(plane, SIDE), x)
        self.partner = (1 - self.core, self.index)
        self.moved = {(axis, by): lax.rem(at + (by + SIDE), SIDE) for axis, at in enumerate(self.at) for by in range(-2, 3)}
        self.peers = {(axis, by): self.place(axis, self.moved[axis, by]) for axis in THREE for by in (-1, 1, 2)}

    def place(self, axis, coord):
        pos = list(self.at)
        pos[axis] = coord
        z, y, x = pos
        return (self.core, (z * SIDE + y) * SIDE + x)

    def shift(self, axis, by):
        return self.moved[axis, by]

    def peer(self, axis, by):
        return self.peers[axis, by]

    def neighbours(self, reach=1):
        return [device for (_, by), device in self.peers.items() if by <= reach]

    def tell(self, sem, devices):
        for device in devices:
            pl.semaphore_signal(sem, inc=1, device_id=device, device_id_type=MESH_ID)

    def barrier(self, devices):
        sem = pltpu.get_barrier_semaphore()
        self.tell(sem, devices)
        pl.semaphore_wait(sem, len(devices))


def pair_of(sems, *at):
    return sems.at[(0,) + at], sems.at[(1,) + at]


def in_order(*calls):
    def run():
        for call in calls:
            call()
    return run


def span(cols):
    (off, width), *rest = cols
    return pl.ds(off, width + sum(w for _, w in rest))


class Gather:
    SEMS = 7

    def __init__(self, net, shard, out, cols, shift, sems, first, direct=False):
        self.net, self.shard, self.out, self.cols, self.moved, self.sems, self.first, self.direct = net, shard, out, cols, shift, sems, first, direct

    def block(self, colour, phase, coord, half=None):
        order = ORDERS[colour]
        off, width = self.cols[colour]
        pick = list(self.net.at)
        for axis in order[:phase]:
            pick[axis] = pl.ds(0, SIDE)
        pick[order[phase]] = coord
        if half is not None and phase:
            pick[order[0]] = pl.ds(half * 2, 2)
        elif half is not None:
            cut = width - width // (2 * TILE) * TILE
            off, width = (off + cut, width - cut) if half else (off, cut)
        return self.out.at[(*pick, slice(None), pl.ds(off, width))] if width else None

    def copy(self, phase, colour, relay, d, by):
        axis = ORDERS[colour][phase]
        far = relay and self.direct
        if far and d:
            return None
        by = 2 if far else by
        back = -by if relay and not far else 0
        dst = src = self.block(colour, phase, self.net.shift(axis, back), d if relay and not far else None)
        if dst is None:
            return None
        if not phase and (far or not relay):
            off, width = self.cols[colour]
            src = self.shard.at[:, pl.ds(off + self.moved, width)]
        return pltpu.make_async_remote_copy(src, dst, *self.sem(phase, relay), device_id=self.net.peer(axis, by), device_id_type=MESH_ID)

    def sem(self, phase, relay):
        return pair_of(self.sems, self.first + 2 * phase + relay)

    def each(self, phase, relay):
        for d, by in BOTH:
            for colour in THREE:
                desc = self.copy(phase, colour, relay, d, by)
                if desc is not None:
                    desc.start()

    def wait(self, phase, relay, side):
        pick = [pl.ds(0, SIDE)] * phase + [pl.ds(0, 2 - relay)] + [0, 0]
        ref = self.out.at[tuple(reversed(pick[:3])) + (slice(None), span(self.cols))]
        pltpu.make_async_copy(ref, ref, self.sem(phase, relay)[side]).wait()

    def own(self):
        at = self.net.at
        cols = span(self.cols)
        src = self.shard.at[:, pl.ds(cols.start + self.moved, cols.size)]
        return pltpu.make_async_copy(src, self.out.at[(*at, slice(None), cols)], self.sems.at[0, self.first + self.SEMS - 1])

    def arrive(self, phase):
        if self.direct:
            self.wait(phase, 0, 1)
        self.wait(phase, 1, 1)

    def start(self, phase):
        if phase:
            self.arrive(phase - 1)
        if phase == 1:
            self.own().wait()
        for relay in range(1 + self.direct):
            self.each(phase, relay)
        if not phase:
            self.own().start()

    def relay(self, phase):
        self.wait(phase, 0, 1)
        self.each(phase, 1)

    def finish(self):
        self.arrive(PHASES[-1])
        for phase in PHASES:
            for relay in TWO:
                self.wait(phase, relay, 0)

    def stages(self):
        steps = (self.start,) if self.direct else (self.start, self.relay)
        return [functools.partial(f, p) for p in PHASES for f in steps] + [self.finish]


class Scatter:
    SEMS = 9

    def __init__(self, net, part, cols, bufs, sems, first, relays=len(PHASES)):
        self.net, self.part, self.cols, self.bufs, self.sems, self.first, self.relays = net, part, cols, bufs, sems, first, relays

    @staticmethod
    def scratch(cols):
        shapes = []
        for _, w in cols:
            shapes += [(3, 2, 2, SIDE, PIECE, w), (3, 2, 2, PIECE, w), (3, 2, PIECE // 2, w)]
        return [pltpu.VMEM(s, jnp.float32) for s in shapes]

    def buf(self, colour, phase):
        return self.bufs[colour * len(PHASES) + phase]

    def block(self, colour, phase, coord, half):
        order = ORDERS[colour]
        off, width = self.cols[colour]
        pick = [pl.ds(0, SIDE)] * 3
        for axis in order[:phase]:
            pick[axis] = self.net.at[axis]
        pick[order[phase]] = coord
        rows = pl.ds(0, PIECE)
        rest = sorted(order[phase + 1:])
        if rest:
            pick[rest[0]] = pl.ds(2 * half, 2)
        else:
            rows = pl.ds(PIECE // 2 * half, PIECE // 2)
        return self.part.at[(*pick, rows, pl.ds(off, width))]

    def copy(self, phase, colour, kind, d, by):
        axis = ORDERS[colour][phase]
        buf = self.buf(colour, phase)
        direct = phase >= self.relays
        if kind == 2 and not direct:
            src = buf.at[0, d]
        elif kind:
            src = self.block(colour, phase, self.net.shift(axis, by), (kind + d) % 2)
        else:
            src = self.block(colour, phase, self.net.shift(axis, 2), d)
            by = 2 if direct else by
        return pltpu.make_async_remote_copy(src, buf.at[kind, d], *self.sem(phase, kind), device_id=self.net.peer(axis, by), device_id_type=MESH_ID)

    def sem(self, phase, kind):
        return pair_of(self.sems, self.first + len(PHASES) * phase + kind)

    def wait(self, phase, kind, side):
        pick = [0] * (phase + 1) + [pl.ds(0, SIDE)] * (2 - phase)
        ref = self.part.at[tuple(pick) + (slice(None), span(self.cols))]
        pltpu.make_async_copy(ref, ref, self.sem(phase, kind)[side]).wait()

    def start(self, phase, kind):
        for d, by in BOTH:
            for colour in THREE:
                self.copy(phase, colour, kind, d, by).start()

    def relay(self, phase):
        self.wait(phase, 0, 1)
        for colour in THREE:
            buf = self.buf(colour, phase)
            for d, by in BOTH:
                buf[0, d] = buf[0, d] + self.block(colour, phase, self.net.shift(ORDERS[colour][phase], by), d)[...]
        self.start(phase, 2)

    def merge(self, phase):
        direct = phase >= self.relays
        for kind in THREE if direct else (1, 2):
            self.wait(phase, kind, 1)
        for colour in THREE:
            buf = self.buf(colour, phase)
            for half in TWO:
                mine = self.block(colour, phase, self.net.at[ORDERS[colour][phase]], half)
                sums = mine[...] + buf[1, 1 - half] + buf[2, half]
                mine[...] = sums + buf[0, half] if direct else sums
        if phase < PHASES[-1]:
            for kind in TWO if phase + 1 < self.relays else THREE:
                self.start(phase + 1, kind)

    def finish(self):
        for phase in PHASES:
            for kind in PHASES:
                self.wait(phase, kind, 0)

    def stages(self):
        calls = [functools.partial(self.start, 0, kind) for kind in TWO]
        for phase in PHASES:
            calls += [functools.partial(self.relay, phase)] * (phase < self.relays) + [functools.partial(self.merge, phase)]
        return calls[:-1] + [in_order(calls[-1], self.finish)]

    def result(self):
        return self.part[self.net.at]


def cut_three(width, off=0, turn=0):
    tiles, ways = width // TILE, len(THREE)
    sizes = [(tiles + (turn - i - 1) % ways) // ways * TILE for i in THREE]
    return [(off + sum(sizes[:i]), s) for i, s in enumerate(sizes)]


def plan(text, *sets):
    left = [iter(s) for s in sets]
    return [(hook, next(left[int(which)])) for hook, field in enumerate(text.split(',')) for which in field]


def halves_of(calls, first=0):
    return [[((when - first) // 2, call) for when, call in calls if when >= first and (when - first) % 2 == odd] for odd in TWO]


def run_at(hook, calls):
    for when, call in calls:
        pl.when(hook == when)(call)


F32, BF16 = jnp.float32, jnp.bfloat16
QB = 256
LANES = TILE
HALF = LANES // 2
CLIP = 8.0
BLOCK = 512
MIB = 2**20


def nt(a, b):
    return lax.dot_general(a, b, (((1,), (1,)), ((), ())), preferred_element_type=F32)


def nn(a, b):
    return jnp.dot(a, b, preferred_element_type=F32)


def tn(a, b):
    return lax.dot_general(a, b, (((0,), (0,)), ((), ())), preferred_element_type=F32)


def along(reduce, values):
    return reduce(values, axis=-1, keepdims=True)


def head_masks(paired):
    lane = lax.broadcasted_iota(jnp.int32, (1, LANES), 1)
    first = lane % HALF < HALF // 2 if paired else lane < HALF
    return first, jnp.logical_not(first)


def causal_tile(key_axis):
    dims = (QB, 2 * QB) if key_axis == 0 else (2 * QB, QB)
    return lax.broadcasted_iota(jnp.int32, dims, key_axis) <= lax.broadcasted_iota(jnp.int32, dims, 1 - key_axis) % QB


def by_head(values, masks):
    return jnp.concatenate([jnp.where(m, values, jnp.zeros((), BF16)) for m in masks], axis=0)


def attend_pair(q_ref, k_ref, v_ref, o_ref, lse_ref):
    masks = head_masks(True)
    key, val = k_ref[...], v_ref[...]
    causal = causal_tile(1)
    first = head_masks(False)[0]
    for lo in reversed(strips(q_ref.shape[0], QB)):
        hi = lo + QB
        query = by_head(q_ref[lo:hi, :], masks)
        diag = jnp.where(causal, nt(query, key[lo:hi]), -1e30)
        top = along(jnp.max, diag)
        if lo:
            past = nt(query, key[:lo])
            top = jnp.maximum(top, along(jnp.max, past))
            past = jnp.exp(past - top)
        diag = jnp.exp(diag - top)
        total = along(jnp.sum, diag)
        if lo:
            total = total + along(jnp.sum, past)
        scale = 1.0 / total
        acc = nn((diag * scale).astype(BF16), val[lo:hi])
        if lo:
            acc = acc + nn((past * scale).astype(BF16), val[:lo])
        o_ref[lo:hi, :] = jnp.where(first, acc[:QB], acc[QB:]).astype(BF16)
        lse = jnp.broadcast_to(top + jnp.log(total), acc.shape).T
        for h in TWO:
            lse_ref[h:h + 1, lo:hi] = lse[:1, h * QB:(h + 1) * QB]


def attend_pair_back(q_ref, k_ref, v_ref, do_ref, lse_ref, dk_ref, dv_ref, put_dq):
    seq = q_ref.shape[0]
    qmask, vmask = head_masks(True), head_masks(False)
    key, val = k_ref[...], v_ref[...]
    key_t = key.astype(F32).T.astype(BF16)
    causal = causal_tile(0)
    first = lax.broadcasted_iota(jnp.int32, (LANES, 1), 0) % HALF < HALF // 2

    def products(lo):
        hi = lo + QB
        query, dout = by_head(q_ref[lo:hi, :], qmask), by_head(do_ref[lo:hi, :], vmask)
        return query, dout, nt(key[:hi], query), nt(val[:hi], dout)

    ahead = products(seq - QB)
    for lo in reversed(strips(seq, QB)):
        hi = lo + QB
        query, dout, score, grad = ahead
        if lo:
            ahead = products(lo - QB)
        prob = jnp.exp(score - jnp.concatenate([lse_ref[h:h + 1, lo:hi] for h in TWO], axis=1))
        diag = jnp.where(causal, prob[lo:], 0.0)
        prob = jnp.concatenate([prob[:lo], diag], axis=0) if lo else diag
        ds = (prob * (grad - jnp.sum(prob * grad, axis=0, keepdims=True))).astype(BF16)
        both = nn(key_t[:, :hi], ds)
        put_dq(lo, hi, jnp.where(first, both[:, :QB], both[:, QB:]).T)
        dv, dk = nn(prob.astype(BF16), dout), nn(ds, query)
        if hi == seq:
            dv_ref[...] = dv
            dk_ref[...] = dk
        else:
            dv_ref[:hi, :] += dv
            dk_ref[:hi, :] += dk


def swap_halves(values):
    return pltpu.roll(values, HALF, axis=1)


COARSE = 32


def tables(seq, head):
    freq = 10000.0 ** (-np.arange(0, head, 2, dtype=np.float64) / head)
    angles = [np.tile(np.arange(seq // COARSE)[:, None] * step * freq, LANES // len(freq)) for step in (1, COARSE)]
    return np.stack([np.stack([np.cos(angle), np.sin(angle)]) for angle in angles]).astype(np.float32)


def spread_tables(table_ref, cos_ref, sin_ref):
    fine_cos, fine_sin = table_ref[0]
    sign = jnp.where(lax.broadcasted_iota(jnp.int32, (1, LANES), 1) < HALF, -1.0, 1.0)

    def body(i):
        rows = aligned(i * COARSE, COARSE)
        cos, sin = table_ref[1, :, pl.ds(i, 1), :]
        cos_ref[rows, :] = fine_cos * cos - fine_sin * sin
        sin_ref[rows, :] = (fine_sin * cos + fine_cos * sin) * sign

    repeat(cos_ref.shape[0] // COARSE, body)


def repeat(count, body):
    def step(i, carry):
        body(i)
        return carry

    lax.fori_loop(0, count, step, 0)


def side_by_side(halves, j):
    return jnp.concatenate([halves[2 * j], halves[2 * j + 1]], axis=1)


def aligned(at, size):
    return pl.ds(pl.multiple_of(at, size), size)


def norm_rows(values):
    mean = along(jnp.mean, values)
    centered = values - mean
    inv = lax.rsqrt(along(jnp.mean, centered * centered) + 1e-5)
    return centered * inv, inv


def norm_grad(grad, normed, inv):
    mean = along(jnp.mean, grad)
    proj = along(jnp.mean, grad * normed)
    return inv * (grad - mean - normed * proj)


def params(collective_id):
    return pltpu.CompilerParams(collective_id=collective_id, has_side_effects=True, vmem_limit_bytes=63 * MIB)


def grid_step():
    return pl.program_id(0), pl.num_programs(0) - 1


def dma(*shape):
    return pltpu.SemaphoreType.DMA(shape)


def shape(dtype, *dims):
    return jax.ShapeDtypeStruct(dims, dtype)


HBM = pl.BlockSpec(memory_space=pltpu.HBM)
WHOLE = pl.BlockSpec(memory_space=pltpu.VMEM)


def lanes(part):
    return slice(LANES * part, LANES * (part + 1))


def strips(width, size):
    return range(0, width, size)


def rows_of(size, width, index):
    return pl.BlockSpec((size, width), lambda step: (index(step), 0))


def fixed(block, index=(0, 0)):
    return pl.BlockSpec(block, lambda *grid: index, pipeline_mode=pl.Buffered(buffer_count=1))


def project_pair(n1_ref, weight, cos_ref, sin_ref, qkv_ref, keep_ref):
    for lo in strips(n1_ref.shape[0], QB):
        rows = slice(lo, lo + QB)
        raw = nn(n1_ref[rows, :], weight)
        keep_ref[rows, :] = (jnp.abs(raw) < CLIP).astype(F32).astype(BF16)
        raw = jnp.clip(raw, -CLIP, CLIP)
        for part in THREE:
            cols = lanes(part)
            tile = raw[:, cols]
            if part < 2:
                tile = tile * cos_ref[rows, :] + swap_halves(tile) * sin_ref[rows, :]
            if not part:
                tile = tile * 0.125
            qkv_ref[rows, cols] = tile.astype(BF16)


def swap_middle(tile):
    quarter = lax.broadcasted_iota(jnp.int32, tile.shape, 1) // (LANES // 4)
    up, down = pltpu.roll(tile, LANES // 4, axis=1), pltpu.roll(tile, LANES - LANES // 4, axis=1)
    return jnp.where(quarter == 1, down, jnp.where(quarter == 2, up, tile))


CHUNK = 256
CHUNK_STEPS = 4
FRONT_PLAN = '014560145260124530,,245,,134,,345,,24,,,,3,,,5,,5'
SCATTER_PLAN = '00,,,,,1,1,,2,0,,,2,12,0,,,,12,0,1,2,012,102,102'
LAST_PLAN = '00,,11,2,0,1,3,22,3,410,,234,4,201,3,402,1342,01,30241'


def to_partner(net, src, dst, send, recv):
    return pltpu.make_async_remote_copy(src, dst, send, recv, device_id=net.partner, device_id_type=MESH_ID)


def front_kernel(x_hbm, qkv_shard, out_shard, ff_shard, down_shard, table_ref, qkv_ref, keep_ref, o_ref, lse_ref, h_hbm, n1_hbm, wq_hbm, wo_hbm, wf_hbm,
                 x_all, n1, w, shards, o_all, part, got, h_buf, wo, sems, gather_sems, load_sem, h_sem, cos_ref, sin_ref, o_buf):
    step, last = grid_step()
    turn = step - 1
    batch, pairs, seq = o_all.shape[:3]
    b, p = turn % batch, turn // batch
    half = CHUNK // 2
    chunks = seq // CHUNK
    ff = down_shard.shape[1]
    net = Torus()
    width = 3 * LANES
    heads_end, out_end = width * pairs, (width + LANES) * pairs
    places = [(w, cut_three(width, width * j), 0) for j in range(pairs)] + [
              (wo_hbm, cut_three(LANES * pairs), heads_end), (wf_hbm, cut_three(3 * ff), out_end)]
    gathers = [Gather(net, shards, out, cols, shift, gather_sems, i * Gather.SEMS, i < pairs) for i, (out, cols, shift) in enumerate(places)]
    strip = x_all.shape[0] // CHUNK_STEPS

    def rows_at(i):
        return aligned(i * strip, strip)

    def load(i):
        return pltpu.make_async_copy(x_hbm.at[rows_at(i)], x_all.at[rows_at(i)], load_sem.at[i])

    def save(i):
        return pltpu.make_async_copy(n1.at[rows_at(i)], n1_hbm.at[rows_at(i)], load_sem.at[i])

    save_weight = pltpu.make_async_copy(w, wq_hbm, load_sem.at[CHUNK_STEPS])

    def normalize(i):
        load(i).wait()
        n1[rows_at(i), :] = norm_rows(x_all[rows_at(i), :].astype(F32))[0].astype(BF16)
        save(i).start()

    def normalize_half(first):
        repeat(CHUNK_STEPS // 2, lambda i: normalize(first + i))

    spread = functools.partial(spread_tables, table_ref, cos_ref, sin_ref)
    calls = plan(FRONT_PLAN, *([*g.stages()] for g in gathers), [in_order(spread, functools.partial(normalize_half, 0)), functools.partial(normalize_half, CHUNK_STEPS // 2)])

    @pl.when(step == 0)
    def _():
        for i in range(CHUNK_STEPS):
            load(i).start()
        for i in THREE:
            heads = qkv_shard[:, i].astype(F32).swapaxes(0, 1)
            for j in range(pairs):
                tile = side_by_side(heads, j)
                shards[:, lanes(3 * j + i)] = (swap_middle(tile) if i < 2 else tile).astype(BF16)
        for j in range(pairs):
            shards[:, lanes(3 * pairs + j)] = side_by_side(out_shard, j)
        both = ff_shard[...].astype(F32)
        for i in range(ff // LANES):
            for j in TWO:
                shards[:, lanes(4 * pairs + 2 * i + j)] = both[:, j, lanes(i)].astype(BF16)
        shards[:, out_end + 2 * ff:] = down_shard[...]
        net.barrier(net.neighbours(2) + [net.partner])
        for when, call in calls:
            if not when:
                call()

    begin, end = halves_of(calls, 1)
    run_at(turn, begin)

    @pl.when(turn >= 0)
    def _():
        weight = w[:, :, :, :, pl.ds(pl.multiple_of(width * p, LANES), width)].reshape(n1.shape[1], width)
        project_pair(n1.at[aligned(b * seq, seq)], weight, cos_ref, sin_ref, qkv_ref, keep_ref)
        q_ref, k_ref, v_ref = (qkv_ref.at[:, pl.ds(LANES * i, LANES)] for i in THREE)
        attend_pair(q_ref, k_ref, v_ref, o_ref, lse_ref.at[0, 0])
        o_all[b, p] = o_ref[...]

    run_at(turn, end)

    def rows_in(c, core):
        return aligned(c * CHUNK + core * half, half)

    def part_copy(b, c):
        return to_partner(net, part.at[b, rows_in(c, 1 - net.core)], got.at[b, c], *pair_of(sems, 0, b, c))

    def rows_out(b, c, core):
        return aligned(b * seq + c * CHUNK + core * half, half)

    def h_copy(b, c, core):
        return to_partner(net, h_buf.at[b, c], h_hbm.at[rows_out(b, c, core)], *pair_of(sems, 1, b, c))

    def h_local(b, c):
        return pltpu.make_async_copy(h_buf.at[b, c], h_hbm.at[rows_out(b, c, net.core)], h_sem.at[b, c])

    def project(b):
        o_buf[...] = jnp.concatenate([o_all[b, j] for j in range(pairs)], axis=1)
        weight = wo[...].reshape(part.shape[2], LANES * pairs)

        def body(c):
            rows = aligned(c * CHUNK, CHUNK)
            part[b, rows, :] = nt(o_buf[rows, :], weight)
            part_copy(b, c).start()

        repeat(chunks, body)

    def combine(b):
        def body(c):
            part_copy(b, c).wait()
            own = rows_in(c, net.core)
            h_buf[b, c] = (x_all[rows_out(b, c, net.core), :].astype(F32) + (part[b, own, :] + got[b, c])).astype(BF16)
            h_copy(b, c, net.core).start()
            h_local(b, c).start()

        repeat(chunks, body)

    def settle():
        for b in range(batch):
            for c in range(chunks):
                h_copy(b, c, net.core).wait_send()
                h_local(b, c).wait()
                h_copy(b, c, 1 - net.core).wait_recv()
        for i in range(CHUNK_STEPS):
            save(i).wait()
        save_weight.wait()

    fetch = pltpu.make_async_copy(wo_hbm, wo, h_sem.at[0, 0])
    run_at(last - step, [(2, fetch.start), (2, save_weight.start), (1, fetch.wait), (0, functools.partial(combine, 0))])

    @pl.when(step + 1 >= last)
    def _():
        project(step + 1 - last)

    run_at(last - step, [(0, functools.partial(combine, 1)), (0, settle)])
    run_at(turn + 1, begin[-1:])


def front(x, qkv_shard, out_shard, ff_shard, down_shard, table, batch, seq, collective_id):
    pairs = len(out_shard) // 2
    rows, d = x.shape
    width = 3 * LANES
    chunks = seq // CHUNK
    vm = pltpu.VMEM
    torus = (SIDE, SIDE, SIDE, PIECE)
    shards = [s.size // PIECE for s in (qkv_shard, out_shard, ff_shard, down_shard)]
    turn = lambda s: jnp.maximum(s - 1, 0)
    head = lambda width: pl.BlockSpec((seq, width), lambda s: (turn(s) % batch, turn(s) // batch))
    return pl.pallas_call(
        front_kernel,
        grid=(1 + batch * pairs,),
        in_specs=[HBM] + [WHOLE] * 5,
        out_specs=[head(width), head(width), head(LANES), pl.BlockSpec((1, 1, 2, seq), lambda s: (turn(s) % batch, turn(s) // batch, 0, 0))] + [HBM] * 5,
        out_shape=[shape(BF16, rows, width * pairs)] * 2 + [shape(BF16, rows, LANES * pairs), shape(F32, batch, pairs, 2, seq), shape(BF16, rows, d), shape(BF16, rows, d),
                   shape(BF16, *torus, shards[0]), shape(BF16, *torus, shards[1]), shape(BF16, *torus, shards[2] + shards[3])],
        scratch_shapes=[vm((rows, d), BF16), vm((rows, d), BF16), vm(torus + (width * pairs,), BF16), vm((PIECE, sum(shards)), BF16),
                        vm((batch, pairs, seq, LANES), BF16), vm((batch, seq, d), F32), vm((batch, chunks, CHUNK // 2, d), F32), vm((batch, chunks, CHUNK // 2, d), BF16),
                        vm(torus + (shards[1],), BF16), dma(2, 2, batch, chunks), dma(2, (pairs + 2) * Gather.SEMS), dma(CHUNK_STEPS + 1), dma(batch, chunks)] + [vm((seq, LANES), F32)] * 2 + [vm((seq, LANES * pairs), BF16)],
        compiler_params=params(collective_id),
        name='front',
    )(x, qkv_shard, out_shard, ff_shard, down_shard, table)


class Exchange:
    def __init__(self, net, rows, partials, results, sems, local_sem):
        self.net, self.rows, self.partials, self.results, self.sems, self.local_sem = net, rows, partials, results, sems, local_sem

    def half(self, core, at=0):
        return aligned(at * self.rows + core * (self.rows // 2), self.rows // 2)

    def part(self, which, at):
        part, got = self.partials[which]
        return to_partner(self.net, part.at[at % 2, self.half(1 - self.net.core)], got.at[at], *pair_of(self.sems, which, at))

    def total(self, which, at):
        part, got = self.partials[which]
        self.part(which, at).wait()
        return part[at % 2, self.half(self.net.core), :] + got[at]

    def results_of(self, at, core, act):
        for i, (buf, hbm) in enumerate(self.results):
            act(buf.at[at % 2], hbm.at[self.half(core, at)], pair_of(self.sems, len(self.partials) + i, at), self.local_sem.at[i, at % 2])

    def publish(self, at):
        def act(buf, rows, sem, local_sem):
            to_partner(self.net, buf, rows, *sem).start()
            pltpu.make_async_copy(buf, rows, local_sem).start()
        self.results_of(at, self.net.core, act)

    def settle(self, at):
        def act(buf, rows, sem, local_sem):
            to_partner(self.net, buf, rows, *sem).wait_send()
            pltpu.make_async_copy(buf, rows, local_sem).wait()
        self.results_of(at, self.net.core, act)
        self.results_of(at, 1 - self.net.core, lambda buf, rows, sem, local_sem: to_partner(self.net, buf, rows, *sem).wait_recv())


def mlp_kernel(blocks, h_ref, gy_ref, wff_ref, wd_ref, y_hbm, gh_hbm, gh32_ref, acts_hbm, n2_ref, gd_hbm,
               saved, grad_down, part_y, part_g, got_y, got_g, y_buf, gh_buf, h_own, gy_own, sems, local_sem, save_sem):
    step, final = grid_step()
    rows, d = h_ref.shape
    ff = wd_ref.shape[1]
    acts = saved.at[step % 2]
    gug, act = acts.at[:, pl.ds(0, 2 * ff)], acts.at[:, pl.ds(2 * ff, ff)]

    def save(at):
        return pltpu.make_async_copy(saved.at[at % 2], acts_hbm.at[aligned(at * rows, rows)], save_sem.at[at % 2])

    save_grad = pltpu.make_async_copy(grad_down, gd_hbm, save_sem.at[2])
    net = Torus()
    swap = Exchange(net, rows, ((part_y, got_y), (part_g, got_g)), ((y_buf, y_hbm), (gh_buf, gh_hbm)), sems, local_sem)

    @pl.when(step == 0)
    def _():
        net.barrier([net.partner])

    @pl.when((step > 1) & (step < blocks))
    def _():
        save(step - 2).wait()

    @pl.when(step < blocks)
    def _():
        n2, _ = norm_rows(h_ref[...].astype(F32))
        n2 = n2.astype(BF16)
        n2_ref[...] = n2
        gy = gy_ref[...]
        for j in strips(ff, QB):
            w = min(QB, ff - j)
            gact = nn(gy, wd_ref[:, j:j + w])
            for i in range(j, j + w, LANES):
                at, mid, end = 2 * i, 2 * i + LANES, 2 * i + QB
                ug = nn(n2, wff_ref[:, at:end])
                up, gate = ug[:, :LANES], ug[:, LANES:]
                sig = 1.0 / (1.0 + jnp.exp(-gate))
                silu = gate * sig
                act[:, i:i + LANES] = (silu * up).astype(BF16)
                ga = gact[:, i - j:i - j + LANES]
                gug[:, at:mid] = (ga * silu).astype(BF16)
                gug[:, mid:end] = (ga * up * sig * (1.0 + gate * (1.0 - sig))).astype(BF16)

        for which, left, right, part in ((0, act, wd_ref, part_y), (1, gug, wff_ref, part_g)):
            for j in strips(d, QB):
                part[step % 2, :, j:j + QB] = nt(left[...], right[j:j + QB, :])
            swap.part(which, step).start()
        save(step).start()
        accumulate(grad_down, step == 0, gy, act)

    @pl.when(step == blocks - 1)
    def _():
        save_grad.start()

    @pl.when(step > 2)
    def _():
        swap.settle(step - 3)

    @pl.when(step > 0)
    def _():
        done = step - 1
        hidden = h_own[...].astype(F32)
        normed, inv = norm_rows(hidden)
        y_buf[done % 2] = (hidden + swap.total(0, done)).astype(BF16)
        gh = gy_own[...].astype(F32) + norm_grad(swap.total(1, done), normed, inv)
        gh32_ref[...] = gh
        gh_buf[done % 2] = gh.astype(BF16)
        swap.publish(done)

    own = swap.half(net.core)
    h_own[...] = h_ref[own, :]
    gy_own[...] = gy_ref[own, :]

    @pl.when(step == blocks)
    def _():
        for at in (blocks - 2, blocks - 1):
            swap.settle(at)
            save(at).wait()
        save_grad.wait()


def mlp(h, gy, weights, collective_id, block=BLOCK):
    rows, d = h.shape
    ff = weights.shape[1] // 3
    half = block // 2
    blocks = rows // block
    torus = (SIDE, SIDE, SIDE, PIECE)
    row = lambda width: rows_of(block, width, lambda i: jnp.minimum(i, blocks - 1))
    vm = pltpu.VMEM
    return pl.pallas_call(
        functools.partial(mlp_kernel, blocks),
        grid=(blocks + 1,),
        in_specs=[row(d), row(d), fixed((d, 2 * ff)), fixed((d, ff), (0, 2))],
        out_specs=[HBM, HBM, rows_of(half, d, lambda i: jnp.maximum(i - 1, 0)), HBM, row(d), HBM],
        out_shape=[shape(BF16, rows, d), shape(BF16, rows, d), shape(F32, rows // 2, d), shape(BF16, rows, 3 * ff), shape(BF16, rows, d), shape(F32, *torus, ff)],
        scratch_shapes=[vm((2, block, 3 * ff), BF16), vm(torus + (ff,), F32)] + [vm((2, block, d), F32)] * 2 + [vm((blocks, half, d), F32)] * 2 + [vm((2, half, d), BF16)] * 2 + [vm((half, d), BF16)] * 2 + [dma(2, 4, blocks), dma(2, 2), dma(3)],
        compiler_params=params(collective_id),
        name='mlp',
    )(h, gy, weights, weights)


def accumulate(part, first, left, right):
    for j in strips(right.shape[1], QB):
        w = min(QB, right.shape[1] - j)
        prod = tn(left, right[:, j:j + w]).reshape(part.shape[:-1] + (w,))
        at = slice(j, j + w)
        part[..., at] = jnp.where(first, 0.0, part[..., at]) + prod


SETS = 3
HEAD_STEP = (SETS - 1) * CHUNK_STEPS


def back_kernel(pairs, gd_hbm, n2_ref, act_ref, qkv_ref, lse_ref, gh_ref, wo_ref, o_ref, keep_ref, table_ref,
                g_ref, gw_ref, gd_ref, gff_ref, cos_ref, sin_ref, do_ref, dk_ref, dv_ref, parts, sems, load_sem, *bufs):
    step, final = grid_step()
    turn = step - HEAD_STEP
    p = turn % pairs
    half = gh_ref.shape[0] // 2
    net = Torus()
    per = len(bufs) // SETS
    scatters = [Scatter(net, parts.at[i], cut_three(parts.shape[-1], turn=i), bufs[per * i:per * i + per], sems, i * Scatter.SEMS) for i in range(SETS)]
    calls = plan(SCATTER_PLAN, *(s.stages() for s in scatters))
    begin, end = halves_of(calls, HEAD_STEP + 1)

    @pl.when(step == 0)
    def _():
        load = pltpu.make_async_copy(gd_hbm, parts.at[0], load_sem.at[0])
        load.start()
        spread_tables(table_ref, cos_ref, sin_ref)
        net.barrier(net.neighbours())
        load.wait()
        for when, call in calls:
            if not when:
                call()

    @pl.when(turn < 0)
    def _():
        accumulate(parts.at[1 + step // CHUNK_STEPS], step % CHUNK_STEPS == 0, n2_ref[...], act_ref)

    run_at(step + 1, [c for c in calls if 0 < c[0] <= HEAD_STEP])

    def put(part, lo, hi, values):
        cols = lanes(part)
        if part < 2:
            values = values * cos_ref[lo:hi, :] - swap_halves(values) * sin_ref[lo:hi, :]
        g_ref[lo:hi, cols] = (values * keep_ref[lo:hi, cols].astype(F32)).astype(BF16)

    def put_dq(lo, hi, dq):
        put(0, lo, hi, dq * 0.125)

    @pl.when(turn >= 0)
    def _():
        @pl.when(p == 0)
        def _():
            gw_ref[...] = jnp.where(turn == 0, 0.0, gw_ref[...])

            def body(i):
                rows = aligned(i * half, half)
                gh = gh_ref[rows, :]
                dout = nn(gh, wo_ref[...]).astype(BF16)
                for j in range(pairs):
                    do_ref[j, rows, :] = dout[:, lanes(j)]
                gw_ref[...] += tn(gh, o_ref[rows, :])

            repeat(len(TWO), body)

        run_at(turn, begin)
        q_ref, k_ref, v_ref = (qkv_ref.at[:, pl.ds(LANES * i, LANES)] for i in THREE)
        attend_pair_back(q_ref, k_ref, v_ref, do_ref.at[p], lse_ref.at[0, 0], dk_ref, dv_ref, put_dq)
        seq = q_ref.shape[0]
        put(1, 0, seq, dk_ref[...])
        put(2, 0, seq, dv_ref[...])
        run_at(turn, end)

    @pl.when(step == final)
    def _():
        gd_ref[...], *halves = [s.result() for s in scatters]
        tiles = jnp.concatenate(halves, axis=1)
        for i in strips(tiles.shape[1], LANES):
            at = i // QB * LANES
            gff_ref[:, i // LANES % 2, at:at + LANES] = tiles[:, i:i + LANES]


def back(gd, n2, acts, qkv, lse, gh, wo_t, o, keep, table, batch, seq, pairs, collective_id):
    rows, d = n2.shape
    ff = acts.shape[1] // SETS
    block = rows // CHUNK_STEPS
    turn = lambda s: jnp.maximum(s - HEAD_STEP, 0)
    head = pl.BlockSpec((seq, 3 * LANES), lambda s: (turn(s) // pairs, turn(s) % pairs))
    late = lambda s: jnp.where(s < HEAD_STEP, s % CHUNK_STEPS, CHUNK_STEPS - 1)
    vm = pltpu.VMEM
    per_seq = lambda width: rows_of(seq, width, lambda s: turn(s) // pairs)
    return pl.pallas_call(
        functools.partial(back_kernel, pairs),
        grid=(HEAD_STEP + batch * pairs,),
        in_specs=[HBM, rows_of(block, d, late), pl.BlockSpec((block, ff), lambda s: (late(s), jnp.minimum(s // CHUNK_STEPS, 1))), head, pl.BlockSpec((1, 1, 2, seq), lambda s: (turn(s) // pairs, turn(s) % pairs, 0, 0)),
                  per_seq(d), fixed(wo_t.shape), per_seq(LANES * pairs), head, WHOLE],
        out_specs=[head, fixed(wo_t.shape), WHOLE, WHOLE],
        out_shape=[shape(BF16, *qkv.shape), shape(F32, *wo_t.shape), shape(F32, PIECE, ff), shape(F32, PIECE, 2, ff)],
        scratch_shapes=[vm((seq, LANES), F32)] * 2 + [vm((pairs, seq, LANES), BF16)] + [vm((seq, LANES), F32)] * 2 + [vm((SETS, SIDE, SIDE, SIDE, PIECE, ff), F32),
                        dma(2, SETS * Scatter.SEMS), dma(1)] + [s for i in range(SETS) for s in Scatter.scratch(cut_three(ff, turn=i))],
        compiler_params=params(collective_id),
        name='back',
    )(gd, n2, acts, qkv, lse, gh, wo_t, o, keep, table)


def last_kernel(pairs, blocks, n1_ref, g_ref, x_ref, g_row, gh_ref, w_ref, gout_hbm, gx_hbm, gout_ref, gw_ref,
                part_out, part_qkv, part, got, buf, sems, scatter_sems, local_sem, *bufs):
    step, final = grid_step()
    turn = step - pairs
    rows, d = x_ref.shape
    net = Torus()
    per = len(bufs) // (pairs + 1)
    parts = [part_out] + [part_qkv.at[j] for j in range(pairs)]
    scatters = [Scatter(net, s, cut_three(s.shape[-1], turn=i), bufs[per * i:per * i + per], scatter_sems, i * Scatter.SEMS, 1 if i > pairs // 2 else len(PHASES)) for i, s in enumerate(parts)]
    calls = plan(LAST_PLAN, *(s.stages() for s in scatters))
    swap = Exchange(net, rows, ((part, got),), ((buf, gx_hbm),), sems, local_sem)

    @pl.when(step == 0)
    def _():
        load = pltpu.make_async_copy(gout_hbm, part_out, local_sem.at[1, 0])
        load.start()
        net.barrier(net.neighbours(2) + [net.partner])
        load.wait()

    begin, end = halves_of(calls)
    run_at(step, begin)

    @pl.when(turn < 0)
    def _():
        size = n1_ref.shape[0] // len(TWO)

        def body(i):
            accumulate(part_qkv.at[step], i == 0, n1_ref[aligned(i * size, size), :], g_ref.at[aligned(i * size, size)])

        repeat(len(TWO), body)

    @pl.when((turn >= 0) & (turn < blocks))
    def _():
        for j in strips(d, QB):
            part[turn % 2, :, j:j + QB] = nt(g_row[...], w_ref[j:j + QB, :])
        swap.part(0, turn).start()

    run_at(step, end)

    @pl.when(turn > 2)
    def _():
        swap.settle(turn - 3)

    @pl.when(turn > 0)
    def _():
        done = turn - 1
        normed, inv = norm_rows(x_ref[swap.half(net.core), :].astype(F32))
        buf[done % 2] = (gh_ref[...] + norm_grad(swap.total(0, done), normed, inv)).astype(BF16)
        swap.publish(done)

    @pl.when(turn == blocks)
    def _():
        for when, call in calls:
            if when > 2 * (pairs + blocks) + 1:
                call()
        for at in (blocks - 2, blocks - 1):
            swap.settle(at)
        out, *sums = [s.result() for s in scatters]
        halves = slice(HALF), slice(HALF, LANES)
        for j in range(pairs):
            for h, cols in enumerate(halves):
                gout_ref[2 * j + h] = out[:, lanes(j)][:, cols]
        for i in THREE:
            tiles = [swap_middle(s[:, lanes(i)]) if i < 2 else s[:, lanes(i)] for s in sums]
            gw_ref[:, i] = jnp.stack([t[:, cols] for t in tiles for cols in halves]).swapaxes(0, 1)


def last(x, n1, g, gh32, w, gout, pairs, collective_id, block=BLOCK):
    rows, d = x.shape
    blocks = rows // block
    late = lambda n, width, by: rows_of(n, width, lambda s: jnp.clip(s - pairs - by, 0, blocks - 1))
    head = pl.BlockSpec((rows, 3 * LANES), lambda s: (0, jnp.minimum(s, pairs - 1)))
    vm = pltpu.VMEM
    half = block // 2
    torus = (SIDE, SIDE, SIDE, PIECE)
    gout = gout.reshape(torus + (-1,))
    return pl.pallas_call(
        functools.partial(last_kernel, pairs, blocks),
        grid=(pairs + blocks + 1,),
        in_specs=[fixed((rows, d)), head, late(block, d, 1), late(block, g.shape[1], 0), late(half, d, 1), fixed(w.shape), HBM],
        out_specs=[HBM, WHOLE, WHOLE],
        out_shape=[shape(BF16, rows, d), shape(F32, 2 * pairs, PIECE, HALF), shape(F32, PIECE, 3, 2 * pairs, HALF)],
        scratch_shapes=[vm(gout.shape, F32), vm((pairs,) + torus + (3 * LANES,), F32), vm((2, block, d), F32), vm((blocks, half, d), F32), vm((2, half, d), BF16),
                        dma(2, 2, blocks), dma(2, (pairs + 1) * Scatter.SEMS), dma(2, 2)] + Scatter.scratch(cut_three(gout.shape[-1])) + Scatter.scratch(cut_three(3 * LANES)) * pairs,
        compiler_params=params(collective_id),
        name='last',
    )(n1, g, x, g, gh32, w, gout)


def hand_over_kernel(*refs):
    count = len(refs) // 2
    for src, dst in zip(refs[:count], refs[count:]):
        dst[...] = src[...]


def hand_over(wide, small, block=BLOCK):
    rows, width = wide[0].shape
    specs = [rows_of(block, width, lambda i: i) for v in wide] + [WHOLE for v in small]
    return pl.pallas_call(
        hand_over_kernel,
        grid=(rows // block,),
        in_specs=specs,
        out_specs=specs,
        out_shape=[shape(v.dtype, *v.shape) for v in wide + small],
        name='hand_over',
    )(*wide, *small)


def device_step(x, grad_y, w_qkv, w_out, w_ff, w_down):
    batch, seq, d = x.shape
    heads, head = w_qkv.shape[2:]
    pairs = heads // 2
    table = jnp.asarray(tables(seq, head))
    ids = iter(range(4))
    x2, gy = (v.reshape(batch * seq, d) for v in (x, grad_y))
    qkv, keep, o, lse, h, n1, *weights = front(x2, w_qkv, w_out.swapaxes(1, 2), w_ff, w_down.T, table, batch, seq, next(ids))
    wq, wo_t, wf = (w.reshape(d, w.shape[-1]) for w in weights)
    y, gh, gh32, acts, n2, gd = mlp(h, gy, wf, next(ids))
    g, gout, gd, gff = back(gd, n2, acts, qkv, lse, gh, wo_t, o, keep, table, batch, seq, pairs, next(ids))
    gx, gout, gqkv = last(x2, n1, g, gh32, wq, gout, pairs, next(ids))
    y, gx, gqkv, gout, gff, gd = hand_over([y, gx], [gqkv, gout, gff, gd])
    return y.reshape(x.shape), gx.reshape(x.shape), gqkv, gout.swapaxes(1, 2), gff, gd.T


def solution(mesh):
    specs = (P('fsdp'), P('fsdp'), P('fsdp', None, 'tp'), P('tp', None, 'fsdp'), P('fsdp', None, 'tp'), P('tp', 'fsdp'))
    return jax.shard_map(device_step, mesh=mesh, in_specs=specs, out_specs=specs, check_vma=False)
```

```python
import functools

import jax
import jax.numpy as jnp
import numpy as np
from jax import lax
from jax.experimental import pallas as pl
from jax.experimental.pallas import tpu as pltpu
from jax.sharding import PartitionSpec as P

MESH_ID = pl.DeviceIdType.MESH
SIDE = 4
TILE = 128
PIECE = 16
ORDERS = ((2, 1, 0), (1, 0, 2), (0, 2, 1))
BOTH = ((0, 1), (1, -1))
PHASES = THREE = range(3)
TWO = range(2)


class Torus:
    def __init__(self):
        self.core = lax.axis_index('tp')
        self.index = lax.axis_index('fsdp')
        plane, x = lax.div(self.index, SIDE), lax.rem(self.index, SIDE)
        self.at = (lax.div(plane, SIDE), lax.rem(plane, SIDE), x)
        self.partner = (1 - self.core, self.index)
        self.moved = {(axis, by): lax.rem(at + (by + SIDE), SIDE) for axis, at in enumerate(self.at) for by in range(-2, 3)}
        self.peers = {(axis, by): self.place(axis, self.moved[axis, by]) for axis in THREE for by in (-1, 1, 2)}

    def place(self, axis, coord):
        pos = list(self.at)
        pos[axis] = coord
        z, y, x = pos
        return (self.core, (z * SIDE + y) * SIDE + x)

    def shift(self, axis, by):
        return self.moved[axis, by]

    def peer(self, axis, by):
        return self.peers[axis, by]

    def neighbours(self, reach=1):
        return [device for (_, by), device in self.peers.items() if by <= reach]

    def tell(self, sem, devices):
        for device in devices:
            pl.semaphore_signal(sem, inc=1, device_id=device, device_id_type=MESH_ID)

    def barrier(self, devices):
        sem = pltpu.get_barrier_semaphore()
        self.tell(sem, devices)
        pl.semaphore_wait(sem, len(devices))


def pair_of(sems, *at):
    return sems.at[(0,) + at], sems.at[(1,) + at]


def in_order(*calls):
    def run():
        for call in calls:
            call()
    return run


def span(cols):
    (off, width), *rest = cols
    return pl.ds(off, width + sum(w for _, w in rest))


class Gather:
    SEMS = 7

    def __init__(self, net, shard, out, cols, shift, sems, first, direct=False):
        self.net, self.shard, self.out, self.cols, self.moved, self.sems, self.first, self.direct = net, shard, out, cols, shift, sems, first, direct

    def block(self, colour, phase, coord, half=None):
        order = ORDERS[colour]
        off, width = self.cols[colour]
        pick = list(self.net.at)
        for axis in order[:phase]:
            pick[axis] = pl.ds(0, SIDE)
        pick[order[phase]] = coord
        if half is not None and phase:
            pick[order[0]] = pl.ds(half * 2, 2)
        elif half is not None:
            cut = width - width // (2 * TILE) * TILE
            off, width = (off + cut, width - cut) if half else (off, cut)
        return self.out.at[(*pick, slice(None), pl.ds(off, width))] if width else None

    def copy(self, phase, colour, relay, d, by):
        axis = ORDERS[colour][phase]
        far = relay and self.direct
        if far and d:
            return None
        by = 2 if far else by
        back = -by if relay and not far else 0
        dst = src = self.block(colour, phase, self.net.shift(axis, back), d if relay and not far else None)
        if dst is None:
            return None
        if not phase and (far or not relay):
            off, width = self.cols[colour]
            src = self.shard.at[:, pl.ds(off + self.moved, width)]
        return pltpu.make_async_remote_copy(src, dst, *self.sem(phase, relay), device_id=self.net.peer(axis, by), device_id_type=MESH_ID)

    def sem(self, phase, relay):
        return pair_of(self.sems, self.first + 2 * phase + relay)

    def each(self, phase, relay):
        for d, by in BOTH:
            for colour in THREE:
                desc = self.copy(phase, colour, relay, d, by)
                if desc is not None:
                    desc.start()

    def wait(self, phase, relay, side):
        pick = [pl.ds(0, SIDE)] * phase + [pl.ds(0, 2 - relay)] + [0, 0]
        ref = self.out.at[tuple(reversed(pick[:3])) + (slice(None), span(self.cols))]
        pltpu.make_async_copy(ref, ref, self.sem(phase, relay)[side]).wait()

    def own(self):
        at = self.net.at
        cols = span(self.cols)
        src = self.shard.at[:, pl.ds(cols.start + self.moved, cols.size)]
        return pltpu.make_async_copy(src, self.out.at[(*at, slice(None), cols)], self.sems.at[0, self.first + self.SEMS - 1])

    def arrive(self, phase):
        if self.direct:
            self.wait(phase, 0, 1)
        self.wait(phase, 1, 1)

    def start(self, phase):
        if phase:
            self.arrive(phase - 1)
        if phase == 1:
            self.own().wait()
        for relay in range(1 + self.direct):
            self.each(phase, relay)
        if not phase:
            self.own().start()

    def relay(self, phase):
        self.wait(phase, 0, 1)
        self.each(phase, 1)

    def finish(self):
        self.arrive(PHASES[-1])
        for phase in PHASES:
            for relay in TWO:
                self.wait(phase, relay, 0)

    def stages(self):
        steps = (self.start,) if self.direct else (self.start, self.relay)
        return [functools.partial(f, p) for p in PHASES for f in steps] + [self.finish]


class Scatter:
    SEMS = 9

    def __init__(self, net, part, cols, bufs, sems, first, relays=len(PHASES)):
        self.net, self.part, self.cols, self.bufs, self.sems, self.first, self.relays = net, part, cols, bufs, sems, first, relays

    @staticmethod
    def scratch(cols):
        shapes = []
        for _, w in cols:
            shapes += [(3, 2, 2, SIDE, PIECE, w), (3, 2, 2, PIECE, w), (3, 2, PIECE // 2, w)]
        return [pltpu.VMEM(s, jnp.float32) for s in shapes]

    def buf(self, colour, phase):
        return self.bufs[colour * len(PHASES) + phase]

    def block(self, colour, phase, coord, half):
        order = ORDERS[colour]
        off, width = self.cols[colour]
        pick = [pl.ds(0, SIDE)] * 3
        for axis in order[:phase]:
            pick[axis] = self.net.at[axis]
        pick[order[phase]] = coord
        rows = pl.ds(0, PIECE)
        rest = sorted(order[phase + 1:])
        if rest:
            pick[rest[0]] = pl.ds(2 * half, 2)
        else:
            rows = pl.ds(PIECE // 2 * half, PIECE // 2)
        return self.part.at[(*pick, rows, pl.ds(off, width))]

    def copy(self, phase, colour, kind, d, by):
        axis = ORDERS[colour][phase]
        buf = self.buf(colour, phase)
        direct = phase >= self.relays
        if kind == 2 and not direct:
            src = buf.at[0, d]
        elif kind:
            src = self.block(colour, phase, self.net.shift(axis, by), (kind + d) % 2)
        else:
            src = self.block(colour, phase, self.net.shift(axis, 2), d)
            by = 2 if direct else by
        return pltpu.make_async_remote_copy(src, buf.at[kind, d], *self.sem(phase, kind), device_id=self.net.peer(axis, by), device_id_type=MESH_ID)

    def sem(self, phase, kind):
        return pair_of(self.sems, self.first + len(PHASES) * phase + kind)

    def wait(self, phase, kind, side):
        pick = [0] * (phase + 1) + [pl.ds(0, SIDE)] * (2 - phase)
        ref = self.part.at[tuple(pick) + (slice(None), span(self.cols))]
        pltpu.make_async_copy(ref, ref, self.sem(phase, kind)[side]).wait()

    def start(self, phase, kind):
        for d, by in BOTH:
            for colour in THREE:
                self.copy(phase, colour, kind, d, by).start()

    def relay(self, phase):
        self.wait(phase, 0, 1)
        for colour in THREE:
            buf = self.buf(colour, phase)
            for d, by in BOTH:
                buf[0, d] = buf[0, d] + self.block(colour, phase, self.net.shift(ORDERS[colour][phase], by), d)[...]
        self.start(phase, 2)

    def merge(self, phase):
        direct = phase >= self.relays
        for kind in THREE if direct else (1, 2):
            self.wait(phase, kind, 1)
        for colour in THREE:
            buf = self.buf(colour, phase)
            for half in TWO:
                mine = self.block(colour, phase, self.net.at[ORDERS[colour][phase]], half)
                sums = mine[...] + buf[1, 1 - half] + buf[2, half]
                mine[...] = sums + buf[0, half] if direct else sums
        if phase < PHASES[-1]:
            for kind in TWO if phase + 1 < self.relays else THREE:
                self.start(phase + 1, kind)

    def finish(self):
        for phase in PHASES:
            for kind in PHASES:
                self.wait(phase, kind, 0)

    def stages(self):
        calls = [functools.partial(self.start, 0, kind) for kind in TWO]
        for phase in PHASES:
            calls += [functools.partial(self.relay, phase)] * (phase < self.relays) + [functools.partial(self.merge, phase)]
        return calls[:-1] + [in_order(calls[-1], self.finish)]

    def result(self):
        return self.part[self.net.at]


def cut_three(width, off=0, turn=0):
    tiles, ways = width // TILE, len(THREE)
    sizes = [(tiles + (turn - i - 1) % ways) // ways * TILE for i in THREE]
    return [(off + sum(sizes[:i]), s) for i, s in enumerate(sizes)]


def plan(text, *sets):
    left = [iter(s) for s in sets]
    return [(hook, next(left[int(which)])) for hook, field in enumerate(text.split(',')) for which in field]


def halves_of(calls, first=0):
    return [[((when - first) // 2, call) for when, call in calls if when >= first and (when - first) % 2 == odd] for odd in TWO]


def run_at(hook, calls):
    for when, call in calls:
        pl.when(hook == when)(call)


F32, BF16 = jnp.float32, jnp.bfloat16
QB = 256
LANES = TILE
HALF = LANES // 2
CLIP = 8.0
BLOCK = 512
MIB = 2**20


def nt(a, b):
    return lax.dot_general(a, b, (((1,), (1,)), ((), ())), preferred_element_type=F32)


def nn(a, b):
    return jnp.dot(a, b, preferred_element_type=F32)


def tn(a, b):
    return lax.dot_general(a, b, (((0,), (0,)), ((), ())), preferred_element_type=F32)


def along(reduce, values):
    return reduce(values, axis=-1, keepdims=True)


def head_masks(paired):
    lane = lax.broadcasted_iota(jnp.int32, (1, LANES), 1)
    first = lane % HALF < HALF // 2 if paired else lane < HALF
    return first, jnp.logical_not(first)


def causal_tile(key_axis):
    dims = (QB, 2 * QB) if key_axis == 0 else (2 * QB, QB)
    return lax.broadcasted_iota(jnp.int32, dims, key_axis) <= lax.broadcasted_iota(jnp.int32, dims, 1 - key_axis) % QB


def by_head(values, masks):
    return jnp.concatenate([jnp.where(m, values, jnp.zeros((), BF16)) for m in masks], axis=0)


def attend_pair(q_ref, k_ref, v_ref, o_ref, lse_ref):
    masks = head_masks(True)
    key, val = k_ref[...], v_ref[...]
    causal = causal_tile(1)
    first, _ = head_masks(False)
    for lo in reversed(strips(q_ref.shape[0], QB)):
        hi = lo + QB
        query = by_head(q_ref[lo:hi, :], masks)
        diag = jnp.where(causal, nt(query, key[lo:hi]), -1e30)
        top = along(jnp.max, diag)
        if lo:
            past = nt(query, key[:lo])
            top = jnp.maximum(top, along(jnp.max, past))
            past = jnp.exp(past - top)
        diag = jnp.exp(diag - top)
        total = along(jnp.sum, diag)
        if lo:
            total = total + along(jnp.sum, past)
        scale = 1.0 / total
        acc = nn((diag * scale).astype(BF16), val[lo:hi])
        if lo:
            acc = acc + nn((past * scale).astype(BF16), val[:lo])
        o_ref[lo:hi, :] = jnp.where(first, acc[:QB], acc[QB:]).astype(BF16)
        lse = jnp.broadcast_to(top + jnp.log(total), acc.shape).T
        for h in TWO:
            lse_ref[h:h + 1, lo:hi] = lse[:1, h * QB:(h + 1) * QB]


def attend_pair_back(q_ref, k_ref, v_ref, do_ref, lse_ref, dk_ref, dv_ref, put_dq):
    seq = q_ref.shape[0]
    qmask, vmask = head_masks(True), head_masks(False)
    key, val = k_ref[...], v_ref[...]
    key_t = key.astype(F32).T.astype(BF16)
    causal = causal_tile(0)
    first = lax.broadcasted_iota(jnp.int32, (LANES, 1), 0) % HALF < HALF // 2

    def products(lo):
        hi = lo + QB
        query, dout = by_head(q_ref[lo:hi, :], qmask), by_head(do_ref[lo:hi, :], vmask)
        return query, dout, nt(key[:hi], query), nt(val[:hi], dout)

    ahead = products(seq - QB)
    for lo in reversed(strips(seq, QB)):
        hi = lo + QB
        query, dout, score, grad = ahead
        if lo:
            ahead = products(lo - QB)
        prob = jnp.exp(score - jnp.concatenate([lse_ref[h:h + 1, lo:hi] for h in TWO], axis=1))
        diag = jnp.where(causal, prob[lo:], 0.0)
        prob = jnp.concatenate([prob[:lo], diag], axis=0) if lo else diag
        ds = (prob * (grad - jnp.sum(prob * grad, axis=0, keepdims=True))).astype(BF16)
        both = nn(key_t[:, :hi], ds)
        put_dq(lo, hi, jnp.where(first, both[:, :QB], both[:, QB:]).T)
        dv, dk = nn(prob.astype(BF16), dout), nn(ds, query)
        if hi == seq:
            dv_ref[...] = dv
            dk_ref[...] = dk
        else:
            dv_ref[:hi, :] += dv
            dk_ref[:hi, :] += dk


def swap_halves(values):
    return pltpu.roll(values, HALF, axis=1)


COARSE = 32


def tables(seq, head):
    freq = 10000.0 ** (-np.arange(0, head, 2, dtype=np.float64) / head)
    angles = [np.tile(np.arange(seq // COARSE)[:, None] * step * freq, LANES // len(freq)) for step in (1, COARSE)]
    return np.stack([np.stack([np.cos(angle), np.sin(angle)]) for angle in angles]).astype(np.float32)


def spread_tables(table_ref, cos_ref, sin_ref):
    fine_cos, fine_sin = table_ref[0]
    sign = jnp.where(lax.broadcasted_iota(jnp.int32, (1, LANES), 1) < HALF, -1.0, 1.0)

    def body(i):
        rows = aligned(i * COARSE, COARSE)
        cos, sin = table_ref[1, :, pl.ds(i, 1), :]
        cos_ref[rows, :] = fine_cos * cos - fine_sin * sin
        sin_ref[rows, :] = (fine_sin * cos + fine_cos * sin) * sign

    repeat(cos_ref.shape[0] // COARSE, body)


def repeat(count, body):
    def step(i, carry):
        body(i)
        return carry

    lax.fori_loop(0, count, step, 0)


def side_by_side(halves, j):
    return jnp.concatenate([halves[2 * j], halves[2 * j + 1]], axis=1)


def aligned(at, size):
    return pl.ds(pl.multiple_of(at, size), size)


def norm_rows(values):
    mean = along(jnp.mean, values)
    centered = values - mean
    inv = lax.rsqrt(along(jnp.mean, centered * centered) + 1e-5)
    return centered * inv, inv


def norm_grad(grad, normed, inv):
    mean = along(jnp.mean, grad)
    proj = along(jnp.mean, grad * normed)
    return inv * (grad - mean - normed * proj)


def params(collective_id):
    return pltpu.CompilerParams(collective_id=collective_id, has_side_effects=True, vmem_limit_bytes=63 * MIB)


def grid_step():
    return pl.program_id(0), pl.num_programs(0) - 1


def dma(*shape):
    return pltpu.SemaphoreType.DMA(shape)


def shape(dtype, *dims):
    return jax.ShapeDtypeStruct(dims, dtype)


HBM = pl.BlockSpec(memory_space=pltpu.HBM)
WHOLE = pl.BlockSpec(memory_space=pltpu.VMEM)


def lanes(part):
    return slice(LANES * part, LANES * (part + 1))


def strips(width, size):
    return range(0, width, size)


def rows_of(size, width, index):
    return pl.BlockSpec((size, width), lambda step: (index(step), 0))


def stats_rows(seq, index):
    return pl.BlockSpec((1, 1, 2, seq), lambda step: (*index(step), 0, 0))


def project_pair(n1_ref, weight, cos_ref, sin_ref, qkv_ref, keep_ref):
    for lo in strips(n1_ref.shape[0], QB):
        rows = slice(lo, lo + QB)
        raw = nn(n1_ref[rows, :], weight)
        keep_ref[rows, :] = (jnp.abs(raw) < CLIP).astype(F32).astype(BF16)
        raw = jnp.clip(raw, -CLIP, CLIP)
        for part in THREE:
            cols = lanes(part)
            tile = raw[:, cols]
            if part < 2:
                tile = tile * cos_ref[rows, :] + swap_halves(tile) * sin_ref[rows, :]
            if not part:
                tile = tile * 0.125
            qkv_ref[rows, cols] = tile.astype(BF16)


def swap_middle(tile):
    quarter = lax.broadcasted_iota(jnp.int32, tile.shape, 1) // (LANES // 4)
    up, down = pltpu.roll(tile, LANES // 4, axis=1), pltpu.roll(tile, LANES - LANES // 4, axis=1)
    return jnp.where(quarter == 1, down, jnp.where(quarter == 2, up, tile))


CHUNK = 256
CHUNK_STEPS = 4
FRONT_PLAN = '014560145260512430,,24,45,13,,345,,24,,,,3,,,5,,5'
SCATTER_PLAN = '00,,,,,1,1,,2,0,,,2,12,0,,,,12,0,1,2,012,102,102'
LAST_PLAN = '00,,11,2,0,1,3,22,3,410,,234,4,201,3,402,1342,01,30241'


def to_partner(net, src, dst, send, recv):
    return pltpu.make_async_remote_copy(src, dst, send, recv, device_id=net.partner, device_id_type=MESH_ID)


def front_kernel(x_hbm, qkv_shard, out_shard, ff_shard, down_shard, table_ref, qkv_ref, keep_ref, o_ref, lse_ref, h_hbm, n1_hbm, wq_hbm, wo_hbm, wf_hbm,
                 x_all, n1, w, shards, o_all, part, got, h_buf, wo, sems, gather_sems, load_sem, h_sem, cos_ref, sin_ref, o_buf):
    step, last = grid_step()
    turn = step - 1
    batch, pairs, seq = o_all.shape[:3]
    b, p = turn % batch, turn // batch
    half = CHUNK // 2
    chunks = seq // CHUNK
    ff = down_shard.shape[1]
    net = Torus()
    width = 3 * LANES
    heads_end, out_end = width * pairs, (width + LANES) * pairs
    places = [(w, cut_three(width, width * j), 0) for j in range(pairs)] + [
              (wo_hbm, cut_three(LANES * pairs), heads_end), (wf_hbm, cut_three(3 * ff), out_end)]
    gathers = [Gather(net, shards, out, cols, shift, gather_sems, i * Gather.SEMS, i < pairs) for i, (out, cols, shift) in enumerate(places)]
    strip = x_all.shape[0] // CHUNK_STEPS

    def rows_at(i):
        return aligned(i * strip, strip)

    def load(i):
        return pltpu.make_async_copy(x_hbm.at[rows_at(i)], x_all.at[rows_at(i)], load_sem.at[i])

    def save(i):
        return pltpu.make_async_copy(n1.at[rows_at(i)], n1_hbm.at[rows_at(i)], load_sem.at[i])

    save_weight = pltpu.make_async_copy(w, wq_hbm, load_sem.at[CHUNK_STEPS])

    def normalize(i):
        load(i).wait()
        n1[rows_at(i), :] = norm_rows(x_all[rows_at(i), :].astype(F32))[0].astype(BF16)
        save(i).start()

    def normalize_half(first):
        repeat(CHUNK_STEPS // 2, lambda i: normalize(first + i))

    spread = functools.partial(spread_tables, table_ref, cos_ref, sin_ref)
    calls = plan(FRONT_PLAN, *([*g.stages()] for g in gathers), [in_order(spread, functools.partial(normalize_half, 0)), functools.partial(normalize_half, CHUNK_STEPS // 2)])

    @pl.when(step == 0)
    def _():
        for i in range(CHUNK_STEPS):
            load(i).start()
        for i in THREE:
            heads = qkv_shard[:, i].astype(F32).swapaxes(0, 1)
            for j in range(pairs):
                tile = side_by_side(heads, j)
                shards[:, lanes(3 * j + i)] = (swap_middle(tile) if i < 2 else tile).astype(BF16)
        for j in range(pairs):
            shards[:, lanes(3 * pairs + j)] = side_by_side(out_shard, j)
        both = ff_shard[...].astype(F32)
        for i in range(ff // LANES):
            for j in TWO:
                shards[:, lanes(4 * pairs + 2 * i + j)] = both[:, j, lanes(i)].astype(BF16)
        shards[:, out_end + 2 * ff:] = down_shard[...]
        net.barrier(net.neighbours(2) + [net.partner])
        for when, call in calls:
            if not when:
                call()

    begin, end = halves_of(calls, 1)
    run_at(turn, begin)

    @pl.when(turn >= 0)
    def _():
        weight = w[:, :, :, :, pl.ds(pl.multiple_of(width * p, LANES), width)].reshape(n1.shape[1], width)
        project_pair(n1.at[aligned(b * seq, seq)], weight, cos_ref, sin_ref, qkv_ref, keep_ref)
        q_ref, k_ref, v_ref = (qkv_ref.at[:, pl.ds(LANES * i, LANES)] for i in THREE)
        attend_pair(q_ref, k_ref, v_ref, o_ref, lse_ref.at[0, 0])
        o_all[b, p] = o_ref[...]

    run_at(turn, end)

    def rows_in(c, core):
        return aligned(c * CHUNK + core * half, half)

    def part_copy(b, c):
        return to_partner(net, part.at[b, rows_in(c, 1 - net.core)], got.at[b, c], *pair_of(sems, 0, b, c))

    def rows_out(b, c, core):
        return aligned(b * seq + c * CHUNK + core * half, half)

    def h_copy(b, c, core):
        return to_partner(net, h_buf.at[b, c], h_hbm.at[rows_out(b, c, core)], *pair_of(sems, 1, b, c))

    def h_local(b, c):
        return pltpu.make_async_copy(h_buf.at[b, c], h_hbm.at[rows_out(b, c, net.core)], h_sem.at[b, c])

    def project(b):
        o_buf[...] = jnp.concatenate([o_all[b, j] for j in range(pairs)], axis=1)
        weight = wo[...].reshape(part.shape[2], LANES * pairs)

        def body(c):
            rows = aligned(c * CHUNK, CHUNK)
            part[b, rows, :] = nt(o_buf[rows, :], weight)
            part_copy(b, c).start()

        repeat(chunks, body)

    def combine(b):
        def body(c):
            part_copy(b, c).wait()
            own = rows_in(c, net.core)
            h_buf[b, c] = (x_all[rows_out(b, c, net.core), :].astype(F32) + (part[b, own, :] + got[b, c])).astype(BF16)
            h_copy(b, c, net.core).start()
            h_local(b, c).start()

        repeat(chunks, body)

    def settle():
        for b in range(batch):
            for c in range(chunks):
                h_copy(b, c, net.core).wait_send()
                h_local(b, c).wait()
                h_copy(b, c, 1 - net.core).wait_recv()
        for i in range(CHUNK_STEPS):
            save(i).wait()
        save_weight.wait()

    fetch = pltpu.make_async_copy(wo_hbm, wo, h_sem.at[0, 0])
    run_at(last - step, [(2, fetch.start), (2, save_weight.start), (1, fetch.wait), (0, functools.partial(combine, 0))])

    @pl.when(step + 1 >= last)
    def _():
        project(step + 1 - last)

    run_at(last - step, [(0, functools.partial(combine, 1)), (0, settle)])
    run_at(turn + 1, begin[-1:])


def front(x, qkv_shard, out_shard, ff_shard, down_shard, table, batch, seq, collective_id):
    pairs = len(out_shard) // 2
    rows, d = x.shape
    width = 3 * LANES
    chunks = seq // CHUNK
    vm = pltpu.VMEM
    torus = (SIDE, SIDE, SIDE, PIECE)
    shards = [s.size // PIECE for s in (qkv_shard, out_shard, ff_shard, down_shard)]
    turn = lambda s: jnp.maximum(s - 1, 0)
    head = lambda width: pl.BlockSpec((seq, width), lambda s: (turn(s) % batch, turn(s) // batch))
    return pl.pallas_call(
        front_kernel,
        grid=(1 + batch * pairs,),
        in_specs=[HBM] + [WHOLE] * 5,
        out_specs=[head(width), head(width), head(LANES), stats_rows(seq, lambda s: (turn(s) % batch, turn(s) // batch))] + [HBM] * 5,
        out_shape=[shape(BF16, rows, width * pairs)] * 2 + [shape(BF16, rows, LANES * pairs), shape(F32, batch, pairs, 2, seq), shape(BF16, rows, d), shape(BF16, rows, d),
                   shape(BF16, *torus, shards[0]), shape(BF16, *torus, shards[1]), shape(BF16, *torus, shards[2] + shards[3])],
        scratch_shapes=[vm((rows, d), BF16), vm((rows, d), BF16), vm(torus + (width * pairs,), BF16), vm((PIECE, sum(shards)), BF16),
                        vm((batch, pairs, seq, LANES), BF16), vm((batch, seq, d), F32), vm((batch, chunks, CHUNK // 2, d), F32), vm((batch, chunks, CHUNK // 2, d), BF16),
                        vm(torus + (shards[1],), BF16), dma(2, 2, batch, chunks), dma(2, (pairs + 2) * Gather.SEMS), dma(CHUNK_STEPS + 1), dma(batch, chunks)] + [vm((seq, LANES), F32)] * 2 + [vm((seq, LANES * pairs), BF16)],
        compiler_params=params(collective_id),
        name='front',
    )(x, qkv_shard, out_shard, ff_shard, down_shard, table)


class Exchange:
    def __init__(self, net, rows, partials, results, sems, local_sem):
        self.net, self.rows, self.partials, self.results, self.sems, self.local_sem = net, rows, partials, results, sems, local_sem

    def half(self, core, at=0):
        return aligned(at * self.rows + core * (self.rows // 2), self.rows // 2)

    def part(self, which, at):
        part, got = self.partials[which]
        return to_partner(self.net, part.at[at % 2, self.half(1 - self.net.core)], got.at[at], *pair_of(self.sems, which, at))

    def total(self, which, at):
        part, got = self.partials[which]
        self.part(which, at).wait()
        return part[at % 2, self.half(self.net.core), :] + got[at]

    def results_of(self, at, core, act):
        for i, (buf, hbm) in enumerate(self.results):
            act(buf.at[at % 2], hbm.at[self.half(core, at)], pair_of(self.sems, len(self.partials) + i, at), self.local_sem.at[i, at % 2])

    def publish(self, at):
        def act(buf, rows, sem, local_sem):
            to_partner(self.net, buf, rows, *sem).start()
            pltpu.make_async_copy(buf, rows, local_sem).start()
        self.results_of(at, self.net.core, act)

    def settle(self, at):
        def act(buf, rows, sem, local_sem):
            to_partner(self.net, buf, rows, *sem).wait_send()
            pltpu.make_async_copy(buf, rows, local_sem).wait()
        self.results_of(at, self.net.core, act)
        self.results_of(at, 1 - self.net.core, lambda buf, rows, sem, local_sem: to_partner(self.net, buf, rows, *sem).wait_recv())

    def settle_tail(self, blocks):
        for at in TWO:
            self.settle(blocks - len(TWO) + at)


def mlp_kernel(blocks, h_ref, gy_ref, weights, y_hbm, gh_hbm, gh32_ref, acts_hbm, n2_ref, gd_hbm,
               wff_ref, wd_ref, saved, grad_down, part_y, part_g, got_y, got_g, y_buf, gh_buf, h_own, gy_own, sems, local_sem, save_sem, load_sem):
    step, final = grid_step()
    rows, d = h_ref.shape
    ff = wd_ref.shape[1]
    acts = saved.at[step % 2]
    gug, act = acts.at[:, pl.ds(0, 2 * ff)], acts.at[:, pl.ds(2 * ff, ff)]

    def save(at):
        return pltpu.make_async_copy(saved.at[at % 2], acts_hbm.at[aligned(at * rows, rows)], save_sem.at[at % 2])

    save_grad = pltpu.make_async_copy(grad_down, gd_hbm, save_sem.at[2])
    net = Torus()
    swap = Exchange(net, rows, ((part_y, got_y), (part_g, got_g)), ((y_buf, y_hbm), (gh_buf, gh_hbm)), sems, local_sem)

    def loads(i):
        out = []
        first, size = cut_three(ff)[i]
        for which, (dst, at) in enumerate(((wd_ref, 2 * ff), (wff_ref, 0))):
            cols = pl.ds((1 + which) * first, (1 + which) * size)
            out.append(pltpu.make_async_copy(weights.at[:, pl.ds(at + cols.start, cols.size)], dst.at[:, cols], load_sem.at[which, i]))
        return out

    @pl.when(step == 0)
    def _():
        for i in THREE:
            for copy in loads(i):
                copy.start()
        net.barrier([net.partner])

    @pl.when((step > 1) & (step < blocks))
    def _():
        save(step - 2).wait()

    @pl.when(step < blocks)
    def _():
        n2, _ = norm_rows(h_ref[...].astype(F32))
        n2 = n2.astype(BF16)
        n2_ref[...] = n2
        gy = gy_ref[...]
        for j in strips(ff, QB):
            w = min(QB, ff - j)
            if j % BLOCK == 0:
                @pl.when(step == 0)
                def _():
                    for copy in loads(j // BLOCK):
                        copy.wait()
            gact = nn(gy, wd_ref[:, j:j + w])
            for i in range(j, j + w, LANES):
                at, mid, end = 2 * i, 2 * i + LANES, 2 * i + QB
                ug = nn(n2, wff_ref[:, at:end])
                up, gate = ug[:, :LANES], ug[:, LANES:]
                sig = 1.0 / (1.0 + jnp.exp(-gate))
                silu = gate * sig
                act[:, i:i + LANES] = (silu * up).astype(BF16)
                ga = gact[:, i - j:i - j + LANES]
                gug[:, at:mid] = (ga * silu).astype(BF16)
                gug[:, mid:end] = (ga * up * sig * (1.0 + gate * (1.0 - sig))).astype(BF16)

        for which, left, right, part in ((0, act, wd_ref, part_y), (1, gug, wff_ref, part_g)):
            for j in strips(d, QB):
                part[step % 2, :, j:j + QB] = nt(left[...], right[j:j + QB, :])
            swap.part(which, step).start()
        save(step).start()
        accumulate(grad_down, step == 0, gy, act)

    @pl.when(step == blocks - 1)
    def _():
        save_grad.start()

    @pl.when(step > 2)
    def _():
        swap.settle(step - 3)

    @pl.when(step > 0)
    def _():
        done = step - 1
        hidden = h_own[...].astype(F32)
        normed, inv = norm_rows(hidden)
        y_buf[done % 2] = (hidden + swap.total(0, done)).astype(BF16)
        gh = gy_own[...].astype(F32) + norm_grad(swap.total(1, done), normed, inv)
        gh32_ref[...] = gh
        gh_buf[done % 2] = gh.astype(BF16)
        swap.publish(done)

    own = swap.half(net.core)
    h_own[...] = h_ref[own, :]
    gy_own[...] = gy_ref[own, :]

    @pl.when(step == blocks)
    def _():
        swap.settle_tail(blocks)
        for at in TWO:
            save(blocks - len(TWO) + at).wait()
        save_grad.wait()


def mlp(h, gy, weights, collective_id, block=BLOCK):
    rows, d = h.shape
    ff = weights.shape[1] // 3
    half = block // 2
    blocks = rows // block
    torus = (SIDE, SIDE, SIDE, PIECE)
    row = lambda width: rows_of(block, width, lambda i: jnp.minimum(i, blocks - 1))
    vm = pltpu.VMEM
    return pl.pallas_call(
        functools.partial(mlp_kernel, blocks),
        grid=(blocks + 1,),
        in_specs=[row(d), row(d), HBM],
        out_specs=[HBM, HBM, rows_of(half, d, lambda i: jnp.maximum(i - 1, 0)), HBM, row(d), HBM],
        out_shape=[shape(BF16, rows, d), shape(BF16, rows, d), shape(F32, rows // 2, d), shape(BF16, rows, 3 * ff), shape(BF16, rows, d), shape(F32, *torus, ff)],
        scratch_shapes=[vm((d, 2 * ff), BF16), vm((d, ff), BF16), vm((2, block, 3 * ff), BF16), vm(torus + (ff,), F32)] + [vm((2, block, d), F32)] * 2 + [vm((blocks, half, d), F32)] * 2 + [vm((2, half, d), BF16)] * 2 + [vm((half, d), BF16)] * 2 + [dma(2, 4, blocks), dma(2, 2), dma(3), dma(2, 3)],
        compiler_params=params(collective_id),
        name='mlp',
    )(h, gy, weights)


def accumulate(part, first, left, right):
    for j in strips(right.shape[1], QB):
        w = min(QB, right.shape[1] - j)
        prod = tn(left, right[:, j:j + w]).reshape(part.shape[:-1] + (w,))
        at = slice(j, j + w)
        part[..., at] = jnp.where(first, 0.0, part[..., at]) + prod


SETS = 3
HEAD_STEP = (SETS - 1) * CHUNK_STEPS


def back_kernel(pairs, gd_hbm, n2_ref, act_ref, qkv_ref, lse_ref, gh_hbm, wo_hbm, o_hbm, keep_ref, table_ref,
                g_ref, gw_ref, gd_ref, gff_ref, cos_ref, sin_ref, do_ref, dk_ref, dv_ref, gh_ref, wo_ref, o_ref, parts, sems, load_sem, *bufs):
    step, final = grid_step()
    turn = step - HEAD_STEP
    p = turn % pairs
    half = gh_ref.shape[0] // 2
    net = Torus()
    per = len(bufs) // SETS
    scatters = [Scatter(net, parts.at[i], cut_three(parts.shape[-1], turn=i), bufs[per * i:per * i + per], sems, i * Scatter.SEMS) for i in range(SETS)]
    calls = plan(SCATTER_PLAN, *(s.stages() for s in scatters))
    begin, end = halves_of(calls, HEAD_STEP + 1)

    def fetch(b):
        rows = aligned(b * 2 * half, 2 * half)
        return [pltpu.make_async_copy(src.at[rows], dst, load_sem.at[i]) for i, (src, dst) in enumerate(((gh_hbm, gh_ref), (o_hbm, o_ref)))]

    load = pltpu.make_async_copy(gd_hbm, parts.at[0], load_sem.at[2])
    fetch_weight = pltpu.make_async_copy(wo_hbm, wo_ref, load_sem.at[3])

    @pl.when(step == 0)
    def _():
        for copy in [load] + fetch(0) + [fetch_weight]:
            copy.start()
        spread_tables(table_ref, cos_ref, sin_ref)
        net.barrier(net.neighbours())
        load.wait()
        for when, call in calls:
            if not when:
                call()

    @pl.when(turn < 0)
    def _():
        accumulate(parts.at[1 + step // CHUNK_STEPS], step % CHUNK_STEPS == 0, n2_ref[...], act_ref)

    run_at(step + 1, [c for c in calls if 0 < c[0] <= HEAD_STEP])

    def put(part, lo, hi, values):
        cols = lanes(part)
        if part < 2:
            values = values * cos_ref[lo:hi, :] - swap_halves(values) * sin_ref[lo:hi, :]
        g_ref[lo:hi, cols] = (values * keep_ref[lo:hi, cols].astype(F32)).astype(BF16)

    put_dq = lambda lo, hi, dq: put(0, lo, hi, dq * 0.125)

    @pl.when(turn >= 0)
    def _():
        @pl.when(p == 0)
        def _():
            pl.when(turn == 0)(fetch_weight.wait)
            for copy in fetch(turn // pairs):
                copy.wait()
            gw_ref[...] = jnp.where(turn == 0, 0.0, gw_ref[...])

            def body(i):
                rows = aligned(i * half, half)
                gh = gh_ref[rows, :]
                dout = nn(gh, wo_ref[...]).astype(BF16)
                for j in range(pairs):
                    do_ref[j, rows, :] = dout[:, lanes(j)]
                gw_ref[...] += tn(gh, o_ref[rows, :])

            repeat(len(TWO), body)

            @pl.when(turn == 0)
            def _():
                for copy in fetch(turn + 1):
                    copy.start()

        run_at(turn, begin)
        q_ref, k_ref, v_ref = (qkv_ref.at[:, pl.ds(LANES * i, LANES)] for i in THREE)
        attend_pair_back(q_ref, k_ref, v_ref, do_ref.at[p], lse_ref.at[0, 0], dk_ref, dv_ref, put_dq)
        for part, grad in ((1, dk_ref), (2, dv_ref)):
            put(part, 0, 2 * half, grad[...])
        run_at(turn, end)

    @pl.when(step == final)
    def _():
        gd_ref[...], *halves = [s.result() for s in scatters]
        tiles = jnp.concatenate(halves, axis=1)
        for i in range(tiles.shape[1] // LANES):
            gff_ref[:, i % 2, lanes(i // 2)] = tiles[:, lanes(i)]


def back(gd, n2, acts, qkv, lse, gh, wo_t, o, keep, table, batch, seq, pairs, collective_id):
    rows, d = n2.shape
    ff = acts.shape[1] // SETS
    block = rows // CHUNK_STEPS
    turn = lambda s: jnp.maximum(s - HEAD_STEP, 0)
    head = pl.BlockSpec((seq, 3 * LANES), lambda s: (turn(s) // pairs, turn(s) % pairs))
    late = lambda s: jnp.where(s < HEAD_STEP, s % CHUNK_STEPS, CHUNK_STEPS - 1)
    vm = pltpu.VMEM
    return pl.pallas_call(
        functools.partial(back_kernel, pairs),
        grid=(HEAD_STEP + batch * pairs,),
        in_specs=[HBM, rows_of(block, d, late), pl.BlockSpec((block, ff), lambda s: (late(s), jnp.minimum(s // CHUNK_STEPS, 1))), head, stats_rows(seq, lambda s: (turn(s) // pairs, turn(s) % pairs)),
                  HBM, HBM, HBM, head, WHOLE],
        out_specs=[head, WHOLE, WHOLE, WHOLE],
        out_shape=[shape(BF16, *qkv.shape), shape(F32, *wo_t.shape), shape(F32, PIECE, ff), shape(F32, PIECE, 2, ff)],
        scratch_shapes=[vm((seq, LANES), F32)] * 2 + [vm((pairs, seq, LANES), BF16)] + [vm((seq, LANES), F32)] * 2 + [vm((seq, d), BF16), vm(wo_t.shape, BF16), vm((seq, LANES * pairs), BF16), vm((SETS, SIDE, SIDE, SIDE, PIECE, ff), F32),
                        dma(2, SETS * Scatter.SEMS), dma(4)] + [s for i in range(SETS) for s in Scatter.scratch(cut_three(ff, turn=i))],
        compiler_params=params(collective_id),
        name='back',
    )(gd, n2, acts, qkv, lse, gh, wo_t, o, keep, table)


def last_kernel(pairs, blocks, n1_hbm, g_ref, x_ref, g_row, gh_ref, w_hbm, gout_hbm, gx_hbm, gout_ref, gw_ref,
                n1_ref, w_ref, part_out, part_qkv, part, got, buf, sems, scatter_sems, local_sem, load_sem, *bufs):
    step, final = grid_step()
    turn = step - pairs
    rows, d = x_ref.shape
    net = Torus()
    per = len(bufs) // (pairs + 1)
    parts = [part_out] + [part_qkv.at[j] for j in range(pairs)]
    scatters = [Scatter(net, s, cut_three(s.shape[-1], turn=i), bufs[per * i:per * i + per], scatter_sems, i * Scatter.SEMS, 1 if i > pairs // 2 else len(PHASES)) for i, s in enumerate(parts)]
    calls = plan(LAST_PLAN, *(s.stages() for s in scatters))
    swap = Exchange(net, rows, ((part, got),), ((buf, gx_hbm),), sems, local_sem)

    loads = [pltpu.make_async_copy(src, dst, load_sem.at[i]) for i, (src, dst) in enumerate(((gout_hbm, part_out), (n1_hbm, n1_ref), (w_hbm, w_ref)))]
    pl.when(turn == 0)(loads[-1].wait)

    @pl.when(step == 0)
    def _():
        for copy in loads:
            copy.start()
        net.barrier(net.neighbours(2) + [net.partner])
        for copy in loads[:-1]:
            copy.wait()

    begin, end = halves_of(calls)
    run_at(step, begin)

    @pl.when(turn < 0)
    def _():
        size = n1_ref.shape[0] // len(TWO)

        def body(i):
            accumulate(part_qkv.at[step], i == 0, n1_ref[aligned(i * size, size), :], g_ref.at[aligned(i * size, size)])

        repeat(len(TWO), body)

    @pl.when((turn >= 0) & (turn < blocks))
    def _():
        for j in strips(d, QB):
            part[turn % 2, :, j:j + QB] = nt(g_row[...], w_ref[j:j + QB, :])
        swap.part(0, turn).start()

    run_at(step, end)

    @pl.when(turn > 2)
    def _():
        swap.settle(turn - 3)

    @pl.when(turn > 0)
    def _():
        done = turn - 1
        normed, inv = norm_rows(x_ref[swap.half(net.core), :].astype(F32))
        buf[done % 2] = (gh_ref[...] + norm_grad(swap.total(0, done), normed, inv)).astype(BF16)
        swap.publish(done)

    @pl.when(turn == blocks)
    def _():
        for when, call in calls:
            if when > 2 * (pairs + blocks) + 1:
                call()
        swap.settle_tail(blocks)
        out, *sums = [s.result() for s in scatters]
        halves = slice(HALF), slice(HALF, LANES)
        for j in range(pairs):
            for h, cols in enumerate(halves):
                gout_ref[2 * j + h] = out[:, lanes(j)][:, cols]
        for i in THREE:
            tiles = [swap_middle(s[:, lanes(i)]) if i < 2 else s[:, lanes(i)] for s in sums]
            gw_ref[:, i] = jnp.stack([t[:, cols] for t in tiles for cols in halves]).swapaxes(0, 1)


def last(x, n1, g, gh32, w, gout, pairs, collective_id, block=BLOCK):
    rows, d = x.shape
    blocks = rows // block
    late = lambda n, width, by: rows_of(n, width, lambda s: jnp.clip(s - pairs - by, 0, blocks - 1))
    head = pl.BlockSpec((rows, 3 * LANES), lambda s: (0, jnp.minimum(s, pairs - 1)))
    vm = pltpu.VMEM
    half = block // 2
    torus = (SIDE, SIDE, SIDE, PIECE)
    gout = gout.reshape(torus + (-1,))
    return pl.pallas_call(
        functools.partial(last_kernel, pairs, blocks),
        grid=(pairs + blocks + 1,),
        in_specs=[HBM, head, late(block, d, 1), late(block, g.shape[1], 0), late(half, d, 1), HBM, HBM],
        out_specs=[HBM, WHOLE, WHOLE],
        out_shape=[shape(BF16, rows, d), shape(F32, 2 * pairs, PIECE, HALF), shape(F32, PIECE, 3, 2 * pairs, HALF)],
        scratch_shapes=[vm((rows, d), BF16), vm(w.shape, BF16), vm(gout.shape, F32), vm((pairs,) + torus + (3 * LANES,), F32), vm((2, block, d), F32), vm((blocks, half, d), F32), vm((2, half, d), BF16),
                        dma(2, 2, blocks), dma(2, (pairs + 1) * Scatter.SEMS), dma(1, 2), dma(3)] + Scatter.scratch(cut_three(gout.shape[-1])) + Scatter.scratch(cut_three(3 * LANES)) * pairs,
        compiler_params=params(collective_id),
        name='last',
    )(n1, g, x, g, gh32, w, gout)


def hand_over_kernel(*refs):
    count = len(refs) // 2
    for src, dst in zip(refs[:count], refs[count:]):
        dst[...] = src[...]


def hand_over(wide, small, block=QB):
    rows, width = wide[0].shape
    specs = [rows_of(block, width, lambda i: i) for v in wide] + [WHOLE for v in small]
    return pl.pallas_call(
        hand_over_kernel,
        grid=(rows // block,),
        in_specs=specs,
        out_specs=specs,
        out_shape=[shape(v.dtype, *v.shape) for v in wide + small],
        name='hand_over',
    )(*wide, *small)


def device_step(x, grad_y, w_qkv, w_out, w_ff, w_down):
    batch, seq, d = x.shape
    heads, head = w_qkv.shape[2:]
    pairs = heads // 2
    table = jnp.asarray(tables(seq, head))
    ids = iter(range(SIDE))
    x2, gy = (v.reshape(batch * seq, d) for v in (x, grad_y))
    qkv, keep, o, lse, h, n1, *weights = front(x2, w_qkv, w_out.swapaxes(1, 2), w_ff, w_down.T, table, batch, seq, next(ids))
    wq, wo_t, wf = (w.reshape(d, w.shape[-1]) for w in weights)
    y, gh, gh32, acts, n2, gd = mlp(h, gy, wf, next(ids))
    g, gout, gd, gff = back(gd, n2, acts, qkv, lse, gh, wo_t, o, keep, table, batch, seq, pairs, next(ids))
    gx, gout, gqkv = last(x2, n1, g, gh32, wq, gout, pairs, next(ids))
    y, gx, gqkv, gout, gff, gd = hand_over([y, gx], [gqkv, gout, gff, gd])
    return y.reshape(x.shape), gx.reshape(x.shape), gqkv, gout.swapaxes(1, 2), gff, gd.T


def solution(mesh):
    specs = (P('fsdp'), P('fsdp'), P('fsdp', None, 'tp'), P('tp', None, 'fsdp'), P('fsdp', None, 'tp'), P('tp', 'fsdp'))
    return jax.shard_map(device_step, mesh=mesh, in_specs=specs, out_specs=specs, check_vma=False)
```

```python
import functools

import jax
import jax.numpy as jnp
import numpy as np
from jax import lax
from jax.experimental import pallas as pl
from jax.experimental.pallas import tpu as pltpu
from jax.sharding import PartitionSpec as P

MESH_ID = pl.DeviceIdType.MESH
SIDE = 4
TILE = 128
PIECE = 16
ORDERS = ((2, 1, 0), (1, 0, 2), (0, 2, 1))
BOTH = ((0, 1), (1, -1))
PHASES = THREE = range(3)
TWO = range(2)


class Torus:
    def __init__(self):
        self.core = lax.axis_index('tp')
        self.index = lax.axis_index('fsdp')
        plane, x = lax.div(self.index, SIDE), lax.rem(self.index, SIDE)
        self.at = (lax.div(plane, SIDE), lax.rem(plane, SIDE), x)
        self.partner = (1 - self.core, self.index)
        self.moved = {(axis, by): lax.rem(at + (by + SIDE), SIDE) for axis, at in enumerate(self.at) for by in range(-2, 3)}
        self.peers = {(axis, by): self.place(axis, self.moved[axis, by]) for axis in THREE for by in (-1, 1, 2)}

    def place(self, axis, coord):
        pos = list(self.at)
        pos[axis] = coord
        z, y, x = pos
        return (self.core, (z * SIDE + y) * SIDE + x)

    def shift(self, axis, by):
        return self.moved[axis, by]

    def peer(self, axis, by):
        return self.peers[axis, by]

    def neighbours(self, reach=1):
        return [device for (_, by), device in self.peers.items() if by <= reach]

    def tell(self, sem, devices):
        for device in devices:
            pl.semaphore_signal(sem, inc=1, device_id=device, device_id_type=MESH_ID)

    def barrier(self, devices):
        sem = pltpu.get_barrier_semaphore()
        self.tell(sem, devices)
        pl.semaphore_wait(sem, len(devices))


def pair_of(sems, *at):
    return sems.at[(0,) + at], sems.at[(1,) + at]


def in_order(*calls):
    def run():
        for call in calls:
            call()
    return run


def span(cols):
    (off, width), *rest = cols
    return pl.ds(off, width + sum(w for _, w in rest))


class Gather:
    SEMS = 7

    def __init__(self, net, shard, out, cols, shift, sems, first, direct=False):
        self.net, self.shard, self.out, self.cols, self.moved, self.sems, self.first, self.direct = net, shard, out, cols, shift, sems, first, direct

    def block(self, colour, phase, coord, half=None):
        order = ORDERS[colour]
        off, width = self.cols[colour]
        pick = list(self.net.at)
        for axis in order[:phase]:
            pick[axis] = pl.ds(0, SIDE)
        pick[order[phase]] = coord
        if half is not None and phase:
            pick[order[0]] = pl.ds(half * 2, 2)
        elif half is not None:
            cut = width - width // (2 * TILE) * TILE
            off, width = (off + cut, width - cut) if half else (off, cut)
        return self.out.at[(*pick, slice(None), pl.ds(off, width))] if width else None

    def copy(self, phase, colour, relay, d, by):
        axis = ORDERS[colour][phase]
        far = relay and self.direct
        if far and d:
            return None
        by = 2 if far else by
        back = -by if relay and not far else 0
        dst = src = self.block(colour, phase, self.net.shift(axis, back), d if relay and not far else None)
        if dst is None:
            return None
        if not phase and (far or not relay):
            off, width = self.cols[colour]
            src = self.shard.at[:, pl.ds(off + self.moved, width)]
        return pltpu.make_async_remote_copy(src, dst, *self.sem(phase, relay), device_id=self.net.peer(axis, by), device_id_type=MESH_ID)

    def sem(self, phase, relay):
        return pair_of(self.sems, self.first + 2 * phase + relay)

    def each(self, phase, relay):
        for d, by in BOTH:
            for colour in THREE:
                desc = self.copy(phase, colour, relay, d, by)
                if desc is not None:
                    desc.start()

    def wait(self, phase, relay, side):
        pick = [pl.ds(0, SIDE)] * phase + [pl.ds(0, 2 - relay)] + [0, 0]
        ref = self.out.at[tuple(reversed(pick[:3])) + (slice(None), span(self.cols))]
        pltpu.make_async_copy(ref, ref, self.sem(phase, relay)[side]).wait()

    def own(self):
        at = self.net.at
        cols = span(self.cols)
        src = self.shard.at[:, pl.ds(cols.start + self.moved, cols.size)]
        return pltpu.make_async_copy(src, self.out.at[(*at, slice(None), cols)], self.sems.at[0, self.first + self.SEMS - 1])

    def arrive(self, phase):
        if self.direct:
            self.wait(phase, 0, 1)
        self.wait(phase, 1, 1)

    def start(self, phase):
        if phase:
            self.arrive(phase - 1)
        if phase == 1:
            self.own().wait()
        for relay in range(1 + self.direct):
            self.each(phase, relay)
        if not phase:
            self.own().start()

    def relay(self, phase):
        self.wait(phase, 0, 1)
        self.each(phase, 1)

    def finish(self):
        self.arrive(PHASES[-1])
        for phase in PHASES:
            for relay in TWO:
                self.wait(phase, relay, 0)

    def stages(self):
        steps = (self.start,) if self.direct else (self.start, self.relay)
        return [functools.partial(f, p) for p in PHASES for f in steps] + [self.finish]


class Scatter:
    SEMS = 9

    def __init__(self, net, part, cols, bufs, sems, first, relays=len(PHASES)):
        self.net, self.part, self.cols, self.bufs, self.sems, self.first, self.relays = net, part, cols, bufs, sems, first, relays

    @staticmethod
    def scratch(cols):
        shapes = []
        for _, w in cols:
            shapes += [(3, 2, 2, SIDE, PIECE, w), (3, 2, 2, PIECE, w), (3, 2, PIECE // 2, w)]
        return [pltpu.VMEM(s, jnp.float32) for s in shapes]

    def buf(self, colour, phase):
        return self.bufs[colour * len(PHASES) + phase]

    def block(self, colour, phase, coord, half):
        order = ORDERS[colour]
        off, width = self.cols[colour]
        pick = [pl.ds(0, SIDE)] * 3
        for axis in order[:phase]:
            pick[axis] = self.net.at[axis]
        pick[order[phase]] = coord
        rows = pl.ds(0, PIECE)
        rest = sorted(order[phase + 1:])
        if rest:
            pick[rest[0]] = pl.ds(2 * half, 2)
        else:
            rows = pl.ds(PIECE // 2 * half, PIECE // 2)
        return self.part.at[(*pick, rows, pl.ds(off, width))]

    def copy(self, phase, colour, kind, d, by):
        axis = ORDERS[colour][phase]
        buf = self.buf(colour, phase)
        direct = phase >= self.relays
        if kind == 2 and not direct:
            src = buf.at[0, d]
        elif kind:
            src = self.block(colour, phase, self.net.shift(axis, by), (kind + d) % 2)
        else:
            src = self.block(colour, phase, self.net.shift(axis, 2), d)
            by = 2 if direct else by
        return pltpu.make_async_remote_copy(src, buf.at[kind, d], *self.sem(phase, kind), device_id=self.net.peer(axis, by), device_id_type=MESH_ID)

    def sem(self, phase, kind):
        return pair_of(self.sems, self.first + len(PHASES) * phase + kind)

    def wait(self, phase, kind, side):
        pick = [0] * (phase + 1) + [pl.ds(0, SIDE)] * (2 - phase)
        ref = self.part.at[tuple(pick) + (slice(None), span(self.cols))]
        pltpu.make_async_copy(ref, ref, self.sem(phase, kind)[side]).wait()

    def start(self, phase, kind):
        for d, by in BOTH:
            for colour in THREE:
                self.copy(phase, colour, kind, d, by).start()

    def relay(self, phase):
        self.wait(phase, 0, 1)
        for colour in THREE:
            buf = self.buf(colour, phase)
            for d, by in BOTH:
                buf[0, d] = buf[0, d] + self.block(colour, phase, self.net.shift(ORDERS[colour][phase], by), d)[...]
        self.start(phase, 2)

    def merge(self, phase):
        direct = phase >= self.relays
        for kind in THREE if direct else (1, 2):
            self.wait(phase, kind, 1)
        for colour in THREE:
            buf = self.buf(colour, phase)
            for half in TWO:
                mine = self.block(colour, phase, self.net.at[ORDERS[colour][phase]], half)
                sums = mine[...] + buf[1, 1 - half] + buf[2, half]
                mine[...] = sums + buf[0, half] if direct else sums
        if phase < PHASES[-1]:
            for kind in TWO if phase + 1 < self.relays else THREE:
                self.start(phase + 1, kind)

    def finish(self):
        for phase in PHASES:
            for kind in PHASES:
                self.wait(phase, kind, 0)

    def stages(self):
        calls = [functools.partial(self.start, 0, kind) for kind in TWO]
        for phase in PHASES:
            calls += [functools.partial(self.relay, phase)] * (phase < self.relays) + [functools.partial(self.merge, phase)]
        return calls[:-1] + [in_order(calls[-1], self.finish)]

    def result(self):
        return self.part[self.net.at]


def cut_three(width, off=0, turn=0):
    tiles, ways = width // TILE, len(THREE)
    sizes = [(tiles + (turn - i - 1) % ways) // ways * TILE for i in THREE]
    return [(off + sum(sizes[:i]), s) for i, s in enumerate(sizes)]


def plan(text, *sets):
    left = [iter(s) for s in sets]
    return [(hook, next(left[int(which)])) for hook, field in enumerate(text.split(',')) for which in field]


def halves_of(calls, first=0):
    return [[((when - first) // 2, call) for when, call in calls if when >= first and (when - first) % 2 == odd] for odd in TWO]


def run_at(hook, calls):
    for when, call in calls:
        pl.when(hook == when)(call)


F32, BF16 = jnp.float32, jnp.bfloat16
QB = 256
LANES = TILE
HALF = LANES // 2
CLIP = 8.0
BLOCK = 512
MIB = 2**20


def nt(a, b):
    return lax.dot_general(a, b, (((1,), (1,)), ((), ())), preferred_element_type=F32)


def nn(a, b):
    return jnp.dot(a, b, preferred_element_type=F32)


def tn(a, b):
    return lax.dot_general(a, b, (((0,), (0,)), ((), ())), preferred_element_type=F32)


def along(reduce, values):
    return reduce(values, axis=-1, keepdims=True)


def head_masks(paired):
    lane = lax.broadcasted_iota(jnp.int32, (1, LANES), 1)
    first = lane % HALF < HALF // 2 if paired else lane < HALF
    return first, jnp.logical_not(first)


def causal_tile(key_axis):
    dims = (QB, 2 * QB) if key_axis == 0 else (2 * QB, QB)
    return lax.broadcasted_iota(jnp.int32, dims, key_axis) <= lax.broadcasted_iota(jnp.int32, dims, 1 - key_axis) % QB


def by_head(values, masks):
    return jnp.concatenate([jnp.where(m, values, jnp.zeros((), BF16)) for m in masks], axis=0)


def attend_pair(q_ref, k_ref, v_ref, o_ref, lse_ref):
    masks = head_masks(True)
    key, val = k_ref[...], v_ref[...]
    causal = causal_tile(1)
    first, _ = head_masks(False)
    for lo in reversed(strips(q_ref.shape[0], QB)):
        hi = lo + QB
        query = by_head(q_ref[lo:hi, :], masks)
        diag = jnp.where(causal, nt(query, key[lo:hi]), -1e30)
        top = along(jnp.max, diag)
        if lo:
            past = nt(query, key[:lo])
            top = jnp.maximum(top, along(jnp.max, past))
            past = jnp.exp(past - top)
        diag = jnp.exp(diag - top)
        total = along(jnp.sum, diag)
        if lo:
            total = total + along(jnp.sum, past)
        scale = 1.0 / total
        acc = nn((diag * scale).astype(BF16), val[lo:hi])
        if lo:
            acc = acc + nn((past * scale).astype(BF16), val[:lo])
        o_ref[lo:hi, :] = jnp.where(first, acc[:QB], acc[QB:]).astype(BF16)
        lse = jnp.broadcast_to(top + jnp.log(total), acc.shape).T
        for h in TWO:
            lse_ref[h:h + 1, lo:hi] = lse[:1, h * QB:(h + 1) * QB]


def attend_pair_back(q_ref, k_ref, v_ref, do_ref, lse_ref, dk_ref, dv_ref, put_dq):
    seq = q_ref.shape[0]
    qmask, vmask = head_masks(True), head_masks(False)
    key, val = k_ref[...], v_ref[...]
    key_t = key.astype(F32).T.astype(BF16)
    causal = causal_tile(0)
    first = lax.broadcasted_iota(jnp.int32, (LANES, 1), 0) % HALF < HALF // 2

    def products(lo):
        hi = lo + QB
        query, dout = by_head(q_ref[lo:hi, :], qmask), by_head(do_ref[lo:hi, :], vmask)
        return query, dout, nt(key[:hi], query), nt(val[:hi], dout)

    ahead = products(seq - QB)
    for lo in reversed(strips(seq, QB)):
        hi = lo + QB
        query, dout, score, grad = ahead
        if lo:
            ahead = products(lo - QB)
        prob = jnp.exp(score - jnp.concatenate([lse_ref[h:h + 1, lo:hi] for h in TWO], axis=1))
        diag = jnp.where(causal, prob[lo:], 0.0)
        prob = jnp.concatenate([prob[:lo], diag], axis=0) if lo else diag
        ds = (prob * (grad - jnp.sum(prob * grad, axis=0, keepdims=True))).astype(BF16)
        both = nn(key_t[:, :hi], ds)
        put_dq(lo, hi, jnp.where(first, both[:, :QB], both[:, QB:]).T)
        dv, dk = nn(prob.astype(BF16), dout), nn(ds, query)
        if hi == seq:
            dv_ref[...] = dv
            dk_ref[...] = dk
        else:
            dv_ref[:hi, :] += dv
            dk_ref[:hi, :] += dk


def swap_halves(values):
    return pltpu.roll(values, HALF, axis=1)


COARSE = 32


def tables(seq, head):
    freq = 10000.0 ** (-np.arange(0, head, 2, dtype=np.float64) / head)
    angles = [np.tile(np.arange(seq // COARSE)[:, None] * step * freq, LANES // len(freq)) for step in (1, COARSE)]
    return np.stack([np.stack([np.cos(angle), np.sin(angle)]) for angle in angles]).astype(np.float32)


def spread_tables(table_ref, cos_ref, sin_ref):
    fine_cos, fine_sin = table_ref[0]
    sign = jnp.where(lax.broadcasted_iota(jnp.int32, (1, LANES), 1) < HALF, -1.0, 1.0)

    def body(i):
        rows = aligned(i * COARSE, COARSE)
        cos, sin = table_ref[1, :, pl.ds(i, 1), :]
        cos_ref[rows, :] = fine_cos * cos - fine_sin * sin
        sin_ref[rows, :] = (fine_sin * cos + fine_cos * sin) * sign

    repeat(cos_ref.shape[0] // COARSE, body)


def repeat(count, body):
    def step(i, carry):
        body(i)
        return carry

    lax.fori_loop(0, count, step, 0)


def side_by_side(halves, j):
    return jnp.concatenate([halves[2 * j], halves[2 * j + 1]], axis=1)


def aligned(at, size):
    return pl.ds(pl.multiple_of(at, size), size)


def norm_rows(values):
    mean = along(jnp.mean, values)
    centered = values - mean
    inv = lax.rsqrt(along(jnp.mean, centered * centered) + 1e-5)
    return centered * inv, inv


def norm_grad(grad, normed, inv):
    mean = along(jnp.mean, grad)
    proj = along(jnp.mean, grad * normed)
    return inv * (grad - mean - normed * proj)


def params(collective_id):
    return pltpu.CompilerParams(collective_id=collective_id, has_side_effects=True, vmem_limit_bytes=63 * MIB)


def grid_step():
    return pl.program_id(0), pl.num_programs(0) - 1


def dma(*shape):
    return pltpu.SemaphoreType.DMA(shape)


def shape(dtype, *dims):
    return jax.ShapeDtypeStruct(dims, dtype)


HBM = pl.BlockSpec(memory_space=pltpu.HBM)
WHOLE = pl.BlockSpec(memory_space=pltpu.VMEM)


def lanes(part):
    return slice(LANES * part, LANES * (part + 1))


def strips(width, size):
    return range(0, width, size)


def rows_of(size, width, index):
    return pl.BlockSpec((size, width), lambda step: (index(step), 0))


def stats_rows(seq, index):
    return pl.BlockSpec((1, 1, 2, seq), lambda step: (*index(step), 0, 0))


def project_pair(n1_ref, weight, cos_ref, sin_ref, qkv_ref, keep_ref):
    for lo in strips(n1_ref.shape[0], QB):
        rows = slice(lo, lo + QB)
        raw = nn(n1_ref[rows, :], weight)
        keep_ref[rows, :] = (jnp.abs(raw) < CLIP).astype(F32).astype(BF16)
        raw = jnp.clip(raw, -CLIP, CLIP)
        for part in THREE:
            cols = lanes(part)
            tile = raw[:, cols]
            if part < 2:
                tile = tile * cos_ref[rows, :] + swap_halves(tile) * sin_ref[rows, :]
            if not part:
                tile = tile * 0.125
            qkv_ref[rows, cols] = tile.astype(BF16)


def swap_middle(tile):
    quarter = lax.broadcasted_iota(jnp.int32, tile.shape, 1) // (LANES // 4)
    up, down = pltpu.roll(tile, LANES // 4, axis=1), pltpu.roll(tile, LANES - LANES // 4, axis=1)
    return jnp.where(quarter == 1, down, jnp.where(quarter == 2, up, tile))


CHUNK = 256
CHUNK_STEPS = 4
FRONT_PLAN = '014560145260512430,,4,5,1234,,345,,24,,,,3,,,5,,5'
SCATTER_PLAN = '00,,,,,1,1,,2,0,,,2,12,0,,,,12,0,1,2,012,102,102'
LAST_PLAN = '00,,11,2,0,1,3,22,3,410,,234,4,201,3,402,1342,01,30241'


def to_partner(net, src, dst, send, recv):
    return pltpu.make_async_remote_copy(src, dst, send, recv, device_id=net.partner, device_id_type=MESH_ID)


def front_kernel(x_hbm, qkv_shard, out_shard, ff_shard, down_shard, table_ref, qkv_ref, keep_ref, o_ref, lse_ref, h_hbm, n1_hbm, wq_hbm, wo_hbm, wf_hbm,
                 x_all, n1, w, shards, o_all, part, got, h_buf, wo, sems, gather_sems, load_sem, h_sem, cos_ref, sin_ref, o_buf):
    step, last = grid_step()
    turn = step - 1
    batch, pairs, seq = o_all.shape[:3]
    b, p = turn % batch, turn // batch
    half = CHUNK // 2
    chunks = seq // CHUNK
    ff = down_shard.shape[1]
    net = Torus()
    width = 3 * LANES
    heads_end, out_end = width * pairs, (width + LANES) * pairs
    places = [(w, cut_three(width, width * j), 0) for j in range(pairs)] + [
              (wo_hbm, cut_three(LANES * pairs), heads_end), (wf_hbm, cut_three(3 * ff), out_end)]
    gathers = [Gather(net, shards, out, cols, shift, gather_sems, i * Gather.SEMS, i < pairs) for i, (out, cols, shift) in enumerate(places)]
    strip = x_all.shape[0] // CHUNK_STEPS

    def rows_at(i):
        return aligned(i * strip, strip)

    def load(i):
        return pltpu.make_async_copy(x_hbm.at[rows_at(i)], x_all.at[rows_at(i)], load_sem.at[i])

    def save(i):
        return pltpu.make_async_copy(n1.at[rows_at(i)], n1_hbm.at[rows_at(i)], load_sem.at[i])

    save_weight = pltpu.make_async_copy(w, wq_hbm, load_sem.at[CHUNK_STEPS])

    def normalize(i):
        load(i).wait()
        n1[rows_at(i), :] = norm_rows(x_all[rows_at(i), :].astype(F32))[0].astype(BF16)
        save(i).start()

    def normalize_half(first):
        repeat(CHUNK_STEPS // 2, lambda i: normalize(first + i))

    spread = functools.partial(spread_tables, table_ref, cos_ref, sin_ref)
    calls = plan(FRONT_PLAN, *([*g.stages()] for g in gathers), [in_order(spread, functools.partial(normalize_half, 0)), functools.partial(normalize_half, CHUNK_STEPS // 2)])

    @pl.when(step == 0)
    def _():
        for i in range(CHUNK_STEPS):
            load(i).start()
        for i in THREE:
            heads = qkv_shard[:, i].astype(F32).swapaxes(0, 1)
            for j in range(pairs):
                tile = side_by_side(heads, j)
                shards[:, lanes(3 * j + i)] = (swap_middle(tile) if i < 2 else tile).astype(BF16)
        for j in range(pairs):
            shards[:, lanes(3 * pairs + j)] = side_by_side(out_shard, j)
        both = ff_shard[...].astype(F32)
        for i in range(ff // LANES):
            for j in TWO:
                shards[:, lanes(4 * pairs + 2 * i + j)] = both[:, j, lanes(i)].astype(BF16)
        shards[:, out_end + 2 * ff:] = down_shard[...]
        net.barrier(net.neighbours(2) + [net.partner])
        for when, call in calls:
            if not when:
                call()

    begin, end = halves_of(calls, 1)
    run_at(turn, begin)

    @pl.when(turn >= 0)
    def _():
        weight = w[:, :, :, :, pl.ds(pl.multiple_of(width * p, LANES), width)].reshape(n1.shape[1], width)
        project_pair(n1.at[aligned(b * seq, seq)], weight, cos_ref, sin_ref, qkv_ref, keep_ref)
        q_ref, k_ref, v_ref = (qkv_ref.at[:, pl.ds(LANES * i, LANES)] for i in THREE)
        attend_pair(q_ref, k_ref, v_ref, o_ref, lse_ref.at[0, 0])
        o_all[b, p] = o_ref[...]

    run_at(turn, end)

    def rows_in(c, core):
        return aligned(c * CHUNK + core * half, half)

    def part_copy(b, c):
        return to_partner(net, part.at[b, rows_in(c, 1 - net.core)], got.at[b, c], *pair_of(sems, 0, b, c))

    def rows_out(b, c, core):
        return aligned(b * seq + c * CHUNK + core * half, half)

    def h_copy(b, c, core):
        return to_partner(net, h_buf.at[b, c], h_hbm.at[rows_out(b, c, core)], *pair_of(sems, 1, b, c))

    def h_local(b, c):
        return pltpu.make_async_copy(h_buf.at[b, c], h_hbm.at[rows_out(b, c, net.core)], h_sem.at[b, c])

    def project(b):
        o_buf[...] = jnp.concatenate([o_all[b, j] for j in range(pairs)], axis=1)
        weight = wo[...].reshape(part.shape[2], LANES * pairs)

        def body(c):
            rows = aligned(c * CHUNK, CHUNK)
            part[b, rows, :] = nt(o_buf[rows, :], weight)
            part_copy(b, c).start()

        repeat(chunks, body)

    def combine(b):
        def body(c):
            part_copy(b, c).wait()
            own = rows_in(c, net.core)
            h_buf[b, c] = (x_all[rows_out(b, c, net.core), :].astype(F32) + (part[b, own, :] + got[b, c])).astype(BF16)
            h_copy(b, c, net.core).start()
            h_local(b, c).start()

        repeat(chunks, body)

    def settle():
        for b in range(batch):
            for c in range(chunks):
                h_copy(b, c, net.core).wait_send()
                h_local(b, c).wait()
                h_copy(b, c, 1 - net.core).wait_recv()
        for i in range(CHUNK_STEPS):
            save(i).wait()
        save_weight.wait()

    fetch = pltpu.make_async_copy(wo_hbm, wo, h_sem.at[0, 0])
    run_at(last - step, [(2, fetch.start), (2, save_weight.start), (1, fetch.wait), (0, functools.partial(combine, 0))])

    @pl.when(step + 1 >= last)
    def _():
        project(step + 1 - last)

    run_at(last - step, [(0, functools.partial(combine, 1)), (0, settle)])
    run_at(turn + 1, begin[-1:])


def front(x, qkv_shard, out_shard, ff_shard, down_shard, table, batch, seq, collective_id):
    pairs = len(out_shard) // 2
    rows, d = x.shape
    width = 3 * LANES
    chunks = seq // CHUNK
    vm = pltpu.VMEM
    torus = (SIDE, SIDE, SIDE, PIECE)
    shards = [s.size // PIECE for s in (qkv_shard, out_shard, ff_shard, down_shard)]
    turn = lambda s: jnp.maximum(s - 1, 0)
    head = lambda width: pl.BlockSpec((seq, width), lambda s: (turn(s) % batch, turn(s) // batch))
    return pl.pallas_call(
        front_kernel,
        grid=(1 + batch * pairs,),
        in_specs=[HBM] + [WHOLE] * 5,
        out_specs=[head(width), head(width), head(LANES), stats_rows(seq, lambda s: (turn(s) % batch, turn(s) // batch))] + [HBM] * 5,
        out_shape=[shape(BF16, rows, width * pairs)] * 2 + [shape(BF16, rows, LANES * pairs), shape(F32, batch, pairs, 2, seq), shape(BF16, rows, d), shape(BF16, rows, d),
                   shape(BF16, *torus, shards[0]), shape(BF16, *torus, shards[1]), shape(BF16, *torus, shards[2] + shards[3])],
        scratch_shapes=[vm((rows, d), BF16), vm((rows, d), BF16), vm(torus + (width * pairs,), BF16), vm((PIECE, sum(shards)), BF16),
                        vm((batch, pairs, seq, LANES), BF16), vm((batch, seq, d), F32), vm((batch, chunks, CHUNK // 2, d), F32), vm((batch, chunks, CHUNK // 2, d), BF16),
                        vm(torus + (shards[1],), BF16), dma(2, 2, batch, chunks), dma(2, (pairs + 2) * Gather.SEMS), dma(CHUNK_STEPS + 1), dma(batch, chunks)] + [vm((seq, LANES), F32)] * 2 + [vm((seq, LANES * pairs), BF16)],
        compiler_params=params(collective_id),
        name='front',
    )(x, qkv_shard, out_shard, ff_shard, down_shard, table)


class Exchange:
    def __init__(self, net, rows, partials, results, sems, local_sem):
        self.net, self.rows, self.partials, self.results, self.sems, self.local_sem = net, rows, partials, results, sems, local_sem

    def half(self, core, at=0):
        return aligned(at * self.rows + core * (self.rows // 2), self.rows // 2)

    def part(self, which, at):
        part, got = self.partials[which]
        return to_partner(self.net, part.at[at % 2, self.half(1 - self.net.core)], got.at[at], *pair_of(self.sems, which, at))

    def total(self, which, at):
        part, got = self.partials[which]
        self.part(which, at).wait()
        return part[at % 2, self.half(self.net.core), :] + got[at]

    def results_of(self, at, core, act):
        for i, (buf, hbm) in enumerate(self.results):
            act(buf.at[at % 2], hbm.at[self.half(core, at)], pair_of(self.sems, len(self.partials) + i, at), self.local_sem.at[i, at % 2])

    def publish(self, at):
        def act(buf, rows, sem, local_sem):
            to_partner(self.net, buf, rows, *sem).start()
            pltpu.make_async_copy(buf, rows, local_sem).start()
        self.results_of(at, self.net.core, act)

    def settle(self, at):
        def act(buf, rows, sem, local_sem):
            to_partner(self.net, buf, rows, *sem).wait_send()
            pltpu.make_async_copy(buf, rows, local_sem).wait()
        self.results_of(at, self.net.core, act)
        self.results_of(at, 1 - self.net.core, lambda buf, rows, sem, local_sem: to_partner(self.net, buf, rows, *sem).wait_recv())

    def settle_tail(self, blocks):
        for at in TWO:
            self.settle(blocks - len(TWO) + at)


def mlp_kernel(blocks, h_ref, gy_ref, weights, y_hbm, gh_hbm, gh32_ref, acts_hbm, n2_ref, gd_hbm,
               wff_ref, wd_ref, saved, grad_down, part_y, part_g, got_y, got_g, y_buf, gh_buf, h_own, gy_own, sems, local_sem, save_sem, load_sem):
    step, final = grid_step()
    rows, d = h_ref.shape
    ff = wd_ref.shape[1]
    acts = saved.at[step % 2]
    gug, act = acts.at[:, pl.ds(0, 2 * ff)], acts.at[:, pl.ds(2 * ff, ff)]

    def save(at):
        return pltpu.make_async_copy(saved.at[at % 2], acts_hbm.at[aligned(at * rows, rows)], save_sem.at[at % 2])

    save_grad = pltpu.make_async_copy(grad_down, gd_hbm, save_sem.at[2])
    net = Torus()
    swap = Exchange(net, rows, ((part_y, got_y), (part_g, got_g)), ((y_buf, y_hbm), (gh_buf, gh_hbm)), sems, local_sem)

    loads = [pltpu.make_async_copy(weights.at[:, pl.ds(at, dst.shape[1])], dst, load_sem.at[i]) for i, (dst, at) in enumerate(((wd_ref, 2 * ff), (wff_ref, 0)))]

    @pl.when(step == 0)
    def _():
        for copy in loads:
            copy.start()
        net.barrier([net.partner])
        for copy in loads:
            copy.wait()

    @pl.when((step > 1) & (step < blocks))
    def _():
        save(step - 2).wait()

    @pl.when(step < blocks)
    def _():
        n2, _ = norm_rows(h_ref[...].astype(F32))
        n2 = n2.astype(BF16)
        n2_ref[...] = n2
        gy = gy_ref[...]
        for j in strips(ff, QB):
            w = min(QB, ff - j)
            gact = nn(gy, wd_ref[:, j:j + w])
            for i in range(j, j + w, LANES):
                at, mid, end = 2 * i, 2 * i + LANES, 2 * i + QB
                ug = nn(n2, wff_ref[:, at:end])
                up, gate = ug[:, :LANES], ug[:, LANES:]
                sig = 1.0 / (1.0 + jnp.exp(-gate))
                silu = gate * sig
                act[:, i:i + LANES] = (silu * up).astype(BF16)
                ga = gact[:, i - j:i - j + LANES]
                gug[:, at:mid] = (ga * silu).astype(BF16)
                gug[:, mid:end] = (ga * up * sig * (1.0 + gate * (1.0 - sig))).astype(BF16)

        for which, left, right, part in ((0, act, wd_ref, part_y), (1, gug, wff_ref, part_g)):
            for j in strips(d, QB):
                part[step % 2, :, j:j + QB] = nt(left[...], right[j:j + QB, :])
            swap.part(which, step).start()
        save(step).start()
        accumulate(grad_down, step == 0, gy, act)

    @pl.when(step == blocks - 1)
    def _():
        save_grad.start()

    @pl.when(step > 2)
    def _():
        swap.settle(step - 3)

    @pl.when(step > 0)
    def _():
        done = step - 1
        hidden = h_own[...].astype(F32)
        normed, inv = norm_rows(hidden)
        y_buf[done % 2] = (hidden + swap.total(0, done)).astype(BF16)
        gh = gy_own[...].astype(F32) + norm_grad(swap.total(1, done), normed, inv)
        gh32_ref[...] = gh
        gh_buf[done % 2] = gh.astype(BF16)
        swap.publish(done)

    own = swap.half(net.core)
    h_own[...] = h_ref[own, :]
    gy_own[...] = gy_ref[own, :]

    @pl.when(step == blocks)
    def _():
        swap.settle_tail(blocks)
        for at in TWO:
            save(blocks - len(TWO) + at).wait()
        save_grad.wait()


def mlp(h, gy, weights, collective_id, block=BLOCK):
    rows, d = h.shape
    ff = weights.shape[1] // 3
    half = block // 2
    blocks = rows // block
    torus = (SIDE, SIDE, SIDE, PIECE)
    row = lambda width: rows_of(block, width, lambda i: jnp.minimum(i, blocks - 1))
    vm = pltpu.VMEM
    return pl.pallas_call(
        functools.partial(mlp_kernel, blocks),
        grid=(blocks + 1,),
        in_specs=[row(d), row(d), HBM],
        out_specs=[HBM, HBM, rows_of(half, d, lambda i: jnp.maximum(i - 1, 0)), HBM, row(d), HBM],
        out_shape=[shape(BF16, rows, d), shape(BF16, rows, d), shape(F32, rows // 2, d), shape(BF16, rows, 3 * ff), shape(BF16, rows, d), shape(F32, *torus, ff)],
        scratch_shapes=[vm((d, 2 * ff), BF16), vm((d, ff), BF16), vm((2, block, 3 * ff), BF16), vm(torus + (ff,), F32)] + [vm((2, block, d), F32)] * 2 + [vm((blocks, half, d), F32)] * 2 + [vm((2, half, d), BF16)] * 2 + [vm((half, d), BF16)] * 2 + [dma(2, 4, blocks), dma(2, 2), dma(3), dma(2)],
        compiler_params=params(collective_id),
        name='mlp',
    )(h, gy, weights)


def accumulate(part, first, left, right):
    for j in strips(right.shape[1], QB):
        w = min(QB, right.shape[1] - j)
        prod = tn(left, right[:, j:j + w]).reshape(part.shape[:-1] + (w,))
        at = slice(j, j + w)
        part[..., at] = jnp.where(first, 0.0, part[..., at]) + prod


SETS = 3
HEAD_STEP = (SETS - 1) * CHUNK_STEPS


def back_kernel(pairs, gd_hbm, n2_ref, act_ref, qkv_ref, lse_ref, gh_hbm, wo_hbm, o_hbm, keep_ref, table_ref,
                g_ref, gw_ref, gd_ref, gff_ref, cos_ref, sin_ref, do_ref, dk_ref, dv_ref, gh_ref, wo_ref, o_ref, parts, sems, load_sem, *bufs):
    step, final = grid_step()
    turn = step - HEAD_STEP
    p = turn % pairs
    half = gh_ref.shape[0] // 2
    net = Torus()
    per = len(bufs) // SETS
    scatters = [Scatter(net, parts.at[i], cut_three(parts.shape[-1], turn=i), bufs[per * i:per * i + per], sems, i * Scatter.SEMS) for i in range(SETS)]
    calls = plan(SCATTER_PLAN, *(s.stages() for s in scatters))
    begin, end = halves_of(calls, HEAD_STEP + 1)

    def fetch(b):
        rows = aligned(b * 2 * half, 2 * half)
        return [pltpu.make_async_copy(src.at[rows], dst, load_sem.at[i]) for i, (src, dst) in enumerate(((gh_hbm, gh_ref), (o_hbm, o_ref)))]

    load = pltpu.make_async_copy(gd_hbm, parts.at[0], load_sem.at[2])
    fetch_weight = pltpu.make_async_copy(wo_hbm, wo_ref, load_sem.at[3])

    @pl.when(step == 0)
    def _():
        for copy in [load] + fetch(0) + [fetch_weight]:
            copy.start()
        spread_tables(table_ref, cos_ref, sin_ref)
        net.barrier(net.neighbours())
        load.wait()
        for when, call in calls:
            if not when:
                call()

    @pl.when(turn < 0)
    def _():
        accumulate(parts.at[1 + step // CHUNK_STEPS], step % CHUNK_STEPS == 0, n2_ref[...], act_ref)

    run_at(step + 1, [c for c in calls if 0 < c[0] <= HEAD_STEP])

    def put(part, lo, hi, values):
        cols = lanes(part)
        if part < 2:
            values = values * cos_ref[lo:hi, :] - swap_halves(values) * sin_ref[lo:hi, :]
        g_ref[lo:hi, cols] = (values * keep_ref[lo:hi, cols].astype(F32)).astype(BF16)

    put_dq = lambda lo, hi, dq: put(0, lo, hi, dq * 0.125)

    @pl.when(turn >= 0)
    def _():
        @pl.when(p == 0)
        def _():
            pl.when(turn == 0)(fetch_weight.wait)
            for copy in fetch(turn // pairs):
                copy.wait()
            gw_ref[...] = jnp.where(turn == 0, 0.0, gw_ref[...])

            def body(i):
                rows = aligned(i * half, half)
                gh = gh_ref[rows, :]
                dout = nn(gh, wo_ref[...]).astype(BF16)
                for j in range(pairs):
                    do_ref[j, rows, :] = dout[:, lanes(j)]
                gw_ref[...] += tn(gh, o_ref[rows, :])

            repeat(len(TWO), body)

            @pl.when(turn == 0)
            def _():
                for copy in fetch(turn + 1):
                    copy.start()

        run_at(turn, begin)
        q_ref, k_ref, v_ref = (qkv_ref.at[:, pl.ds(LANES * i, LANES)] for i in THREE)
        attend_pair_back(q_ref, k_ref, v_ref, do_ref.at[p], lse_ref.at[0, 0], dk_ref, dv_ref, put_dq)
        for part, grad in ((1, dk_ref), (2, dv_ref)):
            put(part, 0, 2 * half, grad[...])
        run_at(turn, end)

    @pl.when(step == final)
    def _():
        gd_ref[...], *halves = [s.result() for s in scatters]
        tiles = jnp.concatenate(halves, axis=1)
        for i in range(tiles.shape[1] // LANES):
            gff_ref[:, i % 2, lanes(i // 2)] = tiles[:, lanes(i)]


def back(gd, n2, acts, qkv, lse, gh, wo_t, o, keep, table, batch, seq, pairs, collective_id):
    rows, d = n2.shape
    ff = acts.shape[1] // SETS
    block = rows // CHUNK_STEPS
    turn = lambda s: jnp.maximum(s - HEAD_STEP, 0)
    head = pl.BlockSpec((seq, 3 * LANES), lambda s: (turn(s) // pairs, turn(s) % pairs))
    late = lambda s: jnp.where(s < HEAD_STEP, s % CHUNK_STEPS, CHUNK_STEPS - 1)
    vm = pltpu.VMEM
    return pl.pallas_call(
        functools.partial(back_kernel, pairs),
        grid=(HEAD_STEP + batch * pairs,),
        in_specs=[HBM, rows_of(block, d, late), pl.BlockSpec((block, ff), lambda s: (late(s), jnp.minimum(s // CHUNK_STEPS, 1))), head, stats_rows(seq, lambda s: (turn(s) // pairs, turn(s) % pairs)),
                  HBM, HBM, HBM, head, WHOLE],
        out_specs=[head, WHOLE, WHOLE, WHOLE],
        out_shape=[shape(BF16, *qkv.shape), shape(F32, *wo_t.shape), shape(F32, PIECE, ff), shape(F32, PIECE, 2, ff)],
        scratch_shapes=[vm((seq, LANES), F32)] * 2 + [vm((pairs, seq, LANES), BF16)] + [vm((seq, LANES), F32)] * 2 + [vm((seq, d), BF16), vm(wo_t.shape, BF16), vm((seq, LANES * pairs), BF16), vm((SETS, SIDE, SIDE, SIDE, PIECE, ff), F32),
                        dma(2, SETS * Scatter.SEMS), dma(4)] + [s for i in range(SETS) for s in Scatter.scratch(cut_three(ff, turn=i))],
        compiler_params=params(collective_id),
        name='back',
    )(gd, n2, acts, qkv, lse, gh, wo_t, o, keep, table)


def last_kernel(pairs, blocks, n1_hbm, g_ref, x_ref, g_row, gh_ref, w_hbm, gout_hbm, gx_hbm, gout_ref, gw_ref,
                n1_ref, w_ref, part_out, part_qkv, part, got, buf, sems, scatter_sems, local_sem, load_sem, *bufs):
    step, final = grid_step()
    turn = step - pairs
    rows, d = x_ref.shape
    net = Torus()
    per = len(bufs) // (pairs + 1)
    parts = [part_out] + [part_qkv.at[j] for j in range(pairs)]
    scatters = [Scatter(net, s, cut_three(s.shape[-1], turn=i), bufs[per * i:per * i + per], scatter_sems, i * Scatter.SEMS, 1 if i > pairs // 2 else len(PHASES)) for i, s in enumerate(parts)]
    calls = plan(LAST_PLAN, *(s.stages() for s in scatters))
    swap = Exchange(net, rows, ((part, got),), ((buf, gx_hbm),), sems, local_sem)

    loads = [pltpu.make_async_copy(src, dst, load_sem.at[i]) for i, (src, dst) in enumerate(((gout_hbm, part_out), (n1_hbm, n1_ref), (w_hbm, w_ref)))]
    pl.when(turn == 0)(loads[-1].wait)

    @pl.when(step == 0)
    def _():
        for copy in loads:
            copy.start()
        net.barrier(net.neighbours(2) + [net.partner])
        for copy in loads[:-1]:
            copy.wait()

    begin, end = halves_of(calls)
    run_at(step, begin)

    @pl.when(turn < 0)
    def _():
        size = n1_ref.shape[0] // len(TWO)

        def body(i):
            accumulate(part_qkv.at[step], i == 0, n1_ref[aligned(i * size, size), :], g_ref.at[aligned(i * size, size)])

        repeat(len(TWO), body)

    @pl.when((turn >= 0) & (turn < blocks))
    def _():
        for j in strips(d, QB):
            part[turn % 2, :, j:j + QB] = nt(g_row[...], w_ref[j:j + QB, :])
        swap.part(0, turn).start()

    run_at(step, end)

    @pl.when(turn > 2)
    def _():
        swap.settle(turn - 3)

    @pl.when(turn > 0)
    def _():
        done = turn - 1
        normed, inv = norm_rows(x_ref[swap.half(net.core), :].astype(F32))
        buf[done % 2] = (gh_ref[...] + norm_grad(swap.total(0, done), normed, inv)).astype(BF16)
        swap.publish(done)

    @pl.when(turn == blocks)
    def _():
        for when, call in calls:
            if when > 2 * (pairs + blocks) + 1:
                call()
        swap.settle_tail(blocks)
        out, *sums = [s.result() for s in scatters]
        halves = slice(HALF), slice(HALF, LANES)
        for j in range(pairs):
            for h, cols in enumerate(halves):
                gout_ref[2 * j + h] = out[:, lanes(j)][:, cols]
        for i in THREE:
            tiles = [swap_middle(s[:, lanes(i)]) if i < 2 else s[:, lanes(i)] for s in sums]
            gw_ref[:, i] = jnp.stack([t[:, cols] for t in tiles for cols in halves]).swapaxes(0, 1)


def last(x, n1, g, gh32, w, gout, pairs, collective_id, block=BLOCK):
    rows, d = x.shape
    blocks = rows // block
    late = lambda n, width, by: rows_of(n, width, lambda s: jnp.clip(s - pairs - by, 0, blocks - 1))
    head = pl.BlockSpec((rows, 3 * LANES), lambda s: (0, jnp.minimum(s, pairs - 1)))
    vm = pltpu.VMEM
    half = block // 2
    torus = (SIDE, SIDE, SIDE, PIECE)
    gout = gout.reshape(torus + (-1,))
    return pl.pallas_call(
        functools.partial(last_kernel, pairs, blocks),
        grid=(pairs + blocks + 1,),
        in_specs=[HBM, head, late(block, d, 1), late(block, g.shape[1], 0), late(half, d, 1), HBM, HBM],
        out_specs=[HBM, WHOLE, WHOLE],
        out_shape=[shape(BF16, rows, d), shape(F32, 2 * pairs, PIECE, HALF), shape(F32, PIECE, 3, 2 * pairs, HALF)],
        scratch_shapes=[vm((rows, d), BF16), vm(w.shape, BF16), vm(gout.shape, F32), vm((pairs,) + torus + (3 * LANES,), F32), vm((2, block, d), F32), vm((blocks, half, d), F32), vm((2, half, d), BF16),
                        dma(2, 2, blocks), dma(2, (pairs + 1) * Scatter.SEMS), dma(1, 2), dma(3)] + Scatter.scratch(cut_three(gout.shape[-1])) + Scatter.scratch(cut_three(3 * LANES)) * pairs,
        compiler_params=params(collective_id),
        name='last',
    )(n1, g, x, g, gh32, w, gout)


def hand_over_kernel(*refs):
    count = len(refs) // 2
    for src, dst in zip(refs[:count], refs[count:]):
        dst[...] = src[...]


def hand_over(wide, small, block=2 * BLOCK):
    rows, width = wide[0].shape
    specs = [rows_of(block, width, lambda i: i) for v in wide] + [WHOLE for v in small]
    return pl.pallas_call(
        hand_over_kernel,
        grid=(rows // block,),
        in_specs=specs,
        out_specs=specs,
        out_shape=[shape(v.dtype, *v.shape) for v in wide + small],
        compiler_params=pltpu.CompilerParams(vmem_limit_bytes=40 * MIB),
        name='hand_over',
    )(*wide, *small)


def device_step(x, grad_y, w_qkv, w_out, w_ff, w_down):
    batch, seq, d = x.shape
    heads, head = w_qkv.shape[2:]
    pairs = heads // 2
    table = jnp.asarray(tables(seq, head))
    ids = iter(range(SIDE))
    x2, gy = (v.reshape(batch * seq, d) for v in (x, grad_y))
    qkv, keep, o, lse, h, n1, *weights = front(x2, w_qkv, w_out.swapaxes(1, 2), w_ff, w_down.T, table, batch, seq, next(ids))
    wq, wo_t, wf = (w.reshape(d, w.shape[-1]) for w in weights)
    y, gh, gh32, acts, n2, gd = mlp(h, gy, wf, next(ids))
    g, gout, gd, gff = back(gd, n2, acts, qkv, lse, gh, wo_t, o, keep, table, batch, seq, pairs, next(ids))
    gx, gout, gqkv = last(x2, n1, g, gh32, wq, gout, pairs, next(ids))
    y, gx, gqkv, gout, gff, gd = hand_over([y, gx], [gqkv, gout, gff, gd])
    return y.reshape(x.shape), gx.reshape(x.shape), gqkv, gout.swapaxes(1, 2), gff, gd.T


def solution(mesh):
    specs = (P('fsdp'), P('fsdp'), P('fsdp', None, 'tp'), P('tp', None, 'fsdp'), P('fsdp', None, 'tp'), P('tp', 'fsdp'))
    return jax.shard_map(device_step, mesh=mesh, in_specs=specs, out_specs=specs, check_vma=False)
```

```python
import functools

import jax
import jax.numpy as jnp
import numpy as np
from jax import lax
from jax.experimental import pallas as pl
from jax.experimental.pallas import tpu as pltpu
from jax.sharding import PartitionSpec as P

MESH_ID = pl.DeviceIdType.MESH
SIDE = 4
TILE = 128
PIECE = 16
ORDERS = ((2, 1, 0), (1, 0, 2), (0, 2, 1))
BOTH = ((0, 1), (1, -1))
PHASES = THREE = range(3)
TWO = range(2)


class Torus:
    def __init__(self):
        self.core = lax.axis_index('tp')
        self.index = lax.axis_index('fsdp')
        plane, x = lax.div(self.index, SIDE), lax.rem(self.index, SIDE)
        self.at = (lax.div(plane, SIDE), lax.rem(plane, SIDE), x)
        self.partner = (1 - self.core, self.index)
        self.moved = {(axis, by): lax.rem(at + (by + SIDE), SIDE) for axis, at in enumerate(self.at) for by in range(-2, 3)}
        self.peers = {(axis, by): self.place(axis, self.moved[axis, by]) for axis in THREE for by in (-1, 1, 2)}

    def place(self, axis, coord):
        pos = list(self.at)
        pos[axis] = coord
        z, y, x = pos
        return (self.core, (z * SIDE + y) * SIDE + x)

    def shift(self, axis, by):
        return self.moved[axis, by]

    def peer(self, axis, by):
        return self.peers[axis, by]

    def neighbours(self, reach=1):
        return [device for (_, by), device in self.peers.items() if by <= reach]

    def tell(self, sem, devices):
        for device in devices:
            pl.semaphore_signal(sem, inc=1, device_id=device, device_id_type=MESH_ID)

    def barrier(self, devices):
        sem = pltpu.get_barrier_semaphore()
        self.tell(sem, devices)
        pl.semaphore_wait(sem, len(devices))


def pair_of(sems, *at):
    return sems.at[(0,) + at], sems.at[(1,) + at]


def in_order(*calls):
    def run():
        for call in calls:
            call()
    return run


def span(cols):
    (off, width), *rest = cols
    return pl.ds(off, width + sum(w for _, w in rest))


class Gather:
    SEMS = 7

    def __init__(self, net, shard, out, cols, shift, sems, first, direct=False):
        self.net, self.shard, self.out, self.cols, self.moved, self.sems, self.first, self.direct = net, shard, out, cols, shift, sems, first, direct

    def block(self, colour, phase, coord, half=None):
        order = ORDERS[colour]
        off, width = self.cols[colour]
        pick = list(self.net.at)
        for axis in order[:phase]:
            pick[axis] = pl.ds(0, SIDE)
        pick[order[phase]] = coord
        if half is not None and phase:
            pick[order[0]] = pl.ds(half * 2, 2)
        elif half is not None:
            cut = width - width // (2 * TILE) * TILE
            off, width = (off + cut, width - cut) if half else (off, cut)
        return self.out.at[(*pick, slice(None), pl.ds(off, width))] if width else None

    def copy(self, phase, colour, relay, d, by):
        axis = ORDERS[colour][phase]
        far = relay and self.direct
        if far and d:
            return None
        by = 2 if far else by
        back = -by if relay and not far else 0
        dst = src = self.block(colour, phase, self.net.shift(axis, back), d if relay and not far else None)
        if dst is None:
            return None
        if not phase and (far or not relay):
            off, width = self.cols[colour]
            src = self.shard.at[:, pl.ds(off + self.moved, width)]
        return pltpu.make_async_remote_copy(src, dst, *self.sem(phase, relay), device_id=self.net.peer(axis, by), device_id_type=MESH_ID)

    def sem(self, phase, relay):
        return pair_of(self.sems, self.first + 2 * phase + relay)

    def each(self, phase, relay):
        for d, by in BOTH:
            for colour in THREE:
                desc = self.copy(phase, colour, relay, d, by)
                if desc is not None:
                    desc.start()

    def wait(self, phase, relay, side):
        pick = [pl.ds(0, SIDE)] * phase + [pl.ds(0, 2 - relay)] + [0, 0]
        ref = self.out.at[tuple(reversed(pick[:3])) + (slice(None), span(self.cols))]
        pltpu.make_async_copy(ref, ref, self.sem(phase, relay)[side]).wait()

    def own(self):
        at = self.net.at
        cols = span(self.cols)
        src = self.shard.at[:, pl.ds(cols.start + self.moved, cols.size)]
        return pltpu.make_async_copy(src, self.out.at[(*at, slice(None), cols)], self.sems.at[0, self.first + self.SEMS - 1])

    def arrive(self, phase):
        if self.direct:
            self.wait(phase, 0, 1)
        self.wait(phase, 1, 1)

    def start(self, phase):
        if phase:
            self.arrive(phase - 1)
        if phase == 1:
            self.own().wait()
        for relay in range(1 + self.direct):
            self.each(phase, relay)
        if not phase:
            self.own().start()

    def relay(self, phase):
        self.wait(phase, 0, 1)
        self.each(phase, 1)

    def finish(self):
        self.arrive(PHASES[-1])
        for phase in PHASES:
            for relay in TWO:
                self.wait(phase, relay, 0)

    def stages(self):
        steps = (self.start,) if self.direct else (self.start, self.relay)
        return [functools.partial(f, p) for p in PHASES for f in steps] + [self.finish]


class Scatter:
    SEMS = 9

    def __init__(self, net, part, cols, bufs, sems, first, relays=len(PHASES)):
        self.net, self.part, self.cols, self.bufs, self.sems, self.first, self.relays = net, part, cols, bufs, sems, first, relays

    @staticmethod
    def scratch(cols):
        shapes = []
        for _, w in cols:
            shapes += [(3, 2, 2, SIDE, PIECE, w), (3, 2, 2, PIECE, w), (3, 2, PIECE // 2, w)]
        return [pltpu.VMEM(s, jnp.float32) for s in shapes]

    def buf(self, colour, phase):
        return self.bufs[colour * len(PHASES) + phase]

    def block(self, colour, phase, coord, half):
        order = ORDERS[colour]
        off, width = self.cols[colour]
        pick = [pl.ds(0, SIDE)] * 3
        for axis in order[:phase]:
            pick[axis] = self.net.at[axis]
        pick[order[phase]] = coord
        rows = pl.ds(0, PIECE)
        rest = sorted(order[phase + 1:])
        if rest:
            pick[rest[0]] = pl.ds(2 * half, 2)
        else:
            rows = pl.ds(PIECE // 2 * half, PIECE // 2)
        return self.part.at[(*pick, rows, pl.ds(off, width))]

    def copy(self, phase, colour, kind, d, by):
        axis = ORDERS[colour][phase]
        buf = self.buf(colour, phase)
        direct = phase >= self.relays
        if kind == 2 and not direct:
            src = buf.at[0, d]
        elif kind:
            src = self.block(colour, phase, self.net.shift(axis, by), (kind + d) % 2)
        else:
            src = self.block(colour, phase, self.net.shift(axis, 2), d)
            by = 2 if direct else by
        return pltpu.make_async_remote_copy(src, buf.at[kind, d], *self.sem(phase, kind), device_id=self.net.peer(axis, by), device_id_type=MESH_ID)

    def sem(self, phase, kind):
        return pair_of(self.sems, self.first + len(PHASES) * phase + kind)

    def wait(self, phase, kind, side):
        pick = [0] * (phase + 1) + [pl.ds(0, SIDE)] * (2 - phase)
        ref = self.part.at[tuple(pick) + (slice(None), span(self.cols))]
        pltpu.make_async_copy(ref, ref, self.sem(phase, kind)[side]).wait()

    def start(self, phase, kind):
        for d, by in BOTH:
            for colour in THREE:
                self.copy(phase, colour, kind, d, by).start()

    def relay(self, phase):
        self.wait(phase, 0, 1)
        for colour in THREE:
            buf = self.buf(colour, phase)
            for d, by in BOTH:
                buf[0, d] = buf[0, d] + self.block(colour, phase, self.net.shift(ORDERS[colour][phase], by), d)[...]
        self.start(phase, 2)

    def merge(self, phase):
        direct = phase >= self.relays
        for kind in THREE if direct else (1, 2):
            self.wait(phase, kind, 1)
        for colour in THREE:
            buf = self.buf(colour, phase)
            for half in TWO:
                mine = self.block(colour, phase, self.net.at[ORDERS[colour][phase]], half)
                sums = mine[...] + buf[1, 1 - half] + buf[2, half]
                mine[...] = sums + buf[0, half] if direct else sums
        if phase < PHASES[-1]:
            for kind in TWO if phase + 1 < self.relays else THREE:
                self.start(phase + 1, kind)

    def finish(self):
        for phase in PHASES:
            for kind in PHASES:
                self.wait(phase, kind, 0)

    def stages(self):
        calls = [functools.partial(self.start, 0, kind) for kind in TWO]
        for phase in PHASES:
            calls += [functools.partial(self.relay, phase)] * (phase < self.relays) + [functools.partial(self.merge, phase)]
        return calls[:-1] + [in_order(calls[-1], self.finish)]

    def result(self):
        return self.part[self.net.at]


def cut_three(width, off=0, turn=0):
    tiles, ways = width // TILE, len(THREE)
    sizes = [(tiles + (turn - i - 1) % ways) // ways * TILE for i in THREE]
    return [(off + sum(sizes[:i]), s) for i, s in enumerate(sizes)]


def plan(text, *sets):
    left = [iter(s) for s in sets]
    return [(hook, next(left[int(which)])) for hook, field in enumerate(text.split(',')) for which in field]


def halves_of(calls, first=0):
    return [[((when - first) // 2, call) for when, call in calls if when >= first and (when - first) % 2 == odd] for odd in TWO]


def run_at(hook, calls):
    for when, call in calls:
        pl.when(hook == when)(call)


F32, BF16 = jnp.float32, jnp.bfloat16
QB = 256
LANES = TILE
HALF = LANES // 2
CLIP = 8.0
BLOCK = 512
MIB = 2**20


def nt(a, b):
    return lax.dot_general(a, b, (((1,), (1,)), ((), ())), preferred_element_type=F32)


def nn(a, b):
    return jnp.dot(a, b, preferred_element_type=F32)


def tn(a, b):
    return lax.dot_general(a, b, (((0,), (0,)), ((), ())), preferred_element_type=F32)


def along(reduce, values):
    return reduce(values, axis=-1, keepdims=True)


def head_masks(paired):
    lane = lax.broadcasted_iota(jnp.int32, (1, LANES), 1)
    first = lane % HALF < HALF // 2 if paired else lane < HALF
    return first, jnp.logical_not(first)


def causal_tile(key_axis):
    dims = (QB, 2 * QB) if key_axis == 0 else (2 * QB, QB)
    return lax.broadcasted_iota(jnp.int32, dims, key_axis) <= lax.broadcasted_iota(jnp.int32, dims, 1 - key_axis) % QB


def by_head(values, masks):
    return jnp.concatenate([jnp.where(m, values, jnp.zeros((), BF16)) for m in masks], axis=0)


def attend_pair(q_ref, k_ref, v_ref, o_ref, lse_ref):
    masks = head_masks(True)
    key, val = k_ref[...], v_ref[...]
    causal = causal_tile(1)
    first, _ = head_masks(False)
    for lo in reversed(strips(q_ref.shape[0], QB)):
        hi = lo + QB
        query = by_head(q_ref[lo:hi, :], masks)
        diag = jnp.where(causal, nt(query, key[lo:hi]), -1e30)
        top = along(jnp.max, diag)
        if lo:
            past = nt(query, key[:lo])
            top = jnp.maximum(top, along(jnp.max, past))
            past = jnp.exp(past - top)
        diag = jnp.exp(diag - top)
        total = along(jnp.sum, diag)
        if lo:
            total = total + along(jnp.sum, past)
        scale = 1.0 / total
        acc = nn((diag * scale).astype(BF16), val[lo:hi])
        if lo:
            acc = acc + nn((past * scale).astype(BF16), val[:lo])
        o_ref[lo:hi, :] = jnp.where(first, acc[:QB], acc[QB:]).astype(BF16)
        lse = jnp.broadcast_to(top + jnp.log(total), acc.shape).T
        for h in TWO:
            lse_ref[h:h + 1, lo:hi] = lse[:1, h * QB:(h + 1) * QB]


def attend_pair_back(q_ref, k_ref, v_ref, do_ref, lse_ref, dk_ref, dv_ref, put_dq):
    seq = q_ref.shape[0]
    qmask, vmask = head_masks(True), head_masks(False)
    key, val = k_ref[...], v_ref[...]
    key_t = key.astype(F32).T.astype(BF16)
    causal = causal_tile(0)
    first = lax.broadcasted_iota(jnp.int32, (LANES, 1), 0) % HALF < HALF // 2

    def products(lo):
        hi = lo + QB
        query, dout = by_head(q_ref[lo:hi, :], qmask), by_head(do_ref[lo:hi, :], vmask)
        return query, dout, nt(key[:hi], query), nt(val[:hi], dout)

    ahead = products(seq - QB)
    for lo in reversed(strips(seq, QB)):
        hi = lo + QB
        query, dout, score, grad = ahead
        if lo:
            ahead = products(lo - QB)
        prob = jnp.exp(score - jnp.concatenate([lse_ref[h:h + 1, lo:hi] for h in TWO], axis=1))
        diag = jnp.where(causal, prob[lo:], 0.0)
        prob = jnp.concatenate([prob[:lo], diag], axis=0) if lo else diag
        ds = (prob * (grad - jnp.sum(prob * grad, axis=0, keepdims=True))).astype(BF16)
        both = nn(key_t[:, :hi], ds)
        put_dq(lo, hi, jnp.where(first, both[:, :QB], both[:, QB:]).T)
        dv, dk = nn(prob.astype(BF16), dout), nn(ds, query)
        if hi == seq:
            dv_ref[...] = dv
            dk_ref[...] = dk
        else:
            dv_ref[:hi, :] += dv
            dk_ref[:hi, :] += dk


def swap_halves(values):
    return pltpu.roll(values, HALF, axis=1)


COARSE = 32


def tables(seq, head):
    freq = 10000.0 ** (-np.arange(0, head, 2, dtype=np.float64) / head)
    angles = [np.tile(np.arange(seq // COARSE)[:, None] * step * freq, LANES // len(freq)) for step in (1, COARSE)]
    return np.stack([np.stack([np.cos(angle), np.sin(angle)]) for angle in angles]).astype(np.float32)


def spread_tables(table_ref, cos_ref, sin_ref):
    fine_cos, fine_sin = table_ref[0]
    sign = jnp.where(lax.broadcasted_iota(jnp.int32, (1, LANES), 1) < HALF, -1.0, 1.0)

    def body(i):
        rows = aligned(i * COARSE, COARSE)
        cos, sin = table_ref[1, :, pl.ds(i, 1), :]
        cos_ref[rows, :] = fine_cos * cos - fine_sin * sin
        sin_ref[rows, :] = (fine_sin * cos + fine_cos * sin) * sign

    repeat(cos_ref.shape[0] // COARSE, body)


def repeat(count, body):
    def step(i, carry):
        body(i)
        return carry

    lax.fori_loop(0, count, step, 0)


def side_by_side(halves, j):
    return jnp.concatenate([halves[2 * j], halves[2 * j + 1]], axis=1)


def aligned(at, size):
    return pl.ds(pl.multiple_of(at, size), size)


def norm_rows(values):
    mean = along(jnp.mean, values)
    centered = values - mean
    inv = lax.rsqrt(along(jnp.mean, centered * centered) + 1e-5)
    return centered * inv, inv


def norm_grad(grad, normed, inv):
    mean = along(jnp.mean, grad)
    proj = along(jnp.mean, grad * normed)
    return inv * (grad - mean - normed * proj)


def params(collective_id):
    return pltpu.CompilerParams(collective_id=collective_id, has_side_effects=True, vmem_limit_bytes=63 * MIB)


def grid_step():
    return pl.program_id(0), pl.num_programs(0) - 1


def dma(*shape):
    return pltpu.SemaphoreType.DMA(shape)


def shape(dtype, *dims):
    return jax.ShapeDtypeStruct(dims, dtype)


HBM = pl.BlockSpec(memory_space=pltpu.HBM)
WHOLE = pl.BlockSpec(memory_space=pltpu.VMEM)


def lanes(part):
    return slice(LANES * part, LANES * (part + 1))


def strips(width, size):
    return range(0, width, size)


def rows_of(size, width, index):
    return pl.BlockSpec((size, width), lambda step: (index(step), 0))


def stats_rows(seq, index):
    return pl.BlockSpec((1, 1, 2, seq), lambda step: (*index(step), 0, 0))


def project_pair(n1_ref, weight, cos_ref, sin_ref, qkv_ref, keep_ref):
    for lo in strips(n1_ref.shape[0], QB):
        rows = slice(lo, lo + QB)
        raw = nn(n1_ref[rows, :], weight)
        keep_ref[rows, :] = (jnp.abs(raw) < CLIP).astype(F32).astype(BF16)
        raw = jnp.clip(raw, -CLIP, CLIP)
        for part in THREE:
            cols = lanes(part)
            tile = raw[:, cols]
            if part < 2:
                tile = tile * cos_ref[rows, :] + swap_halves(tile) * sin_ref[rows, :]
            if not part:
                tile = tile * 0.125
            qkv_ref[rows, cols] = tile.astype(BF16)


def swap_middle(tile):
    quarter = lax.broadcasted_iota(jnp.int32, tile.shape, 1) // (LANES // 4)
    up, down = pltpu.roll(tile, LANES // 4, axis=1), pltpu.roll(tile, LANES - LANES // 4, axis=1)
    return jnp.where(quarter == 1, down, jnp.where(quarter == 2, up, tile))


CHUNK = 256
CHUNK_STEPS = 4
FRONT_PLAN = '014560145260512430,,4,5,1234,,345,,24,,,,3,,,5,,5'
SCATTER_PLAN = '00,,,,,1,1,,2,0,,,2,12,0,,,,12,0,1,2,012,102,102'
LAST_PLAN = '00,,11,2,0,1,3,22,3,410,,234,4,201,3,402,1342,01,30241'


def to_partner(net, src, dst, send, recv):
    return pltpu.make_async_remote_copy(src, dst, send, recv, device_id=net.partner, device_id_type=MESH_ID)


def front_kernel(x_hbm, qkv_shard, out_shard, ff_shard, down_shard, table_ref, qkv_ref, keep_ref, o_ref, lse_ref, h_hbm, n1_hbm, wq_hbm, wo_hbm, wf_hbm,
                 x_all, n1, w, shards, o_all, part, got, h_buf, wo, sems, gather_sems, load_sem, h_sem, cos_ref, sin_ref, o_buf):
    step, last = grid_step()
    turn = step - 1
    batch, pairs, seq = o_all.shape[:3]
    b, p = turn % batch, turn // batch
    half = CHUNK // 2
    chunks = seq // CHUNK
    ff = down_shard.shape[1]
    net = Torus()
    width = 3 * LANES
    heads_end, out_end = width * pairs, (width + LANES) * pairs
    places = [(w, cut_three(width, width * j), 0) for j in range(pairs)] + [
              (wo_hbm, cut_three(LANES * pairs), heads_end), (wf_hbm, cut_three(3 * ff), out_end)]
    gathers = [Gather(net, shards, out, cols, shift, gather_sems, i * Gather.SEMS, i < pairs) for i, (out, cols, shift) in enumerate(places)]
    strip = x_all.shape[0] // CHUNK_STEPS

    def rows_at(i):
        return aligned(i * strip, strip)

    def load(i):
        return pltpu.make_async_copy(x_hbm.at[rows_at(i)], x_all.at[rows_at(i)], load_sem.at[i])

    def save(i):
        return pltpu.make_async_copy(n1.at[rows_at(i)], n1_hbm.at[rows_at(i)], load_sem.at[i])

    save_weight = pltpu.make_async_copy(w, wq_hbm, load_sem.at[CHUNK_STEPS])

    def normalize(i):
        load(i).wait()
        n1[rows_at(i), :] = norm_rows(x_all[rows_at(i), :].astype(F32))[0].astype(BF16)
        save(i).start()

    def normalize_half(first):
        repeat(CHUNK_STEPS // 2, lambda i: normalize(first + i))

    spread = functools.partial(spread_tables, table_ref, cos_ref, sin_ref)
    calls = plan(FRONT_PLAN, *([*g.stages()] for g in gathers), [in_order(spread, functools.partial(normalize_half, 0)), functools.partial(normalize_half, CHUNK_STEPS // 2)])

    @pl.when(step == 0)
    def _():
        for i in range(CHUNK_STEPS):
            load(i).start()
        for i in THREE:
            heads = qkv_shard[:, i].astype(F32).swapaxes(0, 1)
            for j in range(pairs):
                tile = side_by_side(heads, j)
                shards[:, lanes(3 * j + i)] = (swap_middle(tile) if i < 2 else tile).astype(BF16)
        for j in range(pairs):
            shards[:, lanes(3 * pairs + j)] = side_by_side(out_shard, j)
        both = ff_shard[...].astype(F32)
        for i in range(ff // LANES):
            for j in TWO:
                shards[:, lanes(4 * pairs + 2 * i + j)] = both[:, j, lanes(i)].astype(BF16)
        shards[:, out_end + 2 * ff:] = down_shard[...]
        net.barrier(net.neighbours(2) + [net.partner])
        for when, call in calls:
            if not when:
                call()

    begin, end = halves_of(calls, 1)
    run_at(turn, begin)

    @pl.when(turn >= 0)
    def _():
        weight = w[:, :, :, :, pl.ds(pl.multiple_of(width * p, LANES), width)].reshape(n1.shape[1], width)
        project_pair(n1.at[aligned(b * seq, seq)], weight, cos_ref, sin_ref, qkv_ref, keep_ref)
        q_ref, k_ref, v_ref = (qkv_ref.at[:, pl.ds(LANES * i, LANES)] for i in THREE)
        attend_pair(q_ref, k_ref, v_ref, o_ref, lse_ref.at[0, 0])
        o_all[b, p] = o_ref[...]

    run_at(turn, end)

    def rows_in(c, core):
        return aligned(c * CHUNK + core * half, half)

    def part_copy(b, c):
        return to_partner(net, part.at[b, rows_in(c, 1 - net.core)], got.at[b, c], *pair_of(sems, 0, b, c))

    def rows_out(b, c, core):
        return aligned(b * seq + c * CHUNK + core * half, half)

    def h_copy(b, c, core):
        return to_partner(net, h_buf.at[b, c], h_hbm.at[rows_out(b, c, core)], *pair_of(sems, 1, b, c))

    def h_local(b, c):
        return pltpu.make_async_copy(h_buf.at[b, c], h_hbm.at[rows_out(b, c, net.core)], h_sem.at[b, c])

    def project(b):
        o_buf[...] = jnp.concatenate([o_all[b, j] for j in range(pairs)], axis=1)
        weight = wo[...].reshape(part.shape[2], LANES * pairs)

        def body(c):
            rows = aligned(c * CHUNK, CHUNK)
            part[b, rows, :] = nt(o_buf[rows, :], weight)
            part_copy(b, c).start()

        repeat(chunks, body)

    def combine(b):
        def body(c):
            part_copy(b, c).wait()
            own = rows_in(c, net.core)
            h_buf[b, c] = (x_all[rows_out(b, c, net.core), :].astype(F32) + (part[b, own, :] + got[b, c])).astype(BF16)
            h_copy(b, c, net.core).start()
            h_local(b, c).start()

        repeat(chunks, body)

    def settle():
        for b in range(batch):
            for c in range(chunks):
                h_copy(b, c, net.core).wait_send()
                h_local(b, c).wait()
                h_copy(b, c, 1 - net.core).wait_recv()
        for i in range(CHUNK_STEPS):
            save(i).wait()
        save_weight.wait()

    fetch = pltpu.make_async_copy(wo_hbm, wo, h_sem.at[0, 0])
    run_at(last - step, [(2, fetch.start), (2, save_weight.start), (1, fetch.wait), (0, functools.partial(combine, 0))])

    @pl.when(step + 1 >= last)
    def _():
        project(step + 1 - last)

    run_at(last - step, [(0, functools.partial(combine, 1)), (0, settle)])
    run_at(turn + 1, begin[-1:])


def front(x, qkv_shard, out_shard, ff_shard, down_shard, table, batch, seq, collective_id):
    pairs = len(out_shard) // 2
    rows, d = x.shape
    width = 3 * LANES
    chunks = seq // CHUNK
    vm = pltpu.VMEM
    torus = (SIDE, SIDE, SIDE, PIECE)
    shards = [s.size // PIECE for s in (qkv_shard, out_shard, ff_shard, down_shard)]
    turn = lambda s: jnp.maximum(s - 1, 0)
    head = lambda width: pl.BlockSpec((seq, width), lambda s: (turn(s) % batch, turn(s) // batch))
    return pl.pallas_call(
        front_kernel,
        grid=(1 + batch * pairs,),
        in_specs=[HBM] + [WHOLE] * 5,
        out_specs=[head(width), head(width), head(LANES), stats_rows(seq, lambda s: (turn(s) % batch, turn(s) // batch))] + [HBM] * 5,
        out_shape=[shape(BF16, rows, width * pairs)] * 2 + [shape(BF16, rows, LANES * pairs), shape(F32, batch, pairs, 2, seq), shape(BF16, rows, d), shape(BF16, rows, d),
                   shape(BF16, *torus, shards[0]), shape(BF16, *torus, shards[1]), shape(BF16, *torus, shards[2] + shards[3])],
        scratch_shapes=[vm((rows, d), BF16), vm((rows, d), BF16), vm(torus + (width * pairs,), BF16), vm((PIECE, sum(shards)), BF16),
                        vm((batch, pairs, seq, LANES), BF16), vm((batch, seq, d), F32), vm((batch, chunks, CHUNK // 2, d), F32), vm((batch, chunks, CHUNK // 2, d), BF16),
                        vm(torus + (shards[1],), BF16), dma(2, 2, batch, chunks), dma(2, (pairs + 2) * Gather.SEMS), dma(CHUNK_STEPS + 1), dma(batch, chunks)] + [vm((seq, LANES), F32)] * 2 + [vm((seq, LANES * pairs), BF16)],
        compiler_params=params(collective_id),
        name='front',
    )(x, qkv_shard, out_shard, ff_shard, down_shard, table)


class Exchange:
    def __init__(self, net, rows, partials, results, sems, local_sem):
        self.net, self.rows, self.partials, self.results, self.sems, self.local_sem = net, rows, partials, results, sems, local_sem

    def half(self, core, at=0):
        return aligned(at * self.rows + core * (self.rows // 2), self.rows // 2)

    def part(self, which, at):
        part, got = self.partials[which]
        return to_partner(self.net, part.at[at % 2, self.half(1 - self.net.core)], got.at[at], *pair_of(self.sems, which, at))

    def arrive(self, at):
        for which in range(len(self.partials)):
            self.part(which, at).wait()

    def total(self, which, at):
        part, got = self.partials[which]
        return part[at % 2, self.half(self.net.core), :] + got[at]

    def results_of(self, at, core, act):
        for i, (buf, hbm) in enumerate(self.results):
            act(buf.at[at % 2], hbm.at[self.half(core, at)], pair_of(self.sems, len(self.partials) + i, at), self.local_sem.at[i, at % 2])

    def publish(self, at):
        def act(buf, rows, sem, local_sem):
            to_partner(self.net, buf, rows, *sem).start()
            pltpu.make_async_copy(buf, rows, local_sem).start()
        self.results_of(at, self.net.core, act)

    def settle(self, at):
        def act(buf, rows, sem, local_sem):
            to_partner(self.net, buf, rows, *sem).wait_send()
            pltpu.make_async_copy(buf, rows, local_sem).wait()
        self.results_of(at, self.net.core, act)
        self.results_of(at, 1 - self.net.core, lambda buf, rows, sem, local_sem: to_partner(self.net, buf, rows, *sem).wait_recv())

    def settle_tail(self, blocks):
        for at in TWO:
            self.settle(blocks - len(TWO) + at)


def mlp_kernel(blocks, h_ref, gy_ref, weights, y_hbm, gh_hbm, gh32_ref, acts_hbm, n2_ref, gd_hbm,
               wff_ref, wd_ref, saved, grad_down, part_y, part_g, got_y, got_g, y_buf, gh_buf, h_own, gy_own, sems, local_sem, save_sem, load_sem):
    step, final = grid_step()
    rows, d = h_ref.shape
    ff = wd_ref.shape[1]
    acts = saved.at[step % 2]
    gug, act = acts.at[:, pl.ds(0, 2 * ff)], acts.at[:, pl.ds(2 * ff, ff)]

    def save(at):
        return pltpu.make_async_copy(saved.at[at % 2], acts_hbm.at[aligned(at * rows, rows)], save_sem.at[at % 2])

    save_grad = pltpu.make_async_copy(grad_down, gd_hbm, save_sem.at[2])
    net = Torus()
    swap = Exchange(net, rows, ((part_y, got_y), (part_g, got_g)), ((y_buf, y_hbm), (gh_buf, gh_hbm)), sems, local_sem)

    loads = [pltpu.make_async_copy(weights.at[:, pl.ds(at, dst.shape[1])], dst, load_sem.at[i]) for i, (dst, at) in enumerate(((wd_ref, 2 * ff), (wff_ref, 0)))]

    @pl.when(step == 0)
    def _():
        for copy in loads:
            copy.start()
        net.barrier([net.partner])
        for copy in loads:
            copy.wait()

    @pl.when((step > 1) & (step < blocks))
    def _():
        save(step - 2).wait()

    @pl.when(step < blocks)
    def _():
        n2, _ = norm_rows(h_ref[...].astype(F32))
        n2 = n2.astype(BF16)
        n2_ref[...] = n2
        gy = gy_ref[...]
        for j in strips(ff, QB):
            w = min(QB, ff - j)
            gact = nn(gy, wd_ref[:, j:j + w])
            for i in range(j, j + w, LANES):
                at, mid, end = 2 * i, 2 * i + LANES, 2 * i + QB
                ug = nn(n2, wff_ref[:, at:end])
                up, gate = ug[:, :LANES], ug[:, LANES:]
                sig = 1.0 / (1.0 + jnp.exp(-gate))
                silu = gate * sig
                act[:, i:i + LANES] = (silu * up).astype(BF16)
                ga = gact[:, i - j:i - j + LANES]
                gug[:, at:mid] = (ga * silu).astype(BF16)
                gug[:, mid:end] = (ga * up * sig * (1.0 + gate * (1.0 - sig))).astype(BF16)

        for which, left, right, part in ((0, act, wd_ref, part_y), (1, gug, wff_ref, part_g)):
            for j in strips(d, QB):
                part[step % 2, :, j:j + QB] = nt(left[...], right[j:j + QB, :])
            swap.part(which, step).start()
        save(step).start()

    done = (step + blocks) % (blocks + 1)

    @pl.when(step > 2)
    def _():
        swap.settle(step - 3)

    @pl.when(step > 0)
    def _():
        swap.arrive(done)

    def combine():
        hidden = h_own[...].astype(F32)
        normed, inv = norm_rows(hidden)
        y_buf[done % 2] = (hidden + swap.total(0, done)).astype(BF16)
        gh = gy_own[...].astype(F32) + norm_grad(swap.total(1, done), normed, inv)
        gh32_ref[...] = gh
        gh_buf[done % 2] = gh.astype(BF16)

    @pl.when(step < blocks)
    def _():
        accumulate(grad_down, step == 0, gy_ref[...], act)
        combine()

    @pl.when(step == blocks - 1)
    def _():
        save_grad.start()

    pl.when(step == blocks)(combine)

    @pl.when(step > 0)
    def _():
        swap.publish(done)

    own = swap.half(net.core)
    h_own[...] = h_ref[own, :]
    gy_own[...] = gy_ref[own, :]

    @pl.when(step == blocks)
    def _():
        swap.settle_tail(blocks)
        for at in TWO:
            save(blocks - len(TWO) + at).wait()
        save_grad.wait()


def mlp(h, gy, weights, collective_id, block=BLOCK):
    rows, d = h.shape
    ff = weights.shape[1] // 3
    half = block // 2
    blocks = rows // block
    torus = (SIDE, SIDE, SIDE, PIECE)
    row = lambda width: rows_of(block, width, lambda i: jnp.minimum(i, blocks - 1))
    vm = pltpu.VMEM
    return pl.pallas_call(
        functools.partial(mlp_kernel, blocks),
        grid=(blocks + 1,),
        in_specs=[row(d), row(d), HBM],
        out_specs=[HBM, HBM, rows_of(half, d, lambda i: jnp.maximum(i - 1, 0)), HBM, row(d), HBM],
        out_shape=[shape(BF16, rows, d), shape(BF16, rows, d), shape(F32, rows // 2, d), shape(BF16, rows, 3 * ff), shape(BF16, rows, d), shape(F32, *torus, ff)],
        scratch_shapes=[vm((d, 2 * ff), BF16), vm((d, ff), BF16), vm((2, block, 3 * ff), BF16), vm(torus + (ff,), F32)] + [vm((2, block, d), F32)] * 2 + [vm((blocks + 1, half, d), F32)] * 2 + [vm((2, half, d), BF16)] * 2 + [vm((half, d), BF16)] * 2 + [dma(2, 4, blocks), dma(2, 2), dma(3), dma(2)],
        compiler_params=params(collective_id),
        name='mlp',
    )(h, gy, weights)


def accumulate(part, first, left, right):
    for j in strips(right.shape[1], QB):
        w = min(QB, right.shape[1] - j)
        prod = tn(left, right[:, j:j + w]).reshape(part.shape[:-1] + (w,))
        at = slice(j, j + w)
        part[..., at] = jnp.where(first, 0.0, part[..., at]) + prod


SETS = 3
HEAD_STEP = (SETS - 1) * CHUNK_STEPS


def back_kernel(pairs, gd_hbm, n2_ref, act_ref, qkv_ref, lse_ref, gh_hbm, wo_hbm, o_hbm, keep_ref, table_ref,
                g_ref, gw_ref, gd_ref, gff_ref, cos_ref, sin_ref, do_ref, dk_ref, dv_ref, gh_ref, wo_ref, o_ref, parts, sems, load_sem, *bufs):
    step, final = grid_step()
    turn = step - HEAD_STEP
    p = turn % pairs
    half = gh_ref.shape[0] // 2
    net = Torus()
    per = len(bufs) // SETS
    scatters = [Scatter(net, parts.at[i], cut_three(parts.shape[-1], turn=i), bufs[per * i:per * i + per], sems, i * Scatter.SEMS) for i in range(SETS)]
    calls = plan(SCATTER_PLAN, *(s.stages() for s in scatters))
    begin, end = halves_of(calls, HEAD_STEP + 1)

    def fetch(b):
        rows = aligned(b * 2 * half, 2 * half)
        return [pltpu.make_async_copy(src.at[rows], dst, load_sem.at[i]) for i, (src, dst) in enumerate(((gh_hbm, gh_ref), (o_hbm, o_ref)))]

    load = pltpu.make_async_copy(gd_hbm, parts.at[0], load_sem.at[2])
    fetch_weight = pltpu.make_async_copy(wo_hbm, wo_ref, load_sem.at[3])

    @pl.when(step == 0)
    def _():
        for copy in [load] + fetch(0) + [fetch_weight]:
            copy.start()
        spread_tables(table_ref, cos_ref, sin_ref)
        net.barrier(net.neighbours())
        load.wait()
        for when, call in calls:
            if not when:
                call()

    @pl.when(turn < 0)
    def _():
        accumulate(parts.at[1 + step // CHUNK_STEPS], step % CHUNK_STEPS == 0, n2_ref[...], act_ref)

    run_at(step + 1, [c for c in calls if 0 < c[0] <= HEAD_STEP])

    def put(part, lo, hi, values):
        cols = lanes(part)
        if part < 2:
            values = values * cos_ref[lo:hi, :] - swap_halves(values) * sin_ref[lo:hi, :]
        g_ref[lo:hi, cols] = (values * keep_ref[lo:hi, cols].astype(F32)).astype(BF16)

    put_dq = lambda lo, hi, dq: put(0, lo, hi, dq * 0.125)

    @pl.when(turn >= 0)
    def _():
        @pl.when(p == 0)
        def _():
            pl.when(turn == 0)(fetch_weight.wait)
            for copy in fetch(turn // pairs):
                copy.wait()
            gw_ref[...] = jnp.where(turn == 0, 0.0, gw_ref[...])

            def body(i):
                rows = aligned(i * half, half)
                gh = gh_ref[rows, :]
                dout = nn(gh, wo_ref[...]).astype(BF16)
                for j in range(pairs):
                    do_ref[j, rows, :] = dout[:, lanes(j)]
                gw_ref[...] += tn(gh, o_ref[rows, :])

            repeat(len(TWO), body)

            @pl.when(turn == 0)
            def _():
                for copy in fetch(turn + 1):
                    copy.start()

        run_at(turn, begin)
        q_ref, k_ref, v_ref = (qkv_ref.at[:, pl.ds(LANES * i, LANES)] for i in THREE)
        attend_pair_back(q_ref, k_ref, v_ref, do_ref.at[p], lse_ref.at[0, 0], dk_ref, dv_ref, put_dq)
        for part, grad in ((1, dk_ref), (2, dv_ref)):
            put(part, 0, 2 * half, grad[...])
        run_at(turn, end)

    @pl.when(step == final)
    def _():
        gd_ref[...], *halves = [s.result() for s in scatters]
        tiles = jnp.concatenate(halves, axis=1)
        for i in range(tiles.shape[1] // LANES):
            gff_ref[:, i % 2, lanes(i // 2)] = tiles[:, lanes(i)]


def back(gd, n2, acts, qkv, lse, gh, wo_t, o, keep, table, batch, seq, pairs, collective_id):
    rows, d = n2.shape
    ff = acts.shape[1] // SETS
    block = rows // CHUNK_STEPS
    turn = lambda s: jnp.maximum(s - HEAD_STEP, 0)
    head = pl.BlockSpec((seq, 3 * LANES), lambda s: (turn(s) // pairs, turn(s) % pairs))
    late = lambda s: jnp.where(s < HEAD_STEP, s % CHUNK_STEPS, CHUNK_STEPS - 1)
    vm = pltpu.VMEM
    return pl.pallas_call(
        functools.partial(back_kernel, pairs),
        grid=(HEAD_STEP + batch * pairs,),
        in_specs=[HBM, rows_of(block, d, late), pl.BlockSpec((block, ff), lambda s: (late(s), jnp.minimum(s // CHUNK_STEPS, 1))), head, stats_rows(seq, lambda s: (turn(s) // pairs, turn(s) % pairs)),
                  HBM, HBM, HBM, head, WHOLE],
        out_specs=[head, WHOLE, WHOLE, WHOLE],
        out_shape=[shape(BF16, *qkv.shape), shape(F32, *wo_t.shape), shape(F32, PIECE, ff), shape(F32, PIECE, 2, ff)],
        scratch_shapes=[vm((seq, LANES), F32)] * 2 + [vm((pairs, seq, LANES), BF16)] + [vm((seq, LANES), F32)] * 2 + [vm((seq, d), BF16), vm(wo_t.shape, BF16), vm((seq, LANES * pairs), BF16), vm((SETS, SIDE, SIDE, SIDE, PIECE, ff), F32),
                        dma(2, SETS * Scatter.SEMS), dma(4)] + [s for i in range(SETS) for s in Scatter.scratch(cut_three(ff, turn=i))],
        compiler_params=params(collective_id),
        name='back',
    )(gd, n2, acts, qkv, lse, gh, wo_t, o, keep, table)


def last_kernel(pairs, blocks, n1_hbm, g_ref, x_ref, g_row, gh_ref, w_hbm, gout_hbm, gx_hbm, gout_ref, gw_ref,
                n1_ref, w_ref, part_out, part_qkv, part, got, buf, sems, scatter_sems, local_sem, load_sem, *bufs):
    step, final = grid_step()
    turn = step - pairs
    rows, d = x_ref.shape
    net = Torus()
    per = len(bufs) // (pairs + 1)
    parts = [part_out] + [part_qkv.at[j] for j in range(pairs)]
    scatters = [Scatter(net, s, cut_three(s.shape[-1], turn=i), bufs[per * i:per * i + per], scatter_sems, i * Scatter.SEMS, 1 if i > pairs // 2 else len(PHASES)) for i, s in enumerate(parts)]
    calls = plan(LAST_PLAN, *(s.stages() for s in scatters))
    swap = Exchange(net, rows, ((part, got),), ((buf, gx_hbm),), sems, local_sem)

    loads = [pltpu.make_async_copy(src, dst, load_sem.at[i]) for i, (src, dst) in enumerate(((gout_hbm, part_out), (n1_hbm, n1_ref), (w_hbm, w_ref)))]
    pl.when(turn == 0)(loads[-1].wait)

    @pl.when(step == 0)
    def _():
        for copy in loads:
            copy.start()
        net.barrier(net.neighbours(2) + [net.partner])
        for copy in loads[:-1]:
            copy.wait()

    begin, end = halves_of(calls)
    run_at(step, begin)

    @pl.when(turn < 0)
    def _():
        size = n1_ref.shape[0] // len(TWO)

        def body(i):
            accumulate(part_qkv.at[step], i == 0, n1_ref[aligned(i * size, size), :], g_ref.at[aligned(i * size, size)])

        repeat(len(TWO), body)

    @pl.when((turn >= 0) & (turn < blocks))
    def _():
        def body(i):
            cols = aligned(i * QB, QB)
            part[turn % 2, :, cols] = nt(g_row[...], w_ref[cols, :])

        repeat(d // QB, body)
        swap.part(0, turn).start()

    run_at(step, end)

    @pl.when(turn > 2)
    def _():
        swap.settle(turn - 3)

    @pl.when(turn > 0)
    def _():
        done = turn - 1
        swap.arrive(done)
        normed, inv = norm_rows(x_ref[swap.half(net.core), :].astype(F32))
        buf[done % 2] = (gh_ref[...] + norm_grad(swap.total(0, done), normed, inv)).astype(BF16)
        swap.publish(done)

    @pl.when(turn == blocks)
    def _():
        for when, call in calls:
            if when > 2 * (pairs + blocks) + 1:
                call()
        swap.settle_tail(blocks)
        out, *sums = [s.result() for s in scatters]
        halves = slice(HALF), slice(HALF, LANES)
        for j in range(pairs):
            for h, cols in enumerate(halves):
                gout_ref[2 * j + h] = out[:, lanes(j)][:, cols]
        for i in THREE:
            tiles = [swap_middle(s[:, lanes(i)]) if i < 2 else s[:, lanes(i)] for s in sums]
            gw_ref[:, i] = jnp.stack([t[:, cols] for t in tiles for cols in halves]).swapaxes(0, 1)


def last(x, n1, g, gh32, w, gout, pairs, collective_id, block=BLOCK):
    rows, d = x.shape
    blocks = rows // block
    late = lambda n, width, by: rows_of(n, width, lambda s: jnp.clip(s - pairs - by, 0, blocks - 1))
    head = pl.BlockSpec((rows, 3 * LANES), lambda s: (0, jnp.minimum(s, pairs - 1)))
    vm = pltpu.VMEM
    half = block // 2
    torus = (SIDE, SIDE, SIDE, PIECE)
    gout = gout.reshape(torus + (-1,))
    return pl.pallas_call(
        functools.partial(last_kernel, pairs, blocks),
        grid=(pairs + blocks + 1,),
        in_specs=[HBM, head, late(block, d, 1), late(block, g.shape[1], 0), late(half, d, 1), HBM, HBM],
        out_specs=[HBM, WHOLE, WHOLE],
        out_shape=[shape(BF16, rows, d), shape(F32, 2 * pairs, PIECE, HALF), shape(F32, PIECE, 3, 2 * pairs, HALF)],
        scratch_shapes=[vm((rows, d), BF16), vm(w.shape, BF16), vm(gout.shape, F32), vm((pairs,) + torus + (3 * LANES,), F32), vm((2, block, d), F32), vm((blocks, half, d), F32), vm((2, half, d), BF16),
                        dma(2, 2, blocks), dma(2, (pairs + 1) * Scatter.SEMS), dma(1, 2), dma(3)] + Scatter.scratch(cut_three(gout.shape[-1])) + Scatter.scratch(cut_three(3 * LANES)) * pairs,
        compiler_params=params(collective_id),
        name='last',
    )(n1, g, x, g, gh32, w, gout)


def hand_over_kernel(*refs):
    count = len(refs) // 2
    for src, dst in zip(refs[:count], refs[count:]):
        dst[...] = src[...]


def hand_over(wide, small, block=2 * BLOCK):
    rows, width = wide[0].shape
    specs = [rows_of(block, width, lambda i: i) for v in wide] + [WHOLE for v in small]
    return pl.pallas_call(
        hand_over_kernel,
        grid=(rows // block,),
        in_specs=specs,
        out_specs=specs,
        out_shape=[shape(v.dtype, *v.shape) for v in wide + small],
        compiler_params=pltpu.CompilerParams(vmem_limit_bytes=63 * MIB),
        name='hand_over',
    )(*wide, *small)


def device_step(x, grad_y, w_qkv, w_out, w_ff, w_down):
    batch, seq, d = x.shape
    heads, head = w_qkv.shape[2:]
    pairs = heads // 2
    table = jnp.asarray(tables(seq, head))
    ids = iter(range(SIDE))
    x2, gy = (v.reshape(batch * seq, d) for v in (x, grad_y))
    qkv, keep, o, lse, h, n1, *weights = front(x2, w_qkv, w_out.swapaxes(1, 2), w_ff, w_down.T, table, batch, seq, next(ids))
    wq, wo_t, wf = (w.reshape(d, w.shape[-1]) for w in weights)
    y, gh, gh32, acts, n2, gd = mlp(h, gy, wf, next(ids))
    g, gout, gd, gff = back(gd, n2, acts, qkv, lse, gh, wo_t, o, keep, table, batch, seq, pairs, next(ids))
    gx, gout, gqkv = last(x2, n1, g, gh32, wq, gout, pairs, next(ids))
    y, gx, gqkv, gout, gff, gd = hand_over([y, gx], [gqkv, gout, gff, gd])
    return y.reshape(x.shape), gx.reshape(x.shape), gqkv, gout.swapaxes(1, 2), gff, gd.T


def solution(mesh):
    specs = (P('fsdp'), P('fsdp'), P('fsdp', None, 'tp'), P('tp', None, 'fsdp'), P('fsdp', None, 'tp'), P('tp', 'fsdp'))
    return jax.shard_map(device_step, mesh=mesh, in_specs=specs, out_specs=specs, check_vma=False)
```

```python
import functools

import jax
import jax.numpy as jnp
import numpy as np
from jax import lax
from jax.experimental import pallas as pl
from jax.experimental.pallas import tpu as pltpu
from jax.sharding import PartitionSpec as P

MESH_ID = pl.DeviceIdType.MESH
SIDE = 4
TILE = 128
PIECE = 16
ORDERS = ((2, 1, 0), (1, 0, 2), (0, 2, 1))
BOTH = ((0, 1), (1, -1))
PHASES = THREE = range(3)
TWO = range(2)


class Torus:
    def __init__(self):
        self.core = lax.axis_index('tp')
        self.index = lax.axis_index('fsdp')
        plane, x = lax.div(self.index, SIDE), lax.rem(self.index, SIDE)
        self.at = (lax.div(plane, SIDE), lax.rem(plane, SIDE), x)
        self.partner = (1 - self.core, self.index)
        self.moved = {(axis, by): lax.rem(at + (by + SIDE), SIDE) for axis, at in enumerate(self.at) for by in range(-2, 3)}
        self.peers = {(axis, by): self.place(axis, self.moved[axis, by]) for axis in THREE for by in (-1, 1, 2)}

    def place(self, axis, coord):
        pos = list(self.at)
        pos[axis] = coord
        z, y, x = pos
        return (self.core, (z * SIDE + y) * SIDE + x)

    def shift(self, axis, by):
        return self.moved[axis, by]

    def peer(self, axis, by):
        return self.peers[axis, by]

    def neighbours(self, reach=1):
        return [device for (_, by), device in self.peers.items() if by <= reach]

    def tell(self, sem, devices):
        for device in devices:
            pl.semaphore_signal(sem, inc=1, device_id=device, device_id_type=MESH_ID)

    def barrier(self, devices):
        sem = pltpu.get_barrier_semaphore()
        self.tell(sem, devices)
        pl.semaphore_wait(sem, len(devices))


def pair_of(sems, *at):
    return sems.at[(0,) + at], sems.at[(1,) + at]


def in_order(*calls):
    def run():
        for call in calls:
            call()
    return run


def span(cols):
    (off, width), *rest = cols
    return pl.ds(off, width + sum(w for _, w in rest))


class Gather:
    SEMS = 7

    def __init__(self, net, shard, out, cols, shift, sems, first, direct=False):
        self.net, self.shard, self.out, self.cols, self.moved, self.sems, self.first, self.direct = net, shard, out, cols, shift, sems, first, direct

    def block(self, colour, phase, coord, half=None):
        order = ORDERS[colour]
        off, width = self.cols[colour]
        pick = list(self.net.at)
        for axis in order[:phase]:
            pick[axis] = pl.ds(0, SIDE)
        pick[order[phase]] = coord
        if half is not None and phase:
            pick[order[0]] = pl.ds(half * 2, 2)
        elif half is not None:
            cut = width - width // (2 * TILE) * TILE
            off, width = (off + cut, width - cut) if half else (off, cut)
        return self.out.at[(*pick, slice(None), pl.ds(off, width))] if width else None

    def copy(self, phase, colour, relay, d, by):
        axis = ORDERS[colour][phase]
        far = relay and self.direct
        if far and d:
            return None
        by = 2 if far else by
        back = -by if relay and not far else 0
        dst = src = self.block(colour, phase, self.net.shift(axis, back), d if relay and not far else None)
        if dst is None:
            return None
        if not phase and (far or not relay):
            off, width = self.cols[colour]
            src = self.shard.at[:, pl.ds(off + self.moved, width)]
        return pltpu.make_async_remote_copy(src, dst, *self.sem(phase, relay), device_id=self.net.peer(axis, by), device_id_type=MESH_ID)

    def sem(self, phase, relay):
        return pair_of(self.sems, self.first + 2 * phase + relay)

    def each(self, phase, relay):
        for d, by in BOTH:
            for colour in THREE:
                desc = self.copy(phase, colour, relay, d, by)
                if desc is not None:
                    desc.start()

    def wait(self, phase, relay, side):
        pick = [pl.ds(0, SIDE)] * phase + [pl.ds(0, 2 - relay)] + [0, 0]
        ref = self.out.at[tuple(reversed(pick[:3])) + (slice(None), span(self.cols))]
        pltpu.make_async_copy(ref, ref, self.sem(phase, relay)[side]).wait()

    def own(self):
        at = self.net.at
        cols = span(self.cols)
        src = self.shard.at[:, pl.ds(cols.start + self.moved, cols.size)]
        return pltpu.make_async_copy(src, self.out.at[(*at, slice(None), cols)], self.sems.at[0, self.first + self.SEMS - 1])

    def arrive(self, phase):
        if self.direct:
            self.wait(phase, 0, 1)
        self.wait(phase, 1, 1)

    def start(self, phase):
        if phase:
            self.arrive(phase - 1)
        if phase == 1:
            self.own().wait()
        for relay in range(1 + self.direct):
            self.each(phase, relay)
        if not phase:
            self.own().start()

    def relay(self, phase):
        self.wait(phase, 0, 1)
        self.each(phase, 1)

    def finish(self):
        self.arrive(PHASES[-1])
        for phase in PHASES:
            for relay in TWO:
                self.wait(phase, relay, 0)

    def stages(self):
        steps = (self.start,) if self.direct else (self.start, self.relay)
        return [functools.partial(f, p) for p in PHASES for f in steps] + [self.finish]


class Scatter:
    SEMS = 9

    def __init__(self, net, part, cols, bufs, sems, first, relays=len(PHASES)):
        self.net, self.part, self.cols, self.bufs, self.sems, self.first, self.relays = net, part, cols, bufs, sems, first, relays

    @staticmethod
    def scratch(cols):
        shapes = []
        for _, w in cols:
            shapes += [(3, 2, 2, SIDE, PIECE, w), (3, 2, 2, PIECE, w), (3, 2, PIECE // 2, w)]
        return [pltpu.VMEM(s, jnp.float32) for s in shapes]

    def buf(self, colour, phase):
        return self.bufs[colour * len(PHASES) + phase]

    def block(self, colour, phase, coord, half):
        order = ORDERS[colour]
        off, width = self.cols[colour]
        pick = [pl.ds(0, SIDE)] * 3
        for axis in order[:phase]:
            pick[axis] = self.net.at[axis]
        pick[order[phase]] = coord
        rows = pl.ds(0, PIECE)
        rest = sorted(order[phase + 1:])
        if rest:
            pick[rest[0]] = pl.ds(2 * half, 2)
        else:
            rows = pl.ds(PIECE // 2 * half, PIECE // 2)
        return self.part.at[(*pick, rows, pl.ds(off, width))]

    def copy(self, phase, colour, kind, d, by):
        axis = ORDERS[colour][phase]
        buf = self.buf(colour, phase)
        direct = phase >= self.relays
        if kind == 2 and not direct:
            src = buf.at[0, d]
        elif kind:
            src = self.block(colour, phase, self.net.shift(axis, by), (kind + d) % 2)
        else:
            src = self.block(colour, phase, self.net.shift(axis, 2), d)
            by = 2 if direct else by
        return pltpu.make_async_remote_copy(src, buf.at[kind, d], *self.sem(phase, kind), device_id=self.net.peer(axis, by), device_id_type=MESH_ID)

    def sem(self, phase, kind):
        return pair_of(self.sems, self.first + len(PHASES) * phase + kind)

    def wait(self, phase, kind, side):
        pick = [0] * (phase + 1) + [pl.ds(0, SIDE)] * (2 - phase)
        ref = self.part.at[tuple(pick) + (slice(None), span(self.cols))]
        pltpu.make_async_copy(ref, ref, self.sem(phase, kind)[side]).wait()

    def start(self, phase, kind):
        for d, by in BOTH:
            for colour in THREE:
                self.copy(phase, colour, kind, d, by).start()

    def relay(self, phase):
        self.wait(phase, 0, 1)
        for colour in THREE:
            buf = self.buf(colour, phase)
            for d, by in BOTH:
                buf[0, d] = buf[0, d] + self.block(colour, phase, self.net.shift(ORDERS[colour][phase], by), d)[...]
        self.start(phase, 2)

    def merge(self, phase):
        direct = phase >= self.relays
        for kind in THREE if direct else (1, 2):
            self.wait(phase, kind, 1)
        for colour in THREE:
            buf = self.buf(colour, phase)
            for half in TWO:
                mine = self.block(colour, phase, self.net.at[ORDERS[colour][phase]], half)
                sums = mine[...] + buf[1, 1 - half] + buf[2, half]
                mine[...] = sums + buf[0, half] if direct else sums
        if phase < PHASES[-1]:
            for kind in TWO if phase + 1 < self.relays else THREE:
                self.start(phase + 1, kind)

    def finish(self):
        for phase in PHASES:
            for kind in PHASES:
                self.wait(phase, kind, 0)

    def stages(self):
        calls = [functools.partial(self.start, 0, kind) for kind in TWO]
        for phase in PHASES:
            calls += [functools.partial(self.relay, phase)] * (phase < self.relays) + [functools.partial(self.merge, phase)]
        return calls[:-1] + [in_order(calls[-1], self.finish)]

    def result(self):
        return self.part[self.net.at]


def cut_three(width, off=0, turn=0):
    tiles, ways = width // TILE, len(THREE)
    sizes = [(tiles + (turn - i - 1) % ways) // ways * TILE for i in THREE]
    return [(off + sum(sizes[:i]), s) for i, s in enumerate(sizes)]


def plan(text, *sets):
    left = [iter(s) for s in sets]
    return [(hook, next(left[int(which)])) for hook, field in enumerate(text.split(',')) for which in field]


def halves_of(calls, first=0):
    return [[((when - first) // 2, call) for when, call in calls if when >= first and (when - first) % 2 == odd] for odd in TWO]


def run_at(hook, calls):
    for when, call in calls:
        pl.when(hook == when)(call)


F32, BF16 = jnp.float32, jnp.bfloat16
QB = 256
LANES = TILE
HALF = LANES // 2
PAIR = 3 * LANES
CLIP = 8.0
BLOCK = 512
MIB = 2**20


def nt(a, b):
    return lax.dot_general(a, b, (((1,), (1,)), ((), ())), preferred_element_type=F32)


def nn(a, b):
    return jnp.dot(a, b, preferred_element_type=F32)


def tn(a, b):
    return lax.dot_general(a, b, (((0,), (0,)), ((), ())), preferred_element_type=F32)


def along(reduce, values):
    return reduce(values, axis=-1, keepdims=True)


def head_masks(paired):
    lane = lax.broadcasted_iota(jnp.int32, (1, LANES), 1)
    first = lane % HALF < HALF // 2 if paired else lane < HALF
    return first, jnp.logical_not(first)


def causal_tile(key_axis):
    dims = (QB, 2 * QB) if key_axis == 0 else (2 * QB, QB)
    return lax.broadcasted_iota(jnp.int32, dims, key_axis) <= lax.broadcasted_iota(jnp.int32, dims, 1 - key_axis) % QB


def by_head(values, masks):
    return jnp.concatenate([jnp.where(m, values, jnp.zeros((), BF16)) for m in masks], axis=0)


def attend_pair(q_ref, k_ref, v_ref, o_ref, lse_ref):
    masks = head_masks(True)
    key, val = k_ref[...], v_ref[...]
    causal = causal_tile(1)
    first, _ = head_masks(False)
    for lo in reversed(strips(q_ref.shape[0], QB)):
        hi = lo + QB
        query = by_head(q_ref[lo:hi, :], masks)
        diag = jnp.where(causal, nt(query, key[lo:hi]), -1e30)
        top = along(jnp.max, diag)
        if lo:
            past = nt(query, key[:lo])
            top = jnp.maximum(top, along(jnp.max, past))
            past = jnp.exp(past - top)
        diag = jnp.exp(diag - top)
        total = along(jnp.sum, diag)
        if lo:
            total = total + along(jnp.sum, past)
        scale = 1.0 / total
        acc = nn((diag * scale).astype(BF16), val[lo:hi])
        if lo:
            acc = acc + nn((past * scale).astype(BF16), val[:lo])
        o_ref[lo:hi, :] = jnp.where(first, acc[:QB], acc[QB:]).astype(BF16)
        lse = jnp.broadcast_to(top + jnp.log(total), acc.shape).T
        for h in TWO:
            lse_ref[h:h + 1, lo:hi] = lse[:1, h * QB:(h + 1) * QB]


def attend_pair_back(q_ref, k_ref, v_ref, do_ref, lse_ref, dk_ref, dv_ref, put_dq):
    seq = q_ref.shape[0]
    qmask, vmask = head_masks(True), head_masks(False)
    key, val = k_ref[...], v_ref[...]
    key_t = key.astype(F32).T.astype(BF16)
    causal = causal_tile(0)
    first = lax.broadcasted_iota(jnp.int32, (LANES, 1), 0) % HALF < HALF // 2

    def products(lo):
        hi = lo + QB
        query, dout = by_head(q_ref[lo:hi, :], qmask), by_head(do_ref[lo:hi, :], vmask)
        return query, dout, nt(key[:hi], query), nt(val[:hi], dout)

    ahead = products(seq - QB)
    for lo in reversed(strips(seq, QB)):
        hi = lo + QB
        query, dout, score, grad = ahead
        if lo:
            ahead = products(lo - QB)
        prob = jnp.exp(score - jnp.concatenate([lse_ref[h:h + 1, lo:hi] for h in TWO], axis=1))
        diag = jnp.where(causal, prob[lo:], 0.0)
        prob = jnp.concatenate([prob[:lo], diag], axis=0) if lo else diag
        ds = (prob * (grad - jnp.sum(prob * grad, axis=0, keepdims=True))).astype(BF16)
        both = nn(key_t[:, :hi], ds)
        put_dq(lo, hi, jnp.where(first, both[:, :QB], both[:, QB:]).T)
        dv, dk = nn(prob.astype(BF16), dout), nn(ds, query)
        if hi == seq:
            dv_ref[...] = dv
            dk_ref[...] = dk
        else:
            dv_ref[:hi, :] += dv
            dk_ref[:hi, :] += dk


def swap_halves(values):
    return pltpu.roll(values, HALF, axis=1)


COARSE = 32


def tables(seq, head):
    freq = 10000.0 ** (-np.arange(0, head, 2, dtype=np.float64) / head)
    angles = [np.tile(np.arange(seq // COARSE)[:, None] * step * freq, LANES // len(freq)) for step in (1, COARSE)]
    return np.stack([np.stack([np.cos(angle), np.sin(angle)]) for angle in angles]).astype(np.float32)


def spread_tables(table_ref, cos_ref, sin_ref):
    fine_cos, fine_sin = table_ref[0]
    sign = jnp.where(lax.broadcasted_iota(jnp.int32, (1, LANES), 1) < HALF, -1.0, 1.0)

    def body(i):
        rows = aligned(i * COARSE, COARSE)
        cos, sin = table_ref[1, :, pl.ds(i, 1), :]
        cos_ref[rows, :] = fine_cos * cos - fine_sin * sin
        sin_ref[rows, :] = (fine_sin * cos + fine_cos * sin) * sign

    repeat(cos_ref.shape[0] // COARSE, body)


def repeat(count, body):
    def step(i, carry):
        body(i)
        return carry

    lax.fori_loop(0, count, step, 0)


def side_by_side(halves, j):
    return jnp.concatenate([halves[2 * j], halves[2 * j + 1]], axis=1)


def aligned(at, size):
    return pl.ds(pl.multiple_of(at, size), size)


def norm_rows(values):
    mean = along(jnp.mean, values)
    centered = values - mean
    inv = lax.rsqrt(along(jnp.mean, centered * centered) + 1e-5)
    return centered * inv, inv


def norm_grad(grad, normed, inv):
    mean = along(jnp.mean, grad)
    proj = along(jnp.mean, grad * normed)
    return inv * (grad - mean - normed * proj)


def params(collective_id):
    return pltpu.CompilerParams(collective_id=collective_id, has_side_effects=True, vmem_limit_bytes=63 * MIB)


def grid_step():
    return pl.program_id(0), pl.num_programs(0) - 1


def dma(*shape):
    return pltpu.SemaphoreType.DMA(shape)


def shape(dtype, *dims):
    return jax.ShapeDtypeStruct(dims, dtype)


HBM = pl.BlockSpec(memory_space=pltpu.HBM)
WHOLE = pl.BlockSpec(memory_space=pltpu.VMEM)


def lanes(part):
    return slice(LANES * part, LANES * (part + 1))


def strips(width, size):
    return range(0, width, size)


def rows_of(size, width, index):
    return pl.BlockSpec((size, width), lambda step: (index(step), 0))


def stats_rows(seq, index):
    return pl.BlockSpec((1, 1, 2, seq), lambda step: (*index(step), 0, 0))


def project_pair(n1_ref, weight, cos_ref, sin_ref, qkv_ref, keep_ref):
    for lo in strips(n1_ref.shape[0], QB):
        rows = slice(lo, lo + QB)
        raw = nn(n1_ref[rows, :], weight)
        keep_ref[rows, :] = (jnp.abs(raw) < CLIP).astype(F32).astype(BF16)
        raw = jnp.clip(raw, -CLIP, CLIP)
        for part in THREE:
            cols = lanes(part)
            tile = raw[:, cols]
            if part < 2:
                tile = tile * cos_ref[rows, :] + swap_halves(tile) * sin_ref[rows, :]
            if not part:
                tile = tile * 0.125
            qkv_ref[rows, cols] = tile.astype(BF16)


def swap_middle(tile):
    quarter = lax.broadcasted_iota(jnp.int32, tile.shape, 1) // (LANES // 4)
    up, down = pltpu.roll(tile, LANES // 4, axis=1), pltpu.roll(tile, LANES - LANES // 4, axis=1)
    return jnp.where(quarter == 1, down, jnp.where(quarter == 2, up, tile))


CHUNK = 256
CHUNK_STEPS = 4
FRONT_PLAN = '014560145260512430,,4,5,1234,,345,,24,,,,3,,,5,,5'
SCATTER_PLAN = '00,,,,,1,1,,2,0,,,2,12,0,,,,12,0,1,2,012,102,102'
LAST_PLAN = '00,,11,2,0,1,3,22,3,410,,234,4,201,3,402,1342,01,30241'


def to_partner(net, src, dst, send, recv):
    return pltpu.make_async_remote_copy(src, dst, send, recv, device_id=net.partner, device_id_type=MESH_ID)


def front_kernel(x_hbm, qkv_shard, out_shard, ff_shard, down_shard, table_ref, qkv_hbm, keep_hbm, o_hbm, lse_ref, h_hbm, n1_hbm, wq_hbm, wo_hbm, wf_hbm,
                 x_all, n1, w, shards, o_all, part, got, h_buf, wo, sems, gather_sems, load_sem, h_sem, cos_ref, sin_ref, o_buf, qkv_all, keep_all, store_sem):
    step, last = grid_step()
    turn = step - 1
    batch, pairs, seq = o_all.shape[:3]
    b, p = turn % batch, turn // batch
    half = CHUNK // 2
    chunks = seq // CHUNK
    ff = down_shard.shape[1]
    net = Torus()
    width = PAIR
    heads_end, out_end = width * pairs, (width + LANES) * pairs
    places = [(w, cut_three(width, width * j), 0) for j in range(pairs)] + [
              (wo_hbm, cut_three(LANES * pairs), heads_end), (wf_hbm, cut_three(3 * ff), out_end)]
    gathers = [Gather(net, shards, out, cols, shift, gather_sems, i * Gather.SEMS, i < pairs) for i, (out, cols, shift) in enumerate(places)]
    strip = x_all.shape[0] // CHUNK_STEPS

    def rows_at(i):
        return aligned(i * strip, strip)

    def load(i):
        return pltpu.make_async_copy(x_hbm.at[rows_at(i)], x_all.at[rows_at(i)], load_sem.at[i])

    def save(i):
        return pltpu.make_async_copy(n1.at[rows_at(i)], n1_hbm.at[rows_at(i)], load_sem.at[i])

    save_weight = pltpu.make_async_copy(w, wq_hbm, load_sem.at[CHUNK_STEPS])

    def normalize(i):
        load(i).wait()
        n1[rows_at(i), :] = norm_rows(x_all[rows_at(i), :].astype(F32))[0].astype(BF16)
        save(i).start()

    def normalize_half(first):
        repeat(CHUNK_STEPS // 2, lambda i: normalize(first + i))

    spread = functools.partial(spread_tables, table_ref, cos_ref, sin_ref)
    calls = plan(FRONT_PLAN, *([*g.stages()] for g in gathers), [in_order(spread, functools.partial(normalize_half, 0)), functools.partial(normalize_half, CHUNK_STEPS // 2)])

    @pl.when(step == 0)
    def _():
        for i in range(CHUNK_STEPS):
            load(i).start()
        for i in THREE:
            heads = qkv_shard[:, i].astype(F32).swapaxes(0, 1)
            for j in range(pairs):
                tile = side_by_side(heads, j)
                shards[:, lanes(3 * j + i)] = (swap_middle(tile) if i < 2 else tile).astype(BF16)
        for j in range(pairs):
            shards[:, lanes(3 * pairs + j)] = side_by_side(out_shard, j)
        both = ff_shard[...].astype(F32)
        for i in range(ff // LANES):
            for j in TWO:
                shards[:, lanes(4 * pairs + 2 * i + j)] = both[:, j, lanes(i)].astype(BF16)
        shards[:, out_end + 2 * ff:] = down_shard[...]
        net.barrier(net.neighbours(2) + [net.partner])
        for when, call in calls:
            if not when:
                call()

    begin, end = halves_of(calls, 1)
    run_at(turn, begin)

    def store(b, p):
        out = []
        for i, (src, dst) in enumerate(((qkv_all.at[b], qkv_hbm), (keep_all.at[b], keep_hbm), (o_all.at[b, p], o_hbm))):
            size = src.shape[-1]
            out.append(pltpu.make_async_copy(src, dst.at[aligned(b * seq, seq), aligned(p * size, size)], store_sem.at[i, b]))
        return out

    @pl.when(turn >= batch)
    def _():
        for copy in store(b, p - 1):
            copy.wait()

    @pl.when(turn >= 0)
    def _():
        qkv_ref, keep_ref = qkv_all.at[b], keep_all.at[b]
        weight = w[:, :, :, :, pl.ds(pl.multiple_of(width * p, LANES), width)].reshape(n1.shape[1], width)
        project_pair(n1.at[aligned(b * seq, seq)], weight, cos_ref, sin_ref, qkv_ref, keep_ref)
        q_ref, k_ref, v_ref = (qkv_ref.at[:, pl.ds(LANES * i, LANES)] for i in THREE)
        attend_pair(q_ref, k_ref, v_ref, o_all.at[b, p], lse_ref.at[0, 0])
        for copy in store(b, p):
            copy.start()

    run_at(turn, end)

    def rows_in(c, core):
        return aligned(c * CHUNK + core * half, half)

    def part_copy(b, c):
        return to_partner(net, part.at[b, rows_in(c, 1 - net.core)], got.at[b, c], *pair_of(sems, 0, b, c))

    def rows_out(b, c, core):
        return aligned(b * seq + c * CHUNK + core * half, half)

    def h_copy(b, c, core):
        return to_partner(net, h_buf.at[b, c], h_hbm.at[rows_out(b, c, core)], *pair_of(sems, 1, b, c))

    def h_local(b, c):
        return pltpu.make_async_copy(h_buf.at[b, c], h_hbm.at[rows_out(b, c, net.core)], h_sem.at[b, c])

    def project(b):
        o_buf[...] = jnp.concatenate([o_all[b, j] for j in range(pairs)], axis=1)
        weight = wo[...].reshape(part.shape[2], LANES * pairs)

        def body(c):
            rows = aligned(c * CHUNK, CHUNK)
            part[b, rows, :] = nt(o_buf[rows, :], weight)
            part_copy(b, c).start()

        repeat(chunks, body)

    def combine(b):
        def body(c):
            part_copy(b, c).wait()
            own = rows_in(c, net.core)
            h_buf[b, c] = (x_all[rows_out(b, c, net.core), :].astype(F32) + (part[b, own, :] + got[b, c])).astype(BF16)
            h_copy(b, c, net.core).start()
            h_local(b, c).start()

        repeat(chunks, body)

    def settle():
        for b in range(batch):
            for c in range(chunks):
                h_copy(b, c, net.core).wait_send()
                h_local(b, c).wait()
                h_copy(b, c, 1 - net.core).wait_recv()
        for b in range(batch):
            for copy in store(b, pairs - 1):
                copy.wait()
        for i in range(CHUNK_STEPS):
            save(i).wait()
        save_weight.wait()

    fetch = pltpu.make_async_copy(wo_hbm, wo, h_sem.at[0, 0])
    run_at(last - step, [(2, fetch.start), (2, save_weight.start), (1, fetch.wait), (0, functools.partial(combine, 0))])

    @pl.when(step + 1 >= last)
    def _():
        project(step + 1 - last)

    run_at(last - step, [(0, functools.partial(combine, 1)), (0, settle)])
    run_at(turn + 1, begin[-1:])


def front(x, qkv_shard, out_shard, ff_shard, down_shard, table, batch, seq, collective_id):
    pairs = len(out_shard) // 2
    rows, d = x.shape
    width = PAIR
    chunks = seq // CHUNK
    vm = pltpu.VMEM
    torus = (SIDE, SIDE, SIDE, PIECE)
    shards = [s.size // PIECE for s in (qkv_shard, out_shard, ff_shard, down_shard)]
    turn = lambda s: jnp.maximum(s - 1, 0)
    return pl.pallas_call(
        front_kernel,
        grid=(1 + batch * pairs,),
        in_specs=[HBM] + [WHOLE] * 5,
        out_specs=[HBM] * 3 + [stats_rows(seq, lambda s: (turn(s) % batch, turn(s) // batch))] + [HBM] * 5,
        out_shape=[shape(BF16, rows, width * pairs)] * 2 + [shape(BF16, rows, LANES * pairs), shape(F32, batch, pairs, 2, seq), shape(BF16, rows, d), shape(BF16, rows, d),
                   shape(BF16, *torus, shards[0]), shape(BF16, *torus, shards[1]), shape(BF16, *torus, shards[2] + shards[3])],
        scratch_shapes=[vm((rows, d), BF16), vm((rows, d), BF16), vm(torus + (width * pairs,), BF16), vm((PIECE, sum(shards)), BF16),
                        vm((batch, pairs, seq, LANES), BF16), vm((batch, seq, d), F32), vm((batch, chunks, CHUNK // 2, d), F32), vm((batch, chunks, CHUNK // 2, d), BF16),
                        vm(torus + (shards[1],), BF16), dma(2, 2, batch, chunks), dma(2, (pairs + 2) * Gather.SEMS), dma(CHUNK_STEPS + 1), dma(batch, chunks)] + [vm((seq, LANES), F32)] * 2 + [vm((seq, LANES * pairs), BF16)] + [vm((batch, seq, width), BF16)] * 2 + [dma(3, batch)],
        compiler_params=params(collective_id),
        name='front',
    )(x, qkv_shard, out_shard, ff_shard, down_shard, table)


class Exchange:
    def __init__(self, net, rows, partials, results, sems, local_sem):
        self.net, self.rows, self.partials, self.results, self.sems, self.local_sem = net, rows, partials, results, sems, local_sem

    def half(self, core, at=0):
        return aligned(at * self.rows + core * (self.rows // 2), self.rows // 2)

    def part(self, which, at):
        part, got = self.partials[which]
        return to_partner(self.net, part.at[at % 2, self.half(1 - self.net.core)], got.at[at], *pair_of(self.sems, which, at))

    def arrive(self, at):
        for which in range(len(self.partials)):
            self.part(which, at).wait()

    def total(self, which, at):
        part, got = self.partials[which]
        return part[at % 2, self.half(self.net.core), :] + got[at]

    def results_of(self, at, core, act):
        for i, (buf, hbm) in enumerate(self.results):
            act(buf.at[at % 2], hbm.at[self.half(core, at)], pair_of(self.sems, len(self.partials) + i, at), self.local_sem.at[i, at % 2])

    def publish(self, at):
        def act(buf, rows, sem, local_sem):
            to_partner(self.net, buf, rows, *sem).start()
            pltpu.make_async_copy(buf, rows, local_sem).start()
        self.results_of(at, self.net.core, act)

    def settle(self, at):
        def act(buf, rows, sem, local_sem):
            to_partner(self.net, buf, rows, *sem).wait_send()
            pltpu.make_async_copy(buf, rows, local_sem).wait()
        self.results_of(at, self.net.core, act)
        self.results_of(at, 1 - self.net.core, lambda buf, rows, sem, local_sem: to_partner(self.net, buf, rows, *sem).wait_recv())

    def settle_tail(self, blocks):
        for at in TWO:
            self.settle(blocks - len(TWO) + at)


def mlp_kernel(blocks, h_ref, gy_ref, weights, y_hbm, gh_hbm, gh32_ref, acts_hbm, n2_ref, gd_hbm,
               wff_ref, wd_ref, saved, grad_down, part_y, part_g, got_y, got_g, y_buf, gh_buf, h_own, gy_own, sems, local_sem, save_sem, load_sem):
    step, final = grid_step()
    rows, d = h_ref.shape
    ff = wd_ref.shape[1]
    acts = saved.at[step % 2]
    gug, act = acts.at[:, pl.ds(0, 2 * ff)], acts.at[:, pl.ds(2 * ff, ff)]

    def save(at):
        return pltpu.make_async_copy(saved.at[at % 2], acts_hbm.at[aligned(at * rows, rows)], save_sem.at[at % 2])

    save_grad = pltpu.make_async_copy(grad_down, gd_hbm, save_sem.at[2])
    net = Torus()
    swap = Exchange(net, rows, ((part_y, got_y), (part_g, got_g)), ((y_buf, y_hbm), (gh_buf, gh_hbm)), sems, local_sem)

    loads = [pltpu.make_async_copy(weights.at[:, pl.ds(at, dst.shape[1])], dst, load_sem.at[i]) for i, (dst, at) in enumerate(((wd_ref, 2 * ff), (wff_ref, 0)))]

    @pl.when(step == 0)
    def _():
        for copy in loads:
            copy.start()
        net.barrier([net.partner])
        for copy in loads:
            copy.wait()

    @pl.when((step > 1) & (step < blocks))
    def _():
        save(step - 2).wait()

    @pl.when(step < blocks)
    def _():
        n2, _ = norm_rows(h_ref[...].astype(F32))
        n2 = n2.astype(BF16)
        n2_ref[...] = n2
        gy = gy_ref[...]
        for j in strips(ff, QB):
            w = min(QB, ff - j)
            gact = nn(gy, wd_ref[:, j:j + w])
            for i in range(j, j + w, LANES):
                at, mid, end = 2 * i, 2 * i + LANES, 2 * i + QB
                ug = nn(n2, wff_ref[:, at:end])
                up, gate = ug[:, :LANES], ug[:, LANES:]
                sig = 1.0 / (1.0 + jnp.exp(-gate))
                silu = gate * sig
                act[:, i:i + LANES] = (silu * up).astype(BF16)
                ga = gact[:, i - j:i - j + LANES]
                gug[:, at:mid] = (ga * silu).astype(BF16)
                gug[:, mid:end] = (ga * up * sig * (1.0 + gate * (1.0 - sig))).astype(BF16)

        for which, left, right, part in ((0, act, wd_ref, part_y), (1, gug, wff_ref, part_g)):
            for j in strips(d, QB):
                part[step % 2, :, j:j + QB] = nt(left[...], right[j:j + QB, :])
            swap.part(which, step).start()
        save(step).start()

    done = (step + blocks) % (blocks + 1)

    @pl.when(step > 2)
    def _():
        swap.settle(step - 3)

    @pl.when(step > 0)
    def _():
        swap.arrive(done)

    def combine():
        hidden = h_own[...].astype(F32)
        normed, inv = norm_rows(hidden)
        y_buf[done % 2] = (hidden + swap.total(0, done)).astype(BF16)
        gh = gy_own[...].astype(F32) + norm_grad(swap.total(1, done), normed, inv)
        gh32_ref[...] = gh
        gh_buf[done % 2] = gh.astype(BF16)

    @pl.when(step < blocks)
    def _():
        accumulate(grad_down, step == 0, gy_ref[...], act)
        combine()

    @pl.when(step == blocks - 1)
    def _():
        save_grad.start()

    pl.when(step == blocks)(combine)

    @pl.when(step > 0)
    def _():
        swap.publish(done)

    own = swap.half(net.core)
    h_own[...] = h_ref[own, :]
    gy_own[...] = gy_ref[own, :]

    @pl.when(step == blocks)
    def _():
        swap.settle_tail(blocks)
        for at in TWO:
            save(blocks - len(TWO) + at).wait()
        save_grad.wait()


def mlp(h, gy, weights, collective_id, block=BLOCK):
    rows, d = h.shape
    ff = weights.shape[1] // 3
    half = block // 2
    blocks = rows // block
    torus = (SIDE, SIDE, SIDE, PIECE)
    row = lambda width: rows_of(block, width, lambda i: jnp.minimum(i, blocks - 1))
    vm = pltpu.VMEM
    return pl.pallas_call(
        functools.partial(mlp_kernel, blocks),
        grid=(blocks + 1,),
        in_specs=[row(d), row(d), HBM],
        out_specs=[HBM, HBM, rows_of(half, d, lambda i: jnp.maximum(i - 1, 0)), HBM, row(d), HBM],
        out_shape=[shape(BF16, rows, d), shape(BF16, rows, d), shape(F32, rows // 2, d), shape(BF16, rows, 3 * ff), shape(BF16, rows, d), shape(F32, *torus, ff)],
        scratch_shapes=[vm((d, 2 * ff), BF16), vm((d, ff), BF16), vm((2, block, 3 * ff), BF16), vm(torus + (ff,), F32)] + [vm((2, block, d), F32)] * 2 + [vm((blocks + 1, half, d), F32)] * 2 + [vm((2, half, d), BF16)] * 2 + [vm((half, d), BF16)] * 2 + [dma(2, 4, blocks), dma(2, 2), dma(3), dma(2)],
        compiler_params=params(collective_id),
        name='mlp',
    )(h, gy, weights)


def accumulate(part, first, left, right):
    for j in strips(right.shape[1], QB):
        w = min(QB, right.shape[1] - j)
        prod = tn(left, right[:, j:j + w]).reshape(part.shape[:-1] + (w,))
        at = slice(j, j + w)
        part[..., at] = jnp.where(first, 0.0, part[..., at]) + prod


SETS = 3
HEAD_STEP = (SETS - 1) * CHUNK_STEPS


def back_kernel(pairs, gd_hbm, n2_ref, act_ref, qkv_ref, lse_ref, gh_hbm, wo_hbm, o_hbm, keep_ref, table_ref,
                g_ref, gw_ref, gd_ref, gff_ref, cos_ref, sin_ref, do_ref, dk_ref, dv_ref, gh_ref, wo_ref, o_ref, parts, sems, load_sem, *bufs):
    step, final = grid_step()
    turn = step - HEAD_STEP
    p = turn % pairs
    half = gh_ref.shape[0] // 2
    net = Torus()
    per = len(bufs) // SETS
    scatters = [Scatter(net, parts.at[i], cut_three(parts.shape[-1], turn=i), bufs[per * i:per * i + per], sems, i * Scatter.SEMS) for i in range(SETS)]
    calls = plan(SCATTER_PLAN, *(s.stages() for s in scatters))
    begin, end = halves_of(calls, HEAD_STEP + 1)

    def fetch(b):
        rows = aligned(b * 2 * half, 2 * half)
        return [pltpu.make_async_copy(src.at[rows], dst, load_sem.at[i]) for i, (src, dst) in enumerate(((gh_hbm, gh_ref), (o_hbm, o_ref)))]

    load = pltpu.make_async_copy(gd_hbm, parts.at[0], load_sem.at[2])
    fetch_weight = pltpu.make_async_copy(wo_hbm, wo_ref, load_sem.at[3])

    @pl.when(step == 0)
    def _():
        for copy in [load] + fetch(0) + [fetch_weight]:
            copy.start()
        spread_tables(table_ref, cos_ref, sin_ref)
        net.barrier(net.neighbours())
        load.wait()
        for when, call in calls:
            if not when:
                call()

    @pl.when(turn < 0)
    def _():
        accumulate(parts.at[1 + step // CHUNK_STEPS], step % CHUNK_STEPS == 0, n2_ref[...], act_ref)

    run_at(step + 1, [c for c in calls if 0 < c[0] <= HEAD_STEP])

    def put(part, lo, hi, values):
        cols = lanes(part)
        if part < 2:
            values = values * cos_ref[lo:hi, :] - swap_halves(values) * sin_ref[lo:hi, :]
        g_ref[lo:hi, cols] = (values * keep_ref[lo:hi, cols].astype(F32)).astype(BF16)

    put_dq = lambda lo, hi, dq: put(0, lo, hi, dq * 0.125)

    @pl.when(turn >= 0)
    def _():
        @pl.when(p == 0)
        def _():
            pl.when(turn == 0)(fetch_weight.wait)
            for copy in fetch(turn // pairs):
                copy.wait()
            gw_ref[...] = jnp.where(turn == 0, 0.0, gw_ref[...])

            def body(i):
                rows = aligned(i * half, half)
                gh = gh_ref[rows, :]
                dout = nn(gh, wo_ref[...]).astype(BF16)
                for j in range(pairs):
                    do_ref[j, rows, :] = dout[:, lanes(j)]
                gw_ref[...] += tn(gh, o_ref[rows, :])

            repeat(len(TWO), body)

            @pl.when(turn == 0)
            def _():
                for copy in fetch(turn + 1):
                    copy.start()

        run_at(turn, begin)
        q_ref, k_ref, v_ref = (qkv_ref.at[:, pl.ds(LANES * i, LANES)] for i in THREE)
        attend_pair_back(q_ref, k_ref, v_ref, do_ref.at[p], lse_ref.at[0, 0], dk_ref, dv_ref, put_dq)
        for part, grad in ((1, dk_ref), (2, dv_ref)):
            put(part, 0, 2 * half, grad[...])
        run_at(turn, end)

    @pl.when(step == final)
    def _():
        gd_ref[...], *halves = [s.result() for s in scatters]
        tiles = jnp.concatenate(halves, axis=1)
        for i in range(tiles.shape[1] // LANES):
            gff_ref[:, i % 2, lanes(i // 2)] = tiles[:, lanes(i)]


def back(gd, n2, acts, qkv, lse, gh, wo_t, o, keep, table, batch, seq, pairs, collective_id):
    rows, d = n2.shape
    ff = acts.shape[1] // SETS
    block = rows // CHUNK_STEPS
    turn = lambda s: jnp.maximum(s - HEAD_STEP, 0)
    head = pl.BlockSpec((seq, PAIR), lambda s: (turn(s) // pairs, turn(s) % pairs))
    late = lambda s: jnp.where(s < HEAD_STEP, s % CHUNK_STEPS, CHUNK_STEPS - 1)
    vm = pltpu.VMEM
    return pl.pallas_call(
        functools.partial(back_kernel, pairs),
        grid=(HEAD_STEP + batch * pairs,),
        in_specs=[HBM, rows_of(block, d, late), pl.BlockSpec((block, ff), lambda s: (late(s), jnp.minimum(s // CHUNK_STEPS, 1))), head, stats_rows(seq, lambda s: (turn(s) // pairs, turn(s) % pairs)),
                  HBM, HBM, HBM, head, WHOLE],
        out_specs=[head, WHOLE, WHOLE, WHOLE],
        out_shape=[shape(BF16, *qkv.shape), shape(F32, *wo_t.shape), shape(F32, PIECE, ff), shape(F32, PIECE, 2, ff)],
        scratch_shapes=[vm((seq, LANES), F32)] * 2 + [vm((pairs, seq, LANES), BF16)] + [vm((seq, LANES), F32)] * 2 + [vm((seq, d), BF16), vm(wo_t.shape, BF16), vm((seq, LANES * pairs), BF16), vm((SETS, SIDE, SIDE, SIDE, PIECE, ff), F32),
                        dma(2, SETS * Scatter.SEMS), dma(4)] + [s for i in range(SETS) for s in Scatter.scratch(cut_three(ff, turn=i))],
        compiler_params=params(collective_id),
        name='back',
    )(gd, n2, acts, qkv, lse, gh, wo_t, o, keep, table)


def last_kernel(pairs, blocks, n1_hbm, g_ref, x_ref, g_row, gh_ref, w_hbm, gout_hbm, gx_hbm, gout_ref, gw_ref,
                n1_ref, w_ref, part_out, part_qkv, part, got, buf, sems, scatter_sems, local_sem, load_sem, *bufs):
    step, final = grid_step()
    turn = step - pairs
    rows, d = x_ref.shape
    net = Torus()
    per = len(bufs) // (pairs + 1)
    parts = [part_out] + [part_qkv.at[j] for j in range(pairs)]
    scatters = [Scatter(net, s, cut_three(s.shape[-1], turn=i), bufs[per * i:per * i + per], scatter_sems, i * Scatter.SEMS, 1 if i > pairs // 2 else len(PHASES)) for i, s in enumerate(parts)]
    calls = plan(LAST_PLAN, *(s.stages() for s in scatters))
    swap = Exchange(net, rows, ((part, got),), ((buf, gx_hbm),), sems, local_sem)

    loads = [pltpu.make_async_copy(src, dst, load_sem.at[i]) for i, (src, dst) in enumerate(((gout_hbm, part_out), (n1_hbm, n1_ref), (w_hbm, w_ref)))]
    pl.when(turn == 0)(loads[-1].wait)

    @pl.when(step == 0)
    def _():
        for copy in loads:
            copy.start()
        net.barrier(net.neighbours(2) + [net.partner])
        for copy in loads[:-1]:
            copy.wait()

    begin, end = halves_of(calls)
    run_at(step, begin)

    @pl.when(turn < 0)
    def _():
        size = n1_ref.shape[0] // len(TWO)

        def body(i):
            accumulate(part_qkv.at[step], i == 0, n1_ref[aligned(i * size, size), :], g_ref.at[aligned(i * size, size)])

        repeat(len(TWO), body)

    @pl.when((turn >= 0) & (turn < blocks))
    def _():
        def body(i):
            cols = aligned(i * QB, QB)
            part[turn % 2, :, cols] = nt(g_row[...], w_ref[cols, :])

        repeat(d // QB, body)
        swap.part(0, turn).start()

    run_at(step, end)

    @pl.when(turn > 2)
    def _():
        swap.settle(turn - 3)

    @pl.when(turn > 0)
    def _():
        done = turn - 1
        swap.arrive(done)
        normed, inv = norm_rows(x_ref[swap.half(net.core), :].astype(F32))
        buf[done % 2] = (gh_ref[...] + norm_grad(swap.total(0, done), normed, inv)).astype(BF16)
        swap.publish(done)

    @pl.when(turn == blocks)
    def _():
        for when, call in calls:
            if when > 2 * (pairs + blocks) + 1:
                call()
        swap.settle_tail(blocks)
        out, *sums = [s.result() for s in scatters]
        halves = slice(HALF), slice(HALF, LANES)
        for j in range(pairs):
            for h, cols in enumerate(halves):
                gout_ref[2 * j + h] = out[:, lanes(j)][:, cols]
        for i in THREE:
            tiles = [swap_middle(s[:, lanes(i)]) if i < 2 else s[:, lanes(i)] for s in sums]
            gw_ref[:, i] = jnp.stack([t[:, cols] for t in tiles for cols in halves]).swapaxes(0, 1)


def last(x, n1, g, gh32, w, gout, pairs, collective_id, block=BLOCK):
    rows, d = x.shape
    blocks = rows // block
    late = lambda n, width, by: rows_of(n, width, lambda s: jnp.clip(s - pairs - by, 0, blocks - 1))
    head = pl.BlockSpec((rows, PAIR), lambda s: (0, jnp.minimum(s, pairs - 1)))
    vm = pltpu.VMEM
    half = block // 2
    torus = (SIDE, SIDE, SIDE, PIECE)
    gout = gout.reshape(torus + (-1,))
    return pl.pallas_call(
        functools.partial(last_kernel, pairs, blocks),
        grid=(pairs + blocks + 1,),
        in_specs=[HBM, head, late(block, d, 1), late(block, g.shape[1], 0), late(half, d, 1), HBM, HBM],
        out_specs=[HBM, WHOLE, WHOLE],
        out_shape=[shape(BF16, rows, d), shape(F32, 2 * pairs, PIECE, HALF), shape(F32, PIECE, 3, 2 * pairs, HALF)],
        scratch_shapes=[vm((rows, d), BF16), vm(w.shape, BF16), vm(gout.shape, F32), vm((pairs,) + torus + (PAIR,), F32), vm((2, block, d), F32), vm((blocks, half, d), F32), vm((2, half, d), BF16),
                        dma(2, 2, blocks), dma(2, (pairs + 1) * Scatter.SEMS), dma(1, 2), dma(3)] + Scatter.scratch(cut_three(gout.shape[-1])) + Scatter.scratch(cut_three(PAIR)) * pairs,
        compiler_params=params(collective_id),
        name='last',
    )(n1, g, x, g, gh32, w, gout)


def hand_over_kernel(*refs):
    count = len(refs) // 2
    for src, dst in zip(refs[:count], refs[count:]):
        dst[...] = src[...]


def hand_over(wide, small, block=2 * BLOCK):
    rows, width = wide[0].shape
    specs = [rows_of(block, width, lambda i: i) for v in wide] + [WHOLE for v in small]
    return pl.pallas_call(
        hand_over_kernel,
        grid=(rows // block,),
        in_specs=specs,
        out_specs=specs,
        out_shape=[shape(v.dtype, *v.shape) for v in wide + small],
        compiler_params=pltpu.CompilerParams(vmem_limit_bytes=63 * MIB),
        name='hand_over',
    )(*wide, *small)


def device_step(x, grad_y, w_qkv, w_out, w_ff, w_down):
    batch, seq, d = x.shape
    heads, head = w_qkv.shape[2:]
    pairs = heads // 2
    table = jnp.asarray(tables(seq, head))
    ids = iter(range(SIDE))
    x2, gy = (v.reshape(batch * seq, d) for v in (x, grad_y))
    qkv, keep, o, lse, h, n1, *weights = front(x2, w_qkv, w_out.swapaxes(1, 2), w_ff, w_down.T, table, batch, seq, next(ids))
    wq, wo_t, wf = (w.reshape(d, w.shape[-1]) for w in weights)
    y, gh, gh32, acts, n2, gd = mlp(h, gy, wf, next(ids))
    g, gout, gd, gff = back(gd, n2, acts, qkv, lse, gh, wo_t, o, keep, table, batch, seq, pairs, next(ids))
    gx, gout, gqkv = last(x2, n1, g, gh32, wq, gout, pairs, next(ids))
    y, gx, gqkv, gout, gff, gd = hand_over([y, gx], [gqkv, gout, gff, gd])
    return y.reshape(x.shape), gx.reshape(x.shape), gqkv, gout.swapaxes(1, 2), gff, gd.T


def solution(mesh):
    specs = (P('fsdp'), P('fsdp'), P('fsdp', None, 'tp'), P('tp', None, 'fsdp'), P('fsdp', None, 'tp'), P('tp', 'fsdp'))
    return jax.shard_map(device_step, mesh=mesh, in_specs=specs, out_specs=specs, check_vma=False)
```

```python
import functools

import jax
import jax.numpy as jnp
import numpy as np
from jax import lax
from jax.experimental import pallas as pl
from jax.experimental.pallas import tpu as pltpu
from jax.sharding import PartitionSpec as P

MESH_ID = pl.DeviceIdType.MESH
SIDE = 4
TILE = 128
PIECE = 16
ORDERS = ((2, 1, 0), (1, 0, 2), (0, 2, 1))
BOTH = ((0, 1), (1, -1))
PHASES = THREE = range(3)
TWO = range(2)


class Torus:
    def __init__(self):
        self.core = lax.axis_index('tp')
        self.index = lax.axis_index('fsdp')
        plane, x = lax.div(self.index, SIDE), lax.rem(self.index, SIDE)
        self.at = (lax.div(plane, SIDE), lax.rem(plane, SIDE), x)
        self.partner = (1 - self.core, self.index)
        self.moved = {(axis, by): lax.rem(at + (by + SIDE), SIDE) for axis, at in enumerate(self.at) for by in range(-2, 3)}
        self.peers = {(axis, by): self.place(axis, self.moved[axis, by]) for axis in THREE for by in (-1, 1, 2)}

    def place(self, axis, coord):
        pos = list(self.at)
        pos[axis] = coord
        z, y, x = pos
        return (self.core, (z * SIDE + y) * SIDE + x)

    def shift(self, axis, by):
        return self.moved[axis, by]

    def peer(self, axis, by):
        return self.peers[axis, by]

    def neighbours(self, reach=1):
        return [device for (_, by), device in self.peers.items() if by <= reach]

    def tell(self, sem, devices):
        for device in devices:
            pl.semaphore_signal(sem, inc=1, device_id=device, device_id_type=MESH_ID)

    def barrier(self, devices):
        sem = pltpu.get_barrier_semaphore()
        self.tell(sem, devices)
        pl.semaphore_wait(sem, len(devices))


def pair_of(sems, *at):
    return sems.at[(0,) + at], sems.at[(1,) + at]


def in_order(*calls):
    def run():
        for call in calls:
            call()
    return run


def span(cols):
    (off, width), *rest = cols
    return pl.ds(off, width + sum(w for _, w in rest))


class Gather:
    SEMS = 7

    def __init__(self, net, shard, out, cols, shift, sems, first, direct=False):
        self.net, self.shard, self.out, self.cols, self.moved, self.sems, self.first, self.direct = net, shard, out, cols, shift, sems, first, direct

    def block(self, colour, phase, coord, half=None):
        order = ORDERS[colour]
        off, width = self.cols[colour]
        pick = list(self.net.at)
        for axis in order[:phase]:
            pick[axis] = pl.ds(0, SIDE)
        pick[order[phase]] = coord
        if half is not None and phase:
            pick[order[0]] = pl.ds(half * 2, 2)
        elif half is not None:
            cut = width - width // (2 * TILE) * TILE
            off, width = (off + cut, width - cut) if half else (off, cut)
        return self.out.at[(*pick, slice(None), pl.ds(off, width))] if width else None

    def copy(self, phase, colour, relay, d, by):
        axis = ORDERS[colour][phase]
        far = relay and self.direct
        if far and d:
            return None
        by = 2 if far else by
        back = -by if relay and not far else 0
        dst = src = self.block(colour, phase, self.net.shift(axis, back), d if relay and not far else None)
        if dst is None:
            return None
        if not phase and (far or not relay):
            off, width = self.cols[colour]
            src = self.shard.at[:, pl.ds(off + self.moved, width)]
        return pltpu.make_async_remote_copy(src, dst, *self.sem(phase, relay), device_id=self.net.peer(axis, by), device_id_type=MESH_ID)

    def sem(self, phase, relay):
        return pair_of(self.sems, self.first + 2 * phase + relay)

    def each(self, phase, relay):
        for d, by in BOTH:
            for colour in THREE:
                desc = self.copy(phase, colour, relay, d, by)
                if desc is not None:
                    desc.start()

    def wait(self, phase, relay, side):
        pick = [pl.ds(0, SIDE)] * phase + [pl.ds(0, 2 - relay)] + [0, 0]
        ref = self.out.at[tuple(reversed(pick[:3])) + (slice(None), span(self.cols))]
        pltpu.make_async_copy(ref, ref, self.sem(phase, relay)[side]).wait()

    def own(self):
        at = self.net.at
        cols = span(self.cols)
        src = self.shard.at[:, pl.ds(cols.start + self.moved, cols.size)]
        return pltpu.make_async_copy(src, self.out.at[(*at, slice(None), cols)], self.sems.at[0, self.first + self.SEMS - 1])

    def arrive(self, phase):
        if self.direct:
            self.wait(phase, 0, 1)
        self.wait(phase, 1, 1)

    def start(self, phase):
        if phase:
            self.arrive(phase - 1)
        if phase == 1:
            self.own().wait()
        for relay in range(1 + self.direct):
            self.each(phase, relay)
        if not phase:
            self.own().start()

    def relay(self, phase):
        self.wait(phase, 0, 1)
        self.each(phase, 1)

    def finish(self):
        self.arrive(PHASES[-1])
        for phase in PHASES:
            for relay in TWO:
                self.wait(phase, relay, 0)

    def stages(self):
        steps = (self.start,) if self.direct else (self.start, self.relay)
        return [functools.partial(f, p) for p in PHASES for f in steps] + [self.finish]


class Scatter:
    SEMS = 9

    def __init__(self, net, part, cols, bufs, sems, first, relays=len(PHASES)):
        self.net, self.part, self.cols, self.bufs, self.sems, self.first, self.relays = net, part, cols, bufs, sems, first, relays

    @staticmethod
    def scratch(cols):
        shapes = []
        for _, w in cols:
            shapes += [(3, 2, 2, SIDE, PIECE, w), (3, 2, 2, PIECE, w), (3, 2, PIECE // 2, w)]
        return [pltpu.VMEM(s, jnp.float32) for s in shapes]

    def buf(self, colour, phase):
        return self.bufs[colour * len(PHASES) + phase]

    def block(self, colour, phase, coord, half):
        order = ORDERS[colour]
        off, width = self.cols[colour]
        pick = [pl.ds(0, SIDE)] * 3
        for axis in order[:phase]:
            pick[axis] = self.net.at[axis]
        pick[order[phase]] = coord
        rows = pl.ds(0, PIECE)
        rest = sorted(order[phase + 1:])
        if rest:
            pick[rest[0]] = pl.ds(2 * half, 2)
        else:
            rows = pl.ds(PIECE // 2 * half, PIECE // 2)
        return self.part.at[(*pick, rows, pl.ds(off, width))]

    def copy(self, phase, colour, kind, d, by):
        axis = ORDERS[colour][phase]
        buf = self.buf(colour, phase)
        direct = phase >= self.relays
        if kind == 2 and not direct:
            src = buf.at[0, d]
        elif kind:
            src = self.block(colour, phase, self.net.shift(axis, by), (kind + d) % 2)
        else:
            src = self.block(colour, phase, self.net.shift(axis, 2), d)
            by = 2 if direct else by
        return pltpu.make_async_remote_copy(src, buf.at[kind, d], *self.sem(phase, kind), device_id=self.net.peer(axis, by), device_id_type=MESH_ID)

    def sem(self, phase, kind):
        return pair_of(self.sems, self.first + len(PHASES) * phase + kind)

    def wait(self, phase, kind, side):
        pick = [0] * (phase + 1) + [pl.ds(0, SIDE)] * (2 - phase)
        ref = self.part.at[tuple(pick) + (slice(None), span(self.cols))]
        pltpu.make_async_copy(ref, ref, self.sem(phase, kind)[side]).wait()

    def start(self, phase, kind):
        for d, by in BOTH:
            for colour in THREE:
                self.copy(phase, colour, kind, d, by).start()

    def relay(self, phase):
        self.wait(phase, 0, 1)
        for colour in THREE:
            buf = self.buf(colour, phase)
            for d, by in BOTH:
                buf[0, d] = buf[0, d] + self.block(colour, phase, self.net.shift(ORDERS[colour][phase], by), d)[...]
        self.start(phase, 2)

    def merge(self, phase):
        direct = phase >= self.relays
        for kind in THREE if direct else (1, 2):
            self.wait(phase, kind, 1)
        for colour in THREE:
            buf = self.buf(colour, phase)
            for half in TWO:
                mine = self.block(colour, phase, self.net.at[ORDERS[colour][phase]], half)
                sums = mine[...] + buf[1, 1 - half] + buf[2, half]
                mine[...] = sums + buf[0, half] if direct else sums
        if phase < PHASES[-1]:
            for kind in TWO if phase + 1 < self.relays else THREE:
                self.start(phase + 1, kind)

    def finish(self):
        for phase in PHASES:
            for kind in PHASES:
                self.wait(phase, kind, 0)

    def stages(self):
        calls = [functools.partial(self.start, 0, kind) for kind in TWO]
        for phase in PHASES:
            calls += [functools.partial(self.relay, phase)] * (phase < self.relays) + [functools.partial(self.merge, phase)]
        return calls[:-1] + [in_order(calls[-1], self.finish)]

    def result(self):
        return self.part[self.net.at]


def cut_three(width, off=0, turn=0):
    tiles, ways = width // TILE, len(THREE)
    sizes = [(tiles + (turn - i - 1) % ways) // ways * TILE for i in THREE]
    return [(off + sum(sizes[:i]), s) for i, s in enumerate(sizes)]


def plan(text, *sets):
    left = [iter(s) for s in sets]
    return [(hook, next(left[int(which)])) for hook, field in enumerate(text.split(',')) for which in field]


def halves_of(calls, first=0):
    return [[((when - first) // 2, call) for when, call in calls if when >= first and (when - first) % 2 == odd] for odd in TWO]


def run_at(hook, calls):
    for when, call in calls:
        pl.when(hook == when)(call)


F32, BF16 = jnp.float32, jnp.bfloat16
QB = 256
LANES = TILE
HALF = LANES // 2
PAIR = 3 * LANES
CLIP = 8.0
BLOCK = 512
MIB = 2**20


def nt(a, b):
    return lax.dot_general(a, b, (((1,), (1,)), ((), ())), preferred_element_type=F32)


def nn(a, b):
    return jnp.dot(a, b, preferred_element_type=F32)


def tn(a, b):
    return lax.dot_general(a, b, (((0,), (0,)), ((), ())), preferred_element_type=F32)


def along(reduce, values):
    return reduce(values, axis=-1, keepdims=True)


def head_masks(paired):
    lane = lax.broadcasted_iota(jnp.int32, (1, LANES), 1)
    first = lane % HALF < HALF // 2 if paired else lane < HALF
    return first, jnp.logical_not(first)


def causal_tile(key_axis):
    dims = (QB, 2 * QB) if key_axis == 0 else (2 * QB, QB)
    return lax.broadcasted_iota(jnp.int32, dims, key_axis) <= lax.broadcasted_iota(jnp.int32, dims, 1 - key_axis) % QB


def by_head(values, masks):
    return jnp.concatenate([jnp.where(m, values, jnp.zeros((), BF16)) for m in masks], axis=0)


def attend_pair(q_ref, k_ref, v_ref, o_ref, lse_ref):
    masks = head_masks(True)
    key, val = k_ref[...], v_ref[...]
    causal = causal_tile(1)
    first, _ = head_masks(False)
    for lo in reversed(strips(q_ref.shape[0], QB)):
        hi = lo + QB
        query = by_head(q_ref[lo:hi, :], masks)
        diag = jnp.where(causal, nt(query, key[lo:hi]), -1e30)
        top = along(jnp.max, diag)
        if lo:
            past = nt(query, key[:lo])
            top = jnp.maximum(top, along(jnp.max, past))
            past = jnp.exp(past - top)
        diag = jnp.exp(diag - top)
        total = along(jnp.sum, diag)
        if lo:
            total = total + along(jnp.sum, past)
        scale = 1.0 / total
        acc = nn((diag * scale).astype(BF16), val[lo:hi])
        if lo:
            acc = acc + nn((past * scale).astype(BF16), val[:lo])
        o_ref[lo:hi, :] = jnp.where(first, acc[:QB], acc[QB:]).astype(BF16)
        lse = jnp.broadcast_to(top + jnp.log(total), acc.shape).T
        for h in TWO:
            lse_ref[h:h + 1, lo:hi] = lse[:1, h * QB:(h + 1) * QB]


def attend_pair_back(q_ref, k_ref, v_ref, do_ref, lse_ref, dk_ref, dv_ref, put_dq):
    seq = q_ref.shape[0]
    qmask, vmask = head_masks(True), head_masks(False)
    key, val = k_ref[...], v_ref[...]
    key_t = key.astype(F32).T.astype(BF16)
    causal = causal_tile(0)
    first = lax.broadcasted_iota(jnp.int32, (LANES, 1), 0) % HALF < HALF // 2

    def products(lo):
        hi = lo + QB
        query, dout = by_head(q_ref[lo:hi, :], qmask), by_head(do_ref[lo:hi, :], vmask)
        return query, dout, nt(key[:hi], query), nt(val[:hi], dout)

    ahead = products(seq - QB)
    for lo in reversed(strips(seq, QB)):
        hi = lo + QB
        query, dout, score, grad = ahead
        if lo:
            ahead = products(lo - QB)
        prob = jnp.exp(score - jnp.concatenate([lse_ref[h:h + 1, lo:hi] for h in TWO], axis=1))
        diag = jnp.where(causal, prob[lo:], 0.0)
        prob = jnp.concatenate([prob[:lo], diag], axis=0) if lo else diag
        ds = (prob * (grad - jnp.sum(prob * grad, axis=0, keepdims=True))).astype(BF16)
        both = nn(key_t[:, :hi], ds)
        put_dq(lo, hi, jnp.where(first, both[:, :QB], both[:, QB:]).T)
        dv, dk = nn(prob.astype(BF16), dout), nn(ds, query)
        if hi == seq:
            dv_ref[...] = dv
            dk_ref[...] = dk
        else:
            dv_ref[:hi, :] += dv
            dk_ref[:hi, :] += dk


def swap_halves(values):
    return pltpu.roll(values, HALF, axis=1)


COARSE = 32


def tables(seq, head):
    freq = 10000.0 ** (-np.arange(0, head, 2, dtype=np.float64) / head)
    angles = [np.tile(np.arange(seq // COARSE)[:, None] * step * freq, LANES // len(freq)) for step in (1, COARSE)]
    return np.stack([np.stack([np.cos(angle), np.sin(angle)]) for angle in angles]).astype(np.float32)


def spread_tables(table_ref, cos_ref, sin_ref):
    fine_cos, fine_sin = table_ref[0]
    sign = jnp.where(lax.broadcasted_iota(jnp.int32, (1, LANES), 1) < HALF, -1.0, 1.0)

    def body(i):
        rows = aligned(i * COARSE, COARSE)
        cos, sin = table_ref[1, :, pl.ds(i, 1), :]
        cos_ref[rows, :] = fine_cos * cos - fine_sin * sin
        sin_ref[rows, :] = (fine_sin * cos + fine_cos * sin) * sign

    repeat(cos_ref.shape[0] // COARSE, body)


def repeat(count, body):
    def step(i, carry):
        body(i)
        return carry

    lax.fori_loop(0, count, step, 0)


def side_by_side(halves, j):
    return jnp.concatenate([halves[2 * j], halves[2 * j + 1]], axis=1)


def aligned(at, size):
    return pl.ds(pl.multiple_of(at, size), size)


def norm_rows(values):
    mean = along(jnp.mean, values)
    centered = values - mean
    inv = lax.rsqrt(along(jnp.mean, centered * centered) + 1e-5)
    return centered * inv, inv


def norm_grad(grad, normed, inv):
    mean = along(jnp.mean, grad)
    proj = along(jnp.mean, grad * normed)
    return inv * (grad - mean - normed * proj)


def params(collective_id):
    return pltpu.CompilerParams(collective_id=collective_id, has_side_effects=True, vmem_limit_bytes=63 * MIB)


def grid_step():
    return pl.program_id(0), pl.num_programs(0) - 1


def dma(*shape):
    return pltpu.SemaphoreType.DMA(shape)


def shape(dtype, *dims):
    return jax.ShapeDtypeStruct(dims, dtype)


HBM = pl.BlockSpec(memory_space=pltpu.HBM)
WHOLE = pl.BlockSpec(memory_space=pltpu.VMEM)


def lanes(part):
    return slice(LANES * part, LANES * (part + 1))


def strips(width, size):
    return range(0, width, size)


def rows_of(size, width, index):
    return pl.BlockSpec((size, width), lambda step: (index(step), 0))


def stats_rows(seq, index):
    return pl.BlockSpec((1, 1, 2, seq), lambda step: (*index(step), 0, 0))


def project_pair(n1_ref, weight, cos_ref, sin_ref, qkv_ref, keep_ref):
    for lo in strips(n1_ref.shape[0], QB):
        rows = slice(lo, lo + QB)
        raw = nn(n1_ref[rows, :], weight)
        keep_ref[rows, :] = (jnp.abs(raw) < CLIP).astype(F32).astype(BF16)
        raw = jnp.clip(raw, -CLIP, CLIP)
        for part in THREE:
            cols = lanes(part)
            tile = raw[:, cols]
            if part < 2:
                tile = tile * cos_ref[rows, :] + swap_halves(tile) * sin_ref[rows, :]
            if not part:
                tile = tile * 0.125
            qkv_ref[rows, cols] = tile.astype(BF16)


def swap_middle(tile):
    quarter = lax.broadcasted_iota(jnp.int32, tile.shape, 1) // (LANES // 4)
    up, down = pltpu.roll(tile, LANES // 4, axis=1), pltpu.roll(tile, LANES - LANES // 4, axis=1)
    return jnp.where(quarter == 1, down, jnp.where(quarter == 2, up, tile))


CHUNK = 256
CHUNK_STEPS = 4
FRONT_PLAN = '014560145260512430,,4,5,1234,,345,,24,,,,3,,,5,,5'
SCATTER_PLAN = '0,0,,,,1,,1,2,02,,,,1,,,2,0,,1,201,2,10,2012,012'
LAST_PLAN = '00,1,1,,20,13,,2,2,34,10,234,41,,2034,1023,410,2,31402'


def to_partner(net, src, dst, send, recv):
    return pltpu.make_async_remote_copy(src, dst, send, recv, device_id=net.partner, device_id_type=MESH_ID)


def front_kernel(x_hbm, qkv_shard, out_shard, ff_shard, down_shard, table_ref, qkv_hbm, keep_hbm, o_hbm, lse_ref, h_hbm, n1_hbm, wq_hbm, wo_hbm, wf_hbm,
                 x_all, n1, w, shards, o_all, part, got, h_buf, wo, sems, gather_sems, load_sem, h_sem, cos_ref, sin_ref, o_buf, qkv_all, keep_all, store_sem):
    step, last = grid_step()
    turn = step - 1
    batch, pairs, seq = o_all.shape[:3]
    b, p = turn % batch, turn // batch
    half = CHUNK // 2
    chunks = seq // CHUNK
    ff = down_shard.shape[1]
    net = Torus()
    width = PAIR
    heads_end, out_end = width * pairs, (width + LANES) * pairs
    places = [(w, cut_three(width, width * j), 0) for j in range(pairs)] + [
              (wo_hbm, cut_three(LANES * pairs), heads_end), (wf_hbm, cut_three(3 * ff), out_end)]
    gathers = [Gather(net, shards, out, cols, shift, gather_sems, i * Gather.SEMS, i < pairs) for i, (out, cols, shift) in enumerate(places)]
    strip = x_all.shape[0] // CHUNK_STEPS

    def rows_at(i):
        return aligned(i * strip, strip)

    def load(i):
        return pltpu.make_async_copy(x_hbm.at[rows_at(i)], x_all.at[rows_at(i)], load_sem.at[i])

    def save(i):
        return pltpu.make_async_copy(n1.at[rows_at(i)], n1_hbm.at[rows_at(i)], load_sem.at[i])

    save_weight = pltpu.make_async_copy(w, wq_hbm, load_sem.at[CHUNK_STEPS])

    def normalize(i):
        load(i).wait()
        n1[rows_at(i), :] = norm_rows(x_all[rows_at(i), :].astype(F32))[0].astype(BF16)
        save(i).start()

    def normalize_half(first):
        repeat(CHUNK_STEPS // 2, lambda i: normalize(first + i))

    spread = functools.partial(spread_tables, table_ref, cos_ref, sin_ref)
    calls = plan(FRONT_PLAN, *([*g.stages()] for g in gathers), [in_order(spread, functools.partial(normalize_half, 0)), functools.partial(normalize_half, CHUNK_STEPS // 2)])

    @pl.when(step == 0)
    def _():
        for i in range(CHUNK_STEPS):
            load(i).start()
        for i in THREE:
            heads = qkv_shard[:, i].astype(F32).swapaxes(0, 1)
            for j in range(pairs):
                tile = side_by_side(heads, j)
                shards[:, lanes(3 * j + i)] = (swap_middle(tile) if i < 2 else tile).astype(BF16)
        for j in range(pairs):
            shards[:, lanes(3 * pairs + j)] = side_by_side(out_shard, j)
        both = ff_shard[...].astype(F32)
        for i in range(ff // LANES):
            for j in TWO:
                shards[:, lanes(4 * pairs + 2 * i + j)] = both[:, j, lanes(i)].astype(BF16)
        shards[:, out_end + 2 * ff:] = down_shard[...]
        net.barrier(net.neighbours(2) + [net.partner])
        for when, call in calls:
            if not when:
                call()

    begin, end = halves_of(calls, 1)
    run_at(turn, begin)

    def store(b, p):
        out = []
        for i, (src, dst) in enumerate(((qkv_all.at[b], qkv_hbm), (keep_all.at[b], keep_hbm), (o_all.at[b, p], o_hbm))):
            size = src.shape[-1]
            out.append(pltpu.make_async_copy(src, dst.at[aligned(b * seq, seq), aligned(p * size, size)], store_sem.at[i, b]))
        return out

    @pl.when(turn >= batch)
    def _():
        for copy in store(b, p - 1):
            copy.wait()

    @pl.when(turn >= 0)
    def _():
        qkv_ref, keep_ref = qkv_all.at[b], keep_all.at[b]
        weight = w[:, :, :, :, pl.ds(pl.multiple_of(width * p, LANES), width)].reshape(n1.shape[1], width)
        project_pair(n1.at[aligned(b * seq, seq)], weight, cos_ref, sin_ref, qkv_ref, keep_ref)
        q_ref, k_ref, v_ref = (qkv_ref.at[:, pl.ds(LANES * i, LANES)] for i in THREE)
        attend_pair(q_ref, k_ref, v_ref, o_all.at[b, p], lse_ref.at[0, 0])
        for copy in store(b, p):
            copy.start()

    run_at(turn, end)

    def rows_in(c, core):
        return aligned(c * CHUNK + core * half, half)

    def part_copy(b, c):
        return to_partner(net, part.at[b, rows_in(c, 1 - net.core)], got.at[b, c], *pair_of(sems, 0, b, c))

    def rows_out(b, c, core):
        return aligned(b * seq + c * CHUNK + core * half, half)

    def h_copy(b, c, core):
        return to_partner(net, h_buf.at[b, c], h_hbm.at[rows_out(b, c, core)], *pair_of(sems, 1, b, c))

    def h_local(b, c):
        return pltpu.make_async_copy(h_buf.at[b, c], h_hbm.at[rows_out(b, c, net.core)], h_sem.at[b, c])

    def project(b):
        o_buf[...] = jnp.concatenate([o_all[b, j] for j in range(pairs)], axis=1)
        weight = wo[...].reshape(part.shape[2], LANES * pairs)

        def body(c):
            rows = aligned(c * CHUNK, CHUNK)
            part[b, rows, :] = nt(o_buf[rows, :], weight)
            part_copy(b, c).start()

        repeat(chunks, body)

    def combine(b):
        def body(c):
            part_copy(b, c).wait()
            own = rows_in(c, net.core)
            h_buf[b, c] = (x_all[rows_out(b, c, net.core), :].astype(F32) + (part[b, own, :] + got[b, c])).astype(BF16)
            h_copy(b, c, net.core).start()
            h_local(b, c).start()

        repeat(chunks, body)

    def settle():
        for b in range(batch):
            for c in range(chunks):
                h_copy(b, c, net.core).wait_send()
                h_local(b, c).wait()
                h_copy(b, c, 1 - net.core).wait_recv()
        for b in range(batch):
            for copy in store(b, pairs - 1):
                copy.wait()
        for i in range(CHUNK_STEPS):
            save(i).wait()
        save_weight.wait()

    fetch = pltpu.make_async_copy(wo_hbm, wo, h_sem.at[0, 0])
    run_at(last - step, [(2, fetch.start), (2, save_weight.start), (1, fetch.wait), (0, functools.partial(combine, 0))])

    @pl.when(step + 1 >= last)
    def _():
        project(step + 1 - last)

    run_at(last - step, [(0, functools.partial(combine, 1)), (0, settle)])
    run_at(turn + 1, begin[-1:])


def front(x, qkv_shard, out_shard, ff_shard, down_shard, table, batch, seq, collective_id):
    pairs = len(out_shard) // 2
    rows, d = x.shape
    width = PAIR
    chunks = seq // CHUNK
    vm = pltpu.VMEM
    torus = (SIDE, SIDE, SIDE, PIECE)
    shards = [s.size // PIECE for s in (qkv_shard, out_shard, ff_shard, down_shard)]
    turn = lambda s: jnp.maximum(s - 1, 0)
    return pl.pallas_call(
        front_kernel,
        grid=(1 + batch * pairs,),
        in_specs=[HBM] + [WHOLE] * 5,
        out_specs=[HBM] * 3 + [stats_rows(seq, lambda s: (turn(s) % batch, turn(s) // batch))] + [HBM] * 5,
        out_shape=[shape(BF16, rows, width * pairs)] * 2 + [shape(BF16, rows, LANES * pairs), shape(F32, batch, pairs, 2, seq), shape(BF16, rows, d), shape(BF16, rows, d),
                   shape(BF16, *torus, shards[0]), shape(BF16, *torus, shards[1]), shape(BF16, *torus, shards[2] + shards[3])],
        scratch_shapes=[vm((rows, d), BF16), vm((rows, d), BF16), vm(torus + (width * pairs,), BF16), vm((PIECE, sum(shards)), BF16),
                        vm((batch, pairs, seq, LANES), BF16), vm((batch, seq, d), F32), vm((batch, chunks, CHUNK // 2, d), F32), vm((batch, chunks, CHUNK // 2, d), BF16),
                        vm(torus + (shards[1],), BF16), dma(2, 2, batch, chunks), dma(2, (pairs + 2) * Gather.SEMS), dma(CHUNK_STEPS + 1), dma(batch, chunks)] + [vm((seq, LANES), F32)] * 2 + [vm((seq, LANES * pairs), BF16)] + [vm((batch, seq, width), BF16)] * 2 + [dma(3, batch)],
        compiler_params=params(collective_id),
        name='front',
    )(x, qkv_shard, out_shard, ff_shard, down_shard, table)


class Exchange:
    def __init__(self, net, rows, partials, results, sems, local_sem):
        self.net, self.rows, self.partials, self.results, self.sems, self.local_sem = net, rows, partials, results, sems, local_sem

    def half(self, core, at=0):
        return aligned(at * self.rows + core * (self.rows // 2), self.rows // 2)

    def part(self, which, at):
        part, got = self.partials[which]
        return to_partner(self.net, part.at[at % 2, self.half(1 - self.net.core)], got.at[at], *pair_of(self.sems, which, at))

    def arrive(self, at):
        for which in range(len(self.partials)):
            self.part(which, at).wait()

    def total(self, which, at):
        part, got = self.partials[which]
        return part[at % 2, self.half(self.net.core), :] + got[at]

    def results_of(self, at, core, act):
        for i, (buf, hbm) in enumerate(self.results):
            act(buf.at[at % 2], hbm.at[self.half(core, at)], pair_of(self.sems, len(self.partials) + i, at), self.local_sem.at[i, at % 2])

    def publish(self, at):
        def act(buf, rows, sem, local_sem):
            to_partner(self.net, buf, rows, *sem).start()
            pltpu.make_async_copy(buf, rows, local_sem).start()
        self.results_of(at, self.net.core, act)

    def settle(self, at):
        def act(buf, rows, sem, local_sem):
            to_partner(self.net, buf, rows, *sem).wait_send()
            pltpu.make_async_copy(buf, rows, local_sem).wait()
        self.results_of(at, self.net.core, act)
        self.results_of(at, 1 - self.net.core, lambda buf, rows, sem, local_sem: to_partner(self.net, buf, rows, *sem).wait_recv())

    def settle_tail(self, blocks):
        for at in TWO:
            self.settle(blocks - len(TWO) + at)


def mlp_kernel(blocks, h_ref, gy_ref, weights, y_hbm, gh_hbm, gh32_ref, acts_hbm, n2_ref, gd_hbm,
               wff_ref, wd_ref, saved, grad_down, part_y, part_g, got_y, got_g, y_buf, gh_buf, h_own, gy_own, sems, local_sem, save_sem, load_sem):
    step, final = grid_step()
    rows, d = h_ref.shape
    ff = wd_ref.shape[1]
    acts = saved.at[step % 2]
    gug, act = acts.at[:, pl.ds(0, 2 * ff)], acts.at[:, pl.ds(2 * ff, ff)]

    def save(at):
        return pltpu.make_async_copy(saved.at[at % 2], acts_hbm.at[aligned(at * rows, rows)], save_sem.at[at % 2])

    save_grad = pltpu.make_async_copy(grad_down, gd_hbm, save_sem.at[2])
    net = Torus()
    swap = Exchange(net, rows, ((part_y, got_y), (part_g, got_g)), ((y_buf, y_hbm), (gh_buf, gh_hbm)), sems, local_sem)

    loads = [pltpu.make_async_copy(weights.at[:, pl.ds(at, dst.shape[1])], dst, load_sem.at[i]) for i, (dst, at) in enumerate(((wd_ref, 2 * ff), (wff_ref, 0)))]

    @pl.when(step == 0)
    def _():
        for copy in loads:
            copy.start()
        net.barrier([net.partner])
        for copy in loads:
            copy.wait()

    @pl.when((step > 1) & (step < blocks))
    def _():
        save(step - 2).wait()

    @pl.when(step < blocks)
    def _():
        n2, _ = norm_rows(h_ref[...].astype(F32))
        n2 = n2.astype(BF16)
        n2_ref[...] = n2
        gy = gy_ref[...]
        for j in strips(ff, QB):
            w = min(QB, ff - j)
            gact = nn(gy, wd_ref[:, j:j + w])
            for i in range(j, j + w, LANES):
                at, mid, end = 2 * i, 2 * i + LANES, 2 * i + QB
                ug = nn(n2, wff_ref[:, at:end])
                up, gate = ug[:, :LANES], ug[:, LANES:]
                sig = 1.0 / (1.0 + jnp.exp(-gate))
                silu = gate * sig
                act[:, i:i + LANES] = (silu * up).astype(BF16)
                ga = gact[:, i - j:i - j + LANES]
                gug[:, at:mid] = (ga * silu).astype(BF16)
                gug[:, mid:end] = (ga * up * sig * (1.0 + gate * (1.0 - sig))).astype(BF16)

        for which, left, right, part in ((0, act, wd_ref, part_y), (1, gug, wff_ref, part_g)):
            for j in strips(d, QB):
                part[step % 2, :, j:j + QB] = nt(left[...], right[j:j + QB, :])
            swap.part(which, step).start()
        save(step).start()

    done = (step + blocks) % (blocks + 1)

    @pl.when(step > 2)
    def _():
        swap.settle(step - 3)

    @pl.when(step > 0)
    def _():
        swap.arrive(done)

    def combine():
        hidden = h_own[...].astype(F32)
        normed, inv = norm_rows(hidden)
        y_buf[done % 2] = (hidden + swap.total(0, done)).astype(BF16)
        gh = gy_own[...].astype(F32) + norm_grad(swap.total(1, done), normed, inv)
        gh32_ref[...] = gh
        gh_buf[done % 2] = gh.astype(BF16)

    @pl.when(step < blocks)
    def _():
        accumulate(grad_down, step == 0, gy_ref[...], act)
        combine()

    @pl.when(step == blocks - 1)
    def _():
        save_grad.start()

    pl.when(step == blocks)(combine)

    @pl.when(step > 0)
    def _():
        swap.publish(done)

    own = swap.half(net.core)
    h_own[...] = h_ref[own, :]
    gy_own[...] = gy_ref[own, :]

    @pl.when(step == blocks)
    def _():
        swap.settle_tail(blocks)
        for at in TWO:
            save(blocks - len(TWO) + at).wait()
        save_grad.wait()


def mlp(h, gy, weights, collective_id, block=BLOCK):
    rows, d = h.shape
    ff = weights.shape[1] // 3
    half = block // 2
    blocks = rows // block
    torus = (SIDE, SIDE, SIDE, PIECE)
    row = lambda width: rows_of(block, width, lambda i: jnp.minimum(i, blocks - 1))
    vm = pltpu.VMEM
    return pl.pallas_call(
        functools.partial(mlp_kernel, blocks),
        grid=(blocks + 1,),
        in_specs=[row(d), row(d), HBM],
        out_specs=[HBM, HBM, rows_of(half, d, lambda i: jnp.maximum(i - 1, 0)), HBM, row(d), HBM],
        out_shape=[shape(BF16, rows, d), shape(BF16, rows, d), shape(F32, rows // 2, d), shape(BF16, rows, 3 * ff), shape(BF16, rows, d), shape(F32, *torus, ff)],
        scratch_shapes=[vm((d, 2 * ff), BF16), vm((d, ff), BF16), vm((2, block, 3 * ff), BF16), vm(torus + (ff,), F32)] + [vm((2, block, d), F32)] * 2 + [vm((blocks + 1, half, d), F32)] * 2 + [vm((2, half, d), BF16)] * 2 + [vm((half, d), BF16)] * 2 + [dma(2, 4, blocks), dma(2, 2), dma(3), dma(2)],
        compiler_params=params(collective_id),
        name='mlp',
    )(h, gy, weights)


def accumulate(part, first, left, right):
    for j in strips(right.shape[1], QB):
        w = min(QB, right.shape[1] - j)
        prod = tn(left, right[:, j:j + w]).reshape(part.shape[:-1] + (w,))
        at = slice(j, j + w)
        part[..., at] = jnp.where(first, 0.0, part[..., at]) + prod


SETS = 3
HEAD_STEP = (SETS - 1) * CHUNK_STEPS


def back_kernel(pairs, gd_hbm, n2_ref, act_ref, qkv_ref, lse_ref, gh_hbm, wo_hbm, o_hbm, keep_ref, table_ref,
                g_ref, gw_ref, gd_ref, gff_ref, cos_ref, sin_ref, do_ref, dk_ref, dv_ref, gh_ref, wo_ref, o_ref, parts, sems, load_sem, *bufs):
    step, final = grid_step()
    turn = step - HEAD_STEP
    p = turn % pairs
    half = gh_ref.shape[0] // 2
    net = Torus()
    per = len(bufs) // SETS
    scatters = [Scatter(net, parts.at[i], cut_three(parts.shape[-1], turn=i), bufs[per * i:per * i + per], sems, i * Scatter.SEMS) for i in range(SETS)]
    calls = plan(SCATTER_PLAN, *(s.stages() for s in scatters))
    begin, end = halves_of(calls, HEAD_STEP + 1)

    def fetch(b):
        rows = aligned(b * 2 * half, 2 * half)
        return [pltpu.make_async_copy(src.at[rows], dst, load_sem.at[i]) for i, (src, dst) in enumerate(((gh_hbm, gh_ref), (o_hbm, o_ref)))]

    load = pltpu.make_async_copy(gd_hbm, parts.at[0], load_sem.at[2])
    fetch_weight = pltpu.make_async_copy(wo_hbm, wo_ref, load_sem.at[3])

    @pl.when(step == 0)
    def _():
        for copy in [load] + fetch(0) + [fetch_weight]:
            copy.start()
        spread_tables(table_ref, cos_ref, sin_ref)
        net.barrier(net.neighbours())
        load.wait()
        for when, call in calls:
            if not when:
                call()

    @pl.when(turn < 0)
    def _():
        accumulate(parts.at[1 + step // CHUNK_STEPS], step % CHUNK_STEPS == 0, n2_ref[...], act_ref)

    run_at(step + 1, [c for c in calls if 0 < c[0] <= HEAD_STEP])

    def put(part, lo, hi, values):
        cols = lanes(part)
        if part < 2:
            values = values * cos_ref[lo:hi, :] - swap_halves(values) * sin_ref[lo:hi, :]
        g_ref[lo:hi, cols] = (values * keep_ref[lo:hi, cols].astype(F32)).astype(BF16)

    put_dq = lambda lo, hi, dq: put(0, lo, hi, dq * 0.125)

    @pl.when(turn >= 0)
    def _():
        @pl.when(p == 0)
        def _():
            pl.when(turn == 0)(fetch_weight.wait)
            for copy in fetch(turn // pairs):
                copy.wait()
            gw_ref[...] = jnp.where(turn == 0, 0.0, gw_ref[...])

            def body(i):
                rows = aligned(i * half, half)
                gh = gh_ref[rows, :]
                dout = nn(gh, wo_ref[...]).astype(BF16)
                for j in range(pairs):
                    do_ref[j, rows, :] = dout[:, lanes(j)]
                gw_ref[...] += tn(gh, o_ref[rows, :])

            repeat(len(TWO), body)

            @pl.when(turn == 0)
            def _():
                for copy in fetch(turn + 1):
                    copy.start()

        run_at(turn, begin)
        q_ref, k_ref, v_ref = (qkv_ref.at[:, pl.ds(LANES * i, LANES)] for i in THREE)
        attend_pair_back(q_ref, k_ref, v_ref, do_ref.at[p], lse_ref.at[0, 0], dk_ref, dv_ref, put_dq)
        for part, grad in ((1, dk_ref), (2, dv_ref)):
            put(part, 0, 2 * half, grad[...])
        run_at(turn, end)

    @pl.when(step == final)
    def _():
        gd_ref[...], *halves = [s.result() for s in scatters]
        tiles = jnp.concatenate(halves, axis=1)
        for i in range(tiles.shape[1] // LANES):
            gff_ref[:, i % 2, lanes(i // 2)] = tiles[:, lanes(i)]


def back(gd, n2, acts, qkv, lse, gh, wo_t, o, keep, table, batch, seq, pairs, collective_id):
    rows, d = n2.shape
    ff = acts.shape[1] // SETS
    block = rows // CHUNK_STEPS
    turn = lambda s: jnp.maximum(s - HEAD_STEP, 0)
    head = pl.BlockSpec((seq, PAIR), lambda s: (turn(s) // pairs, turn(s) % pairs))
    late = lambda s: jnp.where(s < HEAD_STEP, s % CHUNK_STEPS, CHUNK_STEPS - 1)
    vm = pltpu.VMEM
    return pl.pallas_call(
        functools.partial(back_kernel, pairs),
        grid=(HEAD_STEP + batch * pairs,),
        in_specs=[HBM, rows_of(block, d, late), pl.BlockSpec((block, ff), lambda s: (late(s), jnp.minimum(s // CHUNK_STEPS, 1))), head, stats_rows(seq, lambda s: (turn(s) // pairs, turn(s) % pairs)),
                  HBM, HBM, HBM, head, WHOLE],
        out_specs=[head, WHOLE, WHOLE, WHOLE],
        out_shape=[shape(BF16, *qkv.shape), shape(F32, *wo_t.shape), shape(F32, PIECE, ff), shape(F32, PIECE, 2, ff)],
        scratch_shapes=[vm((seq, LANES), F32)] * 2 + [vm((pairs, seq, LANES), BF16)] + [vm((seq, LANES), F32)] * 2 + [vm((seq, d), BF16), vm(wo_t.shape, BF16), vm((seq, LANES * pairs), BF16), vm((SETS, SIDE, SIDE, SIDE, PIECE, ff), F32),
                        dma(2, SETS * Scatter.SEMS), dma(4)] + [s for i in range(SETS) for s in Scatter.scratch(cut_three(ff, turn=i))],
        compiler_params=params(collective_id),
        name='back',
    )(gd, n2, acts, qkv, lse, gh, wo_t, o, keep, table)


def last_kernel(pairs, blocks, n1_hbm, g_ref, x_ref, g_row, gh_ref, w_hbm, gout_hbm, gx_hbm, gout_ref, gw_ref,
                n1_ref, w_ref, part_out, part_qkv, part, got, buf, sems, scatter_sems, local_sem, load_sem, *bufs):
    step, final = grid_step()
    turn = step - pairs
    rows, d = x_ref.shape
    net = Torus()
    per = len(bufs) // (pairs + 1)
    parts = [part_out] + [part_qkv.at[j] for j in range(pairs)]
    scatters = [Scatter(net, s, cut_three(s.shape[-1], turn=i), bufs[per * i:per * i + per], scatter_sems, i * Scatter.SEMS, 1 if i > pairs // 2 else len(PHASES)) for i, s in enumerate(parts)]
    calls = plan(LAST_PLAN, *(s.stages() for s in scatters))
    swap = Exchange(net, rows, ((part, got),), ((buf, gx_hbm),), sems, local_sem)

    loads = [pltpu.make_async_copy(src, dst, load_sem.at[i]) for i, (src, dst) in enumerate(((gout_hbm, part_out), (n1_hbm, n1_ref), (w_hbm, w_ref)))]
    pl.when(turn == 0)(loads[-1].wait)

    @pl.when(step == 0)
    def _():
        for copy in loads:
            copy.start()
        net.barrier(net.neighbours(2) + [net.partner])
        for copy in loads[:-1]:
            copy.wait()

    begin, end = halves_of(calls)
    run_at(step, begin)

    @pl.when(turn < 0)
    def _():
        size = n1_ref.shape[0] // len(TWO)

        def body(i):
            accumulate(part_qkv.at[step], i == 0, n1_ref[aligned(i * size, size), :], g_ref.at[aligned(i * size, size)])

        repeat(len(TWO), body)

    @pl.when((turn >= 0) & (turn < blocks))
    def _():
        def body(i):
            cols = aligned(i * QB, QB)
            part[turn % 2, :, cols] = nt(g_row[...], w_ref[cols, :])

        repeat(d // QB, body)
        swap.part(0, turn).start()

    run_at(step, end)

    @pl.when(turn > 2)
    def _():
        swap.settle(turn - 3)

    @pl.when(turn > 0)
    def _():
        done = turn - 1
        swap.arrive(done)
        normed, inv = norm_rows(x_ref[swap.half(net.core), :].astype(F32))
        buf[done % 2] = (gh_ref[...] + norm_grad(swap.total(0, done), normed, inv)).astype(BF16)
        swap.publish(done)

    @pl.when(turn == blocks)
    def _():
        for when, call in calls:
            if when > 2 * (pairs + blocks) + 1:
                call()
        swap.settle_tail(blocks)
        out, *sums = [s.result() for s in scatters]
        halves = slice(HALF), slice(HALF, LANES)
        for j in range(pairs):
            for h, cols in enumerate(halves):
                gout_ref[2 * j + h] = out[:, lanes(j)][:, cols]
        for i in THREE:
            tiles = [swap_middle(s[:, lanes(i)]) if i < 2 else s[:, lanes(i)] for s in sums]
            gw_ref[:, i] = jnp.stack([t[:, cols] for t in tiles for cols in halves]).swapaxes(0, 1)


def last(x, n1, g, gh32, w, gout, pairs, collective_id, block=BLOCK):
    rows, d = x.shape
    blocks = rows // block
    late = lambda n, width, by: rows_of(n, width, lambda s: jnp.clip(s - pairs - by, 0, blocks - 1))
    head = pl.BlockSpec((rows, PAIR), lambda s: (0, jnp.minimum(s, pairs - 1)))
    vm = pltpu.VMEM
    half = block // 2
    torus = (SIDE, SIDE, SIDE, PIECE)
    gout = gout.reshape(torus + (-1,))
    return pl.pallas_call(
        functools.partial(last_kernel, pairs, blocks),
        grid=(pairs + blocks + 1,),
        in_specs=[HBM, head, late(block, d, 1), late(block, g.shape[1], 0), late(half, d, 1), HBM, HBM],
        out_specs=[HBM, WHOLE, WHOLE],
        out_shape=[shape(BF16, rows, d), shape(F32, 2 * pairs, PIECE, HALF), shape(F32, PIECE, 3, 2 * pairs, HALF)],
        scratch_shapes=[vm((rows, d), BF16), vm(w.shape, BF16), vm(gout.shape, F32), vm((pairs,) + torus + (PAIR,), F32), vm((2, block, d), F32), vm((blocks, half, d), F32), vm((2, half, d), BF16),
                        dma(2, 2, blocks), dma(2, (pairs + 1) * Scatter.SEMS), dma(1, 2), dma(3)] + Scatter.scratch(cut_three(gout.shape[-1])) + Scatter.scratch(cut_three(PAIR)) * pairs,
        compiler_params=params(collective_id),
        name='last',
    )(n1, g, x, g, gh32, w, gout)


def hand_over_kernel(*refs):
    count = len(refs) // 2
    for src, dst in zip(refs[:count], refs[count:]):
        dst[...] = src[...]


def hand_over(wide, small, block=2 * BLOCK):
    rows, width = wide[0].shape
    specs = [rows_of(block, width, lambda i: i) for v in wide] + [WHOLE for v in small]
    return pl.pallas_call(
        hand_over_kernel,
        grid=(rows // block,),
        in_specs=specs,
        out_specs=specs,
        out_shape=[shape(v.dtype, *v.shape) for v in wide + small],
        compiler_params=pltpu.CompilerParams(vmem_limit_bytes=63 * MIB),
        name='hand_over',
    )(*wide, *small)


def device_step(x, grad_y, w_qkv, w_out, w_ff, w_down):
    batch, seq, d = x.shape
    heads, head = w_qkv.shape[2:]
    pairs = heads // 2
    table = jnp.asarray(tables(seq, head))
    ids = iter(range(SIDE))
    x2, gy = (v.reshape(batch * seq, d) for v in (x, grad_y))
    qkv, keep, o, lse, h, n1, *weights = front(x2, w_qkv, w_out.swapaxes(1, 2), w_ff, w_down.T, table, batch, seq, next(ids))
    wq, wo_t, wf = (w.reshape(d, w.shape[-1]) for w in weights)
    y, gh, gh32, acts, n2, gd = mlp(h, gy, wf, next(ids))
    g, gout, gd, gff = back(gd, n2, acts, qkv, lse, gh, wo_t, o, keep, table, batch, seq, pairs, next(ids))
    gx, gout, gqkv = last(x2, n1, g, gh32, wq, gout, pairs, next(ids))
    y, gx, gqkv, gout, gff, gd = hand_over([y, gx], [gqkv, gout, gff, gd])
    return y.reshape(x.shape), gx.reshape(x.shape), gqkv, gout.swapaxes(1, 2), gff, gd.T


def solution(mesh):
    specs = (P('fsdp'), P('fsdp'), P('fsdp', None, 'tp'), P('tp', None, 'fsdp'), P('fsdp', None, 'tp'), P('tp', 'fsdp'))
    return jax.shard_map(device_step, mesh=mesh, in_specs=specs, out_specs=specs, check_vma=False)
```
